8 devices in a mesh: tp: 2 (over z, y), dp: 4 (over x, core).
Axes of the slice: x: 2, y: 2, z: 1, core: 2. Of those that a mesh axis runs over, the one named last changes fastest.
Arguments:
- x_in: bfloat16 [128, 256, 2048], P('dp')
- dy_in: bfloat16 [128, 256, 2048], P('dp')
- positions: int32 [128, 256], P('dp')
- g_attn: bfloat16 [2048], replicated
- q_gain: bfloat16 [128], replicated
- k_gain: bfloat16 [128], replicated
- w_q: bfloat16 [2048, 2048], P(None, 'tp')
- w_k: bfloat16 [2048, 1024], P(None, 'tp')
- w_v: bfloat16 [2048, 1024], P(None, 'tp')
- w_o: bfloat16 [2048, 2048], P('tp')
Outputs:
- output 1: bfloat16 [128, 256, 2048], P('dp')
- output 2: bfloat16 [128, 256, 2048], P('dp')
- output 3: float32 [2048, 2048], P(None, 'tp')
- output 4: float32 [2048, 1024], P(None, 'tp')
- output 5: float32 [2048, 1024], P(None, 'tp')
- output 6: float32 [2048, 2048], P('tp')
- output 7: float32 [128], replicated
- output 8: float32 [128], replicated
- output 9: float32 [2048], replicated
All inputs are finite; a program needn't handle non-finite values.
Results may differ from the reference program's by a relative error of at most 0.0199202.
Values sent between devices are 32-bit elements.
A program may use at most 1 GiB of HBM per device.

```python
import jax
import jax.numpy as jnp
from jax import lax

BATCH_ROWS = 128
SEQ_LEN = 256
MODEL_DIM = 2048
NUM_HEADS = 16
KV_HEADS = 8
HEAD_DIM = 128
EPS = 1e-6
ROPE_THETA = 1000000.0
GROUP_SIZE = NUM_HEADS // KV_HEADS
ATT_SCALE = HEAD_DIM ** -0.5


def setup_inputs(seed: int = 0) -> dict:
    rng_keys = jax.random.split(jax.random.key(seed), 10)
    tok_shape = (BATCH_ROWS, SEQ_LEN, MODEL_DIM)
    x_in = jax.random.normal(rng_keys[0], tok_shape, jnp.float32).astype(jnp.bfloat16)
    dy_in = jax.random.normal(rng_keys[1], tok_shape, jnp.float32).astype(jnp.bfloat16)
    pos_steps = jax.random.randint(rng_keys[2], (BATCH_ROWS, SEQ_LEN), 1, 4, dtype=jnp.int32)
    positions = (jnp.cumsum(pos_steps, axis=1) - pos_steps[:, :1]).astype(jnp.int32)
    g_attn = (1.0 + 0.4 * jax.random.normal(rng_keys[3], (MODEL_DIM,), jnp.float32)).astype(jnp.bfloat16)
    q_gain = (1.0 + 0.5 * jax.random.normal(rng_keys[4], (HEAD_DIM,), jnp.float32)).astype(jnp.bfloat16)
    k_gain = (1.0 + 0.5 * jax.random.normal(rng_keys[5], (HEAD_DIM,), jnp.float32)).astype(jnp.bfloat16)
    in_scale = MODEL_DIM ** -0.5
    w_q = (jax.random.normal(rng_keys[6], (MODEL_DIM, NUM_HEADS * HEAD_DIM), jnp.float32) * in_scale).astype(jnp.bfloat16)
    w_k = (jax.random.normal(rng_keys[7], (MODEL_DIM, KV_HEADS * HEAD_DIM), jnp.float32) * in_scale).astype(jnp.bfloat16)
    w_v = (jax.random.normal(rng_keys[8], (MODEL_DIM, KV_HEADS * HEAD_DIM), jnp.float32) * in_scale).astype(jnp.bfloat16)
    w_o = (jax.random.normal(rng_keys[9], (NUM_HEADS * HEAD_DIM, MODEL_DIM), jnp.float32) * (NUM_HEADS * HEAD_DIM) ** -0.5).astype(jnp.bfloat16)
    return {"x_in": x_in, "dy_in": dy_in, "positions": positions, "g_attn": g_attn, "q_gain": q_gain, "k_gain": k_gain, "w_q": w_q, "w_k": w_k, "w_v": w_v, "w_o": w_o}


def rope_tables(positions):
    inv_freq = ROPE_THETA ** (-jnp.arange(0, HEAD_DIM, 2, dtype=jnp.float32) / HEAD_DIM)
    angles = positions.astype(jnp.float32)[:, :, None, None] * inv_freq
    return jnp.cos(angles), jnp.sin(angles)


def head_norm_rope(t_proj, weight, cos_tab, sin_tab):
    t_f32 = t_proj.astype(jnp.float32)
    t_hat = t_f32 * lax.rsqrt(jnp.mean(t_f32 * t_f32, axis=-1, keepdims=True) + EPS)
    scaled = t_hat * weight
    half_dim = HEAD_DIM // 2
    low_half = scaled[..., :half_dim]
    high_half = scaled[..., half_dim:]
    return jnp.concatenate([low_half * cos_tab - high_half * sin_tab, high_half * cos_tab + low_half * sin_tab], axis=-1)


def attend_row(row_args):
    q_row, k_row, v_row, do_row = row_args
    q_grp = q_row.reshape(SEQ_LEN, KV_HEADS, GROUP_SIZE, HEAD_DIM).astype(jnp.float32)
    do_grp = do_row.reshape(SEQ_LEN, KV_HEADS, GROUP_SIZE, HEAD_DIM).astype(jnp.float32)
    k_f32 = k_row.astype(jnp.float32)
    v_f32 = v_row.astype(jnp.float32)
    scores = jnp.einsum("qkgd,skd->kgqs", q_grp, k_f32) * ATT_SCALE
    causal = jnp.arange(SEQ_LEN)[:, None] >= jnp.arange(SEQ_LEN)[None, :]
    attn_prob = jax.nn.softmax(jnp.where(causal, scores, -jnp.inf), axis=-1)
    prob_bf = attn_prob.astype(jnp.bfloat16).astype(jnp.float32)
    row_out = jnp.einsum("kgqs,skd->qkgd", prob_bf, v_f32).astype(jnp.bfloat16)
    d_val = jnp.einsum("kgqs,qkgd->skd", prob_bf, do_grp).astype(jnp.bfloat16)
    d_prob = jnp.einsum("qkgd,skd->kgqs", do_grp, v_f32)
    d_score = attn_prob * (d_prob - jnp.sum(d_prob * attn_prob, axis=-1, keepdims=True)) * ATT_SCALE
    ds_bf = d_score.astype(jnp.bfloat16).astype(jnp.float32)
    d_query = jnp.einsum("kgqs,skd->qkgd", ds_bf, k_f32).astype(jnp.bfloat16)
    d_key = jnp.einsum("kgqs,qkgd->skd", ds_bf, q_grp).astype(jnp.bfloat16)
    return (row_out.reshape(SEQ_LEN, NUM_HEADS, HEAD_DIM), d_query.reshape(SEQ_LEN, NUM_HEADS, HEAD_DIM), d_key, d_val)


def reference(x_in, dy_in, positions, g_attn, q_gain, k_gain, w_q, w_k, w_v, w_o):
    x_f32 = x_in.astype(jnp.float32).reshape(-1, MODEL_DIM)
    inv_rms = lax.rsqrt(jnp.mean(x_f32 * x_f32, axis=-1, keepdims=True) + EPS)
    x_hat = x_f32 * inv_rms
    normed = (x_hat * g_attn.astype(jnp.float32)).astype(jnp.bfloat16)
    q_raw = jnp.dot(normed, w_q, preferred_element_type=jnp.float32).astype(jnp.bfloat16).reshape(BATCH_ROWS, SEQ_LEN, NUM_HEADS, HEAD_DIM)
    k_raw = jnp.dot(normed, w_k, preferred_element_type=jnp.float32).astype(jnp.bfloat16).reshape(BATCH_ROWS, SEQ_LEN, KV_HEADS, HEAD_DIM)
    v_proj = jnp.dot(normed, w_v, preferred_element_type=jnp.float32).astype(jnp.bfloat16).reshape(BATCH_ROWS, SEQ_LEN, KV_HEADS, HEAD_DIM)
    cos_tab, sin_tab = rope_tables(positions)
    q_rot, q_pull = jax.vjp(lambda t_proj, weight: head_norm_rope(t_proj, weight, cos_tab, sin_tab), q_raw, q_gain.astype(jnp.float32))
    k_rot, k_pull = jax.vjp(lambda t_proj, weight: head_norm_rope(t_proj, weight, cos_tab, sin_tab), k_raw, k_gain.astype(jnp.float32))
    dy_flat = dy_in.reshape(-1, MODEL_DIM)
    d_out = jnp.dot(dy_flat, w_o.T, preferred_element_type=jnp.float32).astype(jnp.bfloat16).reshape(BATCH_ROWS, SEQ_LEN, NUM_HEADS, HEAD_DIM)
    attn_out, dq_rot, dk_rot, dv_proj = lax.map(attend_row, (q_rot.astype(jnp.bfloat16), k_rot.astype(jnp.bfloat16), v_proj, d_out))
    o_flat = attn_out.reshape(-1, NUM_HEADS * HEAD_DIM)
    attn_sum = jnp.dot(o_flat, w_o, preferred_element_type=jnp.float32)
    y_out = (x_f32 + attn_sum).astype(jnp.bfloat16).reshape(x_in.shape)
    dw_o = jnp.dot(o_flat.T, dy_flat, preferred_element_type=jnp.float32)
    dq_raw, dq_gain = q_pull(dq_rot.astype(jnp.float32))
    dk_raw, dk_gain = k_pull(dk_rot.astype(jnp.float32))
    dq_flat = dq_raw.reshape(-1, NUM_HEADS * HEAD_DIM)
    dk_flat = dk_raw.reshape(-1, KV_HEADS * HEAD_DIM)
    dv_flat = dv_proj.reshape(-1, KV_HEADS * HEAD_DIM)
    dw_q = jnp.dot(normed.T, dq_flat, preferred_element_type=jnp.float32)
    dw_k = jnp.dot(normed.T, dk_flat, preferred_element_type=jnp.float32)
    dw_v = jnp.dot(normed.T, dv_flat, preferred_element_type=jnp.float32)
    d_normed = (jnp.dot(dq_flat, w_q.T, preferred_element_type=jnp.float32) + jnp.dot(dk_flat, w_k.T, preferred_element_type=jnp.float32) + jnp.dot(dv_flat, w_v.T, preferred_element_type=jnp.float32))
    dg_attn = jnp.sum(d_normed * x_hat, axis=0)
    d_scaled = d_normed * g_attn.astype(jnp.float32)
    dx_f32 = dy_flat.astype(jnp.float32) + inv_rms * (d_scaled - x_hat * jnp.mean(d_scaled * x_hat, axis=-1, keepdims=True))
    dx_out = dx_f32.astype(jnp.bfloat16).reshape(x_in.shape)
    return (y_out, dx_out, dw_q, dw_k, dw_v, dw_o, dq_gain, dk_gain, dg_attn)
```

```python
import functools
import jax
import jax.numpy as jnp
from jax import lax
from jax.experimental import pallas as pl
from jax.experimental.pallas import tpu as pltpu
from jax.sharding import PartitionSpec as P


EPS = 1e-6
THETA = 1000000.0
F32 = jnp.float32
BF16 = jnp.bfloat16
HD = 128
NT = (((1,), (1,)), ((), ()))
TN = (((0,), (0,)), ((), ()))
NN = (((1,), (0,)), ((), ()))


def dot(a, b, dims=NN):
    return lax.dot_general(a, b, dims, preferred_element_type=F32)


def weave(*lists):
    order = []
    for n, pieces in enumerate(lists):
        total = sum(c for c, _ in pieces) or 1
        at = 0
        for k, (c, f) in enumerate(pieces):
            order.append(((at + c / 2) / total, n, k, f))
            at += c
    for _, _, _, f in sorted(order, key=lambda e: e[:3]):
        f()


CH = 32


def attn_kernel(own, seq, n_grp, sel_ref, *refs):
    if own:
        (x0_ref, xn_ref, dy_ref, cos_ref, sin_ref, gain_ref, qg_ref, kg_ref, wq_ref, wk_ref, wv_ref, wo_ref,
         n_out, o_out, dq_out, dk_out, dv_out, dgq_out, dgk_out) = refs[:19]
        refs = refs[19:]
    else:
        nin_ref, dy_ref, cos_ref, sin_ref, qg_ref, kg_ref, wq_ref, wk_ref, wv_ref, wo_ref, _, _, _, _, o_out, dq_out, dk_out, dv_out = refs[:18]
        refs = refs[18:]
        n_ref = nin_ref
    (wot_ref, qnew_ref, knew_ref, vnew_ref, raw_ref, inv_ref, rot_ref, do_ref, v_ref, s_ref, dp_ref, p_ref, ds_ref, dkf_ref, dqf_ref, st_ref,
     tab_ref, o_ref, dq_ref, dk_ref, dv_ref) = refs[:21]
    if own:
        n_ref, nn_ref, dgq_ref, dgk_ref = refs[21:]
    half = seq // 2
    scale = HD ** -0.5
    log2e = 1.4426950408889634
    step = pl.program_id(0)

    def norm_rows(src, dst):
        def piece(c):
            def run():
                xf = src[c:c + 32, :].astype(F32)
                inv = lax.rsqrt(jnp.mean(xf * xf, axis=-1, keepdims=True) + EPS)
                dst[c:c + 32, :] = (xf * inv * gain_ref[0:1, :]).astype(BF16)

            return (1.5, run)

        return [piece(c) for c in range(0, seq, 32)]

    def proj(g):
        def q():
            t = dot(n_ref[...], wq_ref[:, g * 2 * HD:(g + 1) * 2 * HD])
            for h in range(2):
                qnew_ref[g % 2, h] = t[:, h * HD:(h + 1) * HD].astype(BF16)

        def k():
            t = dot(n_ref[...], wk_ref[:, g * HD:(g + 2) * HD])
            for h in range(2):
                knew_ref[g + h] = t[:, h * HD:(h + 1) * HD].astype(BF16)

        def v():
            t = dot(n_ref[...], wv_ref[:, g * HD:(g + 2) * HD])
            for h in range(2):
                vnew_ref[g + h] = t[:, h * HD:(h + 1) * HD].astype(BF16)

        def do():
            t = dot(dy_ref[...], wot_ref[:, g * 2 * HD:(g + 1) * 2 * HD])
            for h in range(2):
                do_ref[g, h * half:(h + 1) * half, :] = t[:half, h * HD:(h + 1) * HD].astype(BF16)
                do_ref[g, seq + h * half:seq + (h + 1) * half, :] = t[half:, h * HD:(h + 1) * HD].astype(BF16)

        return [(1, q)] + ([(1, k), (1, v)] if g % 2 == 0 else []) + [(1, do)]

    def stacked(h, c):
        return (h * half + c) if c < half else (seq + h * half + c - half)

    def rope(g):
        cs, sn = (tab_ref.at[2], tab_ref.at[3]) if g == n_grp - 1 else (tab_ref.at[0], tab_ref.at[1])

        def size(h, c):
            def run():
                raw = knew_ref[g, c:c + CH, :] if h == 2 else qnew_ref[g % 2, h, c:c + CH, :]
                raw_ref[g, h, c:c + CH, :] = raw
                t = raw.astype(F32)
                inv_ref[g, h, c:c + CH, :] = jnp.broadcast_to(lax.rsqrt(jnp.mean(t * t, axis=-1, keepdims=True) + EPS), t.shape)

            return (0.4, run)

        def turn(h, c):
            def run():
                t = raw_ref[g, h, c:c + CH, :].astype(F32)
                w = (t * inv_ref[g, h, c:c + CH, :]) * (kg_ref if h == 2 else qg_ref)[0:1, :]
                o = 2 * seq + c if h == 2 else stacked(h, c)
                x = pltpu.roll(w, HD // 2, 1)
                co, si = cs[c:c + CH, :], sn[c:c + CH, :]
                rot_ref[g, o:o + CH, 0:HD] = (w * co + x * si).astype(BF16)
                rot_ref[g, o:o + CH, HD:] = (x * co - w * si).astype(BF16)
                if h == 2:
                    v_ref[g, c:c + CH, :] = vnew_ref[g, c:c + CH, :]

            return (0.6, run)

        return [f(h, c) for f in (size, turn) for h in (2, 0, 1) for c in range(0, seq, CH)]

    def scores(g):
        b = g % 2

        def s():
            s_ref[b, 0:seq, 0:half] = dot(rot_ref[g, 0:seq, 0:HD], rot_ref[g, 2 * seq:2 * seq + half, 0:HD], NT)
            s_ref[b, seq:, :] = dot(rot_ref[g, seq:2 * seq, 0:HD], rot_ref[g, 2 * seq:, 0:HD], NT)

        def dp():
            dp_ref[b, 0:seq, 0:half] = dot(do_ref[g, :seq, :], v_ref[g, :half, :], NT)
            dp_ref[b, seq:, :] = dot(do_ref[g, seq:, :], v_ref[g], NT)

        return [(1, s), (1, dp)]

    def soft(g):
        b = g % 2
        c2 = scale * log2e

        def part(blk, c):
            return slice(blk * seq + c, blk * seq + c + CH), half if blk == 0 else seq

        def masked(blk, c, s):
            row_id = lax.broadcasted_iota(jnp.int32, (CH, half), 0) + (c % half)
            keep = row_id >= lax.broadcasted_iota(jnp.int32, (CH, half), 1)
            if blk == 0:
                return jnp.where(keep, s, -jnp.inf)
            return jnp.concatenate([s[:, :half], jnp.where(keep, s[:, half:], -jnp.inf)], axis=1)

        def wide(ref, rows, width):
            t = ref[rows, :]
            return t if width == half else jnp.concatenate([t, t], axis=1)

        def top(blk, c):
            rows, width = part(blk, c)

            def run():
                m = jnp.max(masked(blk, c, s_ref[b, rows, 0:width]), axis=-1, keepdims=True)
                st_ref[0, rows, :] = jnp.broadcast_to(m * c2, (CH, HD))

            return (0.4 + 0.4 * blk, run)

        def power(blk, c):
            rows, width = part(blk, c)

            def run():
                e = jnp.exp2(masked(blk, c, s_ref[b, rows, 0:width] * c2) - wide(st_ref.at[0], rows, width))
                s_ref[b, rows, 0:width] = e
                st_ref[1, rows, :] = jnp.broadcast_to(1.0 / jnp.sum(e, axis=-1, keepdims=True), (CH, HD))

            return (0.8 + 0.8 * blk, run)

        def prob(blk, c):
            rows, width = part(blk, c)

            def run():
                pr = s_ref[b, rows, 0:width] * wide(st_ref.at[1], rows, width)
                s_ref[b, rows, 0:width] = pr
                p_ref[b, rows, 0:width] = pr.astype(BF16)
                st_ref[2, rows, :] = jnp.broadcast_to(jnp.sum(pr * dp_ref[b, rows, 0:width], axis=-1, keepdims=True), (CH, HD))

            return (0.8 + 0.8 * blk, run)

        def last(blk, c):
            rows, width = part(blk, c)

            def run():
                d = dp_ref[b, rows, 0:width] - wide(st_ref.at[2], rows, width)
                ds_ref[b, rows, 0:width] = (s_ref[b, rows, 0:width] * d * scale).astype(BF16)

            return (0.8 + 0.8 * blk, run)

        return [f(blk, c) for f in (top, power, prob, last) for blk in range(2) for c in range(0, seq, CH)]

    def grads(g):
        b = g % 2
        col, kcol = g * 2 * HD, g * HD

        def dq():
            dqf_ref[b, 0:seq, :] = dot(ds_ref[b, 0:seq, 0:half], rot_ref[g, 2 * seq:2 * seq + half, :])
            dqf_ref[b, seq:, :] = dot(ds_ref[b, seq:, :], rot_ref[g, 2 * seq:, :])

        def dk():
            tb = dot(ds_ref[b, seq:, :], rot_ref[g, seq:2 * seq, :], TN)
            ta = dot(ds_ref[b, 0:seq, 0:half], rot_ref[g, 0:seq, :], TN)
            dkf_ref[b, :half, :] = tb[:half] + ta
            dkf_ref[b, half:, :] = tb[half:]

        def o():
            ta = dot(p_ref[b, 0:seq, 0:half], v_ref[g, :half, :])
            tb = dot(p_ref[b, seq:, :], v_ref[g])
            for h in range(2):
                o_ref[0:half, col + h * HD:col + (h + 1) * HD] = ta[h * half:(h + 1) * half].astype(BF16)
                o_ref[half:seq, col + h * HD:col + (h + 1) * HD] = tb[h * half:(h + 1) * half].astype(BF16)

        def dv():
            tb = dot(p_ref[b, seq:, :], do_ref[g, seq:, :], TN)
            ta = dot(p_ref[b, 0:seq, 0:half], do_ref[g, :seq, :], TN)
            dv_ref[0:half, kcol:kcol + HD] = (tb[:half] + ta).astype(BF16)
            dv_ref[half:seq, kcol:kcol + HD] = tb[half:].astype(BF16)

        return [(1, dq), (1, dk), (1, o), (1, dv)]

    def back(g):
        b = g % 2

        def place(h, c):
            if h == 2:
                return dkf_ref, c, dk_ref, g * HD, kg_ref
            return dqf_ref, stacked(h, c), dq_ref, (2 * g + h) * HD, qg_ref

        def turn(h, c):
            src, o, _, _, g_ref = place(h, c)

            def run():
                d = src[b, o:o + CH, :].astype(BF16).astype(F32)
                that = raw_ref[g, h, c:c + CH, :].astype(F32) * inv_ref[g, h, c:c + CH, :]
                du = d[:, :HD] * tab_ref[2, c:c + CH, :] - d[:, HD:] * tab_ref[3, c:c + CH, :]
                src[b, o:o + CH, 0:HD] = du
                pr = du * that
                if own:
                    dg_ref = dgk_ref if h == 2 else dgq_ref
                    dg_ref[...] += jnp.sum(pr.reshape(CH // 8, 8, HD), axis=0)
                st_ref[3 + h, c:c + CH, :] = jnp.broadcast_to(jnp.mean(pr * g_ref[0:1, :], axis=-1, keepdims=True), (CH, HD))

            return (0.6, run)

        def out(h, c):
            src, o, out_ref, col, g_ref = place(h, c)

            def run():
                inv = inv_ref[g, h, c:c + CH, :]
                that = raw_ref[g, h, c:c + CH, :].astype(F32) * inv
                out_ref[c:c + CH, col:col + HD] = (inv * (src[b, o:o + CH, 0:HD] * g_ref[0:1, :] - that * st_ref[3 + h, c:c + CH, :])).astype(BF16)

            return (0.5, run)

        return [f(h, c) for f in (turn, out) for h in (0, 1, 2) for c in range(0, seq, CH)]

    @pl.when(step == 0)
    def _():
        for c in range(0, wo_ref.shape[0], 256):
            for d in range(0, wo_ref.shape[1], 256):
                wot_ref[d:d + 256, c:c + 256] = wo_ref[c:c + 256, d:d + 256].T
        if own:
            weave(norm_rows(x0_ref, n_ref))

    tab_ref[2:4] = tab_ref[0:2]
    tab_ref[0] = cos_ref[...]
    tab_ref[1] = sin_ref[...]
    if own:
        norms = norm_rows(xn_ref, nn_ref)
    for g in range(n_grp):
        vec = soft((g - 3) % n_grp)
        sc = scores((g - 2) % n_grp)
        vec = vec + rope((g - 1) % n_grp)
        if own:
            vec += norms[g * len(norms) // n_grp:(g + 1) * len(norms) // n_grp]
        vec += back(g)
        gr = grads(g)
        for _, f in gr[:2]:
            f()
        weave(vec, sc + gr[2:] + proj(g))

    for dst, src in ((o_out, o_ref), (dq_out, dq_ref), (dk_out, dk_ref), (dv_out, dv_ref)):
        dst[0] = src[...]
    if own:
        n_out[...] = n_ref[...]
        n_ref[...] = nn_ref[...]
        keep = step > 0
        for dst, acc in ((dgq_out, dgq_ref), (dgk_out, dgk_ref)):
            acc[...] = jnp.where(keep, acc[...], 0.0)
            dst[...] = acc[...]


def attn_call(own, sel, x, dy, cosd, sind, gain, qg, kg, wq, wk, wv, wo, prev=None, seq=256):
    T, D = x.shape
    nq, nk = wq.shape[1], wk.shape[1]
    n_grp = nk // HD
    rows = T // seq
    const = lambda *b: pl.BlockSpec(b, lambda i, s: (0,) * len(b), pipeline_mode=pl.Buffered(1))
    now = lambda c: pl.BlockSpec((seq, c), lambda i, s: (jnp.minimum(i, rows - 1), 0))
    nxt = lambda c: pl.BlockSpec((seq, c), lambda i, s: (jnp.minimum(i + 1, rows - 1), 0))
    out3 = lambda c: pl.BlockSpec((1, seq, c), lambda i, s: (s[0], jnp.maximum(i - 1, 0), 0))
    mid = [now(D), now(HD), now(HD)]
    tail = [const(1, HD), const(1, HD), const(D, nq), const(D, nk), const(D, nk), const(nq, D)]
    shapes = [jax.ShapeDtypeStruct((2, T, c), BF16) for c in (nq, nq, nk, nk)]
    specs = [out3(nq), out3(nq), out3(nk), out3(nk)]
    aliases = {}
    if own:
        in_specs = [const(seq, D), nxt(D)] + mid + [const(1, D)] + tail
        args = [x, x, dy, cosd, sind, gain, qg, kg, wq, wk, wv, wo]
        shapes = [jax.ShapeDtypeStruct((T, D), BF16)] + shapes + [jax.ShapeDtypeStruct((8, HD), F32)] * 2
        specs = [now(D)] + specs + [pl.BlockSpec((8, HD), lambda i, s: (0, 0))] * 2
    else:
        in_specs = [now(D)] + mid + tail + [pl.BlockSpec(memory_space=pl.ANY)] * 4
        args = [x, dy, cosd, sind, qg, kg, wq, wk, wv, wo]
        aliases = {1 + len(args) + i: i for i in range(4)}
        args += list(prev)
    flops = 2 * T * D * (nq + 2 * nk + nq) + 12 * T * nq * seq
    return pl.pallas_call(
        functools.partial(attn_kernel, own, seq, n_grp),
        grid_spec=pltpu.PrefetchScalarGridSpec(
            num_scalar_prefetch=1,
            grid=(rows + 1,),
            in_specs=in_specs,
            out_specs=specs,
            scratch_shapes=[
                pltpu.VMEM((D, nq), BF16),
                pltpu.VMEM((2, 2, seq, HD), BF16),
                pltpu.VMEM((n_grp, seq, HD), BF16),
                pltpu.VMEM((n_grp, seq, HD), BF16),
                pltpu.VMEM((n_grp, 3, seq, HD), BF16),
                pltpu.VMEM((n_grp, 3, seq, HD), F32),
                pltpu.VMEM((n_grp, 3 * seq, 2 * HD), BF16),
                pltpu.VMEM((n_grp, 2 * seq, HD), BF16),
                pltpu.VMEM((n_grp, seq, HD), BF16),
                pltpu.VMEM((2, 2 * seq, seq), F32),
                pltpu.VMEM((2, 2 * seq, seq), F32),
                pltpu.VMEM((2, 2 * seq, seq), BF16),
                pltpu.VMEM((2, 2 * seq, seq), BF16),
                pltpu.VMEM((2, seq, 2 * HD), F32),
                pltpu.VMEM((2, 2 * seq, 2 * HD), F32),
                pltpu.VMEM((6, 2 * seq, HD), F32),
                pltpu.VMEM((4, seq, HD), F32),
            ] + [pltpu.VMEM((seq, c), BF16) for c in (nq, nq, nk, nk)]
            + ([pltpu.VMEM((seq, D), BF16)] * 2 + [pltpu.VMEM((8, HD), F32)] * 2 if own else []),
        ),
        out_shape=shapes,
        input_output_aliases=aliases,
        compiler_params=pltpu.CompilerParams(dimension_semantics=("arbitrary",), vmem_limit_bytes=56 << 20),
        cost_estimate=pl.CostEstimate(flops=flops, bytes_accessed=T * D * 6 + T * (2 * nq + 2 * nk) * 2, transcendentals=T * nq * 2),
        name="attn_own" if own else "attn_other",
    )(sel, *args)


def unpack_kernel(f_ref, q_ref, k_ref, v_ref, o_ref):
    d = q_ref.shape[0]
    nq, nk = q_ref.shape[1], k_ref.shape[1]
    q_ref[...] = f_ref[0, 0:d, 0:nq].astype(BF16)
    k_ref[...] = f_ref[0, 0:d, nq:nq + nk].astype(BF16)
    v_ref[...] = f_ref[0, 0:d, nq + nk:].astype(BF16)
    o_ref[...] = f_ref[0, d:, :].astype(BF16)


def unpack_call(gathered, D, nq, nk):
    n, r, c = gathered.shape
    part = lambda a, b: pl.BlockSpec((a // n, b), lambda i: (i, 0))
    return pl.pallas_call(
        unpack_kernel,
        grid=(n,),
        in_specs=[pl.BlockSpec((1, r, c), lambda i: (i, 0, 0), pipeline_mode=pl.Buffered(1))],
        out_specs=[part(D, nq), part(D, nk), part(D, nk), part(nq, D)],
        out_shape=[jax.ShapeDtypeStruct(s, BF16) for s in ((D, nq), (D, nk), (D, nk), (nq, D))],
        compiler_params=pltpu.CompilerParams(dimension_semantics=("arbitrary",), vmem_limit_bytes=60 << 20),
        cost_estimate=pl.CostEstimate(flops=n * r * c, bytes_accessed=n * r * c * 6, transcendentals=0),
        name="unpack",
    )(gathered)


def dw_kernel(n_out, sel_ref, a_ref, *refs):
    a = a_ref[0] if len(a_ref.shape) == 3 else a_ref[...]
    for b_ref, out_ref in zip(refs[:n_out], refs[n_out:]):
        b = b_ref[0] if len(b_ref.shape) == 3 else b_ref[...]

        @pl.when(pl.program_id(0) == 0)
        def _():
            out_ref[...] = jnp.zeros_like(out_ref)

        out_ref[...] += dot(a, b, TN)


def dw_call(sel, a, bs, tile=1024):
    def spec(v):
        if v.ndim == 3:
            return pl.BlockSpec((1, tile, v.shape[2]), lambda i, s: (s[0], i, 0))
        return pl.BlockSpec((tile, v.shape[1]), lambda i, s: (i, 0))

    T, M = a.shape[-2:]
    width = sum(b.shape[-1] for b in bs)
    return pl.pallas_call(
        functools.partial(dw_kernel, len(bs)),
        grid_spec=pltpu.PrefetchScalarGridSpec(
            num_scalar_prefetch=1,
            grid=(T // tile,),
            in_specs=[spec(a)] + [spec(b) for b in bs],
            out_specs=[pl.BlockSpec((M, b.shape[-1]), lambda i, s: (0, 0)) for b in bs],
        ),
        out_shape=[jax.ShapeDtypeStruct((M, b.shape[-1]), F32) for b in bs],
        compiler_params=pltpu.CompilerParams(dimension_semantics=("arbitrary",), vmem_limit_bytes=56 << 20),
        cost_estimate=pl.CostEstimate(flops=2 * T * M * width, bytes_accessed=2 * T * (M + width) + 4 * M * width, transcendentals=0),
    )(sel, a, *bs)


def out_kernel(m, sel_ref, x_ref, dy_ref, o_ref, dq_ref, dk_ref, dv_ref, gain_ref, *refs):
    own, oth = refs[:4], refs[4:8]
    y_out, dx_out, dg_out, wq_ref, wk_ref, wv_ref, wo_ref, dn_ref, oc_ref, y_ref, dx_ref, st_ref, dg_ref, sem = refs[8:]
    D = x_ref.shape[1]
    step = pl.program_id(0)
    ME = sel_ref[0]

    @pl.when(step == 0)
    def _():
        copies = []
        for k, dst in enumerate((wq_ref, wk_ref, wv_ref, wo_ref)):
            copies.append(pltpu.make_async_copy(own[k], dst.at[ME], sem.at[k]))
            copies.append(pltpu.make_async_copy(oth[k], dst.at[1 - ME], sem.at[4 + k]))
        for c in copies:
            c.start()
        for c in copies:
            c.wait()
        dg_ref[...] = jnp.zeros_like(dg_ref)

    CR = 32
    NC = 256

    def stat(c):
        def run():
            xf = x_ref[c:c + CR, :].astype(F32)
            st_ref[0, c:c + CR, :] = jnp.broadcast_to(lax.rsqrt(jnp.mean(xf * xf, axis=-1, keepdims=True) + EPS), (CR, HD))
            st_ref[1, c:c + CR, :] = jnp.zeros((CR, HD), F32)

        return (1, run)

    def keep(c):
        def run():
            for s in range(2):
                oc_ref[s, c:c + CR, :] = o_ref[s, c:c + CR, :]

        return (0.5, run)

    def dn_dot(n):
        def run():
            cols = slice(n * NC, (n + 1) * NC)
            t = None
            for s in range(2):
                for a_ref, w_ref in ((dq_ref, wq_ref), (dk_ref, wk_ref), (dv_ref, wv_ref)):
                    u = dot(a_ref[s], w_ref[s, cols, :], NT)
                    t = u if t is None else t + u
            dn_ref[:, cols] = t

        return (1, run)

    def wide(v):
        return jnp.concatenate([v] * (NC // HD), axis=1)

    def first(n, c):
        def run():
            cols = slice(n * NC, (n + 1) * NC)
            w = dn_ref[c:c + CR, cols] * (x_ref[c:c + CR, cols].astype(F32) * wide(st_ref[0, c:c + CR, :]))
            dg_ref[:, cols] += jnp.sum(w.reshape(CR // 8, 8, NC), axis=0)
            w = w * gain_ref[0:1, cols]
            st_ref[1, c:c + CR, :] += w[:, :HD] + w[:, HD:]

        return (1, run)

    def mean(c):
        def run():
            st_ref[2, c:c + CR, :] = jnp.broadcast_to(jnp.sum(st_ref[1, c:c + CR, :], axis=-1, keepdims=True) * (1.0 / D), (CR, HD))

        return (0.2, run)

    def second(n, c):
        def run():
            cols = slice(n * NC, (n + 1) * NC)
            inv = wide(st_ref[0, c:c + CR, :])
            xh = x_ref[c:c + CR, cols].astype(F32) * inv
            e = dn_ref[c:c + CR, cols] * gain_ref[0:1, cols]
            dx_ref[c:c + CR, cols] = (dy_ref[c:c + CR, cols].astype(F32) + inv * (e - xh * wide(st_ref[2, c:c + CR, :]))).astype(BF16)

        return (1, run)

    def y_dot(n):
        def run():
            cols = slice(n * NC, (n + 1) * NC)
            t = dot(oc_ref[0], wo_ref[0, :, cols]) + dot(oc_ref[1], wo_ref[1, :, cols])
            y_ref[:, cols] = (x_ref[:, cols].astype(F32) + t).astype(BF16)

        return (1, run)

    nn = D // NC
    rows = range(0, m, CR)
    dn = [dn_dot(n) for n in range(nn)]
    for _, f in dn[:1]:
        f()
    head = [stat(c) for c in rows] + [keep(c) for c in rows]
    weave(head, [dn[1]])
    for n in range(2, nn):
        weave([first(n - 2, c) for c in rows], [dn[n]])
    yd = [y_dot(n) for n in range(nn)]
    weave([first(nn - 2, c) for c in rows], yd[:1])
    weave([first(nn - 1, c) for c in rows] + [mean(c) for c in rows], yd[1:2])
    weave([second(n, c) for n in range(nn) for c in rows], yd[2:])
    y_out[...] = y_ref[...]
    dx_out[...] = dx_ref[...]
    dg_out[...] = dg_ref[...]


def out_call(sel, x, dy, o, dq, dk, dv, gain, own, oth, m=256):
    T, D = x.shape
    nq, nk = dq.shape[2], dk.shape[2]
    row = pl.BlockSpec((m, D), lambda i, s: (i, 0))
    two = lambda c: pl.BlockSpec((2, m, c), lambda i, s: (0, i, 0))
    hbm = pl.BlockSpec(memory_space=pl.ANY)
    return pl.pallas_call(
        functools.partial(out_kernel, m),
        grid_spec=pltpu.PrefetchScalarGridSpec(
            num_scalar_prefetch=1,
            grid=(T // m,),
            in_specs=[row, row, two(nq), two(nq), two(nk), two(nk), pl.BlockSpec((1, D), lambda i, s: (0, 0), pipeline_mode=pl.Buffered(1))] + [hbm] * 8,
            out_specs=[row, row, pl.BlockSpec((8, D), lambda i, s: (0, 0))],
            scratch_shapes=[
                pltpu.VMEM((2, D, nq), BF16),
                pltpu.VMEM((2, D, nk), BF16),
                pltpu.VMEM((2, D, nk), BF16),
                pltpu.VMEM((2, nq, D), BF16),
                pltpu.VMEM((m, D), F32),
                pltpu.VMEM((2, m, nq), BF16),
                pltpu.VMEM((m, D), BF16),
                pltpu.VMEM((m, D), BF16),
                pltpu.VMEM((3, m, HD), F32),
                pltpu.VMEM((8, D), F32),
                pltpu.SemaphoreType.DMA((8,)),
            ],
        ),
        out_shape=[jax.ShapeDtypeStruct((T, D), BF16)] * 2 + [jax.ShapeDtypeStruct((8, D), F32)],
        compiler_params=pltpu.CompilerParams(dimension_semantics=("arbitrary",), vmem_limit_bytes=60 << 20),
        cost_estimate=pl.CostEstimate(flops=2 * T * D * 2 * (2 * nq + 2 * nk), bytes_accessed=T * D * 8 + T * (4 * nq + 4 * nk) * 2, transcendentals=T),
        name="out",
    )(sel, x, dy, o, dq, dk, dv, gain, *own, *oth)


def solution(mesh):
    tok_spec = P("dp", None, None)
    col_spec = P(None, "tp")
    row_spec = P("tp", None)
    n_dp = mesh.shape["dp"]

    def per_device(x_in, dy_in, positions, g_attn, q_gain, k_gain, w_q, w_k, w_v, w_o):
        n_batch, n_seq, D = x_in.shape
        T = n_batch * n_seq
        nq, nk = w_q.shape[1], w_k.shape[1]
        x, dy = x_in.reshape(T, D), dy_in.reshape(T, D)
        me = lax.axis_index("tp").astype(jnp.int32)
        own = me.reshape(1)
        other = 1 - own

        part = lax.axis_index("dp") % 2
        cut = lambda w: lax.dynamic_slice_in_dim(w, part * (w.shape[0] // 2), w.shape[0] // 2, 0)
        share = jnp.concatenate([jnp.concatenate([cut(w_q), cut(w_k), cut(w_v)], axis=1), cut(w_o)], axis=0).astype(F32)
        share = lax.ppermute(share, "tp", [(0, 1), (1, 0)])
        gathered = lax.all_gather(share, "dp", axis_index_groups=[[2 * i, 2 * i + 1] for i in range(n_dp // 2)])

        inv_freq = THETA ** (-jnp.arange(0, HD, 2, dtype=F32) / HD)
        angles = positions.reshape(T, 1).astype(F32) * inv_freq
        cos, sin = jnp.cos(angles), jnp.sin(angles)
        cosd, sind = jnp.concatenate([cos, cos], axis=1), jnp.concatenate([-sin, sin], axis=1)
        gain = g_attn.astype(F32).reshape(1, D)
        qg, kg = q_gain.astype(F32).reshape(1, HD), k_gain.astype(F32).reshape(1, HD)

        n, o, dq, dk, dv, dgq, dgk = attn_call(True, own, x, dy, cosd, sind, gain, qg, kg, w_q, w_k, w_v, w_o, seq=n_seq)
        (dw_o,) = dw_call(own, o, [dy])
        (dw_q,) = dw_call(own, n, [dq])
        dw_k, dw_v = dw_call(own, n, [dk, dv])
        dw_o, dw_q, dw_k, dw_v = lax.psum((dw_o, dw_q, dw_k, dw_v), "dp")
        q_sum, k_sum = lax.psum((jnp.sum(dgq, axis=0), jnp.sum(dgk, axis=0)), ("tp", "dp"))

        theirs = unpack_call(gathered, D, nq, nk)
        o, dq, dk, dv = attn_call(False, other, n, dy, cosd, sind, gain, qg, kg, *theirs, prev=(o, dq, dk, dv), seq=n_seq)
        y, dx, dg = out_call(own, x, dy, o, dq, dk, dv, gain, (w_q, w_k, w_v, w_o), theirs)
        g_sum = lax.psum(jnp.sum(dg, axis=0), "dp")
        return y.reshape(x_in.shape), dx.reshape(x_in.shape), dw_q, dw_k, dw_v, dw_o, q_sum, k_sum, g_sum

    return jax.shard_map(per_device, mesh=mesh, in_specs=(tok_spec, tok_spec, P("dp", None), P(), P(), P(), col_spec, col_spec, col_spec, row_spec), out_specs=(tok_spec, tok_spec, col_spec, col_spec, col_spec, row_spec, P(), P(), P()), check_vma=False)
```

```python
import functools
import jax
import jax.numpy as jnp
from jax import lax
from jax.experimental import pallas as pl
from jax.experimental.pallas import tpu as pltpu
from jax.sharding import PartitionSpec as P


EPS = 1e-6
THETA = 1000000.0
F32 = jnp.float32
BF16 = jnp.bfloat16
HD = 128
NT = (((1,), (1,)), ((), ()))
TN = (((0,), (0,)), ((), ()))
NN = (((1,), (0,)), ((), ()))


def dot(a, b, dims=NN):
    return lax.dot_general(a, b, dims, preferred_element_type=F32)


def weave(*lists):
    order = []
    for n, pieces in enumerate(lists):
        total = sum(c for c, _ in pieces) or 1
        at = 0
        for k, (c, f) in enumerate(pieces):
            order.append(((at + c / 2) / total, n, k, f))
            at += c
    for _, _, _, f in sorted(order, key=lambda e: e[:3]):
        f()


CH = 32


def attn_kernel(own, seq, n_grp, sel_ref, *refs):
    if own:
        (x0_ref, xn_ref, dy_ref, cos_ref, sin_ref, gain_ref, qg_ref, kg_ref, wq_ref, wk_ref, wv_ref, wo_ref,
         n_out, o_out, dq_out, dk_out, dv_out, dgq_out, dgk_out) = refs[:19]
        refs = refs[19:]
    else:
        nin_ref, dy_ref, cos_ref, sin_ref, qg_ref, kg_ref, wq_ref, wk_ref, wv_ref, wo_ref, _, _, _, _, o_out, dq_out, dk_out, dv_out = refs[:18]
        refs = refs[18:]
        n_ref = nin_ref
    (wot_ref, qnew_ref, knew_ref, vnew_ref, raw_ref, inv_ref, rot_ref, do_ref, v_ref, s_ref, dp_ref, p_ref, ds_ref, dkf_ref, dqf_ref, st_ref,
     tab_ref, o_ref, dq_ref, dk_ref, dv_ref) = refs[:21]
    if own:
        n_ref, nn_ref, dgq_ref, dgk_ref = refs[21:]
    half = seq // 2
    scale = HD ** -0.5
    log2e = 1.4426950408889634
    step = pl.program_id(0)

    def norm_rows(src, dst):
        def piece(c):
            def run():
                xf = src[c:c + 32, :].astype(F32)
                inv = lax.rsqrt(jnp.mean(xf * xf, axis=-1, keepdims=True) + EPS)
                dst[c:c + 32, :] = (xf * inv * gain_ref[0:1, :]).astype(BF16)

            return (1.5, run)

        return [piece(c) for c in range(0, seq, 32)]

    def proj(g):
        def q():
            t = dot(n_ref[...], wq_ref[:, g * 2 * HD:(g + 1) * 2 * HD])
            for h in range(2):
                qnew_ref[g % 2, h] = t[:, h * HD:(h + 1) * HD].astype(BF16)

        def k():
            t = dot(n_ref[...], wk_ref[:, g * HD:(g + 2) * HD])
            for h in range(2):
                knew_ref[g + h] = t[:, h * HD:(h + 1) * HD].astype(BF16)

        def v():
            t = dot(n_ref[...], wv_ref[:, g * HD:(g + 2) * HD])
            for h in range(2):
                vnew_ref[g + h] = t[:, h * HD:(h + 1) * HD].astype(BF16)

        def do():
            t = dot(dy_ref[...], wot_ref[:, g * 2 * HD:(g + 1) * 2 * HD])
            for h in range(2):
                do_ref[g, h * half:(h + 1) * half, :] = t[:half, h * HD:(h + 1) * HD].astype(BF16)
                do_ref[g, seq + h * half:seq + (h + 1) * half, :] = t[half:, h * HD:(h + 1) * HD].astype(BF16)

        return [(1, q)] + ([(1, k), (1, v)] if g % 2 == 0 else []) + [(1, do)]

    def stacked(h, c):
        return (h * half + c) if c < half else (seq + h * half + c - half)

    def rope(g):
        cs, sn = (tab_ref.at[2], tab_ref.at[3]) if g == n_grp - 1 else (tab_ref.at[0], tab_ref.at[1])

        def size(h, c):
            def run():
                raw = knew_ref[g, c:c + CH, :] if h == 2 else qnew_ref[g % 2, h, c:c + CH, :]
                raw_ref[g, h, c:c + CH, :] = raw
                t = raw.astype(F32)
                inv_ref[g, h, c:c + CH, :] = jnp.broadcast_to(lax.rsqrt(jnp.mean(t * t, axis=-1, keepdims=True) + EPS), t.shape)

            return (0.4, run)

        def turn(h, c):
            def run():
                t = raw_ref[g, h, c:c + CH, :].astype(F32)
                w = (t * inv_ref[g, h, c:c + CH, :]) * (kg_ref if h == 2 else qg_ref)[0:1, :]
                o = 2 * seq + c if h == 2 else stacked(h, c)
                x = pltpu.roll(w, HD // 2, 1)
                co, si = cs[c:c + CH, :], sn[c:c + CH, :]
                rot_ref[g, o:o + CH, 0:HD] = (w * co + x * si).astype(BF16)
                rot_ref[g, o:o + CH, HD:] = (x * co - w * si).astype(BF16)
                if h == 2:
                    v_ref[g, c:c + CH, :] = vnew_ref[g, c:c + CH, :]

            return (0.6, run)

        return [f(h, c) for f in (size, turn) for h in (2, 0, 1) for c in range(0, seq, CH)]

    def scores(g):
        b = g % 2

        def s():
            s_ref[b, 0:seq, 0:half] = dot(rot_ref[g, 0:seq, 0:HD], rot_ref[g, 2 * seq:2 * seq + half, 0:HD], NT)
            s_ref[b, seq:, :] = dot(rot_ref[g, seq:2 * seq, 0:HD], rot_ref[g, 2 * seq:, 0:HD], NT)

        def dp():
            dp_ref[b, 0:seq, 0:half] = dot(do_ref[g, :seq, :], v_ref[g, :half, :], NT)
            dp_ref[b, seq:, :] = dot(do_ref[g, seq:, :], v_ref[g], NT)

        return [(1, s), (1, dp)]

    def soft(g):
        b = g % 2
        c2 = scale * log2e

        def part(blk, c):
            return slice(blk * seq + c, blk * seq + c + CH), half if blk == 0 else seq

        def masked(blk, c, s):
            row_id = lax.broadcasted_iota(jnp.int32, (CH, half), 0) + (c % half)
            keep = row_id >= lax.broadcasted_iota(jnp.int32, (CH, half), 1)
            if blk == 0:
                return jnp.where(keep, s, -jnp.inf)
            return jnp.concatenate([s[:, :half], jnp.where(keep, s[:, half:], -jnp.inf)], axis=1)

        def wide(ref, rows, width):
            t = ref[rows, :]
            return t if width == half else jnp.concatenate([t, t], axis=1)

        def top(blk, c):
            rows, width = part(blk, c)

            def run():
                m = jnp.max(masked(blk, c, s_ref[b, rows, 0:width]), axis=-1, keepdims=True)
                st_ref[0, rows, :] = jnp.broadcast_to(m * c2, (CH, HD))

            return (0.4 + 0.4 * blk, run)

        def power(blk, c):
            rows, width = part(blk, c)

            def run():
                e = jnp.exp2(masked(blk, c, s_ref[b, rows, 0:width] * c2) - wide(st_ref.at[0], rows, width))
                s_ref[b, rows, 0:width] = e
                st_ref[1, rows, :] = jnp.broadcast_to(1.0 / jnp.sum(e, axis=-1, keepdims=True), (CH, HD))

            return (0.8 + 0.8 * blk, run)

        def prob(blk, c):
            rows, width = part(blk, c)

            def run():
                pr = s_ref[b, rows, 0:width] * wide(st_ref.at[1], rows, width)
                s_ref[b, rows, 0:width] = pr
                p_ref[b, rows, 0:width] = pr.astype(BF16)
                st_ref[2, rows, :] = jnp.broadcast_to(jnp.sum(pr * dp_ref[b, rows, 0:width], axis=-1, keepdims=True), (CH, HD))

            return (0.8 + 0.8 * blk, run)

        def last(blk, c):
            rows, width = part(blk, c)

            def run():
                d = dp_ref[b, rows, 0:width] - wide(st_ref.at[2], rows, width)
                ds_ref[b, rows, 0:width] = (s_ref[b, rows, 0:width] * d * scale).astype(BF16)

            return (0.8 + 0.8 * blk, run)

        return [f(blk, c) for f in (top, power, prob, last) for blk in range(2) for c in range(0, seq, CH)]

    def grads(g):
        b = g % 2
        col, kcol = g * 2 * HD, g * HD

        def dq():
            dqf_ref[b, 0:seq, :] = dot(ds_ref[b, 0:seq, 0:half], rot_ref[g, 2 * seq:2 * seq + half, :])
            dqf_ref[b, seq:, :] = dot(ds_ref[b, seq:, :], rot_ref[g, 2 * seq:, :])

        def dk():
            tb = dot(ds_ref[b, seq:, :], rot_ref[g, seq:2 * seq, :], TN)
            ta = dot(ds_ref[b, 0:seq, 0:half], rot_ref[g, 0:seq, :], TN)
            dkf_ref[b, :half, :] = tb[:half] + ta
            dkf_ref[b, half:, :] = tb[half:]

        def o():
            ta = dot(p_ref[b, 0:seq, 0:half], v_ref[g, :half, :])
            tb = dot(p_ref[b, seq:, :], v_ref[g])
            for h in range(2):
                o_ref[0:half, col + h * HD:col + (h + 1) * HD] = ta[h * half:(h + 1) * half].astype(BF16)
                o_ref[half:seq, col + h * HD:col + (h + 1) * HD] = tb[h * half:(h + 1) * half].astype(BF16)

        def dv():
            tb = dot(p_ref[b, seq:, :], do_ref[g, seq:, :], TN)
            ta = dot(p_ref[b, 0:seq, 0:half], do_ref[g, :seq, :], TN)
            dv_ref[0:half, kcol:kcol + HD] = (tb[:half] + ta).astype(BF16)
            dv_ref[half:seq, kcol:kcol + HD] = tb[half:].astype(BF16)

        return [(1, dq), (1, dk), (1, o), (1, dv)]

    def back(g):
        b = g % 2

        def place(h, c):
            if h == 2:
                return dkf_ref, c, dk_ref, g * HD, kg_ref
            return dqf_ref, stacked(h, c), dq_ref, (2 * g + h) * HD, qg_ref

        def turn(h, c):
            src, o, _, _, g_ref = place(h, c)

            def run():
                d = src[b, o:o + CH, :].astype(BF16).astype(F32)
                that = raw_ref[g, h, c:c + CH, :].astype(F32) * inv_ref[g, h, c:c + CH, :]
                du = d[:, :HD] * tab_ref[2, c:c + CH, :] - d[:, HD:] * tab_ref[3, c:c + CH, :]
                src[b, o:o + CH, 0:HD] = du
                pr = du * that
                if own:
                    dg_ref = dgk_ref if h == 2 else dgq_ref
                    dg_ref[...] += jnp.sum(pr.reshape(CH // 8, 8, HD), axis=0)
                st_ref[3 + h, c:c + CH, :] = jnp.broadcast_to(jnp.mean(pr * g_ref[0:1, :], axis=-1, keepdims=True), (CH, HD))

            return (0.6, run)

        def out(h, c):
            src, o, out_ref, col, g_ref = place(h, c)

            def run():
                inv = inv_ref[g, h, c:c + CH, :]
                that = raw_ref[g, h, c:c + CH, :].astype(F32) * inv
                out_ref[c:c + CH, col:col + HD] = (inv * (src[b, o:o + CH, 0:HD] * g_ref[0:1, :] - that * st_ref[3 + h, c:c + CH, :])).astype(BF16)

            return (0.5, run)

        return [f(h, c) for f in (turn, out) for h in (0, 1, 2) for c in range(0, seq, CH)]

    @pl.when(step == 0)
    def _():
        for c in range(0, wo_ref.shape[0], 256):
            for d in range(0, wo_ref.shape[1], 256):
                wot_ref[d:d + 256, c:c + 256] = wo_ref[c:c + 256, d:d + 256].T
        if own:
            weave(norm_rows(x0_ref, n_ref))

    tab_ref[2:4] = tab_ref[0:2]
    tab_ref[0] = cos_ref[...]
    tab_ref[1] = sin_ref[...]
    if own:
        norms = norm_rows(xn_ref, nn_ref)
    for g in range(n_grp):
        vec = soft((g - 3) % n_grp)
        sc = scores((g - 2) % n_grp)
        vec = vec + rope((g - 1) % n_grp)
        if own:
            vec += norms[g * len(norms) // n_grp:(g + 1) * len(norms) // n_grp]
        vec += back(g)
        gr = grads(g)
        for _, f in gr[:2]:
            f()
        weave(vec, sc + gr[2:] + proj(g))

    for dst, src in ((o_out, o_ref), (dq_out, dq_ref), (dk_out, dk_ref), (dv_out, dv_ref)):
        dst[0] = src[...]
    if own:
        n_out[...] = n_ref[...]
        n_ref[...] = nn_ref[...]
        keep = step > 0
        for dst, acc in ((dgq_out, dgq_ref), (dgk_out, dgk_ref)):
            acc[...] = jnp.where(keep, acc[...], 0.0)
            dst[...] = acc[...]


def attn_call(own, sel, x, dy, cosd, sind, gain, qg, kg, wq, wk, wv, wo, prev=None, seq=256):
    T, D = x.shape
    nq, nk = wq.shape[1], wk.shape[1]
    n_grp = nk // HD
    rows = T // seq
    const = lambda *b: pl.BlockSpec(b, lambda i, s: (0,) * len(b), pipeline_mode=pl.Buffered(1))
    now = lambda c: pl.BlockSpec((seq, c), lambda i, s: (jnp.minimum(i, rows - 1), 0))
    nxt = lambda c: pl.BlockSpec((seq, c), lambda i, s: (jnp.minimum(i + 1, rows - 1), 0))
    out3 = lambda c: pl.BlockSpec((1, seq, c), lambda i, s: (s[0], jnp.maximum(i - 1, 0), 0))
    mid = [now(D), now(HD), now(HD)]
    tail = [const(1, HD), const(1, HD), const(D, nq), const(D, nk), const(D, nk), const(nq, D)]
    shapes = [jax.ShapeDtypeStruct((2, T, c), BF16) for c in (nq, nq, nk, nk)]
    specs = [out3(nq), out3(nq), out3(nk), out3(nk)]
    aliases = {}
    if own:
        in_specs = [const(seq, D), nxt(D)] + mid + [const(1, D)] + tail
        args = [x, x, dy, cosd, sind, gain, qg, kg, wq, wk, wv, wo]
        shapes = [jax.ShapeDtypeStruct((T, D), BF16)] + shapes + [jax.ShapeDtypeStruct((8, HD), F32)] * 2
        specs = [now(D)] + specs + [pl.BlockSpec((8, HD), lambda i, s: (0, 0))] * 2
    else:
        in_specs = [now(D)] + mid + tail + [pl.BlockSpec(memory_space=pl.ANY)] * 4
        args = [x, dy, cosd, sind, qg, kg, wq, wk, wv, wo]
        aliases = {1 + len(args) + i: i for i in range(4)}
        args += list(prev)
    flops = 2 * T * D * (nq + 2 * nk + nq) + 12 * T * nq * seq
    return pl.pallas_call(
        functools.partial(attn_kernel, own, seq, n_grp),
        grid_spec=pltpu.PrefetchScalarGridSpec(
            num_scalar_prefetch=1,
            grid=(rows + 1,),
            in_specs=in_specs,
            out_specs=specs,
            scratch_shapes=[
                pltpu.VMEM((D, nq), BF16),
                pltpu.VMEM((2, 2, seq, HD), BF16),
                pltpu.VMEM((n_grp, seq, HD), BF16),
                pltpu.VMEM((n_grp, seq, HD), BF16),
                pltpu.VMEM((n_grp, 3, seq, HD), BF16),
                pltpu.VMEM((n_grp, 3, seq, HD), F32),
                pltpu.VMEM((n_grp, 3 * seq, 2 * HD), BF16),
                pltpu.VMEM((n_grp, 2 * seq, HD), BF16),
                pltpu.VMEM((n_grp, seq, HD), BF16),
                pltpu.VMEM((2, 2 * seq, seq), F32),
                pltpu.VMEM((2, 2 * seq, seq), F32),
                pltpu.VMEM((2, 2 * seq, seq), BF16),
                pltpu.VMEM((2, 2 * seq, seq), BF16),
                pltpu.VMEM((2, seq, 2 * HD), F32),
                pltpu.VMEM((2, 2 * seq, 2 * HD), F32),
                pltpu.VMEM((6, 2 * seq, HD), F32),
                pltpu.VMEM((4, seq, HD), F32),
            ] + [pltpu.VMEM((seq, c), BF16) for c in (nq, nq, nk, nk)]
            + ([pltpu.VMEM((seq, D), BF16)] * 2 + [pltpu.VMEM((8, HD), F32)] * 2 if own else []),
        ),
        out_shape=shapes,
        input_output_aliases=aliases,
        compiler_params=pltpu.CompilerParams(dimension_semantics=("arbitrary",), vmem_limit_bytes=56 << 20),
        cost_estimate=pl.CostEstimate(flops=flops, bytes_accessed=T * D * 6 + T * (2 * nq + 2 * nk) * 2, transcendentals=T * nq * 2),
        name="attn_own" if own else "attn_other",
    )(sel, *args)


def unpack_kernel(f_ref, q_ref, k_ref, v_ref, o_ref):
    d = q_ref.shape[0]
    nq, nk = q_ref.shape[1], k_ref.shape[1]
    q_ref[...] = f_ref[0, 0:d, 0:nq].astype(BF16)
    k_ref[...] = f_ref[0, 0:d, nq:nq + nk].astype(BF16)
    v_ref[...] = f_ref[0, 0:d, nq + nk:].astype(BF16)
    o_ref[...] = f_ref[0, d:, :].astype(BF16)


def unpack_call(gathered, D, nq, nk):
    n, r, c = gathered.shape
    part = lambda a, b: pl.BlockSpec((a // n, b), lambda i: (i, 0))
    return pl.pallas_call(
        unpack_kernel,
        grid=(n,),
        in_specs=[pl.BlockSpec((1, r, c), lambda i: (i, 0, 0), pipeline_mode=pl.Buffered(1))],
        out_specs=[part(D, nq), part(D, nk), part(D, nk), part(nq, D)],
        out_shape=[jax.ShapeDtypeStruct(s, BF16) for s in ((D, nq), (D, nk), (D, nk), (nq, D))],
        compiler_params=pltpu.CompilerParams(dimension_semantics=("arbitrary",), vmem_limit_bytes=60 << 20),
        cost_estimate=pl.CostEstimate(flops=n * r * c, bytes_accessed=n * r * c * 6, transcendentals=0),
        name="unpack",
    )(gathered)


def dw_kernel(n_out, sel_ref, a_ref, *refs):
    a = a_ref[0] if len(a_ref.shape) == 3 else a_ref[...]
    for b_ref, out_ref in zip(refs[:n_out], refs[n_out:]):
        b = b_ref[0] if len(b_ref.shape) == 3 else b_ref[...]

        @pl.when(pl.program_id(0) == 0)
        def _():
            out_ref[...] = jnp.zeros_like(out_ref)

        out_ref[...] += dot(a, b, TN)


def dw_call(sel, a, bs, tile=1024):
    def spec(v):
        if v.ndim == 3:
            return pl.BlockSpec((1, tile, v.shape[2]), lambda i, s: (s[0], i, 0))
        return pl.BlockSpec((tile, v.shape[1]), lambda i, s: (i, 0))

    T, M = a.shape[-2:]
    width = sum(b.shape[-1] for b in bs)
    return pl.pallas_call(
        functools.partial(dw_kernel, len(bs)),
        grid_spec=pltpu.PrefetchScalarGridSpec(
            num_scalar_prefetch=1,
            grid=(T // tile,),
            in_specs=[spec(a)] + [spec(b) for b in bs],
            out_specs=[pl.BlockSpec((M, b.shape[-1]), lambda i, s: (0, 0)) for b in bs],
        ),
        out_shape=[jax.ShapeDtypeStruct((M, b.shape[-1]), F32) for b in bs],
        compiler_params=pltpu.CompilerParams(dimension_semantics=("arbitrary",), vmem_limit_bytes=56 << 20),
        cost_estimate=pl.CostEstimate(flops=2 * T * M * width, bytes_accessed=2 * T * (M + width) + 4 * M * width, transcendentals=0),
    )(sel, a, *bs)


def out_kernel(m, sel_ref, x_ref, dy_ref, o_ref, dq_ref, dk_ref, dv_ref, gain_ref, *refs):
    own, oth = refs[:4], refs[4:8]
    y_out, dx_out, dg_out, wq_ref, wk_ref, wv_ref, wo_ref, dn_ref, oc_ref, y_ref, dx_ref, st_ref, dg_ref, sem = refs[8:]
    D = x_ref.shape[1]
    step = pl.program_id(0)
    ME = sel_ref[0]

    @pl.when(step == 0)
    def _():
        copies = []
        for k, dst in enumerate((wq_ref, wk_ref, wv_ref, wo_ref)):
            copies.append(pltpu.make_async_copy(own[k], dst.at[ME], sem.at[k]))
            copies.append(pltpu.make_async_copy(oth[k], dst.at[1 - ME], sem.at[4 + k]))
        for c in copies:
            c.start()
        for c in copies:
            c.wait()
        dg_ref[...] = jnp.zeros_like(dg_ref)

    CR = 32
    NC = 256

    def stat(c):
        def run():
            xf = x_ref[c:c + CR, :].astype(F32)
            st_ref[0, c:c + CR, :] = jnp.broadcast_to(lax.rsqrt(jnp.mean(xf * xf, axis=-1, keepdims=True) + EPS), (CR, HD))
            st_ref[1, c:c + CR, :] = jnp.zeros((CR, HD), F32)

        return (1, run)

    def keep(c):
        def run():
            for s in range(2):
                oc_ref[s, c:c + CR, :] = o_ref[s, c:c + CR, :]

        return (0.5, run)

    def dn_dot(n):
        def run():
            cols = slice(n * NC, (n + 1) * NC)
            t = None
            for s in range(2):
                for a_ref, w_ref in ((dq_ref, wq_ref), (dk_ref, wk_ref), (dv_ref, wv_ref)):
                    u = dot(a_ref[s], w_ref[s, cols, :], NT)
                    t = u if t is None else t + u
            dn_ref[:, cols] = t

        return (1, run)

    def wide(v):
        return jnp.concatenate([v] * (NC // HD), axis=1)

    def first(n, c):
        def run():
            cols = slice(n * NC, (n + 1) * NC)
            w = dn_ref[c:c + CR, cols] * (x_ref[c:c + CR, cols].astype(F32) * wide(st_ref[0, c:c + CR, :]))
            dg_ref[:, cols] += jnp.sum(w.reshape(CR // 8, 8, NC), axis=0)
            w = w * gain_ref[0:1, cols]
            st_ref[1, c:c + CR, :] += w[:, :HD] + w[:, HD:]

        return (1, run)

    def mean(c):
        def run():
            st_ref[2, c:c + CR, :] = jnp.broadcast_to(jnp.sum(st_ref[1, c:c + CR, :], axis=-1, keepdims=True) * (1.0 / D), (CR, HD))

        return (0.2, run)

    def second(n, c):
        def run():
            cols = slice(n * NC, (n + 1) * NC)
            inv = wide(st_ref[0, c:c + CR, :])
            xh = x_ref[c:c + CR, cols].astype(F32) * inv
            e = dn_ref[c:c + CR, cols] * gain_ref[0:1, cols]
            dx_ref[c:c + CR, cols] = (dy_ref[c:c + CR, cols].astype(F32) + inv * (e - xh * wide(st_ref[2, c:c + CR, :]))).astype(BF16)

        return (1, run)

    def y_dot(n):
        def run():
            cols = slice(n * NC, (n + 1) * NC)
            t = dot(oc_ref[0], wo_ref[0, :, cols]) + dot(oc_ref[1], wo_ref[1, :, cols])
            y_ref[:, cols] = (x_ref[:, cols].astype(F32) + t).astype(BF16)

        return (1, run)

    nn = D // NC
    rows = range(0, m, CR)
    dn = [dn_dot(n) for n in range(nn)]
    for _, f in dn[:1]:
        f()
    head = [stat(c) for c in rows] + [keep(c) for c in rows]
    weave(head, [dn[1]])
    for n in range(2, nn):
        weave([first(n - 2, c) for c in rows], [dn[n]])
    yd = [y_dot(n) for n in range(nn)]
    weave([first(nn - 2, c) for c in rows], yd[:1])
    weave([first(nn - 1, c) for c in rows] + [mean(c) for c in rows], yd[1:2])
    weave([second(n, c) for n in range(nn) for c in rows], yd[2:])
    y_out[...] = y_ref[...]
    dx_out[...] = dx_ref[...]
    dg_out[...] = dg_ref[...]


def out_call(sel, x, dy, o, dq, dk, dv, gain, own, oth, m=256):
    T, D = x.shape
    nq, nk = dq.shape[2], dk.shape[2]
    row = pl.BlockSpec((m, D), lambda i, s: (i, 0))
    two = lambda c: pl.BlockSpec((2, m, c), lambda i, s: (0, i, 0))
    hbm = pl.BlockSpec(memory_space=pl.ANY)
    return pl.pallas_call(
        functools.partial(out_kernel, m),
        grid_spec=pltpu.PrefetchScalarGridSpec(
            num_scalar_prefetch=1,
            grid=(T // m,),
            in_specs=[row, row, two(nq), two(nq), two(nk), two(nk), pl.BlockSpec((1, D), lambda i, s: (0, 0), pipeline_mode=pl.Buffered(1))] + [hbm] * 8,
            out_specs=[row, row, pl.BlockSpec((8, D), lambda i, s: (0, 0))],
            scratch_shapes=[
                pltpu.VMEM((2, D, nq), BF16),
                pltpu.VMEM((2, D, nk), BF16),
                pltpu.VMEM((2, D, nk), BF16),
                pltpu.VMEM((2, nq, D), BF16),
                pltpu.VMEM((m, D), F32),
                pltpu.VMEM((2, m, nq), BF16),
                pltpu.VMEM((m, D), BF16),
                pltpu.VMEM((m, D), BF16),
                pltpu.VMEM((3, m, HD), F32),
                pltpu.VMEM((8, D), F32),
                pltpu.SemaphoreType.DMA((8,)),
            ],
        ),
        out_shape=[jax.ShapeDtypeStruct((T, D), BF16)] * 2 + [jax.ShapeDtypeStruct((8, D), F32)],
        compiler_params=pltpu.CompilerParams(dimension_semantics=("arbitrary",), vmem_limit_bytes=60 << 20),
        cost_estimate=pl.CostEstimate(flops=2 * T * D * 2 * (2 * nq + 2 * nk), bytes_accessed=T * D * 8 + T * (4 * nq + 4 * nk) * 2, transcendentals=T),
        name="out",
    )(sel, x, dy, o, dq, dk, dv, gain, *own, *oth)


def pack_kernel(sel_ref, q_ref, k_ref, v_ref, o_ref, out_ref):
    d, nq, nk = q_ref.shape[0], q_ref.shape[1], k_ref.shape[1]
    out_ref[0, 0:d, 0:nq] = q_ref[...].astype(F32)
    out_ref[0, 0:d, nq:nq + nk] = k_ref[...].astype(F32)
    out_ref[0, 0:d, nq + nk:] = v_ref[...].astype(F32)
    out_ref[0, d:, :] = o_ref[...].astype(F32)


def pack_call(part, w_q, w_k, w_v, w_o, parts=2, cuts=4):
    D, nq = w_q.shape
    spec = lambda w: pl.BlockSpec((w.shape[0] // (parts * cuts), w.shape[1]), lambda i, s: (s[0] * cuts + i, 0))
    r = (D + nq) // (parts * cuts)
    return pl.pallas_call(
        pack_kernel,
        grid_spec=pltpu.PrefetchScalarGridSpec(
            num_scalar_prefetch=1,
            grid=(cuts,),
            in_specs=[spec(w) for w in (w_q, w_k, w_v, w_o)],
            out_specs=pl.BlockSpec((1, r, D), lambda i, s: (i, 0, 0)),
        ),
        out_shape=jax.ShapeDtypeStruct((cuts, r, D), F32),
        compiler_params=pltpu.CompilerParams(dimension_semantics=("arbitrary",), vmem_limit_bytes=60 << 20),
        cost_estimate=pl.CostEstimate(flops=cuts * r * D, bytes_accessed=cuts * r * D * 6, transcendentals=0),
        name="pack",
    )(part, w_q, w_k, w_v, w_o)


def table_kernel(pos_ref, freq_ref, cos_ref, sin_ref):
    n, seq = pos_ref.shape
    lane = lax.broadcasted_iota(jnp.int32, (HD, HD), 1)
    for r in range(n):
        for h in range(seq // HD):
            p = pos_ref[r:r + 1, h * HD:(h + 1) * HD].astype(F32)
            a = jnp.broadcast_to(p, (HD, HD)).T * freq_ref[0:1, :]
            k = jnp.round(a * 0.6366197723675814)
            x = ((a - k * 1.5703125) - k * 4.837512969970703125e-4) - k * 7.549789948768648e-8
            z = x * x
            s = ((-1.9515295891e-4 * z + 8.3321608736e-3) * z - 1.6666654611e-1) * z * x + x
            c = ((2.443315711809948e-5 * z - 1.388731625493765e-3) * z + 4.166664568298827e-2) * z * z - 0.5 * z + 1.0
            q = k.astype(jnp.int32)
            odd = (q & 1) == 1
            co, si = jnp.where(odd, s, c), jnp.where(odd, c, s)
            rows = slice((r * (seq // HD) + h) * HD, (r * (seq // HD) + h + 1) * HD)
            cos_ref[rows, :] = jnp.where(((q + 1) & 2) == 0, co, -co)
            sin_ref[rows, :] = jnp.where(((q & 2) == 0) == (lane >= HD // 2), si, -si)


def table_call(positions, rows=8):
    n, seq = positions.shape
    freq = THETA ** (-jnp.arange(0, HD, 2, dtype=F32) / HD)
    freq = jnp.concatenate([freq, freq]).reshape(1, HD)
    out = pl.BlockSpec((rows * seq, HD), lambda i: (i, 0))
    return pl.pallas_call(
        table_kernel,
        grid=(n // rows,),
        in_specs=[pl.BlockSpec((rows, seq), lambda i: (i, 0)), pl.BlockSpec((1, HD), lambda i: (0, 0))],
        out_specs=[out, out],
        out_shape=[jax.ShapeDtypeStruct((n * seq, HD), F32)] * 2,
        compiler_params=pltpu.CompilerParams(dimension_semantics=("arbitrary",), vmem_limit_bytes=60 << 20),
        cost_estimate=pl.CostEstimate(flops=n * seq * HD * 30, bytes_accessed=n * seq * HD * 8, transcendentals=0),
        name="table",
    )(positions, freq)


def solution(mesh):
    tok_spec = P("dp", None, None)
    col_spec = P(None, "tp")
    row_spec = P("tp", None)
    n_dp = mesh.shape["dp"]

    def per_device(x_in, dy_in, positions, g_attn, q_gain, k_gain, w_q, w_k, w_v, w_o):
        n_batch, n_seq, D = x_in.shape
        T = n_batch * n_seq
        nq, nk = w_q.shape[1], w_k.shape[1]
        x, dy = x_in.reshape(T, D), dy_in.reshape(T, D)
        me = lax.axis_index("tp").astype(jnp.int32)
        own = me.reshape(1)
        other = 1 - own

        part = (lax.axis_index("dp") % 2).astype(jnp.int32).reshape(1)
        share = pack_call(part, w_q, w_k, w_v, w_o)
        share = lax.ppermute(share, "tp", [(0, 1), (1, 0)])
        gathered = lax.all_gather(share, "dp", axis_index_groups=[[2 * i, 2 * i + 1] for i in range(n_dp // 2)])
        gathered = gathered.reshape(-1, *gathered.shape[2:])

        cosd, sind = table_call(positions)
        gain = g_attn.astype(F32).reshape(1, D)
        qg, kg = q_gain.astype(F32).reshape(1, HD), k_gain.astype(F32).reshape(1, HD)

        n, o, dq, dk, dv, dgq, dgk = attn_call(True, own, x, dy, cosd, sind, gain, qg, kg, w_q, w_k, w_v, w_o, seq=n_seq)
        (dw_o,) = dw_call(own, o, [dy])
        (dw_q,) = dw_call(own, n, [dq])
        dw_k, dw_v = dw_call(own, n, [dk, dv])
        dw_o, dw_q, dw_k, dw_v = lax.psum((dw_o, dw_q, dw_k, dw_v), "dp")

        theirs = unpack_call(gathered, D, nq, nk)
        o, dq, dk, dv = attn_call(False, other, n, dy, cosd, sind, gain, qg, kg, *theirs, prev=(o, dq, dk, dv), seq=n_seq)
        y, dx, dg = out_call(own, x, dy, o, dq, dk, dv, gain, (w_q, w_k, w_v, w_o), theirs)
        small = jnp.sum(jnp.concatenate([0.5 * dg, dgq, dgk], axis=1), axis=0)
        small = lax.psum(small, ("tp", "dp"))
        g_sum, q_sum, k_sum = small[:D], small[D:D + HD], small[D + HD:]
        return y.reshape(x_in.shape), dx.reshape(x_in.shape), dw_q, dw_k, dw_v, dw_o, q_sum, k_sum, g_sum

    return jax.shard_map(per_device, mesh=mesh, in_specs=(tok_spec, tok_spec, P("dp", None), P(), P(), P(), col_spec, col_spec, col_spec, row_spec), out_specs=(tok_spec, tok_spec, col_spec, col_spec, col_spec, row_spec, P(), P(), P()), check_vma=False)
```

```python
import functools
from types import SimpleNamespace
import jax
import jax.numpy as jnp
from jax import lax
from jax.experimental import pallas as pl
from jax.experimental.pallas import tpu as pltpu
from jax.sharding import PartitionSpec as P


EPS = 1e-6
THETA = 1000000.0
F32 = jnp.float32
BF16 = jnp.bfloat16
HD = 128
NT = (((1,), (1,)), ((), ()))
TN = (((0,), (0,)), ((), ()))
NN = (((1,), (0,)), ((), ()))


def dot(a, b, dims=NN):
    return lax.dot_general(a, b, dims, preferred_element_type=F32)


def weave(*lists):
    order = []
    for n, pieces in enumerate(lists):
        total = sum(c for c, _ in pieces) or 1
        at = 0
        for k, (c, f) in enumerate(pieces):
            order.append(((at + c / 2) / total, n, k, f))
            at += c
    for _, _, _, f in sorted(order, key=lambda e: e[:3]):
        f()


CH = 32


def attn_kernel(own, seq, n_grp, sel_ref, *refs):
    if own:
        (x0_ref, xn_ref, dy_ref, cos_ref, sin_ref, gain_ref, qg_ref, kg_ref, wq_ref, wk_ref, wv_ref, wo_ref,
         n_out, o_out, dq_out, dk_out, dv_out, dgq_out, dgk_out) = refs[:19]
        refs = refs[19:]
    else:
        nin_ref, dy_ref, cos_ref, sin_ref, qg_ref, kg_ref, wq_ref, wk_ref, wv_ref, wo_ref, _, _, _, _, o_out, dq_out, dk_out, dv_out = refs[:18]
        refs = refs[18:]
        n_ref = nin_ref
    (wot_ref, qnew_ref, knew_ref, vnew_ref, raw_ref, inv_ref, rot_ref, do_ref, v_ref, s_ref, dp_ref, p_ref, ds_ref, dkf_ref, dqf_ref, st_ref,
     tab_ref, o_ref, dq_ref, dk_ref, dv_ref) = refs[:21]
    if own:
        n_ref, nn_ref, dgq_ref, dgk_ref = refs[21:]
    half = seq // 2
    scale = HD ** -0.5
    log2e = 1.4426950408889634
    step = pl.program_id(0)

    def norm_rows(src, dst):
        def piece(c):
            def run():
                xf = src[c:c + 32, :].astype(F32)
                inv = lax.rsqrt(jnp.mean(xf * xf, axis=-1, keepdims=True) + EPS)
                dst[c:c + 32, :] = (xf * inv * gain_ref[0:1, :]).astype(BF16)

            return (1.5, run)

        return [piece(c) for c in range(0, seq, 32)]

    def proj(g):
        def q():
            t = dot(n_ref[...], wq_ref[:, g * 2 * HD:(g + 1) * 2 * HD])
            for h in range(2):
                qnew_ref[g % 2, h] = t[:, h * HD:(h + 1) * HD].astype(BF16)

        def k():
            t = dot(n_ref[...], wk_ref[:, g * HD:(g + 2) * HD])
            for h in range(2):
                knew_ref[g + h] = t[:, h * HD:(h + 1) * HD].astype(BF16)

        def v():
            t = dot(n_ref[...], wv_ref[:, g * HD:(g + 2) * HD])
            for h in range(2):
                vnew_ref[g + h] = t[:, h * HD:(h + 1) * HD].astype(BF16)

        def do():
            t = dot(dy_ref[...], wot_ref[:, g * 2 * HD:(g + 1) * 2 * HD])
            for h in range(2):
                do_ref[g, h * half:(h + 1) * half, :] = t[:half, h * HD:(h + 1) * HD].astype(BF16)
                do_ref[g, seq + h * half:seq + (h + 1) * half, :] = t[half:, h * HD:(h + 1) * HD].astype(BF16)

        return [(1, q)] + ([(1, k), (1, v)] if g % 2 == 0 else []) + [(1, do)]

    def stacked(h, c):
        return (h * half + c) if c < half else (seq + h * half + c - half)

    def rope(g):
        cs, sn = (tab_ref.at[2], tab_ref.at[3]) if g == n_grp - 1 else (tab_ref.at[0], tab_ref.at[1])

        def size(h, c):
            def run():
                raw = knew_ref[g, c:c + CH, :] if h == 2 else qnew_ref[g % 2, h, c:c + CH, :]
                raw_ref[g, h, c:c + CH, :] = raw
                t = raw.astype(F32)
                inv_ref[g, h, c:c + CH, :] = jnp.broadcast_to(lax.rsqrt(jnp.mean(t * t, axis=-1, keepdims=True) + EPS), t.shape)

            return (0.4, run)

        def turn(h, c):
            def run():
                t = raw_ref[g, h, c:c + CH, :].astype(F32)
                w = (t * inv_ref[g, h, c:c + CH, :]) * (kg_ref if h == 2 else qg_ref)[0:1, :]
                o = 2 * seq + c if h == 2 else stacked(h, c)
                x = pltpu.roll(w, HD // 2, 1)
                co, si = cs[c:c + CH, :], sn[c:c + CH, :]
                rot_ref[g, o:o + CH, 0:HD] = (w * co + x * si).astype(BF16)
                rot_ref[g, o:o + CH, HD:] = (x * co - w * si).astype(BF16)
                if h == 2:
                    v_ref[g, c:c + CH, :] = vnew_ref[g, c:c + CH, :]

            return (0.6, run)

        return [f(h, c) for f in (size, turn) for h in (2, 0, 1) for c in range(0, seq, CH)]

    def scores(g):
        b = g % 2

        def s():
            s_ref[b, 0:seq, 0:half] = dot(rot_ref[g, 0:seq, 0:HD], rot_ref[g, 2 * seq:2 * seq + half, 0:HD], NT)
            s_ref[b, seq:, :] = dot(rot_ref[g, seq:2 * seq, 0:HD], rot_ref[g, 2 * seq:, 0:HD], NT)

        def dp():
            dp_ref[b, 0:seq, 0:half] = dot(do_ref[g, :seq, :], v_ref[g, :half, :], NT)
            dp_ref[b, seq:, :] = dot(do_ref[g, seq:, :], v_ref[g], NT)

        return [(1, s), (1, dp)]

    def soft(g):
        b = g % 2
        c2 = scale * log2e

        def part(blk, c):
            return slice(blk * seq + c, blk * seq + c + CH), half if blk == 0 else seq

        def masked(blk, c, s):
            row_id = lax.broadcasted_iota(jnp.int32, (CH, half), 0) + (c % half)
            keep = row_id >= lax.broadcasted_iota(jnp.int32, (CH, half), 1)
            if blk == 0:
                return jnp.where(keep, s, -jnp.inf)
            return jnp.concatenate([s[:, :half], jnp.where(keep, s[:, half:], -jnp.inf)], axis=1)

        def wide(ref, rows, width):
            t = ref[rows, :]
            return t if width == half else jnp.concatenate([t, t], axis=1)

        def top(blk, c):
            rows, width = part(blk, c)

            def run():
                m = jnp.max(masked(blk, c, s_ref[b, rows, 0:width]), axis=-1, keepdims=True)
                st_ref[0, rows, :] = jnp.broadcast_to(m * c2, (CH, HD))

            return (0.4 + 0.4 * blk, run)

        def power(blk, c):
            rows, width = part(blk, c)

            def run():
                e = jnp.exp2(masked(blk, c, s_ref[b, rows, 0:width] * c2) - wide(st_ref.at[0], rows, width))
                s_ref[b, rows, 0:width] = e
                st_ref[1, rows, :] = jnp.broadcast_to(1.0 / jnp.sum(e, axis=-1, keepdims=True), (CH, HD))

            return (0.8 + 0.8 * blk, run)

        def prob(blk, c):
            rows, width = part(blk, c)

            def run():
                pr = s_ref[b, rows, 0:width] * wide(st_ref.at[1], rows, width)
                s_ref[b, rows, 0:width] = pr
                p_ref[b, rows, 0:width] = pr.astype(BF16)
                st_ref[2, rows, :] = jnp.broadcast_to(jnp.sum(pr * dp_ref[b, rows, 0:width], axis=-1, keepdims=True), (CH, HD))

            return (0.8 + 0.8 * blk, run)

        def last(blk, c):
            rows, width = part(blk, c)

            def run():
                d = dp_ref[b, rows, 0:width] - wide(st_ref.at[2], rows, width)
                ds_ref[b, rows, 0:width] = (s_ref[b, rows, 0:width] * d * scale).astype(BF16)

            return (0.8 + 0.8 * blk, run)

        return [f(blk, c) for f in (top, power, prob, last) for blk in range(2) for c in range(0, seq, CH)]

    def grads(g):
        b = g % 2
        col, kcol = g * 2 * HD, g * HD

        def dq():
            dqf_ref[b, 0:seq, :] = dot(ds_ref[b, 0:seq, 0:half], rot_ref[g, 2 * seq:2 * seq + half, :])
            dqf_ref[b, seq:, :] = dot(ds_ref[b, seq:, :], rot_ref[g, 2 * seq:, :])

        def dk():
            tb = dot(ds_ref[b, seq:, :], rot_ref[g, seq:2 * seq, :], TN)
            ta = dot(ds_ref[b, 0:seq, 0:half], rot_ref[g, 0:seq, :], TN)
            dkf_ref[b, :half, :] = tb[:half] + ta
            dkf_ref[b, half:, :] = tb[half:]

        def o():
            ta = dot(p_ref[b, 0:seq, 0:half], v_ref[g, :half, :])
            tb = dot(p_ref[b, seq:, :], v_ref[g])
            for h in range(2):
                o_ref[0:half, col + h * HD:col + (h + 1) * HD] = ta[h * half:(h + 1) * half].astype(BF16)
                o_ref[half:seq, col + h * HD:col + (h + 1) * HD] = tb[h * half:(h + 1) * half].astype(BF16)

        def dv():
            tb = dot(p_ref[b, seq:, :], do_ref[g, seq:, :], TN)
            ta = dot(p_ref[b, 0:seq, 0:half], do_ref[g, :seq, :], TN)
            dv_ref[0:half, kcol:kcol + HD] = (tb[:half] + ta).astype(BF16)
            dv_ref[half:seq, kcol:kcol + HD] = tb[half:].astype(BF16)

        return [(1, dq), (1, dk), (1, o), (1, dv)]

    def back(g):
        b = g % 2

        def place(h, c):
            if h == 2:
                return dkf_ref, c, dk_ref, g * HD, kg_ref
            return dqf_ref, stacked(h, c), dq_ref, (2 * g + h) * HD, qg_ref

        def turn(h, c):
            src, o, _, _, g_ref = place(h, c)

            def run():
                d = src[b, o:o + CH, :].astype(BF16).astype(F32)
                that = raw_ref[g, h, c:c + CH, :].astype(F32) * inv_ref[g, h, c:c + CH, :]
                du = d[:, :HD] * tab_ref[2, c:c + CH, :] - d[:, HD:] * tab_ref[3, c:c + CH, :]
                src[b, o:o + CH, 0:HD] = du
                pr = du * that
                if own:
                    dg_ref = dgk_ref if h == 2 else dgq_ref
                    dg_ref[...] += jnp.sum(pr.reshape(CH // 8, 8, HD), axis=0)
                st_ref[3 + h, c:c + CH, :] = jnp.broadcast_to(jnp.mean(pr * g_ref[0:1, :], axis=-1, keepdims=True), (CH, HD))

            return (0.6, run)

        def out(h, c):
            src, o, out_ref, col, g_ref = place(h, c)

            def run():
                inv = inv_ref[g, h, c:c + CH, :]
                that = raw_ref[g, h, c:c + CH, :].astype(F32) * inv
                out_ref[c:c + CH, col:col + HD] = (inv * (src[b, o:o + CH, 0:HD] * g_ref[0:1, :] - that * st_ref[3 + h, c:c + CH, :])).astype(BF16)

            return (0.5, run)

        return [f(h, c) for f in (turn, out) for h in (0, 1, 2) for c in range(0, seq, CH)]

    @pl.when(step == 0)
    def _():
        for c in range(0, wo_ref.shape[0], 256):
            for d in range(0, wo_ref.shape[1], 256):
                wot_ref[d:d + 256, c:c + 256] = wo_ref[c:c + 256, d:d + 256].T
        if own:
            weave(norm_rows(x0_ref, n_ref))

    tab_ref[2:4] = tab_ref[0:2]
    tab_ref[0] = cos_ref[...]
    tab_ref[1] = sin_ref[...]
    if own:
        norms = norm_rows(xn_ref, nn_ref)
    for g in range(n_grp):
        vec = soft((g - 3) % n_grp)
        sc = scores((g - 2) % n_grp)
        vec = vec + rope((g - 1) % n_grp)
        if own:
            vec += norms[g * len(norms) // n_grp:(g + 1) * len(norms) // n_grp]
        vec += back(g)
        gr = grads(g)
        for _, f in gr[:2]:
            f()
        weave(vec, sc + gr[2:] + proj(g))

    for dst, src in ((o_out, o_ref), (dq_out, dq_ref), (dk_out, dk_ref), (dv_out, dv_ref)):
        dst[0] = src[...]
    if own:
        n_out[...] = n_ref[...]
        n_ref[...] = nn_ref[...]
        keep = step > 0
        for dst, acc in ((dgq_out, dgq_ref), (dgk_out, dgk_ref)):
            acc[...] = jnp.where(keep, acc[...], 0.0)
            dst[...] = acc[...]


def attn_call(own, sel, x, dy, cosd, sind, gain, qg, kg, wq, wk, wv, wo, prev=None, seq=256):
    T, D = x.shape
    nq, nk = wq.shape[1], wk.shape[1]
    n_grp = nk // HD
    rows = T // seq
    const = lambda *b: pl.BlockSpec(b, lambda i, s: (0,) * len(b), pipeline_mode=pl.Buffered(1))
    now = lambda c: pl.BlockSpec((seq, c), lambda i, s: (jnp.minimum(i, rows - 1), 0))
    nxt = lambda c: pl.BlockSpec((seq, c), lambda i, s: (jnp.minimum(i + 1, rows - 1), 0))
    out3 = lambda c: pl.BlockSpec((1, seq, c), lambda i, s: (s[0], jnp.maximum(i - 1, 0), 0))
    mid = [now(D), now(HD), now(HD)]
    tail = [const(1, HD), const(1, HD), const(D, nq), const(D, nk), const(D, nk), const(nq, D)]
    shapes = [jax.ShapeDtypeStruct((2, T, c), BF16) for c in (nq, nq, nk, nk)]
    specs = [out3(nq), out3(nq), out3(nk), out3(nk)]
    aliases = {}
    if own:
        in_specs = [const(seq, D), nxt(D)] + mid + [const(1, D)] + tail
        args = [x, x, dy, cosd, sind, gain, qg, kg, wq, wk, wv, wo]
        shapes = [jax.ShapeDtypeStruct((T, D), BF16)] + shapes + [jax.ShapeDtypeStruct((8, HD), F32)] * 2
        specs = [now(D)] + specs + [pl.BlockSpec((8, HD), lambda i, s: (0, 0))] * 2
    else:
        in_specs = [now(D)] + mid + tail + [pl.BlockSpec(memory_space=pl.ANY)] * 4
        args = [x, dy, cosd, sind, qg, kg, wq, wk, wv, wo]
        aliases = {1 + len(args) + i: i for i in range(4)}
        args += list(prev)
    flops = 2 * T * D * (nq + 2 * nk + nq) + 12 * T * nq * seq
    return pl.pallas_call(
        functools.partial(attn_kernel, own, seq, n_grp),
        grid_spec=pltpu.PrefetchScalarGridSpec(
            num_scalar_prefetch=1,
            grid=(rows + 1,),
            in_specs=in_specs,
            out_specs=specs,
            scratch_shapes=[
                pltpu.VMEM((D, nq), BF16),
                pltpu.VMEM((2, 2, seq, HD), BF16),
                pltpu.VMEM((n_grp, seq, HD), BF16),
                pltpu.VMEM((n_grp, seq, HD), BF16),
                pltpu.VMEM((n_grp, 3, seq, HD), BF16),
                pltpu.VMEM((n_grp, 3, seq, HD), F32),
                pltpu.VMEM((n_grp, 3 * seq, 2 * HD), BF16),
                pltpu.VMEM((n_grp, 2 * seq, HD), BF16),
                pltpu.VMEM((n_grp, seq, HD), BF16),
                pltpu.VMEM((2, 2 * seq, seq), F32),
                pltpu.VMEM((2, 2 * seq, seq), F32),
                pltpu.VMEM((2, 2 * seq, seq), BF16),
                pltpu.VMEM((2, 2 * seq, seq), BF16),
                pltpu.VMEM((2, seq, 2 * HD), F32),
                pltpu.VMEM((2, 2 * seq, 2 * HD), F32),
                pltpu.VMEM((6, 2 * seq, HD), F32),
                pltpu.VMEM((4, seq, HD), F32),
            ] + [pltpu.VMEM((seq, c), BF16) for c in (nq, nq, nk, nk)]
            + ([pltpu.VMEM((seq, D), BF16)] * 2 + [pltpu.VMEM((8, HD), F32)] * 2 if own else []),
        ),
        out_shape=shapes,
        input_output_aliases=aliases,
        compiler_params=pltpu.CompilerParams(dimension_semantics=("arbitrary",), vmem_limit_bytes=56 << 20),
        cost_estimate=pl.CostEstimate(flops=flops, bytes_accessed=T * D * 6 + T * (2 * nq + 2 * nk) * 2, transcendentals=T * nq * 2),
        name="attn_own" if own else "attn_other",
    )(sel, *args)


def unpack_kernel(f_ref, q_ref, k_ref, v_ref, o_ref):
    d = q_ref.shape[0]
    nq, nk = q_ref.shape[1], k_ref.shape[1]
    q_ref[...] = f_ref[0, 0:d, 0:nq].astype(BF16)
    k_ref[...] = f_ref[0, 0:d, nq:nq + nk].astype(BF16)
    v_ref[...] = f_ref[0, 0:d, nq + nk:].astype(BF16)
    o_ref[...] = f_ref[0, d:, :].astype(BF16)


def unpack_call(gathered, D, nq, nk):
    n, r, c = gathered.shape
    part = lambda a, b: pl.BlockSpec((a // n, b), lambda i: (i, 0))
    return pl.pallas_call(
        unpack_kernel,
        grid=(n,),
        in_specs=[pl.BlockSpec((1, r, c), lambda i: (i, 0, 0))],
        out_specs=[part(D, nq), part(D, nk), part(D, nk), part(nq, D)],
        out_shape=[jax.ShapeDtypeStruct(s, BF16) for s in ((D, nq), (D, nk), (D, nk), (nq, D))],
        compiler_params=pltpu.CompilerParams(dimension_semantics=("arbitrary",), vmem_limit_bytes=60 << 20),
        cost_estimate=pl.CostEstimate(flops=n * r * c, bytes_accessed=n * r * c * 6, transcendentals=0),
        name="unpack",
    )(gathered)


def dw_kernel(n_out, sel_ref, a_ref, *refs):
    a = a_ref[0] if len(a_ref.shape) == 3 else a_ref[...]
    for b_ref, out_ref in zip(refs[:n_out], refs[n_out:]):
        b = b_ref[0] if len(b_ref.shape) == 3 else b_ref[...]

        @pl.when(pl.program_id(0) == 0)
        def _():
            out_ref[...] = jnp.zeros_like(out_ref)

        out_ref[...] += dot(a, b, TN)


def dw_call(sel, a, bs, tile=1024):
    def spec(v):
        if v.ndim == 3:
            return pl.BlockSpec((1, tile, v.shape[2]), lambda i, s: (s[0], i, 0))
        return pl.BlockSpec((tile, v.shape[1]), lambda i, s: (i, 0))

    T, M = a.shape[-2:]
    width = sum(b.shape[-1] for b in bs)
    return pl.pallas_call(
        functools.partial(dw_kernel, len(bs)),
        grid_spec=pltpu.PrefetchScalarGridSpec(
            num_scalar_prefetch=1,
            grid=(T // tile,),
            in_specs=[spec(a)] + [spec(b) for b in bs],
            out_specs=[pl.BlockSpec((M, b.shape[-1]), lambda i, s: (0, 0)) for b in bs],
        ),
        out_shape=[jax.ShapeDtypeStruct((M, b.shape[-1]), F32) for b in bs],
        compiler_params=pltpu.CompilerParams(dimension_semantics=("arbitrary",), vmem_limit_bytes=56 << 20),
        cost_estimate=pl.CostEstimate(flops=2 * T * M * width, bytes_accessed=2 * T * (M + width) + 4 * M * width, transcendentals=0),
    )(sel, a, *bs)


def pack_kernel(sel_ref, q_ref, k_ref, v_ref, o_ref, out_ref):
    d, nq, nk = q_ref.shape[0], q_ref.shape[1], k_ref.shape[1]
    out_ref[0, 0:d, 0:nq] = q_ref[...].astype(F32)
    out_ref[0, 0:d, nq:nq + nk] = k_ref[...].astype(F32)
    out_ref[0, 0:d, nq + nk:] = v_ref[...].astype(F32)
    out_ref[0, d:, :] = o_ref[...].astype(F32)


def pack_call(part, w_q, w_k, w_v, w_o, parts=2, cuts=4):
    D, nq = w_q.shape
    spec = lambda w: pl.BlockSpec((w.shape[0] // (parts * cuts), w.shape[1]), lambda i, s: (s[0] * cuts + i, 0))
    r = (D + nq) // (parts * cuts)
    return pl.pallas_call(
        pack_kernel,
        grid_spec=pltpu.PrefetchScalarGridSpec(
            num_scalar_prefetch=1,
            grid=(cuts,),
            in_specs=[spec(w) for w in (w_q, w_k, w_v, w_o)],
            out_specs=pl.BlockSpec((1, r, D), lambda i, s: (i, 0, 0)),
        ),
        out_shape=jax.ShapeDtypeStruct((cuts, r, D), F32),
        compiler_params=pltpu.CompilerParams(dimension_semantics=("arbitrary",), vmem_limit_bytes=60 << 20),
        cost_estimate=pl.CostEstimate(flops=cuts * r * D, bytes_accessed=cuts * r * D * 6, transcendentals=0),
        name="pack",
    )(part, w_q, w_k, w_v, w_o)


def table_kernel(pos_ref, freq_ref, cos_ref, sin_ref):
    n, seq = pos_ref.shape
    lane = lax.broadcasted_iota(jnp.int32, (HD, HD), 1)
    for r in range(n):
        for h in range(seq // HD):
            p = pos_ref[r:r + 1, h * HD:(h + 1) * HD].astype(F32)
            a = jnp.broadcast_to(p, (HD, HD)).T * freq_ref[0:1, :]
            k = jnp.round(a * 0.6366197723675814)
            x = ((a - k * 1.5703125) - k * 4.837512969970703125e-4) - k * 7.549789948768648e-8
            z = x * x
            s = ((-1.9515295891e-4 * z + 8.3321608736e-3) * z - 1.6666654611e-1) * z * x + x
            c = ((2.443315711809948e-5 * z - 1.388731625493765e-3) * z + 4.166664568298827e-2) * z * z - 0.5 * z + 1.0
            q = k.astype(jnp.int32)
            odd = (q & 1) == 1
            co, si = jnp.where(odd, s, c), jnp.where(odd, c, s)
            rows = slice((r * (seq // HD) + h) * HD, (r * (seq // HD) + h + 1) * HD)
            cos_ref[rows, :] = jnp.where(((q + 1) & 2) == 0, co, -co)
            sin_ref[rows, :] = jnp.where(((q & 2) == 0) == (lane >= HD // 2), si, -si)


def table_call(positions, rows=8):
    n, seq = positions.shape
    freq = THETA ** (-jnp.arange(0, HD, 2, dtype=F32) / HD)
    freq = jnp.concatenate([freq, freq]).reshape(1, HD)
    out = pl.BlockSpec((rows * seq, HD), lambda i: (i, 0))
    return pl.pallas_call(
        table_kernel,
        grid=(n // rows,),
        in_specs=[pl.BlockSpec((rows, seq), lambda i: (i, 0)), pl.BlockSpec((1, HD), lambda i: (0, 0))],
        out_specs=[out, out],
        out_shape=[jax.ShapeDtypeStruct((n * seq, HD), F32)] * 2,
        compiler_params=pltpu.CompilerParams(dimension_semantics=("arbitrary",), vmem_limit_bytes=60 << 20),
        cost_estimate=pl.CostEstimate(flops=n * seq * HD * 30, bytes_accessed=n * seq * HD * 8, transcendentals=0),
        name="table",
    )(positions, freq)


def attn_stages(seq, n_grp, r):
    half = seq // 2
    scale = HD ** -0.5
    log2e = 1.4426950408889634

    def norm_rows(src, dst):
        def piece(c):
            def run():
                xf = src[c:c + 32, :].astype(F32)
                inv = lax.rsqrt(jnp.mean(xf * xf, axis=-1, keepdims=True) + EPS)
                dst[c:c + 32, :] = (xf * inv * r.gain[0:1, :]).astype(BF16)

            return (1.5, run)

        return [piece(c) for c in range(0, seq, 32)]

    def proj(g):
        def q():
            t = dot(r.n[...], r.wq(slice(g * 2 * HD, (g + 1) * 2 * HD)))
            for h in range(2):
                r.qnew[g % 2, h] = t[:, h * HD:(h + 1) * HD].astype(BF16)

        def k():
            t = dot(r.n[...], r.wk(slice(g * HD, (g + 2) * HD)))
            for h in range(2):
                r.knew[g + h] = t[:, h * HD:(h + 1) * HD].astype(BF16)

        def v():
            t = dot(r.n[...], r.wv(slice(g * HD, (g + 2) * HD)))
            for h in range(2):
                r.vnew[g + h] = t[:, h * HD:(h + 1) * HD].astype(BF16)

        def do():
            t = r.do_dot(slice(g * 2 * HD, (g + 1) * 2 * HD))
            for h in range(2):
                r.do[g, h * half:(h + 1) * half, :] = t[:half, h * HD:(h + 1) * HD].astype(BF16)
                r.do[g, seq + h * half:seq + (h + 1) * half, :] = t[half:, h * HD:(h + 1) * HD].astype(BF16)

        return [(1, q)] + ([(1, k), (1, v)] if g % 2 == 0 else []) + [(1, do)]

    def stacked(h, c):
        return (h * half + c) if c < half else (seq + h * half + c - half)

    def rope(g):
        cs, sn = (r.tab.at[2], r.tab.at[3]) if g == n_grp - 1 else (r.tab.at[0], r.tab.at[1])

        def size(h, c):
            def run():
                raw = r.knew[g, c:c + CH, :] if h == 2 else r.qnew[g % 2, h, c:c + CH, :]
                r.raw[g, h, c:c + CH, :] = raw
                t = raw.astype(F32)
                r.inv[g, h, c:c + CH, :] = jnp.broadcast_to(lax.rsqrt(jnp.mean(t * t, axis=-1, keepdims=True) + EPS), t.shape)

            return (0.4, run)

        def turn(h, c):
            def run():
                t = r.raw[g, h, c:c + CH, :].astype(F32)
                w = (t * r.inv[g, h, c:c + CH, :]) * (r.kg if h == 2 else r.qg)[0:1, :]
                o = 2 * seq + c if h == 2 else stacked(h, c)
                x = pltpu.roll(w, HD // 2, 1)
                co, si = cs[c:c + CH, :], sn[c:c + CH, :]
                r.rot[g, o:o + CH, 0:HD] = (w * co + x * si).astype(BF16)
                r.rot[g, o:o + CH, HD:] = (x * co - w * si).astype(BF16)
                if h == 2:
                    r.v[g, c:c + CH, :] = r.vnew[g, c:c + CH, :]

            return (0.6, run)

        return [f(h, c) for f in (size, turn) for h in (2, 0, 1) for c in range(0, seq, CH)]

    def scores(g):
        b = g % 2

        def s():
            r.s[b, 0:seq, 0:half] = dot(r.rot[g, 0:seq, 0:HD], r.rot[g, 2 * seq:2 * seq + half, 0:HD], NT)
            r.s[b, seq:, :] = dot(r.rot[g, seq:2 * seq, 0:HD], r.rot[g, 2 * seq:, 0:HD], NT)

        def dp():
            r.dp[b, 0:seq, 0:half] = dot(r.do[g, :seq, :], r.v[g, :half, :], NT)
            r.dp[b, seq:, :] = dot(r.do[g, seq:, :], r.v[g], NT)

        return [(1, s), (1, dp)]

    def soft(g):
        b = g % 2
        c2 = scale * log2e

        def part(blk, c):
            return slice(blk * seq + c, blk * seq + c + CH), half if blk == 0 else seq

        def masked(blk, c, s):
            row_id = lax.broadcasted_iota(jnp.int32, (CH, half), 0) + (c % half)
            keep = row_id >= lax.broadcasted_iota(jnp.int32, (CH, half), 1)
            if blk == 0:
                return jnp.where(keep, s, -jnp.inf)
            return jnp.concatenate([s[:, :half], jnp.where(keep, s[:, half:], -jnp.inf)], axis=1)

        def wide(ref, rows, width):
            t = ref[rows, :]
            return t if width == half else jnp.concatenate([t, t], axis=1)

        def top(blk, c):
            rows, width = part(blk, c)

            def run():
                m = jnp.max(masked(blk, c, r.s[b, rows, 0:width]), axis=-1, keepdims=True)
                r.st[0, rows, :] = jnp.broadcast_to(m * c2, (CH, HD))

            return (0.4 + 0.4 * blk, run)

        def power(blk, c):
            rows, width = part(blk, c)

            def run():
                e = jnp.exp2(masked(blk, c, r.s[b, rows, 0:width] * c2) - wide(r.st.at[0], rows, width))
                r.s[b, rows, 0:width] = e
                r.st[1, rows, :] = jnp.broadcast_to(1.0 / jnp.sum(e, axis=-1, keepdims=True), (CH, HD))

            return (0.8 + 0.8 * blk, run)

        def prob(blk, c):
            rows, width = part(blk, c)

            def run():
                pr = r.s[b, rows, 0:width] * wide(r.st.at[1], rows, width)
                r.s[b, rows, 0:width] = pr
                r.p[b, rows, 0:width] = pr.astype(BF16)
                r.st[2, rows, :] = jnp.broadcast_to(jnp.sum(pr * r.dp[b, rows, 0:width], axis=-1, keepdims=True), (CH, HD))

            return (0.8 + 0.8 * blk, run)

        def last(blk, c):
            rows, width = part(blk, c)

            def run():
                d = r.dp[b, rows, 0:width] - wide(r.st.at[2], rows, width)
                r.ds[b, rows, 0:width] = (r.s[b, rows, 0:width] * d * scale).astype(BF16)

            return (0.8 + 0.8 * blk, run)

        return [f(blk, c) for f in (top, power, prob, last) for blk in range(2) for c in range(0, seq, CH)]

    def grads(g):
        b = g % 2
        col, kcol = g * 2 * HD, g * HD

        def dq():
            r.dqf[b, 0:seq, :] = dot(r.ds[b, 0:seq, 0:half], r.rot[g, 2 * seq:2 * seq + half, :])
            r.dqf[b, seq:, :] = dot(r.ds[b, seq:, :], r.rot[g, 2 * seq:, :])

        def dk():
            tb = dot(r.ds[b, seq:, :], r.rot[g, seq:2 * seq, :], TN)
            ta = dot(r.ds[b, 0:seq, 0:half], r.rot[g, 0:seq, :], TN)
            r.dkf[b, :half, :] = tb[:half] + ta
            r.dkf[b, half:, :] = tb[half:]

        def o():
            ta = dot(r.p[b, 0:seq, 0:half], r.v[g, :half, :])
            tb = dot(r.p[b, seq:, :], r.v[g])
            for h in range(2):
                r.o[0:half, col + h * HD:col + (h + 1) * HD] = ta[h * half:(h + 1) * half].astype(BF16)
                r.o[half:seq, col + h * HD:col + (h + 1) * HD] = tb[h * half:(h + 1) * half].astype(BF16)

        def dv():
            tb = dot(r.p[b, seq:, :], r.do[g, seq:, :], TN)
            ta = dot(r.p[b, 0:seq, 0:half], r.do[g, :seq, :], TN)
            r.dv[0:half, kcol:kcol + HD] = (tb[:half] + ta).astype(BF16)
            r.dv[half:seq, kcol:kcol + HD] = tb[half:].astype(BF16)

        return [(1, dq), (1, dk), (1, o), (1, dv)]

    def back(g):
        b = g % 2

        def place(h, c):
            if h == 2:
                return r.dkf, c, r.dk, g * HD, r.kg
            return r.dqf, stacked(h, c), r.dq, (2 * g + h) * HD, r.qg

        def turn(h, c):
            src, o, _, _, g_ref = place(h, c)

            def run():
                d = src[b, o:o + CH, :].astype(BF16).astype(F32)
                that = r.raw[g, h, c:c + CH, :].astype(F32) * r.inv[g, h, c:c + CH, :]
                du = d[:, :HD] * r.tab[2, c:c + CH, :] - d[:, HD:] * r.tab[3, c:c + CH, :]
                src[b, o:o + CH, 0:HD] = du
                pr = du * that
                dg_ref = r.dgk if h == 2 else r.dgq
                dg_ref[...] += jnp.sum(pr.reshape(CH // 8, 8, HD), axis=0)
                r.sb[h, c:c + CH, :] = jnp.broadcast_to(jnp.mean(pr * g_ref[0:1, :], axis=-1, keepdims=True), (CH, HD))

            return (0.6, run)

        def out(h, c):
            src, o, out_ref, col, g_ref = place(h, c)

            def run():
                inv = r.inv[g, h, c:c + CH, :]
                that = r.raw[g, h, c:c + CH, :].astype(F32) * inv
                out_ref[c:c + CH, col:col + HD] = (inv * (src[b, o:o + CH, 0:HD] * g_ref[0:1, :] - that * r.sb[h, c:c + CH, :])).astype(BF16)

            return (0.5, run)

        return [f(h, c) for f in (turn, out) for h in (0, 1, 2) for c in range(0, seq, CH)]

    return SimpleNamespace(norm=norm_rows, proj=proj, rope=rope, scores=scores, soft=soft, grads=grads, back=back)


def attn_tick(st, g, n_grp, extra=()):
    vec = st.soft((g - 3) % n_grp) + st.rope((g - 1) % n_grp)
    more = [e for e in extra]
    if more:
        vec = vec + more[0]
    vec = vec + st.back(g)
    gr = st.grads(g)
    for _, f in gr[:2]:
        f()
    weave(vec, st.scores((g - 2) % n_grp) + gr[2:] + st.proj(g), *more[1:])


def attn_scratch(seq, n_grp, nq, nk):
    return dict(
        qnew=pltpu.VMEM((2, 2, seq, HD), BF16),
        knew=pltpu.VMEM((n_grp, seq, HD), BF16),
        vnew=pltpu.VMEM((n_grp, seq, HD), BF16),
        raw=pltpu.VMEM((n_grp, 3, seq, HD), BF16),
        inv=pltpu.VMEM((n_grp, 3, seq, HD), F32),
        rot=pltpu.VMEM((n_grp, 3 * seq, 2 * HD), BF16),
        do=pltpu.VMEM((n_grp, 2 * seq, HD), BF16),
        v=pltpu.VMEM((n_grp, seq, HD), BF16),
        s=pltpu.VMEM((2, 2 * seq, seq), F32),
        dp=pltpu.VMEM((2, 2 * seq, seq), F32),
        p=pltpu.VMEM((2, 2 * seq, seq), BF16),
        ds=pltpu.VMEM((2, 2 * seq, seq), BF16),
        dkf=pltpu.VMEM((2, seq, 2 * HD), F32),
        dqf=pltpu.VMEM((2, 2 * seq, 2 * HD), F32),
        st=pltpu.VMEM((3, 2 * seq, HD), F32),
        sb=pltpu.VMEM((3, seq, HD), F32),
        tab=pltpu.VMEM((4, seq, HD), F32),
        o=pltpu.VMEM((seq, nq), BF16),
        dq=pltpu.VMEM((seq, nq), BF16),
        dk=pltpu.VMEM((seq, nk), BF16),
        dv=pltpu.VMEM((seq, nk), BF16),
    )


def tail_kernel(seq, n_grp, rows, keys, sel_ref, n_in, dy_in, cos_in, sin_in, x_in, dyx_in, gain_ref, qg_ref, kg_ref, *refs):
    own_w, oth_w, own_a = refs[:4], refs[4:8], refs[8:12]
    y_out, dx_out, dg_out, dgq_out, dgk_out = refs[12:17]
    r = SimpleNamespace(n=n_in, dy=dy_in, qg=qg_ref, kg=kg_ref, gain=gain_ref, **dict(zip(keys, refs[17:])))
    step = pl.program_id(0)
    me = sel_ref[0]
    oth = 1 - me
    D = x_in.shape[1]
    r.wq = lambda c: r.wq_all[oth, :, c]
    r.wk = lambda c: r.wk_all[oth, :, c]
    r.wv = lambda c: r.wv_all[oth, :, c]
    r.do_dot = lambda c: dot(dy_in[...], r.wo_all[oth, c, :], NT)
    st = attn_stages(seq, n_grp, r)

    def fetch(row):
        return [pltpu.make_async_copy(src.at[me, pl.ds(row * seq, seq), :], dst, r.sem.at[8 + k])
                for k, (src, dst) in enumerate(zip(own_a, (r.o_own, r.dq_own, r.dk_own, r.dv_own)))]

    @pl.when(step == 0)
    def _():
        copies = []
        for k, dst in enumerate((r.wq_all, r.wk_all, r.wv_all, r.wo_all)):
            copies.append(pltpu.make_async_copy(oth_w[k], dst.at[oth], r.sem.at[4 + k]))
            copies.append(pltpu.make_async_copy(own_w[k], dst.at[me], r.sem.at[k]))
        for c in copies:
            c.start()
        for c in copies:
            c.wait()
        for c in fetch(0):
            c.start()
        r.dg[...] = jnp.zeros_like(r.dg)

    CR, NC = 32, 256
    nn = D // NC
    lines = range(0, seq, CR)

    def wide(v):
        return jnp.concatenate([v] * (NC // HD), axis=1)

    def stat(c):
        def run():
            xf = x_in[c:c + CR, :].astype(F32)
            r.xs[0, c:c + CR, :] = jnp.broadcast_to(lax.rsqrt(jnp.mean(xf * xf, axis=-1, keepdims=True) + EPS), (CR, HD))
            r.xs[1, c:c + CR, :] = jnp.zeros((CR, HD), F32)

        return (1, run)

    def dn_dot(n):
        def run():
            cols = slice(n * NC, (n + 1) * NC)
            t = None
            for s in range(2):
                for a_ref, w_ref in ((r.dqc, r.wq_all), (r.dkc, r.wk_all), (r.dvc, r.wv_all)):
                    u = dot(a_ref[s], w_ref[s, cols, :], NT)
                    t = u if t is None else t + u
            r.dn[:, cols] = t

        return (2, run)

    def first(n, c):
        def run():
            cols = slice(n * NC, (n + 1) * NC)
            w = r.dn[c:c + CR, cols] * (x_in[c:c + CR, cols].astype(F32) * wide(r.xs[0, c:c + CR, :]))
            r.dg[:, cols] += jnp.sum(w.reshape(CR // 8, 8, NC), axis=0)
            w = w * gain_ref[0:1, cols]
            r.xs[1, c:c + CR, :] += w[:, :HD] + w[:, HD:]

        return (1, run)

    def mean(c):
        def run():
            r.xs[2, c:c + CR, :] = jnp.broadcast_to(jnp.sum(r.xs[1, c:c + CR, :], axis=-1, keepdims=True) * (1.0 / D), (CR, HD))

        return (0.2, run)

    def second(n, c):
        def run():
            cols = slice(n * NC, (n + 1) * NC)
            inv = wide(r.xs[0, c:c + CR, :])
            xh = x_in[c:c + CR, cols].astype(F32) * inv
            e = r.dn[c:c + CR, cols] * gain_ref[0:1, cols]
            dx_out[c:c + CR, cols] = (dyx_in[c:c + CR, cols].astype(F32) + inv * (e - xh * wide(r.xs[2, c:c + CR, :]))).astype(BF16)

        return (1.2, run)

    def y_dot(n):
        def run():
            cols = slice(n * NC, (n + 1) * NC)
            t = dot(r.oc[0], r.wo_all[0, :, cols]) + dot(r.oc[1], r.wo_all[1, :, cols])
            y_out[:, cols] = (x_in[:, cols].astype(F32) + t).astype(BF16)

        return (1, run)

    dn = [dn_dot(n) for n in range(nn)]
    yd = [y_dot(n) for n in range(nn)]
    f = [[first(n, c) for c in lines] for n in range(nn)]
    sec = [second(n, c) for n in range(nn) for c in lines]
    out_mat = [dn[:3], dn[3:6], dn[6:], []]
    out_vec = [[stat(c) for c in lines], f[0] + f[1] + f[2], f[3] + f[4] + f[5], f[6] + f[7] + [mean(c) for c in lines]]

    def body(attn, out):
        if attn:
            r.tab[2:4] = r.tab[0:2]
            r.tab[0] = cos_in[...]
            r.tab[1] = sin_in[...]
        for g in range(n_grp):
            if attn:
                attn_tick(st, g, n_grp, ([], out_mat[g], out_vec[g]) if out else ())
            else:
                weave(out_mat[g], out_vec[g])
        if out:
            weave(yd, sec)
        if attn:
            row = jnp.clip(step - 1, 0, rows - 1)
            for c in fetch(row):
                c.wait()
            for dst, theirs, mine in ((r.oc, r.o, r.o_own), (r.dqc, r.dq, r.dq_own), (r.dkc, r.dk, r.dk_own), (r.dvc, r.dv, r.dv_own)):
                dst[oth] = theirs[...]
                dst[me] = mine[...]

            for acc in (r.dgq, r.dgk):
                acc[...] = jnp.where(step > 0, acc[...], 0.0)

            @pl.when(step < rows)
            def _():
                for c in fetch(step):
                    c.start()

    @pl.when(step < 2)
    def _():
        body(True, False)

    @pl.when((step >= 2) & (step <= rows))
    def _():
        body(True, True)

    @pl.when(step > rows)
    def _():
        body(False, True)
        dg_out[...] = r.dg[...]
        dgq_out[...] = r.dgq[...]
        dgk_out[...] = r.dgk[...]


def tail_call(sel, n, x, dy, cosd, sind, o, dq, dk, dv, gain, qg, kg, own, oth, seq=256):
    T, D = x.shape
    nq, nk = dq.shape[2], dk.shape[2]
    n_grp = nk // HD
    rows = T // seq
    lag = lambda k, c: pl.BlockSpec((seq, c), lambda i, s: (jnp.clip(i - k, 0, rows - 1), 0))
    const = lambda *b: pl.BlockSpec(b, lambda i, s: (0,) * len(b), pipeline_mode=pl.Buffered(1))
    hbm = pl.BlockSpec(memory_space=pl.ANY)
    scratch = attn_scratch(seq, n_grp, nq, nk)
    scratch.update(
        wq_all=pltpu.VMEM((2, D, nq), BF16), wk_all=pltpu.VMEM((2, D, nk), BF16), wv_all=pltpu.VMEM((2, D, nk), BF16), wo_all=pltpu.VMEM((2, nq, D), BF16),
        dn=pltpu.VMEM((seq, D), F32), oc=pltpu.VMEM((2, seq, nq), BF16), dqc=pltpu.VMEM((2, seq, nq), BF16), dkc=pltpu.VMEM((2, seq, nk), BF16), dvc=pltpu.VMEM((2, seq, nk), BF16),
        o_own=pltpu.VMEM((seq, nq), BF16), dq_own=pltpu.VMEM((seq, nq), BF16), dk_own=pltpu.VMEM((seq, nk), BF16), dv_own=pltpu.VMEM((seq, nk), BF16),
        xs=pltpu.VMEM((3, seq, HD), F32), dg=pltpu.VMEM((8, D), F32), dgq=pltpu.VMEM((8, HD), F32), dgk=pltpu.VMEM((8, HD), F32), sem=pltpu.SemaphoreType.DMA((12,)))
    flops = 2 * T * D * (nq + 2 * nk + nq) * 3 + 12 * T * nq * seq
    return pl.pallas_call(
        functools.partial(tail_kernel, seq, n_grp, rows, tuple(scratch)),
        grid_spec=pltpu.PrefetchScalarGridSpec(
            num_scalar_prefetch=1,
            grid=(rows + 2,),
            in_specs=[lag(0, D), lag(0, D), lag(0, HD), lag(0, HD), lag(2, D), lag(2, D), const(1, D), const(1, HD), const(1, HD)] + [hbm] * 12,
            out_specs=[lag(2, D), lag(2, D), pl.BlockSpec((8, D), lambda i, s: (0, 0))] + [pl.BlockSpec((8, HD), lambda i, s: (0, 0))] * 2,
            scratch_shapes=list(scratch.values()),
        ),
        out_shape=[jax.ShapeDtypeStruct((T, D), BF16)] * 2 + [jax.ShapeDtypeStruct((8, c), F32) for c in (D, HD, HD)],
        compiler_params=pltpu.CompilerParams(dimension_semantics=("arbitrary",), vmem_limit_bytes=67043328),
        cost_estimate=pl.CostEstimate(flops=flops, bytes_accessed=T * D * 14, transcendentals=T * nq * 2),
        name="tail",
    )(sel, n, dy, cosd, sind, x, dy, gain, qg, kg, *own, *oth, o, dq, dk, dv)


def solution(mesh):
    tok_spec = P("dp", None, None)
    col_spec = P(None, "tp")
    row_spec = P("tp", None)
    n_dp = mesh.shape["dp"]

    def per_device(x_in, dy_in, positions, g_attn, q_gain, k_gain, w_q, w_k, w_v, w_o):
        n_batch, n_seq, D = x_in.shape
        T = n_batch * n_seq
        nq, nk = w_q.shape[1], w_k.shape[1]
        x, dy = x_in.reshape(T, D), dy_in.reshape(T, D)
        me = lax.axis_index("tp").astype(jnp.int32)
        own = me.reshape(1)

        part = (lax.axis_index("dp") % 2).astype(jnp.int32).reshape(1)
        share = pack_call(part, w_q, w_k, w_v, w_o)
        share = lax.ppermute(share, "tp", [(0, 1), (1, 0)])
        gathered = lax.all_gather(share, "dp", axis_index_groups=[[2 * i, 2 * i + 1] for i in range(n_dp // 2)])
        gathered = gathered.reshape(-1, *gathered.shape[2:])

        cosd, sind = table_call(positions)
        gain = g_attn.astype(F32).reshape(1, D)
        qg, kg = q_gain.astype(F32).reshape(1, HD), k_gain.astype(F32).reshape(1, HD)

        n, o, dq, dk, dv, dgq, dgk = attn_call(True, own, x, dy, cosd, sind, gain, qg, kg, w_q, w_k, w_v, w_o, seq=n_seq)
        (dw_o,) = dw_call(own, o, [dy])
        (dw_q,) = dw_call(own, n, [dq])
        dw_k, dw_v = dw_call(own, n, [dk, dv])
        dw_o, dw_q, dw_k, dw_v = lax.psum((dw_o, dw_q, dw_k, dw_v), "dp")

        theirs = unpack_call(gathered, D, nq, nk)
        y, dx, dg, dgq2, dgk2 = tail_call(own, n, x, dy, cosd, sind, o, dq, dk, dv, gain, qg, kg, (w_q, w_k, w_v, w_o), theirs, seq=n_seq)
        small = lax.psum(jnp.sum(jnp.concatenate([dg, dgq + dgq2, dgk + dgk2], axis=1), axis=0), "dp")
        g_sum, q_sum, k_sum = small[:D], small[D:D + HD], small[D + HD:]
        return y.reshape(x_in.shape), dx.reshape(x_in.shape), dw_q, dw_k, dw_v, dw_o, q_sum, k_sum, g_sum

    return jax.shard_map(per_device, mesh=mesh, in_specs=(tok_spec, tok_spec, P("dp", None), P(), P(), P(), col_spec, col_spec, col_spec, row_spec), out_specs=(tok_spec, tok_spec, col_spec, col_spec, col_spec, row_spec, P(), P(), P()), check_vma=False)
```

```python
import functools
from types import SimpleNamespace
import jax
import jax.numpy as jnp
from jax import lax
from jax.experimental import pallas as pl
from jax.experimental.pallas import tpu as pltpu
from jax.sharding import PartitionSpec as P


EPS = 1e-6
THETA = 1000000.0
F32 = jnp.float32
BF16 = jnp.bfloat16
HD = 128
NT = (((1,), (1,)), ((), ()))
TN = (((0,), (0,)), ((), ()))
NN = (((1,), (0,)), ((), ()))


def dot(a, b, dims=NN):
    return lax.dot_general(a, b, dims, preferred_element_type=F32)


def weave(*lists):
    order = []
    for n, pieces in enumerate(lists):
        total = sum(c for c, _ in pieces) or 1
        at = 0
        for k, (c, f) in enumerate(pieces):
            order.append(((at + c / 2) / total, n, k, f))
            at += c
    for _, _, _, f in sorted(order, key=lambda e: e[:3]):
        f()


CH = 32


def attn_kernel(own, seq, n_grp, sel_ref, *refs):
    if own:
        (x0_ref, xn_ref, dy_ref, cos_ref, sin_ref, gain_ref, qg_ref, kg_ref, wq_ref, wk_ref, wv_ref, wo_ref,
         n_out, o_out, dq_out, dk_out, dv_out, dgq_out, dgk_out) = refs[:19]
        refs = refs[19:]
    else:
        nin_ref, dy_ref, cos_ref, sin_ref, qg_ref, kg_ref, wq_ref, wk_ref, wv_ref, wo_ref, _, _, _, _, o_out, dq_out, dk_out, dv_out = refs[:18]
        refs = refs[18:]
        n_ref = nin_ref
    (wot_ref, qnew_ref, knew_ref, vnew_ref, raw_ref, inv_ref, rot_ref, do_ref, v_ref, s_ref, dp_ref, p_ref, ds_ref, dkf_ref, dqf_ref, st_ref,
     tab_ref, o_ref, dq_ref, dk_ref, dv_ref) = refs[:21]
    if own:
        n_ref, nn_ref, dgq_ref, dgk_ref = refs[21:]
    half = seq // 2
    scale = HD ** -0.5
    log2e = 1.4426950408889634
    step = pl.program_id(0)

    def norm_rows(src, dst):
        def piece(c):
            def run():
                xf = src[c:c + 32, :].astype(F32)
                inv = lax.rsqrt(jnp.mean(xf * xf, axis=-1, keepdims=True) + EPS)
                dst[c:c + 32, :] = (xf * inv * gain_ref[0:1, :]).astype(BF16)

            return (1.5, run)

        return [piece(c) for c in range(0, seq, 32)]

    def proj(g):
        def q():
            t = dot(n_ref[...], wq_ref[:, g * 2 * HD:(g + 1) * 2 * HD])
            for h in range(2):
                qnew_ref[g % 2, h] = t[:, h * HD:(h + 1) * HD].astype(BF16)

        def k():
            t = dot(n_ref[...], wk_ref[:, g * HD:(g + 2) * HD])
            for h in range(2):
                knew_ref[g + h] = t[:, h * HD:(h + 1) * HD].astype(BF16)

        def v():
            t = dot(n_ref[...], wv_ref[:, g * HD:(g + 2) * HD])
            for h in range(2):
                vnew_ref[g + h] = t[:, h * HD:(h + 1) * HD].astype(BF16)

        def do():
            t = dot(dy_ref[...], wot_ref[:, g * 2 * HD:(g + 1) * 2 * HD])
            for h in range(2):
                do_ref[g, h * half:(h + 1) * half, :] = t[:half, h * HD:(h + 1) * HD].astype(BF16)
                do_ref[g, seq + h * half:seq + (h + 1) * half, :] = t[half:, h * HD:(h + 1) * HD].astype(BF16)

        return [(1, q)] + ([(1, k), (1, v)] if g % 2 == 0 else []) + [(1, do)]

    def stacked(h, c):
        return (h * half + c) if c < half else (seq + h * half + c - half)

    def rope(g):
        cs, sn = (tab_ref.at[2], tab_ref.at[3]) if g == n_grp - 1 else (tab_ref.at[0], tab_ref.at[1])

        def size(h, c):
            def run():
                raw = knew_ref[g, c:c + CH, :] if h == 2 else qnew_ref[g % 2, h, c:c + CH, :]
                raw_ref[g, h, c:c + CH, :] = raw
                t = raw.astype(F32)
                inv_ref[g, h, c:c + CH, :] = jnp.broadcast_to(lax.rsqrt(jnp.mean(t * t, axis=-1, keepdims=True) + EPS), t.shape)

            return (0.4, run)

        def turn(h, c):
            def run():
                t = raw_ref[g, h, c:c + CH, :].astype(F32)
                w = (t * inv_ref[g, h, c:c + CH, :]) * (kg_ref if h == 2 else qg_ref)[0:1, :]
                o = 2 * seq + c if h == 2 else stacked(h, c)
                x = pltpu.roll(w, HD // 2, 1)
                co, si = cs[c:c + CH, :], sn[c:c + CH, :]
                rot_ref[g, o:o + CH, 0:HD] = (w * co + x * si).astype(BF16)
                rot_ref[g, o:o + CH, HD:] = (x * co - w * si).astype(BF16)
                if h == 2:
                    v_ref[g, c:c + CH, :] = vnew_ref[g, c:c + CH, :]

            return (0.6, run)

        return [f(h, c) for f in (size, turn) for h in (2, 0, 1) for c in range(0, seq, CH)]

    def scores(g):
        b = g % 2

        def s():
            s_ref[b, 0:seq, 0:half] = dot(rot_ref[g, 0:seq, 0:HD], rot_ref[g, 2 * seq:2 * seq + half, 0:HD], NT)
            s_ref[b, seq:, :] = dot(rot_ref[g, seq:2 * seq, 0:HD], rot_ref[g, 2 * seq:, 0:HD], NT)

        def dp():
            dp_ref[b, 0:seq, 0:half] = dot(do_ref[g, :seq, :], v_ref[g, :half, :], NT)
            dp_ref[b, seq:, :] = dot(do_ref[g, seq:, :], v_ref[g], NT)

        return [(1, s), (1, dp)]

    def soft(g):
        b = g % 2
        c2 = scale * log2e

        def part(blk, c):
            return slice(blk * seq + c, blk * seq + c + CH), half if blk == 0 else seq

        def masked(blk, c, s):
            row_id = lax.broadcasted_iota(jnp.int32, (CH, half), 0) + (c % half)
            keep = row_id >= lax.broadcasted_iota(jnp.int32, (CH, half), 1)
            if blk == 0:
                return jnp.where(keep, s, -jnp.inf)
            return jnp.concatenate([s[:, :half], jnp.where(keep, s[:, half:], -jnp.inf)], axis=1)

        def wide(ref, rows, width):
            t = ref[rows, :]
            return t if width == half else jnp.concatenate([t, t], axis=1)

        def top(blk, c):
            rows, width = part(blk, c)

            def run():
                m = jnp.max(masked(blk, c, s_ref[b, rows, 0:width]), axis=-1, keepdims=True)
                st_ref[0, rows, :] = jnp.broadcast_to(m * c2, (CH, HD))

            return (0.4 + 0.4 * blk, run)

        def power(blk, c):
            rows, width = part(blk, c)

            def run():
                e = jnp.exp2(masked(blk, c, s_ref[b, rows, 0:width] * c2) - wide(st_ref.at[0], rows, width))
                s_ref[b, rows, 0:width] = e
                st_ref[1, rows, :] = jnp.broadcast_to(1.0 / jnp.sum(e, axis=-1, keepdims=True), (CH, HD))

            return (0.8 + 0.8 * blk, run)

        def prob(blk, c):
            rows, width = part(blk, c)

            def run():
                pr = s_ref[b, rows, 0:width] * wide(st_ref.at[1], rows, width)
                s_ref[b, rows, 0:width] = pr
                p_ref[b, rows, 0:width] = pr.astype(BF16)
                st_ref[2, rows, :] = jnp.broadcast_to(jnp.sum(pr * dp_ref[b, rows, 0:width], axis=-1, keepdims=True), (CH, HD))

            return (0.8 + 0.8 * blk, run)

        def last(blk, c):
            rows, width = part(blk, c)

            def run():
                d = dp_ref[b, rows, 0:width] - wide(st_ref.at[2], rows, width)
                ds_ref[b, rows, 0:width] = (s_ref[b, rows, 0:width] * d * scale).astype(BF16)

            return (0.8 + 0.8 * blk, run)

        return [f(blk, c) for f in (top, power, prob, last) for blk in range(2) for c in range(0, seq, CH)]

    def grads(g):
        b = g % 2
        col, kcol = g * 2 * HD, g * HD

        def dq():
            dqf_ref[b, 0:seq, :] = dot(ds_ref[b, 0:seq, 0:half], rot_ref[g, 2 * seq:2 * seq + half, :])
            dqf_ref[b, seq:, :] = dot(ds_ref[b, seq:, :], rot_ref[g, 2 * seq:, :])

        def dk():
            tb = dot(ds_ref[b, seq:, :], rot_ref[g, seq:2 * seq, :], TN)
            ta = dot(ds_ref[b, 0:seq, 0:half], rot_ref[g, 0:seq, :], TN)
            dkf_ref[b, :half, :] = tb[:half] + ta
            dkf_ref[b, half:, :] = tb[half:]

        def o():
            ta = dot(p_ref[b, 0:seq, 0:half], v_ref[g, :half, :])
            tb = dot(p_ref[b, seq:, :], v_ref[g])
            for h in range(2):
                o_ref[0:half, col + h * HD:col + (h + 1) * HD] = ta[h * half:(h + 1) * half].astype(BF16)
                o_ref[half:seq, col + h * HD:col + (h + 1) * HD] = tb[h * half:(h + 1) * half].astype(BF16)

        def dv():
            tb = dot(p_ref[b, seq:, :], do_ref[g, seq:, :], TN)
            ta = dot(p_ref[b, 0:seq, 0:half], do_ref[g, :seq, :], TN)
            dv_ref[0:half, kcol:kcol + HD] = (tb[:half] + ta).astype(BF16)
            dv_ref[half:seq, kcol:kcol + HD] = tb[half:].astype(BF16)

        return [(1, dq), (1, dk), (1, o), (1, dv)]

    def back(g):
        b = g % 2

        def place(h, c):
            if h == 2:
                return dkf_ref, c, dk_ref, g * HD, kg_ref
            return dqf_ref, stacked(h, c), dq_ref, (2 * g + h) * HD, qg_ref

        def turn(h, c):
            src, o, _, _, g_ref = place(h, c)

            def run():
                d = src[b, o:o + CH, :].astype(BF16).astype(F32)
                that = raw_ref[g, h, c:c + CH, :].astype(F32) * inv_ref[g, h, c:c + CH, :]
                du = d[:, :HD] * tab_ref[2, c:c + CH, :] - d[:, HD:] * tab_ref[3, c:c + CH, :]
                src[b, o:o + CH, 0:HD] = du
                pr = du * that
                if own:
                    dg_ref = dgk_ref if h == 2 else dgq_ref
                    dg_ref[...] += jnp.sum(pr.reshape(CH // 8, 8, HD), axis=0)
                st_ref[3 + h, c:c + CH, :] = jnp.broadcast_to(jnp.mean(pr * g_ref[0:1, :], axis=-1, keepdims=True), (CH, HD))

            return (0.6, run)

        def out(h, c):
            src, o, out_ref, col, g_ref = place(h, c)

            def run():
                inv = inv_ref[g, h, c:c + CH, :]
                that = raw_ref[g, h, c:c + CH, :].astype(F32) * inv
                out_ref[c:c + CH, col:col + HD] = (inv * (src[b, o:o + CH, 0:HD] * g_ref[0:1, :] - that * st_ref[3 + h, c:c + CH, :])).astype(BF16)

            return (0.5, run)

        return [f(h, c) for f in (turn, out) for h in (0, 1, 2) for c in range(0, seq, CH)]

    @pl.when(step == 0)
    def _():
        for c in range(0, wo_ref.shape[0], 256):
            for d in range(0, wo_ref.shape[1], 256):
                wot_ref[d:d + 256, c:c + 256] = wo_ref[c:c + 256, d:d + 256].T
        if own:
            weave(norm_rows(x0_ref, n_ref))

    tab_ref[2:4] = tab_ref[0:2]
    tab_ref[0] = cos_ref[...]
    tab_ref[1] = sin_ref[...]
    if own:
        norms = norm_rows(xn_ref, nn_ref)
    for g in range(n_grp):
        vec = soft((g - 3) % n_grp)
        sc = scores((g - 2) % n_grp)
        vec = vec + rope((g - 1) % n_grp)
        if own:
            vec += norms[g * len(norms) // n_grp:(g + 1) * len(norms) // n_grp]
        vec += back(g)
        gr = grads(g)
        for _, f in gr[:2]:
            f()
        weave(vec, sc + gr[2:] + proj(g))

    for dst, src in ((o_out, o_ref), (dq_out, dq_ref), (dk_out, dk_ref), (dv_out, dv_ref)):
        dst[0] = src[...]
    if own:
        n_out[...] = n_ref[...]
        n_ref[...] = nn_ref[...]
        keep = step > 0
        for dst, acc in ((dgq_out, dgq_ref), (dgk_out, dgk_ref)):
            acc[...] = jnp.where(keep, acc[...], 0.0)
            dst[...] = acc[...]


def attn_call(own, sel, x, dy, cosd, sind, gain, qg, kg, wq, wk, wv, wo, prev=None, seq=256):
    T, D = x.shape
    nq, nk = wq.shape[1], wk.shape[1]
    n_grp = nk // HD
    rows = T // seq
    const = lambda *b: pl.BlockSpec(b, lambda i, s: (0,) * len(b), pipeline_mode=pl.Buffered(1))
    now = lambda c: pl.BlockSpec((seq, c), lambda i, s: (jnp.minimum(i, rows - 1), 0))
    nxt = lambda c: pl.BlockSpec((seq, c), lambda i, s: (jnp.minimum(i + 1, rows - 1), 0))
    out3 = lambda c: pl.BlockSpec((1, seq, c), lambda i, s: (s[0], jnp.maximum(i - 1, 0), 0))
    mid = [now(D), now(HD), now(HD)]
    tail = [const(1, HD), const(1, HD), const(D, nq), const(D, nk), const(D, nk), const(nq, D)]
    shapes = [jax.ShapeDtypeStruct((2, T, c), BF16) for c in (nq, nq, nk, nk)]
    specs = [out3(nq), out3(nq), out3(nk), out3(nk)]
    aliases = {}
    if own:
        in_specs = [const(seq, D), nxt(D)] + mid + [const(1, D)] + tail
        args = [x, x, dy, cosd, sind, gain, qg, kg, wq, wk, wv, wo]
        shapes = [jax.ShapeDtypeStruct((T, D), BF16)] + shapes + [jax.ShapeDtypeStruct((8, HD), F32)] * 2
        specs = [now(D)] + specs + [pl.BlockSpec((8, HD), lambda i, s: (0, 0))] * 2
    else:
        in_specs = [now(D)] + mid + tail + [pl.BlockSpec(memory_space=pl.ANY)] * 4
        args = [x, dy, cosd, sind, qg, kg, wq, wk, wv, wo]
        aliases = {1 + len(args) + i: i for i in range(4)}
        args += list(prev)
    flops = 2 * T * D * (nq + 2 * nk + nq) + 12 * T * nq * seq
    return pl.pallas_call(
        functools.partial(attn_kernel, own, seq, n_grp),
        grid_spec=pltpu.PrefetchScalarGridSpec(
            num_scalar_prefetch=1,
            grid=(rows + 1,),
            in_specs=in_specs,
            out_specs=specs,
            scratch_shapes=[
                pltpu.VMEM((D, nq), BF16),
                pltpu.VMEM((2, 2, seq, HD), BF16),
                pltpu.VMEM((n_grp, seq, HD), BF16),
                pltpu.VMEM((n_grp, seq, HD), BF16),
                pltpu.VMEM((n_grp, 3, seq, HD), BF16),
                pltpu.VMEM((n_grp, 3, seq, HD), F32),
                pltpu.VMEM((n_grp, 3 * seq, 2 * HD), BF16),
                pltpu.VMEM((n_grp, 2 * seq, HD), BF16),
                pltpu.VMEM((n_grp, seq, HD), BF16),
                pltpu.VMEM((2, 2 * seq, seq), F32),
                pltpu.VMEM((2, 2 * seq, seq), F32),
                pltpu.VMEM((2, 2 * seq, seq), BF16),
                pltpu.VMEM((2, 2 * seq, seq), BF16),
                pltpu.VMEM((2, seq, 2 * HD), F32),
                pltpu.VMEM((2, 2 * seq, 2 * HD), F32),
                pltpu.VMEM((6, 2 * seq, HD), F32),
                pltpu.VMEM((4, seq, HD), F32),
            ] + [pltpu.VMEM((seq, c), BF16) for c in (nq, nq, nk, nk)]
            + ([pltpu.VMEM((seq, D), BF16)] * 2 + [pltpu.VMEM((8, HD), F32)] * 2 if own else []),
        ),
        out_shape=shapes,
        input_output_aliases=aliases,
        compiler_params=pltpu.CompilerParams(dimension_semantics=("arbitrary",), vmem_limit_bytes=56 << 20),
        cost_estimate=pl.CostEstimate(flops=flops, bytes_accessed=T * D * 6 + T * (2 * nq + 2 * nk) * 2, transcendentals=T * nq * 2),
        name="attn_own" if own else "attn_other",
    )(sel, *args)


def unpack_kernel(f_ref, q_ref, k_ref, v_ref, o_ref):
    d = q_ref.shape[0]
    nq, nk = q_ref.shape[1], k_ref.shape[1]
    q_ref[...] = f_ref[0, 0:d, 0:nq].astype(BF16)
    k_ref[...] = f_ref[0, 0:d, nq:nq + nk].astype(BF16)
    v_ref[...] = f_ref[0, 0:d, nq + nk:].astype(BF16)
    o_ref[...] = f_ref[0, d:, :].astype(BF16)


def unpack_call(gathered, D, nq, nk):
    n, r, c = gathered.shape
    part = lambda a, b: pl.BlockSpec((a // n, b), lambda i: (i, 0))
    return pl.pallas_call(
        unpack_kernel,
        grid=(n,),
        in_specs=[pl.BlockSpec((1, r, c), lambda i: (i, 0, 0))],
        out_specs=[part(D, nq), part(D, nk), part(D, nk), part(nq, D)],
        out_shape=[jax.ShapeDtypeStruct(s, BF16) for s in ((D, nq), (D, nk), (D, nk), (nq, D))],
        compiler_params=pltpu.CompilerParams(dimension_semantics=("arbitrary",), vmem_limit_bytes=60 << 20),
        cost_estimate=pl.CostEstimate(flops=n * r * c, bytes_accessed=n * r * c * 6, transcendentals=0),
        name="unpack",
    )(gathered)


def pre_kernel(sel_ref, q_ref, k_ref, v_ref, o_ref, pos_ref, freq_ref, out_ref, cos_ref, sin_ref):
    d, nq, nk = q_ref.shape[0], q_ref.shape[1], k_ref.shape[1]
    out_ref[0, 0:d, 0:nq] = q_ref[...].astype(F32)
    out_ref[0, 0:d, nq:nq + nk] = k_ref[...].astype(F32)
    out_ref[0, 0:d, nq + nk:] = v_ref[...].astype(F32)
    out_ref[0, d:, :] = o_ref[...].astype(F32)
    n, seq = pos_ref.shape
    lane = lax.broadcasted_iota(jnp.int32, (HD, HD), 1)
    for r in range(n):
        for h in range(seq // HD):
            p = pos_ref[r:r + 1, h * HD:(h + 1) * HD].astype(F32)
            a = jnp.broadcast_to(p, (HD, HD)).T * freq_ref[0:1, :]
            k = jnp.round(a * 0.6366197723675814)
            x = ((a - k * 1.5703125) - k * 4.837512969970703125e-4) - k * 7.549789948768648e-8
            z = x * x
            s = ((-1.9515295891e-4 * z + 8.3321608736e-3) * z - 1.6666654611e-1) * z * x + x
            c = ((2.443315711809948e-5 * z - 1.388731625493765e-3) * z + 4.166664568298827e-2) * z * z - 0.5 * z + 1.0
            q = k.astype(jnp.int32)
            odd = (q & 1) == 1
            co, si = jnp.where(odd, s, c), jnp.where(odd, c, s)
            rows = slice((r * (seq // HD) + h) * HD, (r * (seq // HD) + h + 1) * HD)
            cos_ref[rows, :] = jnp.where(((q + 1) & 2) == 0, co, -co)
            sin_ref[rows, :] = jnp.where(((q & 2) == 0) == (lane >= HD // 2), si, -si)


def pre_call(part, w_q, w_k, w_v, w_o, positions, parts=2, cuts=4):
    D, nq = w_q.shape
    n, seq = positions.shape
    rows = n // cuts
    freq = THETA ** (-jnp.arange(0, HD, 2, dtype=F32) / HD)
    freq = jnp.concatenate([freq, freq]).reshape(1, HD)
    spec = lambda w: pl.BlockSpec((w.shape[0] // (parts * cuts), w.shape[1]), lambda i, s: (s[0] * cuts + i, 0))
    r = (D + nq) // (parts * cuts)
    table = pl.BlockSpec((rows * seq, HD), lambda i, s: (i, 0))
    return pl.pallas_call(
        pre_kernel,
        grid_spec=pltpu.PrefetchScalarGridSpec(
            num_scalar_prefetch=1,
            grid=(cuts,),
            in_specs=[spec(w) for w in (w_q, w_k, w_v, w_o)] + [pl.BlockSpec((rows, seq), lambda i, s: (i, 0)), pl.BlockSpec((1, HD), lambda i, s: (0, 0))],
            out_specs=[pl.BlockSpec((1, r, D), lambda i, s: (i, 0, 0)), table, table],
        ),
        out_shape=[jax.ShapeDtypeStruct((cuts, r, D), F32)] + [jax.ShapeDtypeStruct((n * seq, HD), F32)] * 2,
        compiler_params=pltpu.CompilerParams(dimension_semantics=("arbitrary",), vmem_limit_bytes=60 << 20),
        cost_estimate=pl.CostEstimate(flops=n * seq * HD * 30, bytes_accessed=cuts * r * D * 6 + n * seq * HD * 8, transcendentals=0),
        name="pre",
    )(part, w_q, w_k, w_v, w_o, positions, freq)


def dw_kernel(n_b, sel_ref, a_ref, *refs):
    bs, outs, accs, (at_ref, sem) = refs[:n_b], refs[n_b:2 * n_b], refs[2 * n_b:3 * n_b], refs[3 * n_b:]
    flat = lambda ref: ref.at[0] if len(ref.shape) == 3 else ref
    a, bs = flat(a_ref), [flat(b) for b in bs]
    M, tile = at_ref.shape
    step = pl.program_id(0)

    @pl.when(step == 0)
    def _():
        for acc in accs:
            acc[...] = jnp.zeros_like(acc)

    def part(acc, b, c):
        def run():
            acc[:, c:c + 256] += dot(at_ref[...], b[:, c:c + 256])

        return (1, run)

    for c in range(0, M, 256):
        for k in range(0, tile, 256):
            at_ref[c:c + 256, k:k + 256] = a[k:k + 256, c:c + 256].T
    weave([part(acc, b, c) for acc, b in zip(accs, bs) for c in range(0, b.shape[1], 256)])

    @pl.when(step == pl.num_programs(0) - 1)
    def _():
        copies = [pltpu.make_async_copy(acc, out, sem.at[k]) for k, (acc, out) in enumerate(zip(accs, outs))]
        for c in copies:
            c.start()
        for c in copies:
            c.wait()


def dw_call(sel, a, bs, tile):
    def spec(v):
        if v.ndim == 3:
            return pl.BlockSpec((1, tile, v.shape[2]), lambda i, s: (s[0], i, 0))
        return pl.BlockSpec((tile, v.shape[1]), lambda i, s: (i, 0))

    T, M = a.shape[-2:]
    shapes = [(M, b.shape[-1]) for b in bs]
    width = sum(s[1] for s in shapes)
    return pl.pallas_call(
        functools.partial(dw_kernel, len(bs)),
        grid_spec=pltpu.PrefetchScalarGridSpec(
            num_scalar_prefetch=1,
            grid=(T // tile,),
            in_specs=[spec(a)] + [spec(b) for b in bs],
            out_specs=[pl.BlockSpec(memory_space=pl.ANY)] * len(bs),
            scratch_shapes=[pltpu.VMEM(s, F32) for s in shapes] + [pltpu.VMEM((M, tile), BF16), pltpu.SemaphoreType.DMA((len(bs),))],
        ),
        out_shape=[jax.ShapeDtypeStruct(s, F32) for s in shapes],
        compiler_params=pltpu.CompilerParams(dimension_semantics=("arbitrary",), vmem_limit_bytes=60 << 20),
        cost_estimate=pl.CostEstimate(flops=2 * T * M * width, bytes_accessed=2 * T * (M + width) + 4 * M * width, transcendentals=0),
    )(sel, a, *bs)


def attn_stages(seq, n_grp, r):
    half = seq // 2
    scale = HD ** -0.5
    log2e = 1.4426950408889634

    def norm_rows(src, dst):
        def piece(c):
            def run():
                xf = src[c:c + 32, :].astype(F32)
                inv = lax.rsqrt(jnp.mean(xf * xf, axis=-1, keepdims=True) + EPS)
                dst[c:c + 32, :] = (xf * inv * r.gain[0:1, :]).astype(BF16)

            return (1.5, run)

        return [piece(c) for c in range(0, seq, 32)]

    def proj(g):
        def q():
            t = dot(r.n[...], r.wq(slice(g * 2 * HD, (g + 1) * 2 * HD)))
            for h in range(2):
                r.qnew[g % 2, h] = t[:, h * HD:(h + 1) * HD].astype(BF16)

        def k():
            t = dot(r.n[...], r.wk(slice(g * HD, (g + 2) * HD)))
            for h in range(2):
                r.knew[g + h] = t[:, h * HD:(h + 1) * HD].astype(BF16)

        def v():
            t = dot(r.n[...], r.wv(slice(g * HD, (g + 2) * HD)))
            for h in range(2):
                r.vnew[g + h] = t[:, h * HD:(h + 1) * HD].astype(BF16)

        def do():
            t = r.do_dot(slice(g * 2 * HD, (g + 1) * 2 * HD))
            for h in range(2):
                r.do[g, h * half:(h + 1) * half, :] = t[:half, h * HD:(h + 1) * HD].astype(BF16)
                r.do[g, seq + h * half:seq + (h + 1) * half, :] = t[half:, h * HD:(h + 1) * HD].astype(BF16)

        return [(1, q)] + ([(1, k), (1, v)] if g % 2 == 0 else []) + [(1, do)]

    def stacked(h, c):
        return (h * half + c) if c < half else (seq + h * half + c - half)

    def rope(g):
        cs, sn = (r.tab.at[2], r.tab.at[3]) if g == n_grp - 1 else (r.tab.at[0], r.tab.at[1])

        def size(h, c):
            def run():
                raw = r.knew[g, c:c + CH, :] if h == 2 else r.qnew[g % 2, h, c:c + CH, :]
                r.raw[g, h, c:c + CH, :] = raw
                t = raw.astype(F32)
                r.inv[g, h, c:c + CH, :] = jnp.broadcast_to(lax.rsqrt(jnp.mean(t * t, axis=-1, keepdims=True) + EPS), t.shape)

            return (0.4, run)

        def turn(h, c):
            def run():
                t = r.raw[g, h, c:c + CH, :].astype(F32)
                w = (t * r.inv[g, h, c:c + CH, :]) * (r.kg if h == 2 else r.qg)[0:1, :]
                o = 2 * seq + c if h == 2 else stacked(h, c)
                x = pltpu.roll(w, HD // 2, 1)
                co, si = cs[c:c + CH, :], sn[c:c + CH, :]
                r.rot[g, o:o + CH, 0:HD] = (w * co + x * si).astype(BF16)
                r.rot[g, o:o + CH, HD:] = (x * co - w * si).astype(BF16)
                if h == 2:
                    r.v[g, c:c + CH, :] = r.vnew[g, c:c + CH, :]

            return (0.6, run)

        return [f(h, c) for f in (size, turn) for h in (2, 0, 1) for c in range(0, seq, CH)]

    def scores(g):
        b = g % 2

        def s():
            r.s[b, 0:seq, 0:half] = dot(r.rot[g, 0:seq, 0:HD], r.rot[g, 2 * seq:2 * seq + half, 0:HD], NT)
            r.s[b, seq:, :] = dot(r.rot[g, seq:2 * seq, 0:HD], r.rot[g, 2 * seq:, 0:HD], NT)

        def dp():
            r.dp[b, 0:seq, 0:half] = dot(r.do[g, :seq, :], r.v[g, :half, :], NT)
            r.dp[b, seq:, :] = dot(r.do[g, seq:, :], r.v[g], NT)

        return [(1, s), (1, dp)]

    def soft(g):
        b = g % 2
        c2 = scale * log2e

        def part(blk, c):
            return slice(blk * seq + c, blk * seq + c + CH), half if blk == 0 else seq

        def masked(blk, c, s):
            row_id = lax.broadcasted_iota(jnp.int32, (CH, half), 0) + (c % half)
            keep = row_id >= lax.broadcasted_iota(jnp.int32, (CH, half), 1)
            if blk == 0:
                return jnp.where(keep, s, -jnp.inf)
            return jnp.concatenate([s[:, :half], jnp.where(keep, s[:, half:], -jnp.inf)], axis=1)

        def wide(ref, rows, width):
            t = ref[rows, :]
            return t if width == half else jnp.concatenate([t, t], axis=1)

        def top(blk, c):
            rows, width = part(blk, c)

            def run():
                m = jnp.max(masked(blk, c, r.s[b, rows, 0:width]), axis=-1, keepdims=True)
                r.st[0, rows, :] = jnp.broadcast_to(m * c2, (CH, HD))

            return (0.4 + 0.4 * blk, run)

        def power(blk, c):
            rows, width = part(blk, c)

            def run():
                e = jnp.exp2(masked(blk, c, r.s[b, rows, 0:width] * c2) - wide(r.st.at[0], rows, width))
                r.s[b, rows, 0:width] = e
                r.st[1, rows, :] = jnp.broadcast_to(1.0 / jnp.sum(e, axis=-1, keepdims=True), (CH, HD))

            return (0.8 + 0.8 * blk, run)

        def prob(blk, c):
            rows, width = part(blk, c)

            def run():
                pr = r.s[b, rows, 0:width] * wide(r.st.at[1], rows, width)
                r.s[b, rows, 0:width] = pr
                r.p[b, rows, 0:width] = pr.astype(BF16)
                r.st[2, rows, :] = jnp.broadcast_to(jnp.sum(pr * r.dp[b, rows, 0:width], axis=-1, keepdims=True), (CH, HD))

            return (0.8 + 0.8 * blk, run)

        def last(blk, c):
            rows, width = part(blk, c)

            def run():
                d = r.dp[b, rows, 0:width] - wide(r.st.at[2], rows, width)
                r.ds[b, rows, 0:width] = (r.s[b, rows, 0:width] * d * scale).astype(BF16)

            return (0.8 + 0.8 * blk, run)

        return [f(blk, c) for f in (top, power, prob, last) for blk in range(2) for c in range(0, seq, CH)]

    def grads(g):
        b = g % 2
        col, kcol = g * 2 * HD, g * HD

        def dq():
            r.dqf[b, 0:seq, :] = dot(r.ds[b, 0:seq, 0:half], r.rot[g, 2 * seq:2 * seq + half, :])
            r.dqf[b, seq:, :] = dot(r.ds[b, seq:, :], r.rot[g, 2 * seq:, :])

        def dk():
            tb = dot(r.ds[b, seq:, :], r.rot[g, seq:2 * seq, :], TN)
            ta = dot(r.ds[b, 0:seq, 0:half], r.rot[g, 0:seq, :], TN)
            r.dkf[b, :half, :] = tb[:half] + ta
            r.dkf[b, half:, :] = tb[half:]

        def o():
            ta = dot(r.p[b, 0:seq, 0:half], r.v[g, :half, :])
            tb = dot(r.p[b, seq:, :], r.v[g])
            for h in range(2):
                r.o[0:half, col + h * HD:col + (h + 1) * HD] = ta[h * half:(h + 1) * half].astype(BF16)
                r.o[half:seq, col + h * HD:col + (h + 1) * HD] = tb[h * half:(h + 1) * half].astype(BF16)

        def dv():
            tb = dot(r.p[b, seq:, :], r.do[g, seq:, :], TN)
            ta = dot(r.p[b, 0:seq, 0:half], r.do[g, :seq, :], TN)
            r.dv[0:half, kcol:kcol + HD] = (tb[:half] + ta).astype(BF16)
            r.dv[half:seq, kcol:kcol + HD] = tb[half:].astype(BF16)

        return [(1, dq), (1, dk), (1, o), (1, dv)]

    def back(g):
        b = g % 2

        def place(h, c):
            if h == 2:
                return r.dkf, c, r.dk, g * HD, r.kg
            return r.dqf, stacked(h, c), r.dq, (2 * g + h) * HD, r.qg

        def turn(h, c):
            src, o, _, _, g_ref = place(h, c)

            def run():
                d = src[b, o:o + CH, :].astype(BF16).astype(F32)
                that = r.raw[g, h, c:c + CH, :].astype(F32) * r.inv[g, h, c:c + CH, :]
                du = d[:, :HD] * r.tab[2, c:c + CH, :] - d[:, HD:] * r.tab[3, c:c + CH, :]
                src[b, o:o + CH, 0:HD] = du
                pr = du * that
                dg_ref = r.dgk if h == 2 else r.dgq
                dg_ref[...] += jnp.sum(pr.reshape(CH // 8, 8, HD), axis=0)
                r.sb[h, c:c + CH, :] = jnp.broadcast_to(jnp.mean(pr * g_ref[0:1, :], axis=-1, keepdims=True), (CH, HD))

            return (0.6, run)

        def out(h, c):
            src, o, out_ref, col, g_ref = place(h, c)

            def run():
                inv = r.inv[g, h, c:c + CH, :]
                that = r.raw[g, h, c:c + CH, :].astype(F32) * inv
                out_ref[c:c + CH, col:col + HD] = (inv * (src[b, o:o + CH, 0:HD] * g_ref[0:1, :] - that * r.sb[h, c:c + CH, :])).astype(BF16)

            return (0.5, run)

        return [f(h, c) for f in (turn, out) for h in (0, 1, 2) for c in range(0, seq, CH)]

    return SimpleNamespace(norm=norm_rows, proj=proj, rope=rope, scores=scores, soft=soft, grads=grads, back=back)


def attn_tick(st, g, n_grp, extra=()):
    vec = st.soft((g - 3) % n_grp) + st.rope((g - 1) % n_grp)
    more = [e for e in extra]
    if more:
        vec = vec + more[0]
    vec = vec + st.back(g)
    gr = st.grads(g)
    for _, f in gr[:2]:
        f()
    weave(vec, st.scores((g - 2) % n_grp) + gr[2:] + st.proj(g), *more[1:])


def attn_scratch(seq, n_grp, nq, nk):
    return dict(
        qnew=pltpu.VMEM((2, 2, seq, HD), BF16),
        knew=pltpu.VMEM((n_grp, seq, HD), BF16),
        vnew=pltpu.VMEM((n_grp, seq, HD), BF16),
        raw=pltpu.VMEM((n_grp, 3, seq, HD), BF16),
        inv=pltpu.VMEM((n_grp, 3, seq, HD), F32),
        rot=pltpu.VMEM((n_grp, 3 * seq, 2 * HD), BF16),
        do=pltpu.VMEM((n_grp, 2 * seq, HD), BF16),
        v=pltpu.VMEM((n_grp, seq, HD), BF16),
        s=pltpu.VMEM((2, 2 * seq, seq), F32),
        dp=pltpu.VMEM((2, 2 * seq, seq), F32),
        p=pltpu.VMEM((2, 2 * seq, seq), BF16),
        ds=pltpu.VMEM((2, 2 * seq, seq), BF16),
        dkf=pltpu.VMEM((2, seq, 2 * HD), F32),
        dqf=pltpu.VMEM((2, 2 * seq, 2 * HD), F32),
        st=pltpu.VMEM((3, 2 * seq, HD), F32),
        sb=pltpu.VMEM((3, seq, HD), F32),
        tab=pltpu.VMEM((4, seq, HD), F32),
        o=pltpu.VMEM((seq, nq), BF16),
        dq=pltpu.VMEM((seq, nq), BF16),
        dk=pltpu.VMEM((seq, nk), BF16),
        dv=pltpu.VMEM((seq, nk), BF16),
    )


def tail_kernel(seq, n_grp, rows, keys, sel_ref, n_in, dy_in, cos_in, sin_in, x_in, dyx_in, gain_ref, qg_ref, kg_ref, *refs):
    own_w, oth_w, own_a = refs[:4], refs[4:8], refs[8:12]
    y_out, dx_out, dg_out, dgq_out, dgk_out = refs[12:17]
    r = SimpleNamespace(n=n_in, dy=dy_in, qg=qg_ref, kg=kg_ref, gain=gain_ref, **dict(zip(keys, refs[17:])))
    step = pl.program_id(0)
    me = sel_ref[0]
    oth = 1 - me
    D = x_in.shape[1]
    r.wq = lambda c: r.wq_all[oth, :, c]
    r.wk = lambda c: r.wk_all[oth, :, c]
    r.wv = lambda c: r.wv_all[oth, :, c]
    r.do_dot = lambda c: dot(dy_in[...], r.wo_all[oth, c, :], NT)
    st = attn_stages(seq, n_grp, r)

    def fetch(row):
        return [pltpu.make_async_copy(src.at[me, pl.ds(row * seq, seq), :], dst, r.sem.at[8 + k])
                for k, (src, dst) in enumerate(zip(own_a, (r.o_own, r.dq_own, r.dk_own, r.dv_own)))]

    @pl.when(step == 0)
    def _():
        copies = []
        for k, dst in enumerate((r.wq_all, r.wk_all, r.wv_all, r.wo_all)):
            copies.append(pltpu.make_async_copy(oth_w[k], dst.at[oth], r.sem.at[4 + k]))
            copies.append(pltpu.make_async_copy(own_w[k], dst.at[me], r.sem.at[k]))
        for c in copies:
            c.start()
        for c in copies:
            c.wait()
        for c in fetch(0):
            c.start()
        r.dg[...] = jnp.zeros_like(r.dg)

    CR, NC = 32, 256
    nn = D // NC
    lines = range(0, seq, CR)

    def wide(v):
        return jnp.concatenate([v] * (NC // HD), axis=1)

    def stat(c):
        def run():
            xf = x_in[c:c + CR, :].astype(F32)
            r.xs[0, c:c + CR, :] = jnp.broadcast_to(lax.rsqrt(jnp.mean(xf * xf, axis=-1, keepdims=True) + EPS), (CR, HD))
            r.xs[1, c:c + CR, :] = jnp.zeros((CR, HD), F32)

        return (1, run)

    def dn_dot(n):
        def run():
            cols = slice(n * NC, (n + 1) * NC)
            t = None
            for s in range(2):
                for a_ref, w_ref in ((r.dqc, r.wq_all), (r.dkc, r.wk_all), (r.dvc, r.wv_all)):
                    u = dot(a_ref[s], w_ref[s, cols, :], NT)
                    t = u if t is None else t + u
            r.dn[:, cols] = t

        return (2, run)

    def first(n, c):
        def run():
            cols = slice(n * NC, (n + 1) * NC)
            w = r.dn[c:c + CR, cols] * (x_in[c:c + CR, cols].astype(F32) * wide(r.xs[0, c:c + CR, :]))
            r.dg[:, cols] += jnp.sum(w.reshape(CR // 8, 8, NC), axis=0)
            w = w * gain_ref[0:1, cols]
            r.xs[1, c:c + CR, :] += w[:, :HD] + w[:, HD:]

        return (1, run)

    def mean(c):
        def run():
            r.xs[2, c:c + CR, :] = jnp.broadcast_to(jnp.sum(r.xs[1, c:c + CR, :], axis=-1, keepdims=True) * (1.0 / D), (CR, HD))

        return (0.2, run)

    def second(n, c):
        def run():
            cols = slice(n * NC, (n + 1) * NC)
            inv = wide(r.xs[0, c:c + CR, :])
            xh = x_in[c:c + CR, cols].astype(F32) * inv
            e = r.dn[c:c + CR, cols] * gain_ref[0:1, cols]
            dx_out[c:c + CR, cols] = (dyx_in[c:c + CR, cols].astype(F32) + inv * (e - xh * wide(r.xs[2, c:c + CR, :]))).astype(BF16)

        return (1.2, run)

    def y_dot(n):
        def run():
            cols = slice(n * NC, (n + 1) * NC)
            t = dot(r.oc[0], r.wo_all[0, :, cols]) + dot(r.oc[1], r.wo_all[1, :, cols])
            y_out[:, cols] = (x_in[:, cols].astype(F32) + t).astype(BF16)
            r.xs[3 + me, 0:8, :] = t[0:8, :HD]

        return (1, run)

    dn = [dn_dot(n) for n in range(nn)]
    yd = [y_dot(n) for n in range(nn)]
    f = [[first(n, c) for c in lines] for n in range(nn)]
    sec = [second(n, c) for n in range(nn) for c in lines]
    k = nn // 2
    out_mat = [dn[:k], dn[k:], yd[:3], yd[3:]]
    out_vec = [[stat(c) for c in lines], sum(f[:k], []), sum(f[k:], []) + [mean(c) for c in lines], sec]

    def body(attn, out):
        if attn:
            r.tab[2:4] = r.tab[0:2]
            r.tab[0] = cos_in[...]
            r.tab[1] = sin_in[...]
        for g in range(n_grp):
            if attn:
                attn_tick(st, g, n_grp, ([], out_mat[g], out_vec[g]) if out else ())
            else:
                weave(out_mat[g], out_vec[g])
        if attn:
            row = jnp.clip(step - 1, 0, rows - 1)
            for c in fetch(row):
                c.wait()
            for dst, theirs, mine in ((r.oc, r.o, r.o_own), (r.dqc, r.dq, r.dq_own), (r.dkc, r.dk, r.dk_own), (r.dvc, r.dv, r.dv_own)):
                dst[oth] = theirs[...]
                dst[me] = mine[...]

            for acc in (r.dgq, r.dgk):
                acc[...] = jnp.where(step > 0, acc[...], 0.0)

            @pl.when(step < rows)
            def _():
                for c in fetch(step):
                    c.start()

    @pl.when(step < 2)
    def _():
        body(True, False)

    @pl.when((step >= 2) & (step <= rows))
    def _():
        body(True, True)

    @pl.when(step > rows)
    def _():
        body(False, True)
        dg_out[...] = r.dg[...]
        dgq_out[...] = r.dgq[...]
        dgk_out[...] = r.dgk[...]


def tail_call(sel, n, x, dy, cosd, sind, o, dq, dk, dv, gain, qg, kg, own, oth, seq=256):
    T, D = x.shape
    nq, nk = dq.shape[2], dk.shape[2]
    n_grp = nk // HD
    rows = T // seq
    lag = lambda k, c: pl.BlockSpec((seq, c), lambda i, s: (jnp.clip(i - k, 0, rows - 1), 0))
    const = lambda *b: pl.BlockSpec(b, lambda i, s: (0,) * len(b), pipeline_mode=pl.Buffered(1))
    hbm = pl.BlockSpec(memory_space=pl.ANY)
    scratch = attn_scratch(seq, n_grp, nq, nk)
    scratch.update(
        wq_all=pltpu.VMEM((2, D, nq), BF16), wk_all=pltpu.VMEM((2, D, nk), BF16), wv_all=pltpu.VMEM((2, D, nk), BF16), wo_all=pltpu.VMEM((2, nq, D), BF16),
        dn=pltpu.VMEM((seq, D), F32), oc=pltpu.VMEM((2, seq, nq), BF16), dqc=pltpu.VMEM((2, seq, nq), BF16), dkc=pltpu.VMEM((2, seq, nk), BF16), dvc=pltpu.VMEM((2, seq, nk), BF16),
        o_own=pltpu.VMEM((seq, nq), BF16), dq_own=pltpu.VMEM((seq, nq), BF16), dk_own=pltpu.VMEM((seq, nk), BF16), dv_own=pltpu.VMEM((seq, nk), BF16),
        xs=pltpu.VMEM((5, seq, HD), F32), dg=pltpu.VMEM((8, D), F32), dgq=pltpu.VMEM((8, HD), F32), dgk=pltpu.VMEM((8, HD), F32), sem=pltpu.SemaphoreType.DMA((12,)))
    flops = 2 * T * D * (nq + 2 * nk + nq) * 3 + 12 * T * nq * seq
    return pl.pallas_call(
        functools.partial(tail_kernel, seq, n_grp, rows, tuple(scratch)),
        grid_spec=pltpu.PrefetchScalarGridSpec(
            num_scalar_prefetch=1,
            grid=(rows + 2,),
            in_specs=[lag(0, D), lag(0, D), lag(0, HD), lag(0, HD), lag(2, D), lag(2, D), const(1, D), const(1, HD), const(1, HD)] + [hbm] * 12,
            out_specs=[lag(2, D), lag(2, D), pl.BlockSpec((8, D), lambda i, s: (0, 0))] + [pl.BlockSpec((8, HD), lambda i, s: (0, 0))] * 2,
            scratch_shapes=list(scratch.values()),
        ),
        out_shape=[jax.ShapeDtypeStruct((T, D), BF16)] * 2 + [jax.ShapeDtypeStruct((8, c), F32) for c in (D, HD, HD)],
        compiler_params=pltpu.CompilerParams(dimension_semantics=("arbitrary",), vmem_limit_bytes=67043328),
        cost_estimate=pl.CostEstimate(flops=flops, bytes_accessed=T * D * 14, transcendentals=T * nq * 2),
        name="tail",
    )(sel, n, dy, cosd, sind, x, dy, gain, qg, kg, *own, *oth, o, dq, dk, dv)


def solution(mesh):
    tok_spec = P("dp", None, None)
    col_spec = P(None, "tp")
    row_spec = P("tp", None)
    n_dp = mesh.shape["dp"]

    def per_device(x_in, dy_in, positions, g_attn, q_gain, k_gain, w_q, w_k, w_v, w_o):
        n_batch, n_seq, D = x_in.shape
        T = n_batch * n_seq
        nq, nk = w_q.shape[1], w_k.shape[1]
        x, dy = x_in.reshape(T, D), dy_in.reshape(T, D)
        me = lax.axis_index("tp").astype(jnp.int32)
        own = me.reshape(1)

        part = (lax.axis_index("dp") % 2).astype(jnp.int32).reshape(1)
        share, cosd, sind = pre_call(part, w_q, w_k, w_v, w_o, positions)
        share = lax.ppermute(share, "tp", [(0, 1), (1, 0)])
        gathered = lax.all_gather(share, "dp", axis_index_groups=[[2 * i, 2 * i + 1] for i in range(n_dp // 2)])
        gathered = gathered.reshape(-1, *gathered.shape[2:])

        gain = g_attn.astype(F32).reshape(1, D)
        qg, kg = q_gain.astype(F32).reshape(1, HD), k_gain.astype(F32).reshape(1, HD)

        n, o, dq, dk, dv, dgq, dgk = attn_call(True, own, x, dy, cosd, sind, gain, qg, kg, w_q, w_k, w_v, w_o, seq=n_seq)
        dw_q, dw_k, dw_v = dw_call(own, n, [dq, dk, dv], 512)
        (dw_o,) = dw_call(own, o, [dy], 1024)
        dw_o, dw_q, dw_k, dw_v = lax.psum((dw_o, dw_q, dw_k, dw_v), "dp")

        theirs = unpack_call(gathered, D, nq, nk)
        y, dx, dg, dgq2, dgk2 = tail_call(own, n, x, dy, cosd, sind, o, dq, dk, dv, gain, qg, kg, (w_q, w_k, w_v, w_o), theirs, seq=n_seq)
        small = lax.psum(jnp.sum(jnp.concatenate([dg, dgq + dgq2, dgk + dgk2], axis=1), axis=0), "dp")
        g_sum, q_sum, k_sum = small[:D], small[D:D + HD], small[D + HD:]
        return y.reshape(x_in.shape), dx.reshape(x_in.shape), dw_q, dw_k, dw_v, dw_o, q_sum, k_sum, g_sum

    return jax.shard_map(per_device, mesh=mesh, in_specs=(tok_spec, tok_spec, P("dp", None), P(), P(), P(), col_spec, col_spec, col_spec, row_spec), out_specs=(tok_spec, tok_spec, col_spec, col_spec, col_spec, row_spec, P(), P(), P()), check_vma=False)
```

```python
import functools
from types import SimpleNamespace
import jax
import jax.numpy as jnp
from jax import lax
from jax.experimental import pallas as pl
from jax.experimental.pallas import tpu as pltpu
from jax.sharding import PartitionSpec as P


EPS = 1e-6
THETA = 1000000.0
F32 = jnp.float32
BF16 = jnp.bfloat16
HD = 128
NT = (((1,), (1,)), ((), ()))
TN = (((0,), (0,)), ((), ()))
NN = (((1,), (0,)), ((), ()))


def dot(a, b, dims=NN):
    return lax.dot_general(a, b, dims, preferred_element_type=F32)


def weave(*lists):
    order = []
    for n, pieces in enumerate(lists):
        total = sum(c for c, _ in pieces) or 1
        at = 0
        for k, (c, f) in enumerate(pieces):
            order.append(((at + c / 2) / total, n, k, f))
            at += c
    for _, _, _, f in sorted(order, key=lambda e: e[:3]):
        f()


CH = 32


def attn_kernel(own, seq, n_grp, sel_ref, *refs):
    if own:
        (x0_ref, xn_ref, dy_ref, cos_ref, sin_ref, gain_ref, qg_ref, kg_ref, wq_ref, wk_ref, wv_ref, wo_ref,
         n_out, o_out, dq_out, dk_out, dv_out, dgq_out, dgk_out) = refs[:19]
        refs = refs[19:]
    else:
        nin_ref, dy_ref, cos_ref, sin_ref, qg_ref, kg_ref, wq_ref, wk_ref, wv_ref, wo_ref, _, _, _, _, o_out, dq_out, dk_out, dv_out = refs[:18]
        refs = refs[18:]
        n_ref = nin_ref
    (wot_ref, qnew_ref, knew_ref, vnew_ref, raw_ref, inv_ref, rot_ref, do_ref, v_ref, s_ref, dp_ref, p_ref, ds_ref, dkf_ref, dqf_ref, st_ref,
     tab_ref, o_ref, dq_ref, dk_ref, dv_ref) = refs[:21]
    if own:
        n_ref, nn_ref, dgq_ref, dgk_ref = refs[21:]
    half = seq // 2
    scale = HD ** -0.5
    log2e = 1.4426950408889634
    step = pl.program_id(0)

    def norm_rows(src, dst):
        def piece(c):
            def run():
                xf = src[c:c + 32, :].astype(F32)
                inv = lax.rsqrt(jnp.mean(xf * xf, axis=-1, keepdims=True) + EPS)
                dst[c:c + 32, :] = (xf * inv * gain_ref[0:1, :]).astype(BF16)

            return (1.5, run)

        return [piece(c) for c in range(0, seq, 32)]

    def proj(g):
        def q():
            t = dot(n_ref[...], wq_ref[:, g * 2 * HD:(g + 1) * 2 * HD])
            for h in range(2):
                qnew_ref[g % 2, h] = t[:, h * HD:(h + 1) * HD].astype(BF16)

        def k():
            t = dot(n_ref[...], wk_ref[:, g * HD:(g + 2) * HD])
            for h in range(2):
                knew_ref[g + h] = t[:, h * HD:(h + 1) * HD].astype(BF16)

        def v():
            t = dot(n_ref[...], wv_ref[:, g * HD:(g + 2) * HD])
            for h in range(2):
                vnew_ref[g + h] = t[:, h * HD:(h + 1) * HD].astype(BF16)

        def do():
            t = dot(dy_ref[...], wot_ref[:, g * 2 * HD:(g + 1) * 2 * HD])
            for h in range(2):
                do_ref[g, h * half:(h + 1) * half, :] = t[:half, h * HD:(h + 1) * HD].astype(BF16)
                do_ref[g, seq + h * half:seq + (h + 1) * half, :] = t[half:, h * HD:(h + 1) * HD].astype(BF16)

        return [(1, q)] + ([(1, k), (1, v)] if g % 2 == 0 else []) + [(1, do)]

    def stacked(h, c):
        return (h * half + c) if c < half else (seq + h * half + c - half)

    def rope(g):
        cs, sn = (tab_ref.at[2], tab_ref.at[3]) if g == n_grp - 1 else (tab_ref.at[0], tab_ref.at[1])

        def size(h, c):
            def run():
                raw = knew_ref[g, c:c + CH, :] if h == 2 else qnew_ref[g % 2, h, c:c + CH, :]
                raw_ref[g, h, c:c + CH, :] = raw
                t = raw.astype(F32)
                inv_ref[g, h, c:c + CH, :] = jnp.broadcast_to(lax.rsqrt(jnp.mean(t * t, axis=-1, keepdims=True) + EPS), t.shape)

            return (0.4, run)

        def turn(h, c):
            def run():
                t = raw_ref[g, h, c:c + CH, :].astype(F32)
                w = (t * inv_ref[g, h, c:c + CH, :]) * (kg_ref if h == 2 else qg_ref)[0:1, :]
                o = 2 * seq + c if h == 2 else stacked(h, c)
                x = pltpu.roll(w, HD // 2, 1)
                co, si = cs[c:c + CH, :], sn[c:c + CH, :]
                rot_ref[g, o:o + CH, 0:HD] = (w * co + x * si).astype(BF16)
                rot_ref[g, o:o + CH, HD:] = (x * co - w * si).astype(BF16)
                if h == 2:
                    v_ref[g, c:c + CH, :] = vnew_ref[g, c:c + CH, :]

            return (0.6, run)

        return [f(h, c) for f in (size, turn) for h in (2, 0, 1) for c in range(0, seq, CH)]

    def scores(g):
        b = g % 2

        def s():
            s_ref[b, 0:seq, 0:half] = dot(rot_ref[g, 0:seq, 0:HD], rot_ref[g, 2 * seq:2 * seq + half, 0:HD], NT)
            s_ref[b, seq:, :] = dot(rot_ref[g, seq:2 * seq, 0:HD], rot_ref[g, 2 * seq:, 0:HD], NT)

        def dp():
            dp_ref[b, 0:seq, 0:half] = dot(do_ref[g, :seq, :], v_ref[g, :half, :], NT)
            dp_ref[b, seq:, :] = dot(do_ref[g, seq:, :], v_ref[g], NT)

        return [(1, s), (1, dp)]

    def soft(g):
        b = g % 2
        c2 = scale * log2e

        def part(blk, c):
            return slice(blk * seq + c, blk * seq + c + CH), half if blk == 0 else seq

        def masked(blk, c, s):
            row_id = lax.broadcasted_iota(jnp.int32, (CH, half), 0) + (c % half)
            keep = row_id >= lax.broadcasted_iota(jnp.int32, (CH, half), 1)
            if blk == 0:
                return jnp.where(keep, s, -jnp.inf)
            return jnp.concatenate([s[:, :half], jnp.where(keep, s[:, half:], -jnp.inf)], axis=1)

        def wide(ref, rows, width):
            t = ref[rows, :]
            return t if width == half else jnp.concatenate([t, t], axis=1)

        def top(blk, c):
            rows, width = part(blk, c)

            def run():
                m = jnp.max(masked(blk, c, s_ref[b, rows, 0:width]), axis=-1, keepdims=True)
                st_ref[0, rows, :] = jnp.broadcast_to(m * c2, (CH, HD))

            return (0.4 + 0.4 * blk, run)

        def power(blk, c):
            rows, width = part(blk, c)

            def run():
                e = jnp.exp2(masked(blk, c, s_ref[b, rows, 0:width] * c2) - wide(st_ref.at[0], rows, width))
                s_ref[b, rows, 0:width] = e
                st_ref[1, rows, :] = jnp.broadcast_to(1.0 / jnp.sum(e, axis=-1, keepdims=True), (CH, HD))

            return (0.8 + 0.8 * blk, run)

        def prob(blk, c):
            rows, width = part(blk, c)

            def run():
                pr = s_ref[b, rows, 0:width] * wide(st_ref.at[1], rows, width)
                s_ref[b, rows, 0:width] = pr
                p_ref[b, rows, 0:width] = pr.astype(BF16)
                st_ref[2, rows, :] = jnp.broadcast_to(jnp.sum(pr * dp_ref[b, rows, 0:width], axis=-1, keepdims=True), (CH, HD))

            return (0.8 + 0.8 * blk, run)

        def last(blk, c):
            rows, width = part(blk, c)

            def run():
                d = dp_ref[b, rows, 0:width] - wide(st_ref.at[2], rows, width)
                ds_ref[b, rows, 0:width] = (s_ref[b, rows, 0:width] * d * scale).astype(BF16)

            return (0.8 + 0.8 * blk, run)

        return [f(blk, c) for f in (top, power, prob, last) for blk in range(2) for c in range(0, seq, CH)]

    def grads(g):
        b = g % 2
        col, kcol = g * 2 * HD, g * HD

        def dq():
            dqf_ref[b, 0:seq, :] = dot(ds_ref[b, 0:seq, 0:half], rot_ref[g, 2 * seq:2 * seq + half, :])
            dqf_ref[b, seq:, :] = dot(ds_ref[b, seq:, :], rot_ref[g, 2 * seq:, :])

        def dk():
            tb = dot(ds_ref[b, seq:, :], rot_ref[g, seq:2 * seq, :], TN)
            ta = dot(ds_ref[b, 0:seq, 0:half], rot_ref[g, 0:seq, :], TN)
            dkf_ref[b, :half, :] = tb[:half] + ta
            dkf_ref[b, half:, :] = tb[half:]

        def o():
            ta = dot(p_ref[b, 0:seq, 0:half], v_ref[g, :half, :])
            tb = dot(p_ref[b, seq:, :], v_ref[g])
            for h in range(2):
                o_ref[0:half, col + h * HD:col + (h + 1) * HD] = ta[h * half:(h + 1) * half].astype(BF16)
                o_ref[half:seq, col + h * HD:col + (h + 1) * HD] = tb[h * half:(h + 1) * half].astype(BF16)

        def dv():
            tb = dot(p_ref[b, seq:, :], do_ref[g, seq:, :], TN)
            ta = dot(p_ref[b, 0:seq, 0:half], do_ref[g, :seq, :], TN)
            dv_ref[0:half, kcol:kcol + HD] = (tb[:half] + ta).astype(BF16)
            dv_ref[half:seq, kcol:kcol + HD] = tb[half:].astype(BF16)

        return [(1, dq), (1, dk), (1, o), (1, dv)]

    def back(g):
        b = g % 2

        def place(h, c):
            if h == 2:
                return dkf_ref, c, dk_ref, g * HD, kg_ref
            return dqf_ref, stacked(h, c), dq_ref, (2 * g + h) * HD, qg_ref

        def turn(h, c):
            src, o, _, _, g_ref = place(h, c)

            def run():
                d = src[b, o:o + CH, :].astype(BF16).astype(F32)
                that = raw_ref[g, h, c:c + CH, :].astype(F32) * inv_ref[g, h, c:c + CH, :]
                du = d[:, :HD] * tab_ref[2, c:c + CH, :] - d[:, HD:] * tab_ref[3, c:c + CH, :]
                src[b, o:o + CH, 0:HD] = du
                pr = du * that
                if own:
                    dg_ref = dgk_ref if h == 2 else dgq_ref
                    dg_ref[...] += jnp.sum(pr.reshape(CH // 8, 8, HD), axis=0)
                st_ref[3 + h, c:c + CH, :] = jnp.broadcast_to(jnp.mean(pr * g_ref[0:1, :], axis=-1, keepdims=True), (CH, HD))

            return (0.6, run)

        def out(h, c):
            src, o, out_ref, col, g_ref = place(h, c)

            def run():
                inv = inv_ref[g, h, c:c + CH, :]
                that = raw_ref[g, h, c:c + CH, :].astype(F32) * inv
                out_ref[c:c + CH, col:col + HD] = (inv * (src[b, o:o + CH, 0:HD] * g_ref[0:1, :] - that * st_ref[3 + h, c:c + CH, :])).astype(BF16)

            return (0.5, run)

        return [f(h, c) for f in (turn, out) for h in (0, 1, 2) for c in range(0, seq, CH)]

    @pl.when(step == 0)
    def _():
        for c in range(0, wo_ref.shape[0], 256):
            for d in range(0, wo_ref.shape[1], 256):
                wot_ref[d:d + 256, c:c + 256] = wo_ref[c:c + 256, d:d + 256].T
        if own:
            weave(norm_rows(x0_ref, n_ref))

    tab_ref[2:4] = tab_ref[0:2]
    tab_ref[0] = cos_ref[...]
    tab_ref[1] = sin_ref[...]
    if own:
        norms = norm_rows(xn_ref, nn_ref)
    for g in range(n_grp):
        vec = soft((g - 3) % n_grp)
        sc = scores((g - 2) % n_grp)
        vec = vec + rope((g - 1) % n_grp)
        if own:
            vec += norms[g * len(norms) // n_grp:(g + 1) * len(norms) // n_grp]
        vec += back(g)
        gr = grads(g)
        for _, f in gr[:2]:
            f()
        weave(vec, sc + gr[2:] + proj(g))

    for dst, src in ((o_out, o_ref), (dq_out, dq_ref), (dk_out, dk_ref), (dv_out, dv_ref)):
        dst[0] = src[...]
    if own:
        n_out[...] = n_ref[...]
        n_ref[...] = nn_ref[...]
        keep = step > 0
        for dst, acc in ((dgq_out, dgq_ref), (dgk_out, dgk_ref)):
            acc[...] = jnp.where(keep, acc[...], 0.0)
            dst[...] = acc[...]


def attn_call(own, sel, x, dy, cosd, sind, gain, qg, kg, wq, wk, wv, wo, prev=None, seq=256):
    T, D = x.shape
    nq, nk = wq.shape[1], wk.shape[1]
    n_grp = nk // HD
    rows = T // seq
    const = lambda *b: pl.BlockSpec(b, lambda i, s: (0,) * len(b), pipeline_mode=pl.Buffered(1))
    now = lambda c: pl.BlockSpec((seq, c), lambda i, s: (jnp.minimum(i, rows - 1), 0))
    nxt = lambda c: pl.BlockSpec((seq, c), lambda i, s: (jnp.minimum(i + 1, rows - 1), 0))
    out3 = lambda c: pl.BlockSpec((1, seq, c), lambda i, s: (s[0], jnp.maximum(i - 1, 0), 0))
    mid = [now(D), now(HD), now(HD)]
    tail = [const(1, HD), const(1, HD), const(D, nq), const(D, nk), const(D, nk), const(nq, D)]
    shapes = [jax.ShapeDtypeStruct((2, T, c), BF16) for c in (nq, nq, nk, nk)]
    specs = [out3(nq), out3(nq), out3(nk), out3(nk)]
    aliases = {}
    if own:
        in_specs = [const(seq, D), nxt(D)] + mid + [const(1, D)] + tail
        args = [x, x, dy, cosd, sind, gain, qg, kg, wq, wk, wv, wo]
        shapes = [jax.ShapeDtypeStruct((T, D), BF16)] + shapes + [jax.ShapeDtypeStruct((8, HD), F32)] * 2
        specs = [now(D)] + specs + [pl.BlockSpec((8, HD), lambda i, s: (0, 0))] * 2
    else:
        in_specs = [now(D)] + mid + tail + [pl.BlockSpec(memory_space=pl.ANY)] * 4
        args = [x, dy, cosd, sind, qg, kg, wq, wk, wv, wo]
        aliases = {1 + len(args) + i: i for i in range(4)}
        args += list(prev)
    flops = 2 * T * D * (nq + 2 * nk + nq) + 12 * T * nq * seq
    return pl.pallas_call(
        functools.partial(attn_kernel, own, seq, n_grp),
        grid_spec=pltpu.PrefetchScalarGridSpec(
            num_scalar_prefetch=1,
            grid=(rows + 1,),
            in_specs=in_specs,
            out_specs=specs,
            scratch_shapes=[
                pltpu.VMEM((D, nq), BF16),
                pltpu.VMEM((2, 2, seq, HD), BF16),
                pltpu.VMEM((n_grp, seq, HD), BF16),
                pltpu.VMEM((n_grp, seq, HD), BF16),
                pltpu.VMEM((n_grp, 3, seq, HD), BF16),
                pltpu.VMEM((n_grp, 3, seq, HD), F32),
                pltpu.VMEM((n_grp, 3 * seq, 2 * HD), BF16),
                pltpu.VMEM((n_grp, 2 * seq, HD), BF16),
                pltpu.VMEM((n_grp, seq, HD), BF16),
                pltpu.VMEM((2, 2 * seq, seq), F32),
                pltpu.VMEM((2, 2 * seq, seq), F32),
                pltpu.VMEM((2, 2 * seq, seq), BF16),
                pltpu.VMEM((2, 2 * seq, seq), BF16),
                pltpu.VMEM((2, seq, 2 * HD), F32),
                pltpu.VMEM((2, 2 * seq, 2 * HD), F32),
                pltpu.VMEM((6, 2 * seq, HD), F32),
                pltpu.VMEM((4, seq, HD), F32),
            ] + [pltpu.VMEM((seq, c), BF16) for c in (nq, nq, nk, nk)]
            + ([pltpu.VMEM((seq, D), BF16)] * 2 + [pltpu.VMEM((8, HD), F32)] * 2 if own else []),
        ),
        out_shape=shapes,
        input_output_aliases=aliases,
        compiler_params=pltpu.CompilerParams(dimension_semantics=("arbitrary",), vmem_limit_bytes=56 << 20),
        cost_estimate=pl.CostEstimate(flops=flops, bytes_accessed=T * D * 6 + T * (2 * nq + 2 * nk) * 2, transcendentals=T * nq * 2),
        name="attn_own" if own else "attn_other",
    )(sel, *args)


def pre_kernel(sel_ref, q_ref, k_ref, v_ref, o_ref, pos_ref, freq_ref, out_ref, cos_ref, sin_ref):
    d, nq, nk = q_ref.shape[0], q_ref.shape[1], k_ref.shape[1]
    out_ref[0, 0:d, 0:nq] = q_ref[...].astype(F32)
    out_ref[0, 0:d, nq:nq + nk] = k_ref[...].astype(F32)
    out_ref[0, 0:d, nq + nk:] = v_ref[...].astype(F32)
    out_ref[0, d:, :] = o_ref[...].astype(F32)
    n, seq = pos_ref.shape
    lane = lax.broadcasted_iota(jnp.int32, (HD, HD), 1)
    for r in range(n):
        for h in range(seq // HD):
            p = pos_ref[r:r + 1, h * HD:(h + 1) * HD].astype(F32)
            a = jnp.broadcast_to(p, (HD, HD)).T * freq_ref[0:1, :]
            k = jnp.round(a * 0.6366197723675814)
            x = ((a - k * 1.5703125) - k * 4.837512969970703125e-4) - k * 7.549789948768648e-8
            z = x * x
            s = ((-1.9515295891e-4 * z + 8.3321608736e-3) * z - 1.6666654611e-1) * z * x + x
            c = ((2.443315711809948e-5 * z - 1.388731625493765e-3) * z + 4.166664568298827e-2) * z * z - 0.5 * z + 1.0
            q = k.astype(jnp.int32)
            odd = (q & 1) == 1
            co, si = jnp.where(odd, s, c), jnp.where(odd, c, s)
            rows = slice((r * (seq // HD) + h) * HD, (r * (seq // HD) + h + 1) * HD)
            cos_ref[rows, :] = jnp.where(((q + 1) & 2) == 0, co, -co)
            sin_ref[rows, :] = jnp.where(((q & 2) == 0) == (lane >= HD // 2), si, -si)


def pre_call(part, w_q, w_k, w_v, w_o, positions, parts=2, cuts=4):
    D, nq = w_q.shape
    n, seq = positions.shape
    rows = n // cuts
    freq = THETA ** (-jnp.arange(0, HD, 2, dtype=F32) / HD)
    freq = jnp.concatenate([freq, freq]).reshape(1, HD)
    spec = lambda w: pl.BlockSpec((w.shape[0] // (parts * cuts), w.shape[1]), lambda i, s: (s[0] * cuts + i, 0))
    r = (D + nq) // (parts * cuts)
    table = pl.BlockSpec((rows * seq, HD), lambda i, s: (i, 0))
    return pl.pallas_call(
        pre_kernel,
        grid_spec=pltpu.PrefetchScalarGridSpec(
            num_scalar_prefetch=1,
            grid=(cuts,),
            in_specs=[spec(w) for w in (w_q, w_k, w_v, w_o)] + [pl.BlockSpec((rows, seq), lambda i, s: (i, 0)), pl.BlockSpec((1, HD), lambda i, s: (0, 0))],
            out_specs=[pl.BlockSpec((1, r, D), lambda i, s: (i, 0, 0)), table, table],
        ),
        out_shape=[jax.ShapeDtypeStruct((cuts, r, D), F32)] + [jax.ShapeDtypeStruct((n * seq, HD), F32)] * 2,
        compiler_params=pltpu.CompilerParams(dimension_semantics=("arbitrary",), vmem_limit_bytes=60 << 20),
        cost_estimate=pl.CostEstimate(flops=n * seq * HD * 30, bytes_accessed=cuts * r * D * 6 + n * seq * HD * 8, transcendentals=0),
        name="pre",
    )(part, w_q, w_k, w_v, w_o, positions, freq)


def dw_kernel(n_b, unpack, sel_ref, a_ref, *refs):
    if unpack:
        f_ref, parts = refs[n_b], refs[2 * n_b + 1:2 * n_b + 5]
        refs = refs[:n_b] + refs[n_b + 1:2 * n_b + 1] + refs[2 * n_b + 5:]
        q_ref, k_ref, v_ref, o_ref = parts
        per, nq, nk = f_ref.shape[0], q_ref.shape[1], k_ref.shape[1]
        d, e = q_ref.shape[0] // per, o_ref.shape[0] // per
        for j in range(per):
            q_ref[j * d:(j + 1) * d, :] = f_ref[j, 0:d, 0:nq].astype(BF16)
            k_ref[j * d:(j + 1) * d, :] = f_ref[j, 0:d, nq:nq + nk].astype(BF16)
            v_ref[j * d:(j + 1) * d, :] = f_ref[j, 0:d, nq + nk:].astype(BF16)
            o_ref[j * e:(j + 1) * e, :] = f_ref[j, d:, :].astype(BF16)
    bs, outs, accs, (at_ref, sem) = refs[:n_b], refs[n_b:2 * n_b], refs[2 * n_b:3 * n_b], refs[3 * n_b:]
    flat = lambda ref: ref.at[0] if len(ref.shape) == 3 else ref
    a, bs = flat(a_ref), [flat(b) for b in bs]
    M, tile = at_ref.shape
    step = pl.program_id(0)

    @pl.when(step == 0)
    def _():
        for acc in accs:
            acc[...] = jnp.zeros_like(acc)

    def part(acc, b, c):
        def run():
            acc[:, c:c + 256] += dot(at_ref[...], b[:, c:c + 256])

        return (1, run)

    for c in range(0, M, 256):
        for k in range(0, tile, 256):
            at_ref[c:c + 256, k:k + 256] = a[k:k + 256, c:c + 256].T
    weave([part(acc, b, c) for acc, b in zip(accs, bs) for c in range(0, b.shape[1], 256)])

    @pl.when(step == pl.num_programs(0) - 1)
    def _():
        copies = [pltpu.make_async_copy(acc, out, sem.at[k]) for k, (acc, out) in enumerate(zip(accs, outs))]
        for c in copies:
            c.start()
        for c in copies:
            c.wait()


def dw_call(sel, a, bs, tile, gathered=None, nk=0):
    def spec(v):
        if v.ndim == 3:
            return pl.BlockSpec((1, tile, v.shape[2]), lambda i, s: (s[0], i, 0))
        return pl.BlockSpec((tile, v.shape[1]), lambda i, s: (i, 0))

    T, M = a.shape[-2:]
    shapes = [(M, b.shape[-1]) for b in bs]
    width = sum(s[1] for s in shapes)
    steps = T // tile
    more_in, more_out, more_shapes, more = [], [], [], []
    if gathered is not None:
        n, r, D = gathered.shape
        per = n // 2 // steps
        more = [gathered]
        more_in = [pl.BlockSpec((per, r, D), lambda i, s: ((1 - s[0]) * steps + i, 0, 0))]
        nq = D - 2 * nk
        more_shapes = [jax.ShapeDtypeStruct(s, BF16) for s in ((D, nq), (D, nk), (D, nk), (nq, D))]
        more_out = [pl.BlockSpec((s.shape[0] // steps, s.shape[1]), lambda i, s: (i, 0)) for s in more_shapes]
    return pl.pallas_call(
        functools.partial(dw_kernel, len(bs), gathered is not None),
        grid_spec=pltpu.PrefetchScalarGridSpec(
            num_scalar_prefetch=1,
            grid=(steps,),
            in_specs=[spec(a)] + [spec(b) for b in bs] + more_in,
            out_specs=[pl.BlockSpec(memory_space=pl.ANY)] * len(bs) + more_out,
            scratch_shapes=[pltpu.VMEM(s, F32) for s in shapes] + [pltpu.VMEM((M, tile), BF16), pltpu.SemaphoreType.DMA((len(bs),))],
        ),
        out_shape=[jax.ShapeDtypeStruct(s, F32) for s in shapes] + more_shapes,
        compiler_params=pltpu.CompilerParams(dimension_semantics=("arbitrary",), vmem_limit_bytes=60 << 20),
        cost_estimate=pl.CostEstimate(flops=2 * T * M * width, bytes_accessed=2 * T * (M + width) + 4 * M * width, transcendentals=0),
    )(sel, a, *bs, *more)


def attn_stages(seq, n_grp, r):
    half = seq // 2
    scale = HD ** -0.5
    log2e = 1.4426950408889634

    def norm_rows(src, dst):
        def piece(c):
            def run():
                xf = src[c:c + 32, :].astype(F32)
                inv = lax.rsqrt(jnp.mean(xf * xf, axis=-1, keepdims=True) + EPS)
                dst[c:c + 32, :] = (xf * inv * r.gain[0:1, :]).astype(BF16)

            return (1.5, run)

        return [piece(c) for c in range(0, seq, 32)]

    def proj(g):
        def q():
            t = dot(r.n[...], r.wq(slice(g * 2 * HD, (g + 1) * 2 * HD)))
            for h in range(2):
                r.qnew[g % 2, h] = t[:, h * HD:(h + 1) * HD].astype(BF16)

        def k():
            t = dot(r.n[...], r.wk(slice(g * HD, (g + 2) * HD)))
            for h in range(2):
                r.knew[g + h] = t[:, h * HD:(h + 1) * HD].astype(BF16)

        def v():
            t = dot(r.n[...], r.wv(slice(g * HD, (g + 2) * HD)))
            for h in range(2):
                r.vnew[g + h] = t[:, h * HD:(h + 1) * HD].astype(BF16)

        def do():
            t = r.do_dot(slice(g * 2 * HD, (g + 1) * 2 * HD))
            for h in range(2):
                r.do[g, h * half:(h + 1) * half, :] = t[:half, h * HD:(h + 1) * HD].astype(BF16)
                r.do[g, seq + h * half:seq + (h + 1) * half, :] = t[half:, h * HD:(h + 1) * HD].astype(BF16)

        return [(1, q)] + ([(1, k), (1, v)] if g % 2 == 0 else []) + [(1, do)]

    def stacked(h, c):
        return (h * half + c) if c < half else (seq + h * half + c - half)

    def rope(g):
        cs, sn = (r.tab.at[2], r.tab.at[3]) if g == n_grp - 1 else (r.tab.at[0], r.tab.at[1])

        def size(h, c):
            def run():
                raw = r.knew[g, c:c + CH, :] if h == 2 else r.qnew[g % 2, h, c:c + CH, :]
                r.raw[g, h, c:c + CH, :] = raw
                t = raw.astype(F32)
                r.inv[g, h, c:c + CH, :] = jnp.broadcast_to(lax.rsqrt(jnp.mean(t * t, axis=-1, keepdims=True) + EPS), t.shape)

            return (0.4, run)

        def turn(h, c):
            def run():
                t = r.raw[g, h, c:c + CH, :].astype(F32)
                w = (t * r.inv[g, h, c:c + CH, :]) * (r.kg if h == 2 else r.qg)[0:1, :]
                o = 2 * seq + c if h == 2 else stacked(h, c)
                x = pltpu.roll(w, HD // 2, 1)
                co, si = cs[c:c + CH, :], sn[c:c + CH, :]
                r.rot[g, o:o + CH, 0:HD] = (w * co + x * si).astype(BF16)
                r.rot[g, o:o + CH, HD:] = (x * co - w * si).astype(BF16)
                if h == 2:
                    r.v[g, c:c + CH, :] = r.vnew[g, c:c + CH, :]

            return (0.6, run)

        return [f(h, c) for f in (size, turn) for h in (2, 0, 1) for c in range(0, seq, CH)]

    def scores(g):
        b = g % 2

        def s():
            r.s[b, 0:seq, 0:half] = dot(r.rot[g, 0:seq, 0:HD], r.rot[g, 2 * seq:2 * seq + half, 0:HD], NT)
            r.s[b, seq:, :] = dot(r.rot[g, seq:2 * seq, 0:HD], r.rot[g, 2 * seq:, 0:HD], NT)

        def dp():
            r.dp[b, 0:seq, 0:half] = dot(r.do[g, :seq, :], r.v[g, :half, :], NT)
            r.dp[b, seq:, :] = dot(r.do[g, seq:, :], r.v[g], NT)

        return [(1, s), (1, dp)]

    def soft(g):
        b = g % 2
        c2 = scale * log2e

        def part(blk, c):
            return slice(blk * seq + c, blk * seq + c + CH), half if blk == 0 else seq

        def masked(blk, c, s):
            row_id = lax.broadcasted_iota(jnp.int32, (CH, half), 0) + (c % half)
            keep = row_id >= lax.broadcasted_iota(jnp.int32, (CH, half), 1)
            if blk == 0:
                return jnp.where(keep, s, -jnp.inf)
            return jnp.concatenate([s[:, :half], jnp.where(keep, s[:, half:], -jnp.inf)], axis=1)

        def wide(ref, rows, width):
            t = ref[rows, :]
            return t if width == half else jnp.concatenate([t, t], axis=1)

        def top(blk, c):
            rows, width = part(blk, c)

            def run():
                m = jnp.max(masked(blk, c, r.s[b, rows, 0:width]), axis=-1, keepdims=True)
                r.st[0, rows, :] = jnp.broadcast_to(m * c2, (CH, HD))

            return (0.4 + 0.4 * blk, run)

        def power(blk, c):
            rows, width = part(blk, c)

            def run():
                e = jnp.exp2(masked(blk, c, r.s[b, rows, 0:width] * c2) - wide(r.st.at[0], rows, width))
                r.s[b, rows, 0:width] = e
                r.st[1, rows, :] = jnp.broadcast_to(1.0 / jnp.sum(e, axis=-1, keepdims=True), (CH, HD))

            return (0.8 + 0.8 * blk, run)

        def prob(blk, c):
            rows, width = part(blk, c)

            def run():
                pr = r.s[b, rows, 0:width] * wide(r.st.at[1], rows, width)
                r.s[b, rows, 0:width] = pr
                r.p[b, rows, 0:width] = pr.astype(BF16)
                r.st[2, rows, :] = jnp.broadcast_to(jnp.sum(pr * r.dp[b, rows, 0:width], axis=-1, keepdims=True), (CH, HD))

            return (0.8 + 0.8 * blk, run)

        def last(blk, c):
            rows, width = part(blk, c)

            def run():
                d = r.dp[b, rows, 0:width] - wide(r.st.at[2], rows, width)
                r.ds[b, rows, 0:width] = (r.s[b, rows, 0:width] * d * scale).astype(BF16)

            return (0.8 + 0.8 * blk, run)

        return [f(blk, c) for f in (top, power, prob, last) for blk in range(2) for c in range(0, seq, CH)]

    def grads(g):
        b = g % 2
        col, kcol = g * 2 * HD, g * HD

        def dq():
            r.dqf[b, 0:seq, :] = dot(r.ds[b, 0:seq, 0:half], r.rot[g, 2 * seq:2 * seq + half, :])
            r.dqf[b, seq:, :] = dot(r.ds[b, seq:, :], r.rot[g, 2 * seq:, :])

        def dk():
            tb = dot(r.ds[b, seq:, :], r.rot[g, seq:2 * seq, :], TN)
            ta = dot(r.ds[b, 0:seq, 0:half], r.rot[g, 0:seq, :], TN)
            r.dkf[b, :half, :] = tb[:half] + ta
            r.dkf[b, half:, :] = tb[half:]

        def o():
            ta = dot(r.p[b, 0:seq, 0:half], r.v[g, :half, :])
            tb = dot(r.p[b, seq:, :], r.v[g])
            for h in range(2):
                r.o[0:half, col + h * HD:col + (h + 1) * HD] = ta[h * half:(h + 1) * half].astype(BF16)
                r.o[half:seq, col + h * HD:col + (h + 1) * HD] = tb[h * half:(h + 1) * half].astype(BF16)

        def dv():
            tb = dot(r.p[b, seq:, :], r.do[g, seq:, :], TN)
            ta = dot(r.p[b, 0:seq, 0:half], r.do[g, :seq, :], TN)
            r.dv[0:half, kcol:kcol + HD] = (tb[:half] + ta).astype(BF16)
            r.dv[half:seq, kcol:kcol + HD] = tb[half:].astype(BF16)

        return [(1, dq), (1, dk), (1, o), (1, dv)]

    def back(g):
        b = g % 2

        def place(h, c):
            if h == 2:
                return r.dkf, c, r.dk, g * HD, r.kg
            return r.dqf, stacked(h, c), r.dq, (2 * g + h) * HD, r.qg

        def turn(h, c):
            src, o, _, _, g_ref = place(h, c)

            def run():
                d = src[b, o:o + CH, :].astype(BF16).astype(F32)
                that = r.raw[g, h, c:c + CH, :].astype(F32) * r.inv[g, h, c:c + CH, :]
                du = d[:, :HD] * r.tab[2, c:c + CH, :] - d[:, HD:] * r.tab[3, c:c + CH, :]
                src[b, o:o + CH, 0:HD] = du
                pr = du * that
                dg_ref = r.dgk if h == 2 else r.dgq
                dg_ref[...] += jnp.sum(pr.reshape(CH // 8, 8, HD), axis=0)
                r.sb[h, c:c + CH, :] = jnp.broadcast_to(jnp.mean(pr * g_ref[0:1, :], axis=-1, keepdims=True), (CH, HD))

            return (0.6, run)

        def out(h, c):
            src, o, out_ref, col, g_ref = place(h, c)

            def run():
                inv = r.inv[g, h, c:c + CH, :]
                that = r.raw[g, h, c:c + CH, :].astype(F32) * inv
                out_ref[c:c + CH, col:col + HD] = (inv * (src[b, o:o + CH, 0:HD] * g_ref[0:1, :] - that * r.sb[h, c:c + CH, :])).astype(BF16)

            return (0.5, run)

        return [f(h, c) for f in (turn, out) for h in (0, 1, 2) for c in range(0, seq, CH)]

    return SimpleNamespace(norm=norm_rows, proj=proj, rope=rope, scores=scores, soft=soft, grads=grads, back=back)


def attn_tick(st, g, n_grp, extra=()):
    vec = st.soft((g - 3) % n_grp) + st.rope((g - 1) % n_grp)
    more = [e for e in extra]
    if more:
        vec = vec + more[0]
    vec = vec + st.back(g)
    gr = st.grads(g)
    for _, f in gr[:2]:
        f()
    weave(vec, st.scores((g - 2) % n_grp) + gr[2:] + st.proj(g), *more[1:])


def attn_scratch(seq, n_grp, nq, nk):
    return dict(
        qnew=pltpu.VMEM((2, 2, seq, HD), BF16),
        knew=pltpu.VMEM((n_grp, seq, HD), BF16),
        vnew=pltpu.VMEM((n_grp, seq, HD), BF16),
        raw=pltpu.VMEM((n_grp, 3, seq, HD), BF16),
        inv=pltpu.VMEM((n_grp, 3, seq, HD), F32),
        rot=pltpu.VMEM((n_grp, 3 * seq, 2 * HD), BF16),
        do=pltpu.VMEM((n_grp, 2 * seq, HD), BF16),
        v=pltpu.VMEM((n_grp, seq, HD), BF16),
        s=pltpu.VMEM((2, 2 * seq, seq), F32),
        dp=pltpu.VMEM((2, 2 * seq, seq), F32),
        p=pltpu.VMEM((2, 2 * seq, seq), BF16),
        ds=pltpu.VMEM((2, 2 * seq, seq), BF16),
        dkf=pltpu.VMEM((2, seq, 2 * HD), F32),
        dqf=pltpu.VMEM((2, 2 * seq, 2 * HD), F32),
        st=pltpu.VMEM((3, 2 * seq, HD), F32),
        sb=pltpu.VMEM((3, seq, HD), F32),
        tab=pltpu.VMEM((4, seq, HD), F32),
        o=pltpu.VMEM((seq, nq), BF16),
        dq=pltpu.VMEM((seq, nq), BF16),
        dk=pltpu.VMEM((seq, nk), BF16),
        dv=pltpu.VMEM((seq, nk), BF16),
    )


def tail_kernel(seq, n_grp, rows, keys, sel_ref, n_in, dy_in, cos_in, sin_in, x_in, dyx_in, gain_ref, qg_ref, kg_ref, *refs):
    own_w, oth_w, own_a = refs[:4], refs[4:8], refs[8:12]
    y_out, dx_out, dg_out, dgq_out, dgk_out = refs[12:17]
    r = SimpleNamespace(n=n_in, dy=dy_in, qg=qg_ref, kg=kg_ref, gain=gain_ref, **dict(zip(keys, refs[17:])))
    step = pl.program_id(0)
    me = sel_ref[0]
    oth = 1 - me
    D = x_in.shape[1]
    r.wq = lambda c: r.wq_all[oth, :, c]
    r.wk = lambda c: r.wk_all[oth, :, c]
    r.wv = lambda c: r.wv_all[oth, :, c]
    r.do_dot = lambda c: dot(dy_in[...], r.wo_all[oth, c, :], NT)
    st = attn_stages(seq, n_grp, r)

    def fetch(row):
        return [pltpu.make_async_copy(src.at[me, pl.ds(row * seq, seq), :], dst, r.sem.at[8 + k])
                for k, (src, dst) in enumerate(zip(own_a, (r.o_own, r.dq_own, r.dk_own, r.dv_own)))]

    @pl.when(step == 0)
    def _():
        copies = []
        for k, dst in enumerate((r.wq_all, r.wk_all, r.wv_all, r.wo_all)):
            copies.append(pltpu.make_async_copy(oth_w[k], dst.at[oth], r.sem.at[4 + k]))
            copies.append(pltpu.make_async_copy(own_w[k], dst.at[me], r.sem.at[k]))
        for c in copies:
            c.start()
        for c in copies:
            c.wait()
        for c in fetch(0):
            c.start()
        r.dg[...] = jnp.zeros_like(r.dg)

    CR, NC = 32, 256
    nn = D // NC
    lines = range(0, seq, CR)

    def wide(v):
        return jnp.concatenate([v] * (NC // HD), axis=1)

    def stat(c):
        def run():
            xf = x_in[c:c + CR, :].astype(F32)
            r.xs[0, c:c + CR, :] = jnp.broadcast_to(lax.rsqrt(jnp.mean(xf * xf, axis=-1, keepdims=True) + EPS), (CR, HD))
            r.xs[1, c:c + CR, :] = jnp.zeros((CR, HD), F32)

        return (1, run)

    def dn_dot(n):
        def run():
            cols = slice(n * NC, (n + 1) * NC)
            t = None
            for s in range(2):
                for a_ref, w_ref in ((r.dqc, r.wq_all), (r.dkc, r.wk_all), (r.dvc, r.wv_all)):
                    u = dot(a_ref[s], w_ref[s, cols, :], NT)
                    t = u if t is None else t + u
            r.dn[:, cols] = t

        return (2, run)

    def first(n, c):
        def run():
            cols = slice(n * NC, (n + 1) * NC)
            w = r.dn[c:c + CR, cols] * (x_in[c:c + CR, cols].astype(F32) * wide(r.xs[0, c:c + CR, :]))
            r.dg[:, cols] += jnp.sum(w.reshape(CR // 8, 8, NC), axis=0)
            w = w * gain_ref[0:1, cols]
            r.xs[1, c:c + CR, :] += w[:, :HD] + w[:, HD:]

        return (1, run)

    def mean(c):
        def run():
            r.xs[2, c:c + CR, :] = jnp.broadcast_to(jnp.sum(r.xs[1, c:c + CR, :], axis=-1, keepdims=True) * (1.0 / D), (CR, HD))

        return (0.2, run)

    def second(n, c):
        def run():
            cols = slice(n * NC, (n + 1) * NC)
            inv = wide(r.xs[0, c:c + CR, :])
            xh = x_in[c:c + CR, cols].astype(F32) * inv
            e = r.dn[c:c + CR, cols] * gain_ref[0:1, cols]
            dx_out[c:c + CR, cols] = (dyx_in[c:c + CR, cols].astype(F32) + inv * (e - xh * wide(r.xs[2, c:c + CR, :]))).astype(BF16)

        return (1.2, run)

    def y_dot(n):
        def run():
            cols = slice(n * NC, (n + 1) * NC)
            t = dot(r.oc[0], r.wo_all[0, :, cols]) + dot(r.oc[1], r.wo_all[1, :, cols])
            y_out[:, cols] = (x_in[:, cols].astype(F32) + t).astype(BF16)

        return (1, run)

    dn = [dn_dot(n) for n in range(nn)]
    yd = [y_dot(n) for n in range(nn)]
    f = [[first(n, c) for c in lines] for n in range(nn)]
    sec = [second(n, c) for n in range(nn) for c in lines]
    out_mat = [dn[:3], dn[3:6], dn[6:], []]
    out_vec = [[stat(c) for c in lines], f[0] + f[1] + f[2], f[3] + f[4] + f[5], f[6] + f[7] + [mean(c) for c in lines]]

    def body(attn, out):
        if attn:
            r.tab[2:4] = r.tab[0:2]
            r.tab[0] = cos_in[...]
            r.tab[1] = sin_in[...]
        for g in range(n_grp):
            if attn:
                attn_tick(st, g, n_grp, ([], out_mat[g], out_vec[g]) if out else ())
            else:
                weave(out_mat[g], out_vec[g])
        if out:
            weave(yd, sec)
        if attn:
            row = jnp.clip(step - 1, 0, rows - 1)
            for c in fetch(row):
                c.wait()
            for dst, theirs, mine in ((r.oc, r.o, r.o_own), (r.dqc, r.dq, r.dq_own), (r.dkc, r.dk, r.dk_own), (r.dvc, r.dv, r.dv_own)):
                dst[oth] = theirs[...]
                dst[me] = mine[...]

            for acc in (r.dgq, r.dgk):
                acc[...] = jnp.where(step > 0, acc[...], 0.0)

            @pl.when(step < rows)
            def _():
                for c in fetch(step):
                    c.start()

    @pl.when(step < 2)
    def _():
        body(True, False)

    @pl.when((step >= 2) & (step <= rows))
    def _():
        body(True, True)

    @pl.when(step > rows)
    def _():
        body(False, True)
        dg_out[...] = r.dg[...]
        dgq_out[...] = r.dgq[...]
        dgk_out[...] = r.dgk[...]


def tail_call(sel, n, x, dy, cosd, sind, o, dq, dk, dv, gain, qg, kg, own, oth, seq=256):
    T, D = x.shape
    nq, nk = dq.shape[2], dk.shape[2]
    n_grp = nk // HD
    rows = T // seq
    lag = lambda k, c: pl.BlockSpec((seq, c), lambda i, s: (jnp.clip(i - k, 0, rows - 1), 0))
    const = lambda *b: pl.BlockSpec(b, lambda i, s: (0,) * len(b), pipeline_mode=pl.Buffered(1))
    hbm = pl.BlockSpec(memory_space=pl.ANY)
    scratch = attn_scratch(seq, n_grp, nq, nk)
    scratch.update(
        wq_all=pltpu.VMEM((2, D, nq), BF16), wk_all=pltpu.VMEM((2, D, nk), BF16), wv_all=pltpu.VMEM((2, D, nk), BF16), wo_all=pltpu.VMEM((2, nq, D), BF16),
        dn=pltpu.VMEM((seq, D), F32), oc=pltpu.VMEM((2, seq, nq), BF16), dqc=pltpu.VMEM((2, seq, nq), BF16), dkc=pltpu.VMEM((2, seq, nk), BF16), dvc=pltpu.VMEM((2, seq, nk), BF16),
        o_own=pltpu.VMEM((seq, nq), BF16), dq_own=pltpu.VMEM((seq, nq), BF16), dk_own=pltpu.VMEM((seq, nk), BF16), dv_own=pltpu.VMEM((seq, nk), BF16),
        xs=pltpu.VMEM((3, seq, HD), F32), dg=pltpu.VMEM((8, D), F32), dgq=pltpu.VMEM((8, HD), F32), dgk=pltpu.VMEM((8, HD), F32), sem=pltpu.SemaphoreType.DMA((12,)))
    flops = 2 * T * D * (nq + 2 * nk + nq) * 3 + 12 * T * nq * seq
    return pl.pallas_call(
        functools.partial(tail_kernel, seq, n_grp, rows, tuple(scratch)),
        grid_spec=pltpu.PrefetchScalarGridSpec(
            num_scalar_prefetch=1,
            grid=(rows + 2,),
            in_specs=[lag(0, D), lag(0, D), lag(0, HD), lag(0, HD), lag(2, D), lag(2, D), const(1, D), const(1, HD), const(1, HD)] + [hbm] * 12,
            out_specs=[lag(2, D), lag(2, D), pl.BlockSpec((8, D), lambda i, s: (0, 0))] + [pl.BlockSpec((8, HD), lambda i, s: (0, 0))] * 2,
            scratch_shapes=list(scratch.values()),
        ),
        out_shape=[jax.ShapeDtypeStruct((T, D), BF16)] * 2 + [jax.ShapeDtypeStruct((8, c), F32) for c in (D, HD, HD)],
        compiler_params=pltpu.CompilerParams(dimension_semantics=("arbitrary",), vmem_limit_bytes=67043328),
        cost_estimate=pl.CostEstimate(flops=flops, bytes_accessed=T * D * 14, transcendentals=T * nq * 2),
        name="tail",
    )(sel, n, dy, cosd, sind, x, dy, gain, qg, kg, *own, *oth, o, dq, dk, dv)


def solution(mesh):
    tok_spec = P("dp", None, None)
    col_spec = P(None, "tp")
    row_spec = P("tp", None)
    n_dp = mesh.shape["dp"]

    def per_device(x_in, dy_in, positions, g_attn, q_gain, k_gain, w_q, w_k, w_v, w_o):
        n_batch, n_seq, D = x_in.shape
        T = n_batch * n_seq
        nk = w_k.shape[1]
        x, dy = x_in.reshape(T, D), dy_in.reshape(T, D)
        me = lax.axis_index("tp").astype(jnp.int32)
        own = me.reshape(1)

        part = lax.axis_index("dp").astype(jnp.int32).reshape(1)
        share, cosd, sind = pre_call(part, w_q, w_k, w_v, w_o, positions, parts=n_dp)
        gathered = lax.all_gather(share, ("tp", "dp"), tiled=True)

        gain = g_attn.astype(F32).reshape(1, D)
        qg, kg = q_gain.astype(F32).reshape(1, HD), k_gain.astype(F32).reshape(1, HD)

        n, o, dq, dk, dv, dgq, dgk = attn_call(True, own, x, dy, cosd, sind, gain, qg, kg, w_q, w_k, w_v, w_o, seq=n_seq)
        dw_q, dw_k, dw_v = dw_call(own, n, [dq, dk, dv], 512)
        dw_o, *theirs = dw_call(own, o, [dy], 1024, gathered=gathered, nk=nk)
        dw_o, dw_q, dw_k, dw_v = lax.psum((dw_o, dw_q, dw_k, dw_v), "dp")

        y, dx, dg, dgq2, dgk2 = tail_call(own, n, x, dy, cosd, sind, o, dq, dk, dv, gain, qg, kg, (w_q, w_k, w_v, w_o), theirs, seq=n_seq)
        small = lax.psum(jnp.sum(jnp.concatenate([dg, dgq + dgq2, dgk + dgk2], axis=1), axis=0), "dp")
        g_sum, q_sum, k_sum = small[:D], small[D:D + HD], small[D + HD:]
        return y.reshape(x_in.shape), dx.reshape(x_in.shape), dw_q, dw_k, dw_v, dw_o, q_sum, k_sum, g_sum

    return jax.shard_map(per_device, mesh=mesh, in_specs=(tok_spec, tok_spec, P("dp", None), P(), P(), P(), col_spec, col_spec, col_spec, row_spec), out_specs=(tok_spec, tok_spec, col_spec, col_spec, col_spec, row_spec, P(), P(), P()), check_vma=False)
```

```python
import functools
from types import SimpleNamespace
import jax
import jax.numpy as jnp
from jax import lax
from jax.experimental import pallas as pl
from jax.experimental.pallas import tpu as pltpu
from jax.sharding import PartitionSpec as P


EPS = 1e-6
THETA = 1000000.0
F32 = jnp.float32
BF16 = jnp.bfloat16
HD = 128
NT = (((1,), (1,)), ((), ()))
TN = (((0,), (0,)), ((), ()))
NN = (((1,), (0,)), ((), ()))


def dot(a, b, dims=NN):
    return lax.dot_general(a, b, dims, preferred_element_type=F32)


def weave(*lists):
    order = []
    for n, pieces in enumerate(lists):
        total = sum(c for c, _ in pieces) or 1
        at = 0
        for k, (c, f) in enumerate(pieces):
            order.append(((at + c / 2) / total, n, k, f))
            at += c
    for _, _, _, f in sorted(order, key=lambda e: e[:3]):
        f()


CH = 32


def attn_kernel(own, seq, n_grp, sel_ref, *refs):
    if own:
        (x0_ref, xn_ref, dy_ref, cos_ref, sin_ref, gain_ref, qg_ref, kg_ref, wq_ref, wk_ref, wv_ref, wo_ref,
         n_out, o_out, dq_out, dk_out, dv_out, dgq_out, dgk_out) = refs[:19]
        refs = refs[19:]
    else:
        nin_ref, dy_ref, cos_ref, sin_ref, qg_ref, kg_ref, wq_ref, wk_ref, wv_ref, wo_ref, _, _, _, _, o_out, dq_out, dk_out, dv_out = refs[:18]
        refs = refs[18:]
        n_ref = nin_ref
    (wot_ref, qnew_ref, knew_ref, vnew_ref, raw_ref, inv_ref, rot_ref, do_ref, v_ref, s_ref, dp_ref, p_ref, ds_ref, dkf_ref, dqf_ref, st_ref,
     tab_ref, o_ref, dq_ref, dk_ref, dv_ref) = refs[:21]
    if own:
        n_ref, nn_ref, dgq_ref, dgk_ref = refs[21:]
    half = seq // 2
    scale = HD ** -0.5
    log2e = 1.4426950408889634
    step = pl.program_id(0)

    def norm_rows(src, dst):
        def piece(c):
            def run():
                xf = src[c:c + 32, :].astype(F32)
                inv = lax.rsqrt(jnp.mean(xf * xf, axis=-1, keepdims=True) + EPS)
                dst[c:c + 32, :] = (xf * inv * gain_ref[0:1, :]).astype(BF16)

            return (1.5, run)

        return [piece(c) for c in range(0, seq, 32)]

    def proj(g):
        def q():
            t = dot(n_ref[...], wq_ref[:, g * 2 * HD:(g + 1) * 2 * HD])
            for h in range(2):
                qnew_ref[g % 2, h] = t[:, h * HD:(h + 1) * HD].astype(BF16)

        def k():
            t = dot(n_ref[...], wk_ref[:, g * HD:(g + 2) * HD])
            for h in range(2):
                knew_ref[g + h] = t[:, h * HD:(h + 1) * HD].astype(BF16)

        def v():
            t = dot(n_ref[...], wv_ref[:, g * HD:(g + 2) * HD])
            for h in range(2):
                vnew_ref[g + h] = t[:, h * HD:(h + 1) * HD].astype(BF16)

        def do():
            t = dot(dy_ref[...], wot_ref[:, g * 2 * HD:(g + 1) * 2 * HD])
            for h in range(2):
                do_ref[g, h * half:(h + 1) * half, :] = t[:half, h * HD:(h + 1) * HD].astype(BF16)
                do_ref[g, seq + h * half:seq + (h + 1) * half, :] = t[half:, h * HD:(h + 1) * HD].astype(BF16)

        return [(1, q)] + ([(1, k), (1, v)] if g % 2 == 0 else []) + [(1, do)]

    def stacked(h, c):
        return (h * half + c) if c < half else (seq + h * half + c - half)

    def rope(g):
        cs, sn = (tab_ref.at[2], tab_ref.at[3]) if g == n_grp - 1 else (tab_ref.at[0], tab_ref.at[1])

        def size(h, c):
            def run():
                raw = knew_ref[g, c:c + CH, :] if h == 2 else qnew_ref[g % 2, h, c:c + CH, :]
                raw_ref[g, h, c:c + CH, :] = raw
                t = raw.astype(F32)
                inv_ref[g, h, c:c + CH, :] = jnp.broadcast_to(lax.rsqrt(jnp.mean(t * t, axis=-1, keepdims=True) + EPS), t.shape)

            return (0.4, run)

        def turn(h, c):
            def run():
                t = raw_ref[g, h, c:c + CH, :].astype(F32)
                w = (t * inv_ref[g, h, c:c + CH, :]) * (kg_ref if h == 2 else qg_ref)[0:1, :]
                o = 2 * seq + c if h == 2 else stacked(h, c)
                x = pltpu.roll(w, HD // 2, 1)
                co, si = cs[c:c + CH, :], sn[c:c + CH, :]
                rot_ref[g, o:o + CH, 0:HD] = (w * co + x * si).astype(BF16)
                rot_ref[g, o:o + CH, HD:] = (x * co - w * si).astype(BF16)
                if h == 2:
                    v_ref[g, c:c + CH, :] = vnew_ref[g, c:c + CH, :]

            return (0.6, run)

        return [f(h, c) for f in (size, turn) for h in (2, 0, 1) for c in range(0, seq, CH)]

    def scores(g):
        b = g % 2

        def s():
            s_ref[b, 0:seq, 0:half] = dot(rot_ref[g, 0:seq, 0:HD], rot_ref[g, 2 * seq:2 * seq + half, 0:HD], NT)
            s_ref[b, seq:, :] = dot(rot_ref[g, seq:2 * seq, 0:HD], rot_ref[g, 2 * seq:, 0:HD], NT)

        def dp():
            dp_ref[b, 0:seq, 0:half] = dot(do_ref[g, :seq, :], v_ref[g, :half, :], NT)
            dp_ref[b, seq:, :] = dot(do_ref[g, seq:, :], v_ref[g], NT)

        return [(1, s), (1, dp)]

    def soft(g):
        b = g % 2
        c2 = scale * log2e

        def part(blk, c):
            return slice(blk * seq + c, blk * seq + c + CH), half if blk == 0 else seq

        def masked(blk, c, s):
            row_id = lax.broadcasted_iota(jnp.int32, (CH, half), 0) + (c % half)
            keep = row_id >= lax.broadcasted_iota(jnp.int32, (CH, half), 1)
            if blk == 0:
                return jnp.where(keep, s, -jnp.inf)
            return jnp.concatenate([s[:, :half], jnp.where(keep, s[:, half:], -jnp.inf)], axis=1)

        def wide(ref, rows, width):
            t = ref[rows, :]
            return t if width == half else jnp.concatenate([t, t], axis=1)

        def top(blk, c):
            rows, width = part(blk, c)

            def run():
                m = jnp.max(masked(blk, c, s_ref[b, rows, 0:width]), axis=-1, keepdims=True)
                st_ref[0, rows, :] = jnp.broadcast_to(m * c2, (CH, HD))

            return (0.4 + 0.4 * blk, run)

        def power(blk, c):
            rows, width = part(blk, c)

            def run():
                e = jnp.exp2(masked(blk, c, s_ref[b, rows, 0:width] * c2) - wide(st_ref.at[0], rows, width))
                s_ref[b, rows, 0:width] = e
                st_ref[1, rows, :] = jnp.broadcast_to(1.0 / jnp.sum(e, axis=-1, keepdims=True), (CH, HD))

            return (0.8 + 0.8 * blk, run)

        def prob(blk, c):
            rows, width = part(blk, c)

            def run():
                pr = s_ref[b, rows, 0:width] * wide(st_ref.at[1], rows, width)
                s_ref[b, rows, 0:width] = pr
                p_ref[b, rows, 0:width] = pr.astype(BF16)
                st_ref[2, rows, :] = jnp.broadcast_to(jnp.sum(pr * dp_ref[b, rows, 0:width], axis=-1, keepdims=True), (CH, HD))

            return (0.8 + 0.8 * blk, run)

        def last(blk, c):
            rows, width = part(blk, c)

            def run():
                d = dp_ref[b, rows, 0:width] - wide(st_ref.at[2], rows, width)
                ds_ref[b, rows, 0:width] = (s_ref[b, rows, 0:width] * d * scale).astype(BF16)

            return (0.8 + 0.8 * blk, run)

        return [f(blk, c) for f in (top, power, prob, last) for blk in range(2) for c in range(0, seq, CH)]

    def grads(g):
        b = g % 2
        col, kcol = g * 2 * HD, g * HD

        def dq():
            dqf_ref[b, 0:seq, :] = dot(ds_ref[b, 0:seq, 0:half], rot_ref[g, 2 * seq:2 * seq + half, :])
            dqf_ref[b, seq:, :] = dot(ds_ref[b, seq:, :], rot_ref[g, 2 * seq:, :])

        def dk():
            tb = dot(ds_ref[b, seq:, :], rot_ref[g, seq:2 * seq, :], TN)
            ta = dot(ds_ref[b, 0:seq, 0:half], rot_ref[g, 0:seq, :], TN)
            dkf_ref[b, :half, :] = tb[:half] + ta
            dkf_ref[b, half:, :] = tb[half:]

        def o():
            ta = dot(p_ref[b, 0:seq, 0:half], v_ref[g, :half, :])
            tb = dot(p_ref[b, seq:, :], v_ref[g])
            for h in range(2):
                o_ref[0:half, col + h * HD:col + (h + 1) * HD] = ta[h * half:(h + 1) * half].astype(BF16)
                o_ref[half:seq, col + h * HD:col + (h + 1) * HD] = tb[h * half:(h + 1) * half].astype(BF16)

        def dv():
            tb = dot(p_ref[b, seq:, :], do_ref[g, seq:, :], TN)
            ta = dot(p_ref[b, 0:seq, 0:half], do_ref[g, :seq, :], TN)
            dv_ref[0:half, kcol:kcol + HD] = (tb[:half] + ta).astype(BF16)
            dv_ref[half:seq, kcol:kcol + HD] = tb[half:].astype(BF16)

        return [(1, dq), (1, dk), (1, o), (1, dv)]

    def back(g):
        b = g % 2

        def place(h, c):
            if h == 2:
                return dkf_ref, c, dk_ref, g * HD, kg_ref
            return dqf_ref, stacked(h, c), dq_ref, (2 * g + h) * HD, qg_ref

        def turn(h, c):
            src, o, _, _, g_ref = place(h, c)

            def run():
                d = src[b, o:o + CH, :].astype(BF16).astype(F32)
                that = raw_ref[g, h, c:c + CH, :].astype(F32) * inv_ref[g, h, c:c + CH, :]
                du = d[:, :HD] * tab_ref[2, c:c + CH, :] - d[:, HD:] * tab_ref[3, c:c + CH, :]
                src[b, o:o + CH, 0:HD] = du
                pr = du * that
                if own:
                    dg_ref = dgk_ref if h == 2 else dgq_ref
                    dg_ref[...] += jnp.sum(pr.reshape(CH // 8, 8, HD), axis=0)
                st_ref[3 + h, c:c + CH, :] = jnp.broadcast_to(jnp.mean(pr * g_ref[0:1, :], axis=-1, keepdims=True), (CH, HD))

            return (0.6, run)

        def out(h, c):
            src, o, out_ref, col, g_ref = place(h, c)

            def run():
                inv = inv_ref[g, h, c:c + CH, :]
                that = raw_ref[g, h, c:c + CH, :].astype(F32) * inv
                out_ref[c:c + CH, col:col + HD] = (inv * (src[b, o:o + CH, 0:HD] * g_ref[0:1, :] - that * st_ref[3 + h, c:c + CH, :])).astype(BF16)

            return (0.5, run)

        return [f(h, c) for f in (turn, out) for h in (0, 1, 2) for c in range(0, seq, CH)]

    @pl.when(step == 0)
    def _():
        @pl.loop(0, wo_ref.shape[0] // 256)
        def _(j):
            c = pl.ds(pl.multiple_of(j * 256, 256), 256)
            for d in range(0, wo_ref.shape[1], 256):
                wot_ref[d:d + 256, c] = wo_ref[c, d:d + 256].T

        if own:
            weave(norm_rows(x0_ref, n_ref))

    tab_ref[2:4] = tab_ref[0:2]
    tab_ref[0] = cos_ref[...]
    tab_ref[1] = sin_ref[...]
    if own:
        norms = norm_rows(xn_ref, nn_ref)
    for g in range(n_grp):
        vec = soft((g - 3) % n_grp)
        sc = scores((g - 2) % n_grp)
        vec = vec + rope((g - 1) % n_grp)
        if own:
            vec += norms[g * len(norms) // n_grp:(g + 1) * len(norms) // n_grp]
        vec += back(g)
        gr = grads(g)
        for _, f in gr[:2]:
            f()
        weave(vec, sc + gr[2:] + proj(g))

    for dst, src in ((o_out, o_ref), (dq_out, dq_ref), (dk_out, dk_ref), (dv_out, dv_ref)):
        dst[0] = src[...]
    if own:
        n_out[...] = n_ref[...]
        n_ref[...] = nn_ref[...]
        keep = step > 0
        for dst, acc in ((dgq_out, dgq_ref), (dgk_out, dgk_ref)):
            acc[...] = jnp.where(keep, acc[...], 0.0)
            dst[...] = acc[...]


def attn_call(own, sel, x, dy, cosd, sind, gain, qg, kg, wq, wk, wv, wo, prev=None, seq=256):
    T, D = x.shape
    nq, nk = wq.shape[1], wk.shape[1]
    n_grp = nk // HD
    rows = T // seq
    const = lambda *b: pl.BlockSpec(b, lambda i, s: (0,) * len(b), pipeline_mode=pl.Buffered(1))
    now = lambda c: pl.BlockSpec((seq, c), lambda i, s: (jnp.minimum(i, rows - 1), 0))
    nxt = lambda c: pl.BlockSpec((seq, c), lambda i, s: (jnp.minimum(i + 1, rows - 1), 0))
    out3 = lambda c: pl.BlockSpec((1, seq, c), lambda i, s: (s[0], jnp.maximum(i - 1, 0), 0))
    mid = [now(D), now(HD), now(HD)]
    tail = [const(1, HD), const(1, HD), const(D, nq), const(D, nk), const(D, nk), const(nq, D)]
    shapes = [jax.ShapeDtypeStruct((2, T, c), BF16) for c in (nq, nq, nk, nk)]
    specs = [out3(nq), out3(nq), out3(nk), out3(nk)]
    aliases = {}
    if own:
        in_specs = [const(seq, D), nxt(D)] + mid + [const(1, D)] + tail
        args = [x, x, dy, cosd, sind, gain, qg, kg, wq, wk, wv, wo]
        shapes = [jax.ShapeDtypeStruct((T, D), BF16)] + shapes + [jax.ShapeDtypeStruct((8, HD), F32)] * 2
        specs = [now(D)] + specs + [pl.BlockSpec((8, HD), lambda i, s: (0, 0))] * 2
    else:
        in_specs = [now(D)] + mid + tail + [pl.BlockSpec(memory_space=pl.ANY)] * 4
        args = [x, dy, cosd, sind, qg, kg, wq, wk, wv, wo]
        aliases = {1 + len(args) + i: i for i in range(4)}
        args += list(prev)
    flops = 2 * T * D * (nq + 2 * nk + nq) + 12 * T * nq * seq
    return pl.pallas_call(
        functools.partial(attn_kernel, own, seq, n_grp),
        grid_spec=pltpu.PrefetchScalarGridSpec(
            num_scalar_prefetch=1,
            grid=(rows + 1,),
            in_specs=in_specs,
            out_specs=specs,
            scratch_shapes=[
                pltpu.VMEM((D, nq), BF16),
                pltpu.VMEM((2, 2, seq, HD), BF16),
                pltpu.VMEM((n_grp, seq, HD), BF16),
                pltpu.VMEM((n_grp, seq, HD), BF16),
                pltpu.VMEM((n_grp, 3, seq, HD), BF16),
                pltpu.VMEM((n_grp, 3, seq, HD), F32),
                pltpu.VMEM((n_grp, 3 * seq, 2 * HD), BF16),
                pltpu.VMEM((n_grp, 2 * seq, HD), BF16),
                pltpu.VMEM((n_grp, seq, HD), BF16),
                pltpu.VMEM((2, 2 * seq, seq), F32),
                pltpu.VMEM((2, 2 * seq, seq), F32),
                pltpu.VMEM((2, 2 * seq, seq), BF16),
                pltpu.VMEM((2, 2 * seq, seq), BF16),
                pltpu.VMEM((2, seq, 2 * HD), F32),
                pltpu.VMEM((2, 2 * seq, 2 * HD), F32),
                pltpu.VMEM((6, 2 * seq, HD), F32),
                pltpu.VMEM((4, seq, HD), F32),
            ] + [pltpu.VMEM((seq, c), BF16) for c in (nq, nq, nk, nk)]
            + ([pltpu.VMEM((seq, D), BF16)] * 2 + [pltpu.VMEM((8, HD), F32)] * 2 if own else []),
        ),
        out_shape=shapes,
        input_output_aliases=aliases,
        compiler_params=pltpu.CompilerParams(dimension_semantics=("arbitrary",), vmem_limit_bytes=56 << 20),
        cost_estimate=pl.CostEstimate(flops=flops, bytes_accessed=T * D * 6 + T * (2 * nq + 2 * nk) * 2, transcendentals=T * nq * 2),
        name="attn_own" if own else "attn_other",
    )(sel, *args)


def pre_kernel(sel_ref, q_ref, k_ref, v_ref, o_ref, pos_ref, freq_ref, out_ref, cos_ref, sin_ref):
    d, nq, nk = q_ref.shape[0], q_ref.shape[1], k_ref.shape[1]
    out_ref[0, 0:d, 0:nq] = q_ref[...].astype(F32)
    out_ref[0, 0:d, nq:nq + nk] = k_ref[...].astype(F32)
    out_ref[0, 0:d, nq + nk:] = v_ref[...].astype(F32)
    out_ref[0, d:, :] = o_ref[...].astype(F32)
    n, seq = pos_ref.shape
    lane = lax.broadcasted_iota(jnp.int32, (HD, HD), 1)
    for r in range(n):
        for h in range(seq // HD):
            p = pos_ref[r:r + 1, h * HD:(h + 1) * HD].astype(F32)
            a = jnp.broadcast_to(p, (HD, HD)).T * freq_ref[0:1, :]
            k = jnp.round(a * 0.6366197723675814)
            x = ((a - k * 1.5703125) - k * 4.837512969970703125e-4) - k * 7.549789948768648e-8
            z = x * x
            s = ((-1.9515295891e-4 * z + 8.3321608736e-3) * z - 1.6666654611e-1) * z * x + x
            c = ((2.443315711809948e-5 * z - 1.388731625493765e-3) * z + 4.166664568298827e-2) * z * z - 0.5 * z + 1.0
            q = k.astype(jnp.int32)
            odd = (q & 1) == 1
            co, si = jnp.where(odd, s, c), jnp.where(odd, c, s)
            rows = slice((r * (seq // HD) + h) * HD, (r * (seq // HD) + h + 1) * HD)
            cos_ref[rows, :] = jnp.where(((q + 1) & 2) == 0, co, -co)
            sin_ref[rows, :] = jnp.where(((q & 2) == 0) == (lane >= HD // 2), si, -si)


def pre_call(part, w_q, w_k, w_v, w_o, positions, parts=2, cuts=4):
    D, nq = w_q.shape
    n, seq = positions.shape
    rows = n // cuts
    freq = THETA ** (-jnp.arange(0, HD, 2, dtype=F32) / HD)
    freq = jnp.concatenate([freq, freq]).reshape(1, HD)
    spec = lambda w: pl.BlockSpec((w.shape[0] // (parts * cuts), w.shape[1]), lambda i, s: (s[0] * cuts + i, 0))
    r = (D + nq) // (parts * cuts)
    table = pl.BlockSpec((rows * seq, HD), lambda i, s: (i, 0))
    return pl.pallas_call(
        pre_kernel,
        grid_spec=pltpu.PrefetchScalarGridSpec(
            num_scalar_prefetch=1,
            grid=(cuts,),
            in_specs=[spec(w) for w in (w_q, w_k, w_v, w_o)] + [pl.BlockSpec((rows, seq), lambda i, s: (i, 0)), pl.BlockSpec((1, HD), lambda i, s: (0, 0))],
            out_specs=[pl.BlockSpec((1, r, D), lambda i, s: (i, 0, 0)), table, table],
        ),
        out_shape=[jax.ShapeDtypeStruct((cuts, r, D), F32)] + [jax.ShapeDtypeStruct((n * seq, HD), F32)] * 2,
        compiler_params=pltpu.CompilerParams(dimension_semantics=("arbitrary",), vmem_limit_bytes=60 << 20),
        cost_estimate=pl.CostEstimate(flops=n * seq * HD * 30, bytes_accessed=cuts * r * D * 6 + n * seq * HD * 8, transcendentals=0),
        name="pre",
    )(part, w_q, w_k, w_v, w_o, positions, freq)


def dw_kernel(n_b, unpack, sel_ref, a_ref, *refs):
    if unpack:
        f_ref, parts = refs[n_b], refs[2 * n_b + 1:2 * n_b + 5]
        refs = refs[:n_b] + refs[n_b + 1:2 * n_b + 1] + refs[2 * n_b + 5:]
        q_ref, k_ref, v_ref, o_ref = parts
        per, nq, nk = f_ref.shape[0], q_ref.shape[1], k_ref.shape[1]
        d, e = q_ref.shape[0] // per, o_ref.shape[0] // per
        for j in range(per):
            q_ref[j * d:(j + 1) * d, :] = f_ref[j, 0:d, 0:nq].astype(BF16)
            k_ref[j * d:(j + 1) * d, :] = f_ref[j, 0:d, nq:nq + nk].astype(BF16)
            v_ref[j * d:(j + 1) * d, :] = f_ref[j, 0:d, nq + nk:].astype(BF16)
            o_ref[j * e:(j + 1) * e, :] = f_ref[j, d:, :].astype(BF16)
    bs, outs, accs, (at_ref, sem) = refs[:n_b], refs[n_b:2 * n_b], refs[2 * n_b:3 * n_b], refs[3 * n_b:]
    flat = lambda ref: ref.at[0] if len(ref.shape) == 3 else ref
    a, bs = flat(a_ref), [flat(b) for b in bs]
    M, tile = at_ref.shape
    step = pl.program_id(0)

    @pl.when(step == 0)
    def _():
        for acc in accs:
            @pl.loop(0, M // 64)
            def _(j):
                acc[pl.ds(pl.multiple_of(j * 64, 64), 64), :] = jnp.zeros((64, acc.shape[1]), F32)

    def part(acc, b, c):
        def run():
            acc[:, c:c + 256] += dot(at_ref[...], b[:, c:c + 256])

        return (1, run)

    for c in range(0, M, 256):
        for k in range(0, tile, 256):
            at_ref[c:c + 256, k:k + 256] = a[k:k + 256, c:c + 256].T
    weave([part(acc, b, c) for acc, b in zip(accs, bs) for c in range(0, b.shape[1], 256)])

    @pl.when(step == pl.num_programs(0) - 1)
    def _():
        copies = [pltpu.make_async_copy(acc, out, sem.at[k]) for k, (acc, out) in enumerate(zip(accs, outs))]
        for c in copies:
            c.start()
        for c in copies:
            c.wait()


def dw_call(sel, a, bs, tile, gathered=None, nk=0):
    def spec(v):
        if v.ndim == 3:
            return pl.BlockSpec((1, tile, v.shape[2]), lambda i, s: (s[0], i, 0))
        return pl.BlockSpec((tile, v.shape[1]), lambda i, s: (i, 0))

    T, M = a.shape[-2:]
    shapes = [(M, b.shape[-1]) for b in bs]
    width = sum(s[1] for s in shapes)
    steps = T // tile
    more_in, more_out, more_shapes, more = [], [], [], []
    if gathered is not None:
        n, r, D = gathered.shape
        per = n // 2 // steps
        more = [gathered]
        more_in = [pl.BlockSpec((per, r, D), lambda i, s: ((1 - s[0]) * steps + i, 0, 0))]
        nq = D - 2 * nk
        more_shapes = [jax.ShapeDtypeStruct(s, BF16) for s in ((D, nq), (D, nk), (D, nk), (nq, D))]
        more_out = [pl.BlockSpec((s.shape[0] // steps, s.shape[1]), lambda i, s: (i, 0)) for s in more_shapes]
    return pl.pallas_call(
        functools.partial(dw_kernel, len(bs), gathered is not None),
        grid_spec=pltpu.PrefetchScalarGridSpec(
            num_scalar_prefetch=1,
            grid=(steps,),
            in_specs=[spec(a)] + [spec(b) for b in bs] + more_in,
            out_specs=[pl.BlockSpec(memory_space=pl.ANY)] * len(bs) + more_out,
            scratch_shapes=[pltpu.VMEM(s, F32) for s in shapes] + [pltpu.VMEM((M, tile), BF16), pltpu.SemaphoreType.DMA((len(bs),))],
        ),
        out_shape=[jax.ShapeDtypeStruct(s, F32) for s in shapes] + more_shapes,
        compiler_params=pltpu.CompilerParams(dimension_semantics=("arbitrary",), vmem_limit_bytes=60 << 20),
        cost_estimate=pl.CostEstimate(flops=2 * T * M * width, bytes_accessed=2 * T * (M + width) + 4 * M * width, transcendentals=0),
    )(sel, a, *bs, *more)


def attn_stages(seq, n_grp, r):
    half = seq // 2
    scale = HD ** -0.5
    log2e = 1.4426950408889634

    def norm_rows(src, dst):
        def piece(c):
            def run():
                xf = src[c:c + 32, :].astype(F32)
                inv = lax.rsqrt(jnp.mean(xf * xf, axis=-1, keepdims=True) + EPS)
                dst[c:c + 32, :] = (xf * inv * r.gain[0:1, :]).astype(BF16)

            return (1.5, run)

        return [piece(c) for c in range(0, seq, 32)]

    def proj(g):
        def q():
            t = dot(r.n[...], r.wq(slice(g * 2 * HD, (g + 1) * 2 * HD)))
            for h in range(2):
                r.qnew[g % 2, h] = t[:, h * HD:(h + 1) * HD].astype(BF16)

        def k():
            t = dot(r.n[...], r.wk(slice(g * HD, (g + 2) * HD)))
            for h in range(2):
                r.knew[g + h] = t[:, h * HD:(h + 1) * HD].astype(BF16)

        def v():
            t = dot(r.n[...], r.wv(slice(g * HD, (g + 2) * HD)))
            for h in range(2):
                r.vnew[g + h] = t[:, h * HD:(h + 1) * HD].astype(BF16)

        def do():
            t = r.do_dot(slice(g * 2 * HD, (g + 1) * 2 * HD))
            for h in range(2):
                r.do[g, h * half:(h + 1) * half, :] = t[:half, h * HD:(h + 1) * HD].astype(BF16)
                r.do[g, seq + h * half:seq + (h + 1) * half, :] = t[half:, h * HD:(h + 1) * HD].astype(BF16)

        return [(1, q)] + ([(1, k), (1, v)] if g % 2 == 0 else []) + [(1, do)]

    def stacked(h, c):
        return (h * half + c) if c < half else (seq + h * half + c - half)

    def rope(g):
        cs, sn = (r.tab.at[2], r.tab.at[3]) if g == n_grp - 1 else (r.tab.at[0], r.tab.at[1])

        def size(h, c):
            def run():
                raw = r.knew[g, c:c + CH, :] if h == 2 else r.qnew[g % 2, h, c:c + CH, :]
                r.raw[g, h, c:c + CH, :] = raw
                t = raw.astype(F32)
                r.inv[g, h, c:c + CH, :] = jnp.broadcast_to(lax.rsqrt(jnp.mean(t * t, axis=-1, keepdims=True) + EPS), t.shape)

            return (0.4, run)

        def turn(h, c):
            def run():
                t = r.raw[g, h, c:c + CH, :].astype(F32)
                w = (t * r.inv[g, h, c:c + CH, :]) * (r.kg if h == 2 else r.qg)[0:1, :]
                o = 2 * seq + c if h == 2 else stacked(h, c)
                x = pltpu.roll(w, HD // 2, 1)
                co, si = cs[c:c + CH, :], sn[c:c + CH, :]
                r.rot[g, o:o + CH, 0:HD] = (w * co + x * si).astype(BF16)
                r.rot[g, o:o + CH, HD:] = (x * co - w * si).astype(BF16)
                if h == 2:
                    r.v[g, c:c + CH, :] = r.vnew[g, c:c + CH, :]

            return (0.6, run)

        return [f(h, c) for f in (size, turn) for h in (2, 0, 1) for c in range(0, seq, CH)]

    def scores(g):
        b = g % 2

        def s():
            r.s[b, 0:seq, 0:half] = dot(r.rot[g, 0:seq, 0:HD], r.rot[g, 2 * seq:2 * seq + half, 0:HD], NT)
            r.s[b, seq:, :] = dot(r.rot[g, seq:2 * seq, 0:HD], r.rot[g, 2 * seq:, 0:HD], NT)

        def dp():
            r.dp[b, 0:seq, 0:half] = dot(r.do[g, :seq, :], r.v[g, :half, :], NT)
            r.dp[b, seq:, :] = dot(r.do[g, seq:, :], r.v[g], NT)

        return [(1, s), (1, dp)]

    def soft(g):
        b = g % 2
        c2 = scale * log2e

        def part(blk, c):
            return slice(blk * seq + c, blk * seq + c + CH), half if blk == 0 else seq

        def masked(blk, c, s):
            row_id = lax.broadcasted_iota(jnp.int32, (CH, half), 0) + (c % half)
            keep = row_id >= lax.broadcasted_iota(jnp.int32, (CH, half), 1)
            if blk == 0:
                return jnp.where(keep, s, -jnp.inf)
            return jnp.concatenate([s[:, :half], jnp.where(keep, s[:, half:], -jnp.inf)], axis=1)

        def wide(ref, rows, width):
            t = ref[rows, :]
            return t if width == half else jnp.concatenate([t, t], axis=1)

        def top(blk, c):
            rows, width = part(blk, c)

            def run():
                m = jnp.max(masked(blk, c, r.s[b, rows, 0:width]), axis=-1, keepdims=True)
                r.st[0, rows, :] = jnp.broadcast_to(m * c2, (CH, HD))

            return (0.4 + 0.4 * blk, run)

        def power(blk, c):
            rows, width = part(blk, c)

            def run():
                e = jnp.exp2(masked(blk, c, r.s[b, rows, 0:width] * c2) - wide(r.st.at[0], rows, width))
                r.s[b, rows, 0:width] = e
                r.st[1, rows, :] = jnp.broadcast_to(1.0 / jnp.sum(e, axis=-1, keepdims=True), (CH, HD))

            return (0.8 + 0.8 * blk, run)

        def prob(blk, c):
            rows, width = part(blk, c)

            def run():
                pr = r.s[b, rows, 0:width] * wide(r.st.at[1], rows, width)
                r.s[b, rows, 0:width] = pr
                r.p[b, rows, 0:width] = pr.astype(BF16)
                r.st[2, rows, :] = jnp.broadcast_to(jnp.sum(pr * r.dp[b, rows, 0:width], axis=-1, keepdims=True), (CH, HD))

            return (0.8 + 0.8 * blk, run)

        def last(blk, c):
            rows, width = part(blk, c)

            def run():
                d = r.dp[b, rows, 0:width] - wide(r.st.at[2], rows, width)
                r.ds[b, rows, 0:width] = (r.s[b, rows, 0:width] * d * scale).astype(BF16)

            return (0.8 + 0.8 * blk, run)

        return [f(blk, c) for f in (top, power, prob, last) for blk in range(2) for c in range(0, seq, CH)]

    def grads(g):
        b = g % 2
        col, kcol = g * 2 * HD, g * HD

        def dq():
            r.dqf[b, 0:seq, :] = dot(r.ds[b, 0:seq, 0:half], r.rot[g, 2 * seq:2 * seq + half, :])
            r.dqf[b, seq:, :] = dot(r.ds[b, seq:, :], r.rot[g, 2 * seq:, :])

        def dk():
            tb = dot(r.ds[b, seq:, :], r.rot[g, seq:2 * seq, :], TN)
            ta = dot(r.ds[b, 0:seq, 0:half], r.rot[g, 0:seq, :], TN)
            r.dkf[b, :half, :] = tb[:half] + ta
            r.dkf[b, half:, :] = tb[half:]

        def o():
            ta = dot(r.p[b, 0:seq, 0:half], r.v[g, :half, :])
            tb = dot(r.p[b, seq:, :], r.v[g])
            for h in range(2):
                r.o[0:half, col + h * HD:col + (h + 1) * HD] = ta[h * half:(h + 1) * half].astype(BF16)
                r.o[half:seq, col + h * HD:col + (h + 1) * HD] = tb[h * half:(h + 1) * half].astype(BF16)

        def dv():
            tb = dot(r.p[b, seq:, :], r.do[g, seq:, :], TN)
            ta = dot(r.p[b, 0:seq, 0:half], r.do[g, :seq, :], TN)
            r.dv[0:half, kcol:kcol + HD] = (tb[:half] + ta).astype(BF16)
            r.dv[half:seq, kcol:kcol + HD] = tb[half:].astype(BF16)

        return [(1, dq), (1, dk), (1, o), (1, dv)]

    def back(g):
        b = g % 2

        def place(h, c):
            if h == 2:
                return r.dkf, c, r.dk, g * HD, r.kg
            return r.dqf, stacked(h, c), r.dq, (2 * g + h) * HD, r.qg

        def turn(h, c):
            src, o, _, _, g_ref = place(h, c)

            def run():
                d = src[b, o:o + CH, :].astype(BF16).astype(F32)
                that = r.raw[g, h, c:c + CH, :].astype(F32) * r.inv[g, h, c:c + CH, :]
                du = d[:, :HD] * r.tab[2, c:c + CH, :] - d[:, HD:] * r.tab[3, c:c + CH, :]
                src[b, o:o + CH, 0:HD] = du
                pr = du * that
                dg_ref = r.dgk if h == 2 else r.dgq
                dg_ref[...] += jnp.sum(pr.reshape(CH // 8, 8, HD), axis=0)
                r.sb[h, c:c + CH, :] = jnp.broadcast_to(jnp.mean(pr * g_ref[0:1, :], axis=-1, keepdims=True), (CH, HD))

            return (0.6, run)

        def out(h, c):
            src, o, out_ref, col, g_ref = place(h, c)

            def run():
                inv = r.inv[g, h, c:c + CH, :]
                that = r.raw[g, h, c:c + CH, :].astype(F32) * inv
                out_ref[c:c + CH, col:col + HD] = (inv * (src[b, o:o + CH, 0:HD] * g_ref[0:1, :] - that * r.sb[h, c:c + CH, :])).astype(BF16)

            return (0.5, run)

        return [f(h, c) for f in (turn, out) for h in (0, 1, 2) for c in range(0, seq, CH)]

    return SimpleNamespace(norm=norm_rows, proj=proj, rope=rope, scores=scores, soft=soft, grads=grads, back=back)


def attn_tick(st, g, n_grp):
    vec = st.soft((g - 3) % n_grp) + st.rope((g - 1) % n_grp) + st.back(g)
    gr = st.grads(g)
    for _, f in gr[:2]:
        f()
    weave(vec, st.scores((g - 2) % n_grp) + gr[2:] + st.proj(g))


def attn_scratch(seq, n_grp):
    return dict(
        qnew=pltpu.VMEM((2, 2, seq, HD), BF16),
        knew=pltpu.VMEM((n_grp, seq, HD), BF16),
        vnew=pltpu.VMEM((n_grp, seq, HD), BF16),
        raw=pltpu.VMEM((n_grp, 3, seq, HD), BF16),
        inv=pltpu.VMEM((n_grp, 3, seq, HD), F32),
        rot=pltpu.VMEM((n_grp, 3 * seq, 2 * HD), BF16),
        do=pltpu.VMEM((n_grp, 2 * seq, HD), BF16),
        v=pltpu.VMEM((n_grp, seq, HD), BF16),
        s=pltpu.VMEM((2, 2 * seq, seq), F32),
        dp=pltpu.VMEM((2, 2 * seq, seq), F32),
        p=pltpu.VMEM((2, 2 * seq, seq), BF16),
        ds=pltpu.VMEM((2, 2 * seq, seq), BF16),
        dkf=pltpu.VMEM((2, seq, 2 * HD), F32),
        dqf=pltpu.VMEM((2, 2 * seq, 2 * HD), F32),
        st=pltpu.VMEM((3, 2 * seq, HD), F32),
        sb=pltpu.VMEM((3, seq, HD), F32),
        tab=pltpu.VMEM((4, seq, HD), F32),
    )


def tail_kernel(seq, n_grp, rows, keys, sel_ref, n_in, dy_in, cos_in, sin_in, x_in, dyx_in, gain_ref, qg_ref, kg_ref, *refs):
    own_w, oth_w, own_a = refs[:4], refs[4:8], refs[8:12]
    y_out, dx_out, dg_out, dgq_out, dgk_out = refs[12:17]
    r = SimpleNamespace(n=n_in, dy=dy_in, qg=qg_ref, kg=kg_ref, gain=gain_ref, **dict(zip(keys, refs[17:])))
    step = pl.program_id(0)
    me = sel_ref[0]
    oth = 1 - me
    D = x_in.shape[1]
    r.wq = lambda c: r.wq_all[oth, :, c]
    r.wk = lambda c: r.wk_all[oth, :, c]
    r.wv = lambda c: r.wv_all[oth, :, c]
    r.do_dot = lambda c: dot(dy_in[...], r.wo_all[oth, c, :], NT)
    r.o, r.dq, r.dk, r.dv = r.oc.at[oth], r.dqc.at[oth], r.dkc.at[oth], r.dvc.at[oth]
    st = attn_stages(seq, n_grp, r)

    def fetch(row):
        return [pltpu.make_async_copy(src.at[me, pl.ds(row * seq, seq), :], dst.at[me], r.sem.at[8 + k])
                for k, (src, dst) in enumerate(zip(own_a, (r.oc, r.dqc, r.dkc, r.dvc)))]

    weights = (r.wq_all, r.wk_all, r.wv_all, r.wo_all)
    theirs = [pltpu.make_async_copy(oth_w[k], dst.at[oth], r.sem.at[4 + k]) for k, dst in enumerate(weights)]
    mine = [pltpu.make_async_copy(own_w[k], dst.at[me], r.sem.at[k]) for k, dst in enumerate(weights)]

    @pl.when(step == 0)
    def _():
        for c in theirs + mine:
            c.start()
        r.dg[...] = jnp.zeros_like(r.dg)
        for c in theirs:
            c.wait()

    @pl.when(step > 0)
    def _():
        for c in fetch(step - 1):
            c.start()

    CR, NC = 32, 256
    nn = D // NC
    lines = range(0, seq, CR)

    def wide(v):
        return jnp.concatenate([v] * (NC // HD), axis=1)

    def stat(c):
        def run():
            xf = x_in[c:c + CR, :].astype(F32)
            r.xs[0, c:c + CR, :] = jnp.broadcast_to(lax.rsqrt(jnp.mean(xf * xf, axis=-1, keepdims=True) + EPS), (CR, HD))
            r.xs[1, c:c + CR, :] = jnp.zeros((CR, HD), F32)

        return (1, run)

    def dn_dot(n):
        def run():
            cols = slice(n * NC, (n + 1) * NC)
            t = None
            for s in range(2):
                for a_ref, w_ref in ((r.dqc, r.wq_all), (r.dkc, r.wk_all), (r.dvc, r.wv_all)):
                    u = dot(a_ref[s], w_ref[s, cols, :], NT)
                    t = u if t is None else t + u
            r.dn[:, cols] = t

        return (2, run)

    def first(n, c):
        def run():
            cols = slice(n * NC, (n + 1) * NC)
            w = r.dn[c:c + CR, cols] * (x_in[c:c + CR, cols].astype(F32) * wide(r.xs[0, c:c + CR, :]))
            r.dg[:, cols] += jnp.sum(w.reshape(CR // 8, 8, NC), axis=0)
            w = w * gain_ref[0:1, cols]
            r.xs[1, c:c + CR, :] += w[:, :HD] + w[:, HD:]

        return (1, run)

    def mean(c):
        def run():
            r.xs[2, c:c + CR, :] = jnp.broadcast_to(jnp.sum(r.xs[1, c:c + CR, :], axis=-1, keepdims=True) * (1.0 / D), (CR, HD))

        return (0.2, run)

    def second(n, c):
        def run():
            cols = slice(n * NC, (n + 1) * NC)
            inv = wide(r.xs[0, c:c + CR, :])
            xh = x_in[c:c + CR, cols].astype(F32) * inv
            e = r.dn[c:c + CR, cols] * gain_ref[0:1, cols]
            dx_out[c:c + CR, cols] = (dyx_in[c:c + CR, cols].astype(F32) + inv * (e - xh * wide(r.xs[2, c:c + CR, :]))).astype(BF16)

        return (1.2, run)

    def y_dot(n):
        def run():
            cols = slice(n * NC, (n + 1) * NC)
            t = dot(r.oc[0], r.wo_all[0, :, cols]) + dot(r.oc[1], r.wo_all[1, :, cols])
            y_out[:, cols] = (x_in[:, cols].astype(F32) + t).astype(BF16)

        return (1, run)

    r.tab[2:4] = r.tab[0:2]
    r.tab[0] = cos_in[...]
    r.tab[1] = sin_in[...]
    for g in range(n_grp):
        attn_tick(st, g, n_grp)
    for acc in (r.dgq, r.dgk):
        acc[...] = jnp.where(step > 0, acc[...], 0.0)

    @pl.when(step == 0)
    def _():
        for c in mine:
            c.wait()

    @pl.when(step > 0)
    def _():
        for c in fetch(step - 1):
            c.wait()
        dn = [dn_dot(n) for n in range(nn)]
        yd = [y_dot(n) for n in range(nn)]
        for _, f in dn[:1]:
            f()
        weave([stat(c) for c in lines], dn[1:2])
        for n in range(2, nn):
            weave([first(n - 2, c) for c in lines], dn[n:n + 1])
        weave([first(nn - 2, c) for c in lines], yd[:1])
        weave([first(nn - 1, c) for c in lines] + [mean(c) for c in lines], yd[1:2])
        weave([second(n, c) for n in range(nn) for c in lines], yd[2:])

    @pl.when(step == rows)
    def _():
        dg_out[...] = r.dg[...]
        dgq_out[...] = r.dgq[...]
        dgk_out[...] = r.dgk[...]


def tail_call(sel, n, x, dy, cosd, sind, o, dq, dk, dv, gain, qg, kg, own, oth, seq=256):
    T, D = x.shape
    nq, nk = dq.shape[2], dk.shape[2]
    n_grp = nk // HD
    rows = T // seq
    lag = lambda k, c: pl.BlockSpec((seq, c), lambda i, s: (jnp.clip(i - k, 0, rows - 1), 0))
    const = lambda *b: pl.BlockSpec(b, lambda i, s: (0,) * len(b), pipeline_mode=pl.Buffered(1))
    hbm = pl.BlockSpec(memory_space=pl.ANY)
    scratch = attn_scratch(seq, n_grp)
    scratch.update(
        wq_all=pltpu.VMEM((2, D, nq), BF16), wk_all=pltpu.VMEM((2, D, nk), BF16), wv_all=pltpu.VMEM((2, D, nk), BF16), wo_all=pltpu.VMEM((2, nq, D), BF16),
        dn=pltpu.VMEM((seq, D), F32), oc=pltpu.VMEM((2, seq, nq), BF16), dqc=pltpu.VMEM((2, seq, nq), BF16), dkc=pltpu.VMEM((2, seq, nk), BF16), dvc=pltpu.VMEM((2, seq, nk), BF16),
        xs=pltpu.VMEM((3, seq, HD), F32), dg=pltpu.VMEM((8, D), F32), dgq=pltpu.VMEM((8, HD), F32), dgk=pltpu.VMEM((8, HD), F32), sem=pltpu.SemaphoreType.DMA((12,)))
    flops = 2 * T * D * (nq + 2 * nk + nq) * 3 + 12 * T * nq * seq
    return pl.pallas_call(
        functools.partial(tail_kernel, seq, n_grp, rows, tuple(scratch)),
        grid_spec=pltpu.PrefetchScalarGridSpec(
            num_scalar_prefetch=1,
            grid=(rows + 1,),
            in_specs=[lag(0, D), lag(0, D), lag(0, HD), lag(0, HD), lag(1, D), lag(1, D), const(1, D), const(1, HD), const(1, HD)] + [hbm] * 12,
            out_specs=[lag(1, D), lag(1, D), pl.BlockSpec((8, D), lambda i, s: (0, 0))] + [pl.BlockSpec((8, HD), lambda i, s: (0, 0))] * 2,
            scratch_shapes=list(scratch.values()),
        ),
        out_shape=[jax.ShapeDtypeStruct((T, D), BF16)] * 2 + [jax.ShapeDtypeStruct((8, c), F32) for c in (D, HD, HD)],
        compiler_params=pltpu.CompilerParams(dimension_semantics=("arbitrary",), vmem_limit_bytes=67043328),
        cost_estimate=pl.CostEstimate(flops=flops, bytes_accessed=T * D * 14, transcendentals=T * nq * 2),
        name="tail",
    )(sel, n, dy, cosd, sind, x, dy, gain, qg, kg, *own, *oth, o, dq, dk, dv)


def solution(mesh):
    tok_spec = P("dp", None, None)
    col_spec = P(None, "tp")
    row_spec = P("tp", None)
    n_dp = mesh.shape["dp"]

    def per_device(x_in, dy_in, positions, g_attn, q_gain, k_gain, w_q, w_k, w_v, w_o):
        n_batch, n_seq, D = x_in.shape
        T = n_batch * n_seq
        nk = w_k.shape[1]
        x, dy = x_in.reshape(T, D), dy_in.reshape(T, D)
        me = lax.axis_index("tp").astype(jnp.int32)
        own = me.reshape(1)

        part = lax.axis_index("dp").astype(jnp.int32).reshape(1)
        share, cosd, sind = pre_call(part, w_q, w_k, w_v, w_o, positions, parts=n_dp)
        gathered = lax.all_gather(share, ("tp", "dp"), tiled=True)

        gain = g_attn.astype(F32).reshape(1, D)
        qg, kg = q_gain.astype(F32).reshape(1, HD), k_gain.astype(F32).reshape(1, HD)

        n, o, dq, dk, dv, dgq, dgk = attn_call(True, own, x, dy, cosd, sind, gain, qg, kg, w_q, w_k, w_v, w_o, seq=n_seq)
        dw_q, dw_k, dw_v = dw_call(own, n, [dq, dk, dv], 512)
        dw_o, *theirs = dw_call(own, o, [dy], 1024, gathered=gathered, nk=nk)
        dw_o, dw_q, dw_k, dw_v = lax.psum((dw_o, dw_q, dw_k, dw_v), "dp")

        y, dx, dg, dgq2, dgk2 = tail_call(own, n, x, dy, cosd, sind, o, dq, dk, dv, gain, qg, kg, (w_q, w_k, w_v, w_o), theirs, seq=n_seq)
        small = lax.psum(jnp.sum(jnp.concatenate([dg, dgq + dgq2, dgk + dgk2], axis=1), axis=0), "dp")
        g_sum, q_sum, k_sum = small[:D], small[D:D + HD], small[D + HD:]
        return y.reshape(x_in.shape), dx.reshape(x_in.shape), dw_q, dw_k, dw_v, dw_o, q_sum, k_sum, g_sum

    return jax.shard_map(per_device, mesh=mesh, in_specs=(tok_spec, tok_spec, P("dp", None), P(), P(), P(), col_spec, col_spec, col_spec, row_spec), out_specs=(tok_spec, tok_spec, col_spec, col_spec, col_spec, row_spec, P(), P(), P()), check_vma=False)
```

```python
import functools
from types import SimpleNamespace
import jax
import jax.numpy as jnp
from jax import lax
from jax.experimental import pallas as pl
from jax.experimental.pallas import tpu as pltpu
from jax.sharding import PartitionSpec as P


EPS = 1e-6
THETA = 1000000.0
F32 = jnp.float32
BF16 = jnp.bfloat16
HD = 128
NT = (((1,), (1,)), ((), ()))
TN = (((0,), (0,)), ((), ()))
NN = (((1,), (0,)), ((), ()))


def dot(a, b, dims=NN):
    return lax.dot_general(a, b, dims, preferred_element_type=F32)


def weave(*lists):
    order = []
    for n, pieces in enumerate(lists):
        total = sum(c for c, _ in pieces) or 1
        at = 0
        for k, (c, f) in enumerate(pieces):
            order.append(((at + c / 2) / total, n, k, f))
            at += c
    for _, _, _, f in sorted(order, key=lambda e: e[:3]):
        f()


CH = 32


def attn_kernel(own, seq, n_grp, sel_ref, *refs):
    if own:
        (x0_ref, xn_ref, dy_ref, cos_ref, sin_ref, gain_ref, qg_ref, kg_ref, wq_ref, wk_ref, wv_ref, wo_ref,
         n_out, o_out, dq_out, dk_out, dv_out, dgq_out, dgk_out) = refs[:19]
        refs = refs[19:]
    else:
        nin_ref, dy_ref, cos_ref, sin_ref, qg_ref, kg_ref, wq_ref, wk_ref, wv_ref, wo_ref, _, _, _, _, o_out, dq_out, dk_out, dv_out = refs[:18]
        refs = refs[18:]
        n_ref = nin_ref
    (wot_ref, qnew_ref, knew_ref, vnew_ref, raw_ref, inv_ref, rot_ref, do_ref, v_ref, s_ref, dp_ref, p_ref, ds_ref, dkf_ref, dqf_ref, st_ref,
     tab_ref, o_ref, dq_ref, dk_ref, dv_ref) = refs[:21]
    if own:
        n_ref, nn_ref, dgq_ref, dgk_ref = refs[21:]
    half = seq // 2
    scale = HD ** -0.5
    log2e = 1.4426950408889634
    step = pl.program_id(0)

    def norm_rows(src, dst):
        def piece(c):
            def run():
                xf = src[c:c + 32, :].astype(F32)
                inv = lax.rsqrt(jnp.mean(xf * xf, axis=-1, keepdims=True) + EPS)
                dst[c:c + 32, :] = (xf * inv * gain_ref[0:1, :]).astype(BF16)

            return (1.5, run)

        return [piece(c) for c in range(0, seq, 32)]

    def proj(g):
        def q():
            t = dot(n_ref[...], wq_ref[:, g * 2 * HD:(g + 1) * 2 * HD])
            for h in range(2):
                qnew_ref[g % 2, h] = t[:, h * HD:(h + 1) * HD].astype(BF16)

        def k():
            t = dot(n_ref[...], wk_ref[:, g * HD:(g + 2) * HD])
            for h in range(2):
                knew_ref[g + h] = t[:, h * HD:(h + 1) * HD].astype(BF16)

        def v():
            t = dot(n_ref[...], wv_ref[:, g * HD:(g + 2) * HD])
            for h in range(2):
                vnew_ref[g + h] = t[:, h * HD:(h + 1) * HD].astype(BF16)

        def do():
            t = dot(dy_ref[...], wot_ref[:, g * 2 * HD:(g + 1) * 2 * HD])
            for h in range(2):
                do_ref[g, h * half:(h + 1) * half, :] = t[:half, h * HD:(h + 1) * HD].astype(BF16)
                do_ref[g, seq + h * half:seq + (h + 1) * half, :] = t[half:, h * HD:(h + 1) * HD].astype(BF16)

        return [(1, q)] + ([(1, k), (1, v)] if g % 2 == 0 else []) + [(1, do)]

    def stacked(h, c):
        return (h * half + c) if c < half else (seq + h * half + c - half)

    def rope(g):
        cs, sn = (tab_ref.at[2], tab_ref.at[3]) if g == n_grp - 1 else (tab_ref.at[0], tab_ref.at[1])

        def size(h, c):
            def run():
                raw = knew_ref[g, c:c + CH, :] if h == 2 else qnew_ref[g % 2, h, c:c + CH, :]
                raw_ref[g, h, c:c + CH, :] = raw
                t = raw.astype(F32)
                inv_ref[g, h, c:c + CH, :] = jnp.broadcast_to(lax.rsqrt(jnp.mean(t * t, axis=-1, keepdims=True) + EPS), t.shape)

            return (0.4, run)

        def turn(h, c):
            def run():
                t = raw_ref[g, h, c:c + CH, :].astype(F32)
                w = (t * inv_ref[g, h, c:c + CH, :]) * (kg_ref if h == 2 else qg_ref)[0:1, :]
                o = 2 * seq + c if h == 2 else stacked(h, c)
                x = pltpu.roll(w, HD // 2, 1)
                co, si = cs[c:c + CH, :], sn[c:c + CH, :]
                rot_ref[g, o:o + CH, 0:HD] = (w * co + x * si).astype(BF16)
                rot_ref[g, o:o + CH, HD:] = (x * co - w * si).astype(BF16)
                if h == 2:
                    v_ref[g, c:c + CH, :] = vnew_ref[g, c:c + CH, :]

            return (0.6, run)

        return [f(h, c) for f in (size, turn) for h in (2, 0, 1) for c in range(0, seq, CH)]

    def scores(g):
        b = g % 2

        def s():
            s_ref[b, 0:seq, 0:half] = dot(rot_ref[g, 0:seq, 0:HD], rot_ref[g, 2 * seq:2 * seq + half, 0:HD], NT)
            s_ref[b, seq:, :] = dot(rot_ref[g, seq:2 * seq, 0:HD], rot_ref[g, 2 * seq:, 0:HD], NT)

        def dp():
            dp_ref[b, 0:seq, 0:half] = dot(do_ref[g, :seq, :], v_ref[g, :half, :], NT)
            dp_ref[b, seq:, :] = dot(do_ref[g, seq:, :], v_ref[g], NT)

        return [(1, s), (1, dp)]

    def soft(g):
        b = g % 2
        c2 = scale * log2e

        def part(blk, c):
            return slice(blk * seq + c, blk * seq + c + CH), half if blk == 0 else seq

        def masked(blk, c, s):
            row_id = lax.broadcasted_iota(jnp.int32, (CH, half), 0) + (c % half)
            keep = row_id >= lax.broadcasted_iota(jnp.int32, (CH, half), 1)
            if blk == 0:
                return jnp.where(keep, s, -jnp.inf)
            return jnp.concatenate([s[:, :half], jnp.where(keep, s[:, half:], -jnp.inf)], axis=1)

        def wide(ref, rows, width):
            t = ref[rows, :]
            return t if width == half else jnp.concatenate([t, t], axis=1)

        def top(blk, c):
            rows, width = part(blk, c)

            def run():
                m = jnp.max(masked(blk, c, s_ref[b, rows, 0:width]), axis=-1, keepdims=True)
                st_ref[0, rows, :] = jnp.broadcast_to(m * c2, (CH, HD))

            return (0.4 + 0.4 * blk, run)

        def power(blk, c):
            rows, width = part(blk, c)

            def run():
                e = jnp.exp2(masked(blk, c, s_ref[b, rows, 0:width] * c2) - wide(st_ref.at[0], rows, width))
                s_ref[b, rows, 0:width] = e
                st_ref[1, rows, :] = jnp.broadcast_to(1.0 / jnp.sum(e, axis=-1, keepdims=True), (CH, HD))

            return (0.8 + 0.8 * blk, run)

        def prob(blk, c):
            rows, width = part(blk, c)

            def run():
                pr = s_ref[b, rows, 0:width] * wide(st_ref.at[1], rows, width)
                s_ref[b, rows, 0:width] = pr
                p_ref[b, rows, 0:width] = pr.astype(BF16)
                st_ref[2, rows, :] = jnp.broadcast_to(jnp.sum(pr * dp_ref[b, rows, 0:width], axis=-1, keepdims=True), (CH, HD))

            return (0.8 + 0.8 * blk, run)

        def last(blk, c):
            rows, width = part(blk, c)

            def run():
                d = dp_ref[b, rows, 0:width] - wide(st_ref.at[2], rows, width)
                ds_ref[b, rows, 0:width] = (s_ref[b, rows, 0:width] * d * scale).astype(BF16)

            return (0.8 + 0.8 * blk, run)

        return [f(blk, c) for f in (top, power, prob, last) for blk in range(2) for c in range(0, seq, CH)]

    def grads(g):
        b = g % 2
        col, kcol = g * 2 * HD, g * HD

        def dq():
            dqf_ref[b, 0:seq, :] = dot(ds_ref[b, 0:seq, 0:half], rot_ref[g, 2 * seq:2 * seq + half, :])
            dqf_ref[b, seq:, :] = dot(ds_ref[b, seq:, :], rot_ref[g, 2 * seq:, :])

        def dk():
            tb = dot(ds_ref[b, seq:, :], rot_ref[g, seq:2 * seq, :], TN)
            ta = dot(ds_ref[b, 0:seq, 0:half], rot_ref[g, 0:seq, :], TN)
            dkf_ref[b, :half, :] = tb[:half] + ta
            dkf_ref[b, half:, :] = tb[half:]

        def o():
            ta = dot(p_ref[b, 0:seq, 0:half], v_ref[g, :half, :])
            tb = dot(p_ref[b, seq:, :], v_ref[g])
            for h in range(2):
                o_ref[0:half, col + h * HD:col + (h + 1) * HD] = ta[h * half:(h + 1) * half].astype(BF16)
                o_ref[half:seq, col + h * HD:col + (h + 1) * HD] = tb[h * half:(h + 1) * half].astype(BF16)

        def dv():
            tb = dot(p_ref[b, seq:, :], do_ref[g, seq:, :], TN)
            ta = dot(p_ref[b, 0:seq, 0:half], do_ref[g, :seq, :], TN)
            dv_ref[0:half, kcol:kcol + HD] = (tb[:half] + ta).astype(BF16)
            dv_ref[half:seq, kcol:kcol + HD] = tb[half:].astype(BF16)

        return [(1, dq), (1, dk), (1, o), (1, dv)]

    def back(g):
        b = g % 2

        def place(h, c):
            if h == 2:
                return dkf_ref, c, dk_ref, g * HD, kg_ref
            return dqf_ref, stacked(h, c), dq_ref, (2 * g + h) * HD, qg_ref

        def turn(h, c):
            src, o, _, _, g_ref = place(h, c)

            def run():
                d = src[b, o:o + CH, :].astype(BF16).astype(F32)
                that = raw_ref[g, h, c:c + CH, :].astype(F32) * inv_ref[g, h, c:c + CH, :]
                du = d[:, :HD] * tab_ref[2, c:c + CH, :] - d[:, HD:] * tab_ref[3, c:c + CH, :]
                src[b, o:o + CH, 0:HD] = du
                pr = du * that
                if own:
                    dg_ref = dgk_ref if h == 2 else dgq_ref
                    dg_ref[...] += jnp.sum(pr.reshape(CH // 8, 8, HD), axis=0)
                st_ref[3 + h, c:c + CH, :] = jnp.broadcast_to(jnp.mean(pr * g_ref[0:1, :], axis=-1, keepdims=True), (CH, HD))

            return (0.6, run)

        def out(h, c):
            src, o, out_ref, col, g_ref = place(h, c)

            def run():
                inv = inv_ref[g, h, c:c + CH, :]
                that = raw_ref[g, h, c:c + CH, :].astype(F32) * inv
                out_ref[c:c + CH, col:col + HD] = (inv * (src[b, o:o + CH, 0:HD] * g_ref[0:1, :] - that * st_ref[3 + h, c:c + CH, :])).astype(BF16)

            return (0.5, run)

        return [f(h, c) for f in (turn, out) for h in (0, 1, 2) for c in range(0, seq, CH)]

    @pl.when(step == 0)
    def _():
        @pl.loop(0, wo_ref.shape[0] // 256)
        def _(j):
            c = pl.ds(pl.multiple_of(j * 256, 256), 256)
            for d in range(0, wo_ref.shape[1], 256):
                wot_ref[d:d + 256, c] = wo_ref[c, d:d + 256].T

        if own:
            weave(norm_rows(x0_ref, n_ref))

    tab_ref[2:4] = tab_ref[0:2]
    tab_ref[0] = cos_ref[...]
    tab_ref[1] = sin_ref[...]
    if own:
        norms = norm_rows(xn_ref, nn_ref)
    for g in range(n_grp):
        vec = soft((g - 3) % n_grp)
        sc = scores((g - 2) % n_grp)
        vec = vec + rope((g - 1) % n_grp)
        if own:
            vec += norms[g * len(norms) // n_grp:(g + 1) * len(norms) // n_grp]
        vec += back(g)
        gr = grads(g)
        for _, f in gr[:2]:
            f()
        weave(vec, sc + gr[2:] + proj(g))

    for dst, src in ((o_out, o_ref), (dq_out, dq_ref), (dk_out, dk_ref), (dv_out, dv_ref)):
        dst[0] = src[...]
    if own:
        n_out[...] = n_ref[...]
        n_ref[...] = nn_ref[...]
        keep = step > 0
        for dst, acc in ((dgq_out, dgq_ref), (dgk_out, dgk_ref)):
            acc[...] = jnp.where(keep, acc[...], 0.0)
            dst[...] = acc[...]


def attn_call(own, sel, x, dy, cosd, sind, gain, qg, kg, wq, wk, wv, wo, prev=None, seq=256):
    T, D = x.shape
    nq, nk = wq.shape[1], wk.shape[1]
    n_grp = nk // HD
    rows = T // seq
    const = lambda *b: pl.BlockSpec(b, lambda i, s: (0,) * len(b), pipeline_mode=pl.Buffered(1))
    now = lambda c: pl.BlockSpec((seq, c), lambda i, s: (jnp.minimum(i, rows - 1), 0))
    nxt = lambda c: pl.BlockSpec((seq, c), lambda i, s: (jnp.minimum(i + 1, rows - 1), 0))
    out3 = lambda c: pl.BlockSpec((1, seq, c), lambda i, s: (s[0], jnp.maximum(i - 1, 0), 0))
    mid = [now(D), now(HD), now(HD)]
    tail = [const(1, HD), const(1, HD), const(D, nq), const(D, nk), const(D, nk), const(nq, D)]
    shapes = [jax.ShapeDtypeStruct((2, T, c), BF16) for c in (nq, nq, nk, nk)]
    specs = [out3(nq), out3(nq), out3(nk), out3(nk)]
    aliases = {}
    if own:
        in_specs = [const(seq, D), nxt(D)] + mid + [const(1, D)] + tail
        args = [x, x, dy, cosd, sind, gain, qg, kg, wq, wk, wv, wo]
        shapes = [jax.ShapeDtypeStruct((T, D), BF16)] + shapes + [jax.ShapeDtypeStruct((8, HD), F32)] * 2
        specs = [now(D)] + specs + [pl.BlockSpec((8, HD), lambda i, s: (0, 0))] * 2
    else:
        in_specs = [now(D)] + mid + tail + [pl.BlockSpec(memory_space=pl.ANY)] * 4
        args = [x, dy, cosd, sind, qg, kg, wq, wk, wv, wo]
        aliases = {1 + len(args) + i: i for i in range(4)}
        args += list(prev)
    flops = 2 * T * D * (nq + 2 * nk + nq) + 12 * T * nq * seq
    return pl.pallas_call(
        functools.partial(attn_kernel, own, seq, n_grp),
        grid_spec=pltpu.PrefetchScalarGridSpec(
            num_scalar_prefetch=1,
            grid=(rows + 1,),
            in_specs=in_specs,
            out_specs=specs,
            scratch_shapes=[
                pltpu.VMEM((D, nq), BF16),
                pltpu.VMEM((2, 2, seq, HD), BF16),
                pltpu.VMEM((n_grp, seq, HD), BF16),
                pltpu.VMEM((n_grp, seq, HD), BF16),
                pltpu.VMEM((n_grp, 3, seq, HD), BF16),
                pltpu.VMEM((n_grp, 3, seq, HD), F32),
                pltpu.VMEM((n_grp, 3 * seq, 2 * HD), BF16),
                pltpu.VMEM((n_grp, 2 * seq, HD), BF16),
                pltpu.VMEM((n_grp, seq, HD), BF16),
                pltpu.VMEM((2, 2 * seq, seq), F32),
                pltpu.VMEM((2, 2 * seq, seq), F32),
                pltpu.VMEM((2, 2 * seq, seq), BF16),
                pltpu.VMEM((2, 2 * seq, seq), BF16),
                pltpu.VMEM((2, seq, 2 * HD), F32),
                pltpu.VMEM((2, 2 * seq, 2 * HD), F32),
                pltpu.VMEM((6, 2 * seq, HD), F32),
                pltpu.VMEM((4, seq, HD), F32),
            ] + [pltpu.VMEM((seq, c), BF16) for c in (nq, nq, nk, nk)]
            + ([pltpu.VMEM((seq, D), BF16)] * 2 + [pltpu.VMEM((8, HD), F32)] * 2 if own else []),
        ),
        out_shape=shapes,
        input_output_aliases=aliases,
        compiler_params=pltpu.CompilerParams(dimension_semantics=("arbitrary",), vmem_limit_bytes=56 << 20),
        cost_estimate=pl.CostEstimate(flops=flops, bytes_accessed=T * D * 6 + T * (2 * nq + 2 * nk) * 2, transcendentals=T * nq * 2),
        name="attn_own" if own else "attn_other",
    )(sel, *args)


def pre_kernel(sel_ref, q_ref, k_ref, v_ref, o_ref, pos_ref, freq_ref, out_ref, cos_ref, sin_ref):
    d, nq, nk = q_ref.shape[0], q_ref.shape[1], k_ref.shape[1]
    out_ref[0, 0:d, 0:nq] = q_ref[...].astype(F32)
    out_ref[0, 0:d, nq:nq + nk] = k_ref[...].astype(F32)
    out_ref[0, 0:d, nq + nk:] = v_ref[...].astype(F32)
    out_ref[0, d:, :] = o_ref[...].astype(F32)
    n, seq = pos_ref.shape
    lane = lax.broadcasted_iota(jnp.int32, (HD, HD), 1)
    for r in range(n):
        for h in range(seq // HD):
            p = pos_ref[r:r + 1, h * HD:(h + 1) * HD].astype(F32)
            a = jnp.broadcast_to(p, (HD, HD)).T * freq_ref[0:1, :]
            k = jnp.round(a * 0.6366197723675814)
            x = ((a - k * 1.5703125) - k * 4.837512969970703125e-4) - k * 7.549789948768648e-8
            z = x * x
            s = ((-1.9515295891e-4 * z + 8.3321608736e-3) * z - 1.6666654611e-1) * z * x + x
            c = ((2.443315711809948e-5 * z - 1.388731625493765e-3) * z + 4.166664568298827e-2) * z * z - 0.5 * z + 1.0
            q = k.astype(jnp.int32)
            odd = (q & 1) == 1
            co, si = jnp.where(odd, s, c), jnp.where(odd, c, s)
            rows = slice((r * (seq // HD) + h) * HD, (r * (seq // HD) + h + 1) * HD)
            cos_ref[rows, :] = jnp.where(((q + 1) & 2) == 0, co, -co)
            sin_ref[rows, :] = jnp.where(((q & 2) == 0) == (lane >= HD // 2), si, -si)


def pre_call(part, w_q, w_k, w_v, w_o, positions, parts=2, cuts=4):
    D, nq = w_q.shape
    n, seq = positions.shape
    rows = n // cuts
    freq = THETA ** (-jnp.arange(0, HD, 2, dtype=F32) / HD)
    freq = jnp.concatenate([freq, freq]).reshape(1, HD)
    spec = lambda w: pl.BlockSpec((w.shape[0] // (parts * cuts), w.shape[1]), lambda i, s: (s[0] * cuts + i, 0))
    r = (D + nq) // (parts * cuts)
    table = pl.BlockSpec((rows * seq, HD), lambda i, s: (i, 0))
    return pl.pallas_call(
        pre_kernel,
        grid_spec=pltpu.PrefetchScalarGridSpec(
            num_scalar_prefetch=1,
            grid=(cuts,),
            in_specs=[spec(w) for w in (w_q, w_k, w_v, w_o)] + [pl.BlockSpec((rows, seq), lambda i, s: (i, 0)), pl.BlockSpec((1, HD), lambda i, s: (0, 0))],
            out_specs=[pl.BlockSpec((1, r, D), lambda i, s: (i, 0, 0)), table, table],
        ),
        out_shape=[jax.ShapeDtypeStruct((cuts, r, D), F32)] + [jax.ShapeDtypeStruct((n * seq, HD), F32)] * 2,
        compiler_params=pltpu.CompilerParams(dimension_semantics=("arbitrary",), vmem_limit_bytes=60 << 20),
        cost_estimate=pl.CostEstimate(flops=n * seq * HD * 30, bytes_accessed=cuts * r * D * 6 + n * seq * HD * 8, transcendentals=0),
        name="pre",
    )(part, w_q, w_k, w_v, w_o, positions, freq)


def dw_kernel(n_b, unpack, sel_ref, a_ref, *refs):
    if unpack:
        f_ref, parts = refs[n_b], refs[2 * n_b + 1:2 * n_b + 5]
        refs = refs[:n_b] + refs[n_b + 1:2 * n_b + 1] + refs[2 * n_b + 5:]
        q_ref, k_ref, v_ref, o_ref = parts
        per, nq, nk = f_ref.shape[0], q_ref.shape[1], k_ref.shape[1]
        d, e = q_ref.shape[0] // per, o_ref.shape[0] // per
        for j in range(per):
            q_ref[j * d:(j + 1) * d, :] = f_ref[j, 0:d, 0:nq].astype(BF16)
            k_ref[j * d:(j + 1) * d, :] = f_ref[j, 0:d, nq:nq + nk].astype(BF16)
            v_ref[j * d:(j + 1) * d, :] = f_ref[j, 0:d, nq + nk:].astype(BF16)
            o_ref[j * e:(j + 1) * e, :] = f_ref[j, d:, :].astype(BF16)
    bs, outs, accs, (at_ref, sem) = refs[:n_b], refs[n_b:2 * n_b], refs[2 * n_b:3 * n_b], refs[3 * n_b:]
    flat = lambda ref: ref.at[0] if len(ref.shape) == 3 else ref
    a, bs = flat(a_ref), [flat(b) for b in bs]
    M, tile = at_ref.shape
    step = pl.program_id(0)

    @pl.when(step == 0)
    def _():
        for acc in accs:
            @pl.loop(0, M // 64)
            def _(j):
                acc[pl.ds(pl.multiple_of(j * 64, 64), 64), :] = jnp.zeros((64, acc.shape[1]), F32)

    def part(acc, b, c):
        def run():
            acc[:, c:c + 256] += dot(at_ref[...], b[:, c:c + 256])

        return (1, run)

    for c in range(0, M, 256):
        for k in range(0, tile, 256):
            at_ref[c:c + 256, k:k + 256] = a[k:k + 256, c:c + 256].T
    weave([part(acc, b, c) for acc, b in zip(accs, bs) for c in range(0, b.shape[1], 256)])

    @pl.when(step == pl.num_programs(0) - 1)
    def _():
        copies = [pltpu.make_async_copy(acc, out, sem.at[k]) for k, (acc, out) in enumerate(zip(accs, outs))]
        for c in copies:
            c.start()
        for c in copies:
            c.wait()


def dw_call(sel, a, bs, tile, gathered=None, nk=0):
    def spec(v):
        if v.ndim == 3:
            return pl.BlockSpec((1, tile, v.shape[2]), lambda i, s: (s[0], i, 0))
        return pl.BlockSpec((tile, v.shape[1]), lambda i, s: (i, 0))

    T, M = a.shape[-2:]
    shapes = [(M, b.shape[-1]) for b in bs]
    width = sum(s[1] for s in shapes)
    steps = T // tile
    more_in, more_out, more_shapes, more = [], [], [], []
    if gathered is not None:
        n, r, D = gathered.shape
        per = n // 2 // steps
        more = [gathered]
        more_in = [pl.BlockSpec((per, r, D), lambda i, s: ((1 - s[0]) * steps + i, 0, 0))]
        nq = D - 2 * nk
        more_shapes = [jax.ShapeDtypeStruct(s, BF16) for s in ((D, nq), (D, nk), (D, nk), (nq, D))]
        more_out = [pl.BlockSpec((s.shape[0] // steps, s.shape[1]), lambda i, s: (i, 0)) for s in more_shapes]
    return pl.pallas_call(
        functools.partial(dw_kernel, len(bs), gathered is not None),
        grid_spec=pltpu.PrefetchScalarGridSpec(
            num_scalar_prefetch=1,
            grid=(steps,),
            in_specs=[spec(a)] + [spec(b) for b in bs] + more_in,
            out_specs=[pl.BlockSpec(memory_space=pl.ANY)] * len(bs) + more_out,
            scratch_shapes=[pltpu.VMEM(s, F32) for s in shapes] + [pltpu.VMEM((M, tile), BF16), pltpu.SemaphoreType.DMA((len(bs),))],
        ),
        out_shape=[jax.ShapeDtypeStruct(s, F32) for s in shapes] + more_shapes,
        compiler_params=pltpu.CompilerParams(dimension_semantics=("arbitrary",), vmem_limit_bytes=60 << 20),
        cost_estimate=pl.CostEstimate(flops=2 * T * M * width, bytes_accessed=2 * T * (M + width) + 4 * M * width, transcendentals=0),
    )(sel, a, *bs, *more)


def sum_kernel(n, widths, part_ref, *refs):
    outs, (slots, local_sem, send_sem, recv_sem) = refs[:-4], refs[-4:]
    me = lax.axis_index("dp")
    barrier = pltpu.get_barrier_semaphore()
    for k in range(1, n):
        pl.semaphore_signal(barrier, inc=1, device_id={"dp": lax.rem(me + k, n)}, device_id_type=pl.DeviceIdType.MESH)
    mine = pltpu.make_async_copy(part_ref, slots.at[0], local_sem)
    mine.start()
    pl.semaphore_wait(barrier, n - 1)
    copies = []
    for k in range(1, n):
        copies.append(pltpu.make_async_remote_copy(
            src_ref=part_ref, dst_ref=slots.at[k], send_sem=send_sem.at[k - 1], recv_sem=recv_sem.at[k - 1],
            device_id={"dp": lax.rem(me + k, n)}, device_id_type=pl.DeviceIdType.MESH))
    for c in copies:
        c.start()
    mine.wait()
    for c in copies:
        c.wait()
    total = slots[lax.rem(me + n, n)]
    for a in range(1, n):
        total = total + slots[lax.rem(me + n - a, n)]
    total = jnp.sum(total, axis=0, keepdims=True)
    at = 0
    for out, w in zip(outs, widths):
        out[...] = total[:, at:at + w]
        at += w


def sum_call(part, widths, n):
    return pl.pallas_call(
        functools.partial(sum_kernel, n, widths),
        in_specs=[pl.BlockSpec(memory_space=pl.ANY)],
        out_specs=[pl.BlockSpec(memory_space=pltpu.VMEM)] * len(widths),
        out_shape=[jax.ShapeDtypeStruct((1, w), F32) for w in widths],
        scratch_shapes=[pltpu.VMEM((n, *part.shape), F32), pltpu.SemaphoreType.DMA, pltpu.SemaphoreType.DMA((n - 1,)), pltpu.SemaphoreType.DMA((n - 1,))],
        compiler_params=pltpu.CompilerParams(collective_id=0, has_side_effects=True),
        cost_estimate=pl.CostEstimate(flops=n * part.size, bytes_accessed=8 * n * part.size, transcendentals=0),
        name="small_sum",
    )(part)


def copy_kernel(n, *refs):
    for src, dst in zip(refs[:n], refs[n:]):
        dst[...] = src[...]


def copy_call(arrays, steps=8):
    specs = [pl.BlockSpec((a.shape[0] // steps, a.shape[1]), lambda i: (i, 0)) for a in arrays]
    return pl.pallas_call(
        functools.partial(copy_kernel, len(arrays)),
        grid=(steps,),
        in_specs=specs,
        out_specs=specs,
        out_shape=[jax.ShapeDtypeStruct(a.shape, a.dtype) for a in arrays],
        compiler_params=pltpu.CompilerParams(dimension_semantics=("arbitrary",), vmem_limit_bytes=60 << 20),
        cost_estimate=pl.CostEstimate(flops=0, bytes_accessed=8 * sum(a.size for a in arrays), transcendentals=0),
        name="results",
    )(*arrays)


def attn_stages(seq, n_grp, r):
    half = seq // 2
    scale = HD ** -0.5
    log2e = 1.4426950408889634

    def norm_rows(src, dst):
        def piece(c):
            def run():
                xf = src[c:c + 32, :].astype(F32)
                inv = lax.rsqrt(jnp.mean(xf * xf, axis=-1, keepdims=True) + EPS)
                dst[c:c + 32, :] = (xf * inv * r.gain[0:1, :]).astype(BF16)

            return (1.5, run)

        return [piece(c) for c in range(0, seq, 32)]

    def proj(g):
        def q():
            t = dot(r.n[...], r.wq(slice(g * 2 * HD, (g + 1) * 2 * HD)))
            for h in range(2):
                r.qnew[g % 2, h] = t[:, h * HD:(h + 1) * HD].astype(BF16)

        def k():
            t = dot(r.n[...], r.wk(slice(g * HD, (g + 2) * HD)))
            for h in range(2):
                r.knew[g + h] = t[:, h * HD:(h + 1) * HD].astype(BF16)

        def v():
            t = dot(r.n[...], r.wv(slice(g * HD, (g + 2) * HD)))
            for h in range(2):
                r.vnew[g + h] = t[:, h * HD:(h + 1) * HD].astype(BF16)

        def do():
            t = r.do_dot(slice(g * 2 * HD, (g + 1) * 2 * HD))
            for h in range(2):
                r.do[g, h * half:(h + 1) * half, :] = t[:half, h * HD:(h + 1) * HD].astype(BF16)
                r.do[g, seq + h * half:seq + (h + 1) * half, :] = t[half:, h * HD:(h + 1) * HD].astype(BF16)

        return [(1, q)] + ([(1, k), (1, v)] if g % 2 == 0 else []) + [(1, do)]

    def stacked(h, c):
        return (h * half + c) if c < half else (seq + h * half + c - half)

    def rope(g):
        cs, sn = (r.tab.at[2], r.tab.at[3]) if g == n_grp - 1 else (r.tab.at[0], r.tab.at[1])

        def size(h, c):
            def run():
                raw = r.knew[g, c:c + CH, :] if h == 2 else r.qnew[g % 2, h, c:c + CH, :]
                r.raw[g, h, c:c + CH, :] = raw
                t = raw.astype(F32)
                r.inv[g, h, c:c + CH, :] = jnp.broadcast_to(lax.rsqrt(jnp.mean(t * t, axis=-1, keepdims=True) + EPS), t.shape)

            return (0.4, run)

        def turn(h, c):
            def run():
                t = r.raw[g, h, c:c + CH, :].astype(F32)
                w = (t * r.inv[g, h, c:c + CH, :]) * (r.kg if h == 2 else r.qg)[0:1, :]
                o = 2 * seq + c if h == 2 else stacked(h, c)
                x = pltpu.roll(w, HD // 2, 1)
                co, si = cs[c:c + CH, :], sn[c:c + CH, :]
                r.rot[g, o:o + CH, 0:HD] = (w * co + x * si).astype(BF16)
                r.rot[g, o:o + CH, HD:] = (x * co - w * si).astype(BF16)
                if h == 2:
                    r.v[g, c:c + CH, :] = r.vnew[g, c:c + CH, :]

            return (0.6, run)

        return [f(h, c) for f in (size, turn) for h in (2, 0, 1) for c in range(0, seq, CH)]

    def scores(g):
        b = g % 2

        def s():
            r.s[b, 0:seq, 0:half] = dot(r.rot[g, 0:seq, 0:HD], r.rot[g, 2 * seq:2 * seq + half, 0:HD], NT)
            r.s[b, seq:, :] = dot(r.rot[g, seq:2 * seq, 0:HD], r.rot[g, 2 * seq:, 0:HD], NT)

        def dp():
            r.dp[b, 0:seq, 0:half] = dot(r.do[g, :seq, :], r.v[g, :half, :], NT)
            r.dp[b, seq:, :] = dot(r.do[g, seq:, :], r.v[g], NT)

        return [(1, s), (1, dp)]

    def soft(g):
        b = g % 2
        c2 = scale * log2e

        def part(blk, c):
            return slice(blk * seq + c, blk * seq + c + CH), half if blk == 0 else seq

        def masked(blk, c, s):
            row_id = lax.broadcasted_iota(jnp.int32, (CH, half), 0) + (c % half)
            keep = row_id >= lax.broadcasted_iota(jnp.int32, (CH, half), 1)
            if blk == 0:
                return jnp.where(keep, s, -jnp.inf)
            return jnp.concatenate([s[:, :half], jnp.where(keep, s[:, half:], -jnp.inf)], axis=1)

        def wide(ref, rows, width):
            t = ref[rows, :]
            return t if width == half else jnp.concatenate([t, t], axis=1)

        def top(blk, c):
            rows, width = part(blk, c)

            def run():
                m = jnp.max(masked(blk, c, r.s[b, rows, 0:width]), axis=-1, keepdims=True)
                r.st[0, rows, :] = jnp.broadcast_to(m * c2, (CH, HD))

            return (0.4 + 0.4 * blk, run)

        def power(blk, c):
            rows, width = part(blk, c)

            def run():
                e = jnp.exp2(masked(blk, c, r.s[b, rows, 0:width] * c2) - wide(r.st.at[0], rows, width))
                r.s[b, rows, 0:width] = e
                r.st[1, rows, :] = jnp.broadcast_to(1.0 / jnp.sum(e, axis=-1, keepdims=True), (CH, HD))

            return (0.8 + 0.8 * blk, run)

        def prob(blk, c):
            rows, width = part(blk, c)

            def run():
                pr = r.s[b, rows, 0:width] * wide(r.st.at[1], rows, width)
                r.s[b, rows, 0:width] = pr
                r.p[b, rows, 0:width] = pr.astype(BF16)
                r.st[2, rows, :] = jnp.broadcast_to(jnp.sum(pr * r.dp[b, rows, 0:width], axis=-1, keepdims=True), (CH, HD))

            return (0.8 + 0.8 * blk, run)

        def last(blk, c):
            rows, width = part(blk, c)

            def run():
                d = r.dp[b, rows, 0:width] - wide(r.st.at[2], rows, width)
                r.ds[b, rows, 0:width] = (r.s[b, rows, 0:width] * d * scale).astype(BF16)

            return (0.8 + 0.8 * blk, run)

        return [f(blk, c) for f in (top, power, prob, last) for blk in range(2) for c in range(0, seq, CH)]

    def grads(g):
        b = g % 2
        col, kcol = g * 2 * HD, g * HD

        def dq():
            r.dqf[b, 0:seq, :] = dot(r.ds[b, 0:seq, 0:half], r.rot[g, 2 * seq:2 * seq + half, :])
            r.dqf[b, seq:, :] = dot(r.ds[b, seq:, :], r.rot[g, 2 * seq:, :])

        def dk():
            tb = dot(r.ds[b, seq:, :], r.rot[g, seq:2 * seq, :], TN)
            ta = dot(r.ds[b, 0:seq, 0:half], r.rot[g, 0:seq, :], TN)
            r.dkf[b, :half, :] = tb[:half] + ta
            r.dkf[b, half:, :] = tb[half:]

        def o():
            ta = dot(r.p[b, 0:seq, 0:half], r.v[g, :half, :])
            tb = dot(r.p[b, seq:, :], r.v[g])
            for h in range(2):
                r.o[0:half, col + h * HD:col + (h + 1) * HD] = ta[h * half:(h + 1) * half].astype(BF16)
                r.o[half:seq, col + h * HD:col + (h + 1) * HD] = tb[h * half:(h + 1) * half].astype(BF16)

        def dv():
            tb = dot(r.p[b, seq:, :], r.do[g, seq:, :], TN)
            ta = dot(r.p[b, 0:seq, 0:half], r.do[g, :seq, :], TN)
            r.dv[0:half, kcol:kcol + HD] = (tb[:half] + ta).astype(BF16)
            r.dv[half:seq, kcol:kcol + HD] = tb[half:].astype(BF16)

        return [(1, dq), (1, dk), (1, o), (1, dv)]

    def back(g):
        b = g % 2

        def place(h, c):
            if h == 2:
                return r.dkf, c, r.dk, g * HD, r.kg
            return r.dqf, stacked(h, c), r.dq, (2 * g + h) * HD, r.qg

        def turn(h, c):
            src, o, _, _, g_ref = place(h, c)

            def run():
                d = src[b, o:o + CH, :].astype(BF16).astype(F32)
                that = r.raw[g, h, c:c + CH, :].astype(F32) * r.inv[g, h, c:c + CH, :]
                du = d[:, :HD] * r.tab[2, c:c + CH, :] - d[:, HD:] * r.tab[3, c:c + CH, :]
                src[b, o:o + CH, 0:HD] = du
                pr = du * that
                dg_ref = r.dgk if h == 2 else r.dgq
                dg_ref[...] += jnp.sum(pr.reshape(CH // 8, 8, HD), axis=0)
                r.sb[h, c:c + CH, :] = jnp.broadcast_to(jnp.mean(pr * g_ref[0:1, :], axis=-1, keepdims=True), (CH, HD))

            return (0.6, run)

        def out(h, c):
            src, o, out_ref, col, g_ref = place(h, c)

            def run():
                inv = r.inv[g, h, c:c + CH, :]
                that = r.raw[g, h, c:c + CH, :].astype(F32) * inv
                out_ref[c:c + CH, col:col + HD] = (inv * (src[b, o:o + CH, 0:HD] * g_ref[0:1, :] - that * r.sb[h, c:c + CH, :])).astype(BF16)

            return (0.5, run)

        return [f(h, c) for f in (turn, out) for h in (0, 1, 2) for c in range(0, seq, CH)]

    return SimpleNamespace(norm=norm_rows, proj=proj, rope=rope, scores=scores, soft=soft, grads=grads, back=back)


def attn_tick(st, g, n_grp):
    vec = st.soft((g - 3) % n_grp) + st.rope((g - 1) % n_grp) + st.back(g)
    gr = st.grads(g)
    for _, f in gr[:2]:
        f()
    weave(vec, st.scores((g - 2) % n_grp) + gr[2:] + st.proj(g))


def attn_scratch(seq, n_grp):
    return dict(
        qnew=pltpu.VMEM((2, 2, seq, HD), BF16),
        knew=pltpu.VMEM((n_grp, seq, HD), BF16),
        vnew=pltpu.VMEM((n_grp, seq, HD), BF16),
        raw=pltpu.VMEM((n_grp, 3, seq, HD), BF16),
        inv=pltpu.VMEM((n_grp, 3, seq, HD), F32),
        rot=pltpu.VMEM((n_grp, 3 * seq, 2 * HD), BF16),
        do=pltpu.VMEM((n_grp, 2 * seq, HD), BF16),
        v=pltpu.VMEM((n_grp, seq, HD), BF16),
        s=pltpu.VMEM((2, 2 * seq, seq), F32),
        dp=pltpu.VMEM((2, 2 * seq, seq), F32),
        p=pltpu.VMEM((2, 2 * seq, seq), BF16),
        ds=pltpu.VMEM((2, 2 * seq, seq), BF16),
        dkf=pltpu.VMEM((2, seq, 2 * HD), F32),
        dqf=pltpu.VMEM((2, 2 * seq, 2 * HD), F32),
        st=pltpu.VMEM((3, 2 * seq, HD), F32),
        sb=pltpu.VMEM((3, seq, HD), F32),
        tab=pltpu.VMEM((4, seq, HD), F32),
    )


def tail_kernel(seq, n_grp, rows, keys, sel_ref, n_in, dy_in, cos_in, sin_in, x_in, dyx_in, gain_ref, qg_ref, kg_ref, dgq_own, dgk_own, *refs):
    own_w, oth_w, own_a = refs[:4], refs[4:8], refs[8:12]
    y_out, dx_out, sums_out = refs[12:15]
    r = SimpleNamespace(n=n_in, dy=dy_in, qg=qg_ref, kg=kg_ref, gain=gain_ref, **dict(zip(keys, refs[15:])))
    step = pl.program_id(0)
    me = sel_ref[0]
    oth = 1 - me
    D = x_in.shape[1]
    r.wq = lambda c: r.wq_all[oth, :, c]
    r.wk = lambda c: r.wk_all[oth, :, c]
    r.wv = lambda c: r.wv_all[oth, :, c]
    r.do_dot = lambda c: dot(dy_in[...], r.wo_all[oth, c, :], NT)
    r.o, r.dq, r.dk, r.dv = r.oc.at[oth], r.dqc.at[oth], r.dkc.at[oth], r.dvc.at[oth]
    st = attn_stages(seq, n_grp, r)

    def fetch(row):
        return [pltpu.make_async_copy(src.at[me, pl.ds(row * seq, seq), :], dst.at[me], r.sem.at[8 + k])
                for k, (src, dst) in enumerate(zip(own_a, (r.oc, r.dqc, r.dkc, r.dvc)))]

    weights = (r.wq_all, r.wk_all, r.wv_all, r.wo_all)
    theirs = [pltpu.make_async_copy(oth_w[k], dst.at[oth], r.sem.at[4 + k]) for k, dst in enumerate(weights)]
    mine = [pltpu.make_async_copy(own_w[k], dst.at[me], r.sem.at[k]) for k, dst in enumerate(weights)]

    @pl.when(step == 0)
    def _():
        for c in theirs + mine:
            c.start()
        r.dg[...] = jnp.zeros_like(r.dg)
        for c in theirs:
            c.wait()

    @pl.when(step > 0)
    def _():
        for c in fetch(step - 1):
            c.start()

    CR, NC = 32, 256
    nn = D // NC
    lines = range(0, seq, CR)

    def wide(v):
        return jnp.concatenate([v] * (NC // HD), axis=1)

    def stat(c):
        def run():
            xf = x_in[c:c + CR, :].astype(F32)
            r.xs[0, c:c + CR, :] = jnp.broadcast_to(lax.rsqrt(jnp.mean(xf * xf, axis=-1, keepdims=True) + EPS), (CR, HD))
            r.xs[1, c:c + CR, :] = jnp.zeros((CR, HD), F32)

        return (1, run)

    def dn_dot(n):
        def run():
            cols = slice(n * NC, (n + 1) * NC)
            t = None
            for s in range(2):
                for a_ref, w_ref in ((r.dqc, r.wq_all), (r.dkc, r.wk_all), (r.dvc, r.wv_all)):
                    u = dot(a_ref[s], w_ref[s, cols, :], NT)
                    t = u if t is None else t + u
            r.dn[:, cols] = t

        return (2, run)

    def first(n, c):
        def run():
            cols = slice(n * NC, (n + 1) * NC)
            w = r.dn[c:c + CR, cols] * (x_in[c:c + CR, cols].astype(F32) * wide(r.xs[0, c:c + CR, :]))
            r.dg[:, cols] += jnp.sum(w.reshape(CR // 8, 8, NC), axis=0)
            w = w * gain_ref[0:1, cols]
            r.xs[1, c:c + CR, :] += w[:, :HD] + w[:, HD:]

        return (1, run)

    def mean(c):
        def run():
            r.xs[2, c:c + CR, :] = jnp.broadcast_to(jnp.sum(r.xs[1, c:c + CR, :], axis=-1, keepdims=True) * (1.0 / D), (CR, HD))

        return (0.2, run)

    def second(n, c):
        def run():
            cols = slice(n * NC, (n + 1) * NC)
            inv = wide(r.xs[0, c:c + CR, :])
            xh = x_in[c:c + CR, cols].astype(F32) * inv
            e = r.dn[c:c + CR, cols] * gain_ref[0:1, cols]
            dx_out[c:c + CR, cols] = (dyx_in[c:c + CR, cols].astype(F32) + inv * (e - xh * wide(r.xs[2, c:c + CR, :]))).astype(BF16)

        return (1.2, run)

    def y_dot(n):
        def run():
            cols = slice(n * NC, (n + 1) * NC)
            t = dot(r.oc[0], r.wo_all[0, :, cols]) + dot(r.oc[1], r.wo_all[1, :, cols])
            y_out[:, cols] = (x_in[:, cols].astype(F32) + t).astype(BF16)

        return (1, run)

    r.tab[2:4] = r.tab[0:2]
    r.tab[0] = cos_in[...]
    r.tab[1] = sin_in[...]
    for g in range(n_grp):
        attn_tick(st, g, n_grp)
    for acc in (r.dgq, r.dgk):
        acc[...] = jnp.where(step > 0, acc[...], 0.0)

    @pl.when(step == 0)
    def _():
        for c in mine:
            c.wait()

    @pl.when(step > 0)
    def _():
        for c in fetch(step - 1):
            c.wait()
        dn = [dn_dot(n) for n in range(nn)]
        yd = [y_dot(n) for n in range(nn)]
        for _, f in dn[:1]:
            f()
        weave([stat(c) for c in lines], dn[1:2])
        for n in range(2, nn):
            weave([first(n - 2, c) for c in lines], dn[n:n + 1])
        weave([first(nn - 2, c) for c in lines], yd[:1])
        weave([first(nn - 1, c) for c in lines] + [mean(c) for c in lines], yd[1:2])
        weave([second(n, c) for n in range(nn) for c in lines], yd[2:])

    @pl.when(step == rows)
    def _():
        sums_out[:, 0:D] = r.dg[...]
        sums_out[:, D:D + HD] = r.dgq[...] + dgq_own[...]
        sums_out[:, D + HD:] = r.dgk[...] + dgk_own[...]


def tail_call(sel, n, x, dy, cosd, sind, o, dq, dk, dv, gain, qg, kg, dgq, dgk, own, oth, seq=256):
    T, D = x.shape
    nq, nk = dq.shape[2], dk.shape[2]
    n_grp = nk // HD
    rows = T // seq
    lag = lambda k, c: pl.BlockSpec((seq, c), lambda i, s: (jnp.clip(i - k, 0, rows - 1), 0))
    const = lambda *b: pl.BlockSpec(b, lambda i, s: (0,) * len(b), pipeline_mode=pl.Buffered(1))
    hbm = pl.BlockSpec(memory_space=pl.ANY)
    scratch = attn_scratch(seq, n_grp)
    scratch.update(
        wq_all=pltpu.VMEM((2, D, nq), BF16), wk_all=pltpu.VMEM((2, D, nk), BF16), wv_all=pltpu.VMEM((2, D, nk), BF16), wo_all=pltpu.VMEM((2, nq, D), BF16),
        dn=pltpu.VMEM((seq, D), F32), oc=pltpu.VMEM((2, seq, nq), BF16), dqc=pltpu.VMEM((2, seq, nq), BF16), dkc=pltpu.VMEM((2, seq, nk), BF16), dvc=pltpu.VMEM((2, seq, nk), BF16),
        xs=pltpu.VMEM((3, seq, HD), F32), dg=pltpu.VMEM((8, D), F32), dgq=pltpu.VMEM((8, HD), F32), dgk=pltpu.VMEM((8, HD), F32), sem=pltpu.SemaphoreType.DMA((12,)))
    flops = 2 * T * D * (nq + 2 * nk + nq) * 3 + 12 * T * nq * seq
    return pl.pallas_call(
        functools.partial(tail_kernel, seq, n_grp, rows, tuple(scratch)),
        grid_spec=pltpu.PrefetchScalarGridSpec(
            num_scalar_prefetch=1,
            grid=(rows + 1,),
            in_specs=[lag(0, D), lag(0, D), lag(0, HD), lag(0, HD), lag(1, D), lag(1, D), const(1, D), const(1, HD), const(1, HD), const(8, HD), const(8, HD)] + [hbm] * 12,
            out_specs=[lag(1, D), lag(1, D), pl.BlockSpec((8, D + 2 * HD), lambda i, s: (0, 0))],
            scratch_shapes=list(scratch.values()),
        ),
        out_shape=[jax.ShapeDtypeStruct((T, D), BF16)] * 2 + [jax.ShapeDtypeStruct((8, D + 2 * HD), F32)],
        compiler_params=pltpu.CompilerParams(dimension_semantics=("arbitrary",), vmem_limit_bytes=67043328),
        cost_estimate=pl.CostEstimate(flops=flops, bytes_accessed=T * D * 14, transcendentals=T * nq * 2),
        name="tail",
    )(sel, n, dy, cosd, sind, x, dy, gain, qg, kg, dgq, dgk, *own, *oth, o, dq, dk, dv)


def solution(mesh):
    tok_spec = P("dp", None, None)
    col_spec = P(None, "tp")
    row_spec = P("tp", None)
    n_dp = mesh.shape["dp"]

    def per_device(x_in, dy_in, positions, g_attn, q_gain, k_gain, w_q, w_k, w_v, w_o):
        n_batch, n_seq, D = x_in.shape
        T = n_batch * n_seq
        nk = w_k.shape[1]
        x, dy = x_in.reshape(T, D), dy_in.reshape(T, D)
        me = lax.axis_index("tp").astype(jnp.int32)
        own = me.reshape(1)

        part = lax.axis_index("dp").astype(jnp.int32).reshape(1)
        share, cosd, sind = pre_call(part, w_q, w_k, w_v, w_o, positions, parts=n_dp)
        gathered = lax.all_gather(share, ("tp", "dp"), tiled=True)

        gain = g_attn.astype(F32).reshape(1, D)
        qg, kg = q_gain.astype(F32).reshape(1, HD), k_gain.astype(F32).reshape(1, HD)

        n, o, dq, dk, dv, dgq, dgk = attn_call(True, own, x, dy, cosd, sind, gain, qg, kg, w_q, w_k, w_v, w_o, seq=n_seq)
        dw_q, dw_k, dw_v = dw_call(own, n, [dq, dk, dv], 512)
        dw_o, *theirs = dw_call(own, o, [dy], 1024, gathered=gathered, nk=nk)
        dw_o, dw_q, dw_k, dw_v = lax.psum((dw_o, dw_q, dw_k, dw_v), "dp")

        y, dx, sums = tail_call(own, n, x, dy, cosd, sind, o, dq, dk, dv, gain, qg, kg, dgq, dgk, (w_q, w_k, w_v, w_o), theirs, seq=n_seq)
        g_sum, q_sum, k_sum = (t.reshape(-1) for t in sum_call(sums, (D, HD, HD), n_dp))
        dw_o, dw_q, dw_k, dw_v = copy_call((dw_o, dw_q, dw_k, dw_v))
        return y.reshape(x_in.shape), dx.reshape(x_in.shape), dw_q, dw_k, dw_v, dw_o, q_sum, k_sum, g_sum

    return jax.shard_map(per_device, mesh=mesh, in_specs=(tok_spec, tok_spec, P("dp", None), P(), P(), P(), col_spec, col_spec, col_spec, row_spec), out_specs=(tok_spec, tok_spec, col_spec, col_spec, col_spec, row_spec, P(), P(), P()), check_vma=False)
```

```python
import functools
from types import SimpleNamespace
import jax
import jax.numpy as jnp
from jax import lax
from jax.experimental import pallas as pl
from jax.experimental.pallas import tpu as pltpu
from jax.sharding import PartitionSpec as P


EPS = 1e-6
THETA = 1000000.0
F32 = jnp.float32
BF16 = jnp.bfloat16
HD = 128
NT = (((1,), (1,)), ((), ()))
TN = (((0,), (0,)), ((), ()))
NN = (((1,), (0,)), ((), ()))


def dot(a, b, dims=NN):
    return lax.dot_general(a, b, dims, preferred_element_type=F32)


def weave(*lists):
    order = []
    for n, pieces in enumerate(lists):
        total = sum(c for c, _ in pieces) or 1
        at = 0
        for k, (c, f) in enumerate(pieces):
            order.append(((at + c / 2) / total, n, k, f))
            at += c
    for _, _, _, f in sorted(order, key=lambda e: e[:3]):
        f()


CH = 32


def attn_kernel(own, seq, n_grp, sel_ref, *refs):
    if own:
        (x0_ref, xn_ref, dy_ref, cos_ref, sin_ref, gain_ref, qg_ref, kg_ref, wq_ref, wk_ref, wv_ref, wo_ref,
         n_out, o_out, dq_out, dk_out, dv_out, dgq_out, dgk_out) = refs[:19]
        refs = refs[19:]
    else:
        nin_ref, dy_ref, cos_ref, sin_ref, qg_ref, kg_ref, wq_ref, wk_ref, wv_ref, wo_ref, _, _, _, _, o_out, dq_out, dk_out, dv_out = refs[:18]
        refs = refs[18:]
        n_ref = nin_ref
    (wot_ref, qnew_ref, knew_ref, vnew_ref, raw_ref, inv_ref, rot_ref, do_ref, v_ref, s_ref, dp_ref, p_ref, ds_ref, dkf_ref, dqf_ref, st_ref,
     tab_ref, o_ref, dq_ref, dk_ref, dv_ref) = refs[:21]
    if own:
        n_ref, nn_ref, dgq_ref, dgk_ref = refs[21:]
    half = seq // 2
    scale = HD ** -0.5
    log2e = 1.4426950408889634
    step = pl.program_id(0)

    def norm_rows(src, dst):
        def piece(c):
            def run():
                xf = src[c:c + 32, :].astype(F32)
                inv = lax.rsqrt(jnp.mean(xf * xf, axis=-1, keepdims=True) + EPS)
                dst[c:c + 32, :] = (xf * inv * gain_ref[0:1, :]).astype(BF16)

            return (1.5, run)

        return [piece(c) for c in range(0, seq, 32)]

    def proj(g):
        def q():
            t = dot(n_ref[...], wq_ref[:, g * 2 * HD:(g + 1) * 2 * HD])
            for h in range(2):
                qnew_ref[g % 2, h] = t[:, h * HD:(h + 1) * HD].astype(BF16)

        def k():
            t = dot(n_ref[...], wk_ref[:, g * HD:(g + 2) * HD])
            for h in range(2):
                knew_ref[g + h] = t[:, h * HD:(h + 1) * HD].astype(BF16)

        def v():
            t = dot(n_ref[...], wv_ref[:, g * HD:(g + 2) * HD])
            for h in range(2):
                vnew_ref[g + h] = t[:, h * HD:(h + 1) * HD].astype(BF16)

        def do():
            t = dot(dy_ref[...], wot_ref[:, g * 2 * HD:(g + 1) * 2 * HD])
            for h in range(2):
                do_ref[g, h * half:(h + 1) * half, :] = t[:half, h * HD:(h + 1) * HD].astype(BF16)
                do_ref[g, seq + h * half:seq + (h + 1) * half, :] = t[half:, h * HD:(h + 1) * HD].astype(BF16)

        return [(1, q)] + ([(1, k), (1, v)] if g % 2 == 0 else []) + [(1, do)]

    def stacked(h, c):
        return (h * half + c) if c < half else (seq + h * half + c - half)

    def rope(g):
        cs, sn = (tab_ref.at[2], tab_ref.at[3]) if g == n_grp - 1 else (tab_ref.at[0], tab_ref.at[1])

        def size(h, c):
            def run():
                raw = knew_ref[g, c:c + CH, :] if h == 2 else qnew_ref[g % 2, h, c:c + CH, :]
                raw_ref[g, h, c:c + CH, :] = raw
                t = raw.astype(F32)
                inv_ref[g, h, c:c + CH, :] = jnp.broadcast_to(lax.rsqrt(jnp.mean(t * t, axis=-1, keepdims=True) + EPS), t.shape)

            return (0.4, run)

        def turn(h, c):
            def run():
                t = raw_ref[g, h, c:c + CH, :].astype(F32)
                w = (t * inv_ref[g, h, c:c + CH, :]) * (kg_ref if h == 2 else qg_ref)[0:1, :]
                o = 2 * seq + c if h == 2 else stacked(h, c)
                x = pltpu.roll(w, HD // 2, 1)
                co, si = cs[c:c + CH, :], sn[c:c + CH, :]
                rot_ref[g, o:o + CH, 0:HD] = (w * co + x * si).astype(BF16)
                rot_ref[g, o:o + CH, HD:] = (x * co - w * si).astype(BF16)
                if h == 2:
                    v_ref[g, c:c + CH, :] = vnew_ref[g, c:c + CH, :]

            return (0.6, run)

        return [f(h, c) for f in (size, turn) for h in (2, 0, 1) for c in range(0, seq, CH)]

    def scores(g):
        b = g % 2

        def s():
            s_ref[b, 0:seq, 0:half] = dot(rot_ref[g, 0:seq, 0:HD], rot_ref[g, 2 * seq:2 * seq + half, 0:HD], NT)
            s_ref[b, seq:, :] = dot(rot_ref[g, seq:2 * seq, 0:HD], rot_ref[g, 2 * seq:, 0:HD], NT)

        def dp():
            dp_ref[b, 0:seq, 0:half] = dot(do_ref[g, :seq, :], v_ref[g, :half, :], NT)
            dp_ref[b, seq:, :] = dot(do_ref[g, seq:, :], v_ref[g], NT)

        return [(1, s), (1, dp)]

    def soft(g):
        b = g % 2
        c2 = scale * log2e

        def part(blk, c):
            return slice(blk * seq + c, blk * seq + c + CH), half if blk == 0 else seq

        def masked(blk, c, s):
            row_id = lax.broadcasted_iota(jnp.int32, (CH, half), 0) + (c % half)
            keep = row_id >= lax.broadcasted_iota(jnp.int32, (CH, half), 1)
            if blk == 0:
                return jnp.where(keep, s, -jnp.inf)
            return jnp.concatenate([s[:, :half], jnp.where(keep, s[:, half:], -jnp.inf)], axis=1)

        def wide(ref, rows, width):
            t = ref[rows, :]
            return t if width == half else jnp.concatenate([t, t], axis=1)

        def top(blk, c):
            rows, width = part(blk, c)

            def run():
                m = jnp.max(masked(blk, c, s_ref[b, rows, 0:width]), axis=-1, keepdims=True)
                st_ref[0, rows, :] = jnp.broadcast_to(m * c2, (CH, HD))

            return (0.4 + 0.4 * blk, run)

        def power(blk, c):
            rows, width = part(blk, c)

            def run():
                e = jnp.exp2(masked(blk, c, s_ref[b, rows, 0:width] * c2) - wide(st_ref.at[0], rows, width))
                s_ref[b, rows, 0:width] = e
                st_ref[1, rows, :] = jnp.broadcast_to(1.0 / jnp.sum(e, axis=-1, keepdims=True), (CH, HD))

            return (0.8 + 0.8 * blk, run)

        def prob(blk, c):
            rows, width = part(blk, c)

            def run():
                pr = s_ref[b, rows, 0:width] * wide(st_ref.at[1], rows, width)
                s_ref[b, rows, 0:width] = pr
                p_ref[b, rows, 0:width] = pr.astype(BF16)
                st_ref[2, rows, :] = jnp.broadcast_to(jnp.sum(pr * dp_ref[b, rows, 0:width], axis=-1, keepdims=True), (CH, HD))

            return (0.8 + 0.8 * blk, run)

        def last(blk, c):
            rows, width = part(blk, c)

            def run():
                d = dp_ref[b, rows, 0:width] - wide(st_ref.at[2], rows, width)
                ds_ref[b, rows, 0:width] = (s_ref[b, rows, 0:width] * d * scale).astype(BF16)

            return (0.8 + 0.8 * blk, run)

        return [f(blk, c) for f in (top, power, prob, last) for blk in range(2) for c in range(0, seq, CH)]

    def grads(g):
        b = g % 2
        col, kcol = g * 2 * HD, g * HD

        def dq():
            dqf_ref[b, 0:seq, :] = dot(ds_ref[b, 0:seq, 0:half], rot_ref[g, 2 * seq:2 * seq + half, :])
            dqf_ref[b, seq:, :] = dot(ds_ref[b, seq:, :], rot_ref[g, 2 * seq:, :])

        def dk():
            tb = dot(ds_ref[b, seq:, :], rot_ref[g, seq:2 * seq, :], TN)
            ta = dot(ds_ref[b, 0:seq, 0:half], rot_ref[g, 0:seq, :], TN)
            dkf_ref[b, :half, :] = tb[:half] + ta
            dkf_ref[b, half:, :] = tb[half:]

        def o():
            ta = dot(p_ref[b, 0:seq, 0:half], v_ref[g, :half, :])
            tb = dot(p_ref[b, seq:, :], v_ref[g])
            for h in range(2):
                o_ref[0:half, col + h * HD:col + (h + 1) * HD] = ta[h * half:(h + 1) * half].astype(BF16)
                o_ref[half:seq, col + h * HD:col + (h + 1) * HD] = tb[h * half:(h + 1) * half].astype(BF16)

        def dv():
            tb = dot(p_ref[b, seq:, :], do_ref[g, seq:, :], TN)
            ta = dot(p_ref[b, 0:seq, 0:half], do_ref[g, :seq, :], TN)
            dv_ref[0:half, kcol:kcol + HD] = (tb[:half] + ta).astype(BF16)
            dv_ref[half:seq, kcol:kcol + HD] = tb[half:].astype(BF16)

        return [(1, dq), (1, dk), (1, o), (1, dv)]

    def back(g):
        b = g % 2

        def place(h, c):
            if h == 2:
                return dkf_ref, c, dk_ref, g * HD, kg_ref
            return dqf_ref, stacked(h, c), dq_ref, (2 * g + h) * HD, qg_ref

        def turn(h, c):
            src, o, _, _, g_ref = place(h, c)

            def run():
                d = src[b, o:o + CH, :].astype(BF16).astype(F32)
                that = raw_ref[g, h, c:c + CH, :].astype(F32) * inv_ref[g, h, c:c + CH, :]
                du = d[:, :HD] * tab_ref[2, c:c + CH, :] - d[:, HD:] * tab_ref[3, c:c + CH, :]
                src[b, o:o + CH, 0:HD] = du
                pr = du * that
                if own:
                    dg_ref = dgk_ref if h == 2 else dgq_ref
                    dg_ref[...] += jnp.sum(pr.reshape(CH // 8, 8, HD), axis=0)
                st_ref[3 + h, c:c + CH, :] = jnp.broadcast_to(jnp.mean(pr * g_ref[0:1, :], axis=-1, keepdims=True), (CH, HD))

            return (0.6, run)

        def out(h, c):
            src, o, out_ref, col, g_ref = place(h, c)

            def run():
                inv = inv_ref[g, h, c:c + CH, :]
                that = raw_ref[g, h, c:c + CH, :].astype(F32) * inv
                out_ref[c:c + CH, col:col + HD] = (inv * (src[b, o:o + CH, 0:HD] * g_ref[0:1, :] - that * st_ref[3 + h, c:c + CH, :])).astype(BF16)

            return (0.5, run)

        return [f(h, c) for f in (turn, out) for h in (0, 1, 2) for c in range(0, seq, CH)]

    @pl.when(step == 0)
    def _():
        @pl.loop(0, wo_ref.shape[0] // 256)
        def _(j):
            c = pl.ds(pl.multiple_of(j * 256, 256), 256)
            for d in range(0, wo_ref.shape[1], 256):
                wot_ref[d:d + 256, c] = wo_ref[c, d:d + 256].T

        if own:
            weave(norm_rows(x0_ref, n_ref))

    tab_ref[2:4] = tab_ref[0:2]
    tab_ref[0] = cos_ref[...]
    tab_ref[1] = sin_ref[...]
    if own:
        norms = norm_rows(xn_ref, nn_ref)
    for g in range(n_grp):
        sc = scores((g - 2) % n_grp)
        gr = grads(g)
        nm = norms[g * len(norms) // n_grp:(g + 1) * len(norms) // n_grp] if own else []
        for _, f in gr[:2]:
            f()
        weave(soft((g - 3) % n_grp), rope((g - 1) % n_grp) + nm, back(g), sc + gr[2:] + proj(g))

    for dst, src in ((o_out, o_ref), (dq_out, dq_ref), (dk_out, dk_ref), (dv_out, dv_ref)):
        dst[0] = src[...]
    if own:
        n_out[...] = n_ref[...]
        n_ref[...] = nn_ref[...]
        keep = step > 0
        for dst, acc in ((dgq_out, dgq_ref), (dgk_out, dgk_ref)):
            acc[...] = jnp.where(keep, acc[...], 0.0)
            dst[...] = acc[...]


def attn_call(own, sel, x, dy, cosd, sind, gain, qg, kg, wq, wk, wv, wo, prev=None, seq=256):
    T, D = x.shape
    nq, nk = wq.shape[1], wk.shape[1]
    n_grp = nk // HD
    rows = T // seq
    const = lambda *b: pl.BlockSpec(b, lambda i, s: (0,) * len(b), pipeline_mode=pl.Buffered(1))
    now = lambda c: pl.BlockSpec((seq, c), lambda i, s: (jnp.minimum(i, rows - 1), 0))
    nxt = lambda c: pl.BlockSpec((seq, c), lambda i, s: (jnp.minimum(i + 1, rows - 1), 0))
    out3 = lambda c: pl.BlockSpec((1, seq, c), lambda i, s: (s[0], jnp.maximum(i - 1, 0), 0))
    mid = [now(D), now(HD), now(HD)]
    tail = [const(1, HD), const(1, HD), const(D, nq), const(D, nk), const(D, nk), const(nq, D)]
    shapes = [jax.ShapeDtypeStruct((2, T, c), BF16) for c in (nq, nq, nk, nk)]
    specs = [out3(nq), out3(nq), out3(nk), out3(nk)]
    aliases = {}
    if own:
        in_specs = [const(seq, D), nxt(D)] + mid + [const(1, D)] + tail
        args = [x, x, dy, cosd, sind, gain, qg, kg, wq, wk, wv, wo]
        shapes = [jax.ShapeDtypeStruct((T, D), BF16)] + shapes + [jax.ShapeDtypeStruct((8, HD), F32)] * 2
        specs = [now(D)] + specs + [pl.BlockSpec((8, HD), lambda i, s: (0, 0))] * 2
    else:
        in_specs = [now(D)] + mid + tail + [pl.BlockSpec(memory_space=pl.ANY)] * 4
        args = [x, dy, cosd, sind, qg, kg, wq, wk, wv, wo]
        aliases = {1 + len(args) + i: i for i in range(4)}
        args += list(prev)
    flops = 2 * T * D * (nq + 2 * nk + nq) + 12 * T * nq * seq
    return pl.pallas_call(
        functools.partial(attn_kernel, own, seq, n_grp),
        grid_spec=pltpu.PrefetchScalarGridSpec(
            num_scalar_prefetch=1,
            grid=(rows + 1,),
            in_specs=in_specs,
            out_specs=specs,
            scratch_shapes=[
                pltpu.VMEM((D, nq), BF16),
                pltpu.VMEM((2, 2, seq, HD), BF16),
                pltpu.VMEM((n_grp, seq, HD), BF16),
                pltpu.VMEM((n_grp, seq, HD), BF16),
                pltpu.VMEM((n_grp, 3, seq, HD), BF16),
                pltpu.VMEM((n_grp, 3, seq, HD), F32),
                pltpu.VMEM((n_grp, 3 * seq, 2 * HD), BF16),
                pltpu.VMEM((n_grp, 2 * seq, HD), BF16),
                pltpu.VMEM((n_grp, seq, HD), BF16),
                pltpu.VMEM((2, 2 * seq, seq), F32),
                pltpu.VMEM((2, 2 * seq, seq), F32),
                pltpu.VMEM((2, 2 * seq, seq), BF16),
                pltpu.VMEM((2, 2 * seq, seq), BF16),
                pltpu.VMEM((2, seq, 2 * HD), F32),
                pltpu.VMEM((2, 2 * seq, 2 * HD), F32),
                pltpu.VMEM((6, 2 * seq, HD), F32),
                pltpu.VMEM((4, seq, HD), F32),
            ] + [pltpu.VMEM((seq, c), BF16) for c in (nq, nq, nk, nk)]
            + ([pltpu.VMEM((seq, D), BF16)] * 2 + [pltpu.VMEM((8, HD), F32)] * 2 if own else []),
        ),
        out_shape=shapes,
        input_output_aliases=aliases,
        compiler_params=pltpu.CompilerParams(dimension_semantics=("arbitrary",), vmem_limit_bytes=56 << 20),
        cost_estimate=pl.CostEstimate(flops=flops, bytes_accessed=T * D * 6 + T * (2 * nq + 2 * nk) * 2, transcendentals=T * nq * 2),
        name="attn_own" if own else "attn_other",
    )(sel, *args)


def pre_kernel(sel_ref, q_ref, k_ref, v_ref, o_ref, pos_ref, freq_ref, out_ref, cos_ref, sin_ref):
    d, nq, nk = q_ref.shape[0], q_ref.shape[1], k_ref.shape[1]
    out_ref[0, 0:d, 0:nq] = q_ref[...].astype(F32)
    out_ref[0, 0:d, nq:nq + nk] = k_ref[...].astype(F32)
    out_ref[0, 0:d, nq + nk:] = v_ref[...].astype(F32)
    out_ref[0, d:, :] = o_ref[...].astype(F32)
    n, seq = pos_ref.shape
    lane = lax.broadcasted_iota(jnp.int32, (HD, HD), 1)
    for r in range(n):
        for h in range(seq // HD):
            p = pos_ref[r:r + 1, h * HD:(h + 1) * HD].astype(F32)
            a = jnp.broadcast_to(p, (HD, HD)).T * freq_ref[0:1, :]
            k = jnp.round(a * 0.6366197723675814)
            x = ((a - k * 1.5703125) - k * 4.837512969970703125e-4) - k * 7.549789948768648e-8
            z = x * x
            s = ((-1.9515295891e-4 * z + 8.3321608736e-3) * z - 1.6666654611e-1) * z * x + x
            c = ((2.443315711809948e-5 * z - 1.388731625493765e-3) * z + 4.166664568298827e-2) * z * z - 0.5 * z + 1.0
            q = k.astype(jnp.int32)
            odd = (q & 1) == 1
            co, si = jnp.where(odd, s, c), jnp.where(odd, c, s)
            rows = slice((r * (seq // HD) + h) * HD, (r * (seq // HD) + h + 1) * HD)
            cos_ref[rows, :] = jnp.where(((q + 1) & 2) == 0, co, -co)
            sin_ref[rows, :] = jnp.where(((q & 2) == 0) == (lane >= HD // 2), si, -si)


def pre_call(part, w_q, w_k, w_v, w_o, positions, parts=2, cuts=4):
    D, nq = w_q.shape
    n, seq = positions.shape
    rows = n // cuts
    freq = THETA ** (-jnp.arange(0, HD, 2, dtype=F32) / HD)
    freq = jnp.concatenate([freq, freq]).reshape(1, HD)
    spec = lambda w: pl.BlockSpec((w.shape[0] // (parts * cuts), w.shape[1]), lambda i, s: (s[0] * cuts + i, 0))
    r = (D + nq) // (parts * cuts)
    table = pl.BlockSpec((rows * seq, HD), lambda i, s: (i, 0))
    return pl.pallas_call(
        pre_kernel,
        grid_spec=pltpu.PrefetchScalarGridSpec(
            num_scalar_prefetch=1,
            grid=(cuts,),
            in_specs=[spec(w) for w in (w_q, w_k, w_v, w_o)] + [pl.BlockSpec((rows, seq), lambda i, s: (i, 0)), pl.BlockSpec((1, HD), lambda i, s: (0, 0))],
            out_specs=[pl.BlockSpec((1, r, D), lambda i, s: (i, 0, 0)), table, table],
        ),
        out_shape=[jax.ShapeDtypeStruct((cuts, r, D), F32)] + [jax.ShapeDtypeStruct((n * seq, HD), F32)] * 2,
        compiler_params=pltpu.CompilerParams(dimension_semantics=("arbitrary",), vmem_limit_bytes=60 << 20),
        cost_estimate=pl.CostEstimate(flops=n * seq * HD * 30, bytes_accessed=cuts * r * D * 6 + n * seq * HD * 8, transcendentals=0),
        name="pre",
    )(part, w_q, w_k, w_v, w_o, positions, freq)


def dw_kernel(n_b, unpack, sel_ref, a_ref, *refs):
    if unpack:
        f_ref, parts = refs[n_b], refs[2 * n_b + 1:2 * n_b + 5]
        refs = refs[:n_b] + refs[n_b + 1:2 * n_b + 1] + refs[2 * n_b + 5:]
        q_ref, k_ref, v_ref, o_ref = parts
        per, nq, nk = f_ref.shape[0], q_ref.shape[1], k_ref.shape[1]
        d, e = q_ref.shape[0] // per, o_ref.shape[0] // per
        for j in range(per):
            q_ref[j * d:(j + 1) * d, :] = f_ref[j, 0:d, 0:nq].astype(BF16)
            k_ref[j * d:(j + 1) * d, :] = f_ref[j, 0:d, nq:nq + nk].astype(BF16)
            v_ref[j * d:(j + 1) * d, :] = f_ref[j, 0:d, nq + nk:].astype(BF16)
            o_ref[j * e:(j + 1) * e, :] = f_ref[j, d:, :].astype(BF16)
    bs, outs, accs, (at_ref, sem) = refs[:n_b], refs[n_b:2 * n_b], refs[2 * n_b:3 * n_b], refs[3 * n_b:]
    flat = lambda ref: ref.at[0] if len(ref.shape) == 3 else ref
    a, bs = flat(a_ref), [flat(b) for b in bs]
    M, tile = at_ref.shape
    step = pl.program_id(0)

    @pl.when(step == 0)
    def _():
        for acc in accs:
            @pl.loop(0, M // 64)
            def _(j):
                acc[pl.ds(pl.multiple_of(j * 64, 64), 64), :] = jnp.zeros((64, acc.shape[1]), F32)

    def part(acc, b, c):
        def run():
            acc[:, c:c + 256] += dot(at_ref[...], b[:, c:c + 256])

        return (1, run)

    for c in range(0, M, 256):
        for k in range(0, tile, 256):
            at_ref[c:c + 256, k:k + 256] = a[k:k + 256, c:c + 256].T
    weave([part(acc, b, c) for acc, b in zip(accs, bs) for c in range(0, b.shape[1], 256)])

    @pl.when(step == pl.num_programs(0) - 1)
    def _():
        copies = [pltpu.make_async_copy(acc, out, sem.at[k]) for k, (acc, out) in enumerate(zip(accs, outs))]
        for c in copies:
            c.start()
        for c in copies:
            c.wait()


def dw_call(sel, a, bs, tile, gathered=None, nk=0):
    def spec(v):
        if v.ndim == 3:
            return pl.BlockSpec((1, tile, v.shape[2]), lambda i, s: (s[0], i, 0))
        return pl.BlockSpec((tile, v.shape[1]), lambda i, s: (i, 0))

    T, M = a.shape[-2:]
    shapes = [(M, b.shape[-1]) for b in bs]
    width = sum(s[1] for s in shapes)
    steps = T // tile
    more_in, more_out, more_shapes, more = [], [], [], []
    if gathered is not None:
        n, r, D = gathered.shape
        per = n // 2 // steps
        more = [gathered]
        more_in = [pl.BlockSpec((per, r, D), lambda i, s: ((1 - s[0]) * steps + i, 0, 0))]
        nq = D - 2 * nk
        more_shapes = [jax.ShapeDtypeStruct(s, BF16) for s in ((D, nq), (D, nk), (D, nk), (nq, D))]
        more_out = [pl.BlockSpec((s.shape[0] // steps, s.shape[1]), lambda i, s: (i, 0)) for s in more_shapes]
    return pl.pallas_call(
        functools.partial(dw_kernel, len(bs), gathered is not None),
        grid_spec=pltpu.PrefetchScalarGridSpec(
            num_scalar_prefetch=1,
            grid=(steps,),
            in_specs=[spec(a)] + [spec(b) for b in bs] + more_in,
            out_specs=[pl.BlockSpec(memory_space=pl.ANY)] * len(bs) + more_out,
            scratch_shapes=[pltpu.VMEM(s, F32) for s in shapes] + [pltpu.VMEM((M, tile), BF16), pltpu.SemaphoreType.DMA((len(bs),))],
        ),
        out_shape=[jax.ShapeDtypeStruct(s, F32) for s in shapes] + more_shapes,
        compiler_params=pltpu.CompilerParams(dimension_semantics=("arbitrary",), vmem_limit_bytes=60 << 20),
        cost_estimate=pl.CostEstimate(flops=2 * T * M * width, bytes_accessed=2 * T * (M + width) + 4 * M * width, transcendentals=0),
    )(sel, a, *bs, *more)


def sum_kernel(n, widths, part_ref, *refs):
    outs, (slots, local_sem, send_sem, recv_sem) = refs[:-4], refs[-4:]
    me = lax.axis_index("dp")
    barrier = pltpu.get_barrier_semaphore()
    for k in range(1, n):
        pl.semaphore_signal(barrier, inc=1, device_id={"dp": lax.rem(me + k, n)}, device_id_type=pl.DeviceIdType.MESH)
    mine = pltpu.make_async_copy(part_ref, slots.at[0], local_sem)
    mine.start()
    pl.semaphore_wait(barrier, n - 1)
    copies = []
    for k in range(1, n):
        copies.append(pltpu.make_async_remote_copy(
            src_ref=part_ref, dst_ref=slots.at[k], send_sem=send_sem.at[k - 1], recv_sem=recv_sem.at[k - 1],
            device_id={"dp": lax.rem(me + k, n)}, device_id_type=pl.DeviceIdType.MESH))
    for c in copies:
        c.start()
    mine.wait()
    for c in copies:
        c.wait()
    total = slots[lax.rem(me + n, n)]
    for a in range(1, n):
        total = total + slots[lax.rem(me + n - a, n)]
    total = jnp.sum(total, axis=0, keepdims=True)
    at = 0
    for out, w in zip(outs, widths):
        out[...] = total[:, at:at + w]
        at += w


def sum_call(part, widths, n):
    return pl.pallas_call(
        functools.partial(sum_kernel, n, widths),
        in_specs=[pl.BlockSpec(memory_space=pl.ANY)],
        out_specs=[pl.BlockSpec(memory_space=pltpu.VMEM)] * len(widths),
        out_shape=[jax.ShapeDtypeStruct((1, w), F32) for w in widths],
        scratch_shapes=[pltpu.VMEM((n, *part.shape), F32), pltpu.SemaphoreType.DMA, pltpu.SemaphoreType.DMA((n - 1,)), pltpu.SemaphoreType.DMA((n - 1,))],
        compiler_params=pltpu.CompilerParams(collective_id=0, has_side_effects=True),
        cost_estimate=pl.CostEstimate(flops=n * part.size, bytes_accessed=8 * n * part.size, transcendentals=0),
        name="small_sum",
    )(part)


def copy_kernel(n, *refs):
    for src, dst in zip(refs[:n], refs[n:]):
        dst[...] = src[...]


def copy_call(arrays, steps=8):
    specs = [pl.BlockSpec((a.shape[0] // steps, a.shape[1]), lambda i: (i, 0)) for a in arrays]
    return pl.pallas_call(
        functools.partial(copy_kernel, len(arrays)),
        grid=(steps,),
        in_specs=specs,
        out_specs=specs,
        out_shape=[jax.ShapeDtypeStruct(a.shape, a.dtype) for a in arrays],
        compiler_params=pltpu.CompilerParams(dimension_semantics=("arbitrary",), vmem_limit_bytes=60 << 20),
        cost_estimate=pl.CostEstimate(flops=0, bytes_accessed=8 * sum(a.size for a in arrays), transcendentals=0),
        name="results",
    )(*arrays)


def attn_stages(seq, n_grp, r):
    half = seq // 2
    scale = HD ** -0.5
    log2e = 1.4426950408889634

    def norm_rows(src, dst):
        def piece(c):
            def run():
                xf = src[c:c + 32, :].astype(F32)
                inv = lax.rsqrt(jnp.mean(xf * xf, axis=-1, keepdims=True) + EPS)
                dst[c:c + 32, :] = (xf * inv * r.gain[0:1, :]).astype(BF16)

            return (1.5, run)

        return [piece(c) for c in range(0, seq, 32)]

    def proj(g):
        def q():
            t = dot(r.n[...], r.wq(slice(g * 2 * HD, (g + 1) * 2 * HD)))
            for h in range(2):
                r.qnew[g % 2, h] = t[:, h * HD:(h + 1) * HD].astype(BF16)

        def k():
            t = dot(r.n[...], r.wk(slice(g * HD, (g + 2) * HD)))
            for h in range(2):
                r.knew[g + h] = t[:, h * HD:(h + 1) * HD].astype(BF16)

        def v():
            t = dot(r.n[...], r.wv(slice(g * HD, (g + 2) * HD)))
            for h in range(2):
                r.vnew[g + h] = t[:, h * HD:(h + 1) * HD].astype(BF16)

        def do():
            t = r.do_dot(slice(g * 2 * HD, (g + 1) * 2 * HD))
            for h in range(2):
                r.do[g, h * half:(h + 1) * half, :] = t[:half, h * HD:(h + 1) * HD].astype(BF16)
                r.do[g, seq + h * half:seq + (h + 1) * half, :] = t[half:, h * HD:(h + 1) * HD].astype(BF16)

        return [(1, q)] + ([(1, k), (1, v)] if g % 2 == 0 else []) + [(1, do)]

    def stacked(h, c):
        return (h * half + c) if c < half else (seq + h * half + c - half)

    def rope(g):
        cs, sn = (r.tab.at[2], r.tab.at[3]) if g == n_grp - 1 else (r.tab.at[0], r.tab.at[1])

        def size(h, c):
            def run():
                raw = r.knew[g, c:c + CH, :] if h == 2 else r.qnew[g % 2, h, c:c + CH, :]
                r.raw[g, h, c:c + CH, :] = raw
                t = raw.astype(F32)
                r.inv[g, h, c:c + CH, :] = jnp.broadcast_to(lax.rsqrt(jnp.mean(t * t, axis=-1, keepdims=True) + EPS), t.shape)

            return (0.4, run)

        def turn(h, c):
            def run():
                t = r.raw[g, h, c:c + CH, :].astype(F32)
                w = (t * r.inv[g, h, c:c + CH, :]) * (r.kg if h == 2 else r.qg)[0:1, :]
                o = 2 * seq + c if h == 2 else stacked(h, c)
                x = pltpu.roll(w, HD // 2, 1)
                co, si = cs[c:c + CH, :], sn[c:c + CH, :]
                r.rot[g, o:o + CH, 0:HD] = (w * co + x * si).astype(BF16)
                r.rot[g, o:o + CH, HD:] = (x * co - w * si).astype(BF16)
                if h == 2:
                    r.v[g, c:c + CH, :] = r.vnew[g, c:c + CH, :]

            return (0.6, run)

        return [f(h, c) for f in (size, turn) for h in (2, 0, 1) for c in range(0, seq, CH)]

    def scores(g):
        b = g % 2

        def s():
            r.s[b, 0:seq, 0:half] = dot(r.rot[g, 0:seq, 0:HD], r.rot[g, 2 * seq:2 * seq + half, 0:HD], NT)
            r.s[b, seq:, :] = dot(r.rot[g, seq:2 * seq, 0:HD], r.rot[g, 2 * seq:, 0:HD], NT)

        def dp():
            r.dp[b, 0:seq, 0:half] = dot(r.do[g, :seq, :], r.v[g, :half, :], NT)
            r.dp[b, seq:, :] = dot(r.do[g, seq:, :], r.v[g], NT)

        return [(1, s), (1, dp)]

    def soft(g):
        b = g % 2
        c2 = scale * log2e

        def part(blk, c):
            return slice(blk * seq + c, blk * seq + c + CH), half if blk == 0 else seq

        def masked(blk, c, s):
            row_id = lax.broadcasted_iota(jnp.int32, (CH, half), 0) + (c % half)
            keep = row_id >= lax.broadcasted_iota(jnp.int32, (CH, half), 1)
            if blk == 0:
                return jnp.where(keep, s, -jnp.inf)
            return jnp.concatenate([s[:, :half], jnp.where(keep, s[:, half:], -jnp.inf)], axis=1)

        def wide(ref, rows, width):
            t = ref[rows, :]
            return t if width == half else jnp.concatenate([t, t], axis=1)

        def top(blk, c):
            rows, width = part(blk, c)

            def run():
                m = jnp.max(masked(blk, c, r.s[b, rows, 0:width]), axis=-1, keepdims=True)
                r.st[0, rows, :] = jnp.broadcast_to(m * c2, (CH, HD))

            return (0.4 + 0.4 * blk, run)

        def power(blk, c):
            rows, width = part(blk, c)

            def run():
                e = jnp.exp2(masked(blk, c, r.s[b, rows, 0:width] * c2) - wide(r.st.at[0], rows, width))
                r.s[b, rows, 0:width] = e
                r.st[1, rows, :] = jnp.broadcast_to(1.0 / jnp.sum(e, axis=-1, keepdims=True), (CH, HD))

            return (0.8 + 0.8 * blk, run)

        def prob(blk, c):
            rows, width = part(blk, c)

            def run():
                pr = r.s[b, rows, 0:width] * wide(r.st.at[1], rows, width)
                r.s[b, rows, 0:width] = pr
                r.p[b, rows, 0:width] = pr.astype(BF16)
                r.st[2, rows, :] = jnp.broadcast_to(jnp.sum(pr * r.dp[b, rows, 0:width], axis=-1, keepdims=True), (CH, HD))

            return (0.8 + 0.8 * blk, run)

        def last(blk, c):
            rows, width = part(blk, c)

            def run():
                d = r.dp[b, rows, 0:width] - wide(r.st.at[2], rows, width)
                r.ds[b, rows, 0:width] = (r.s[b, rows, 0:width] * d * scale).astype(BF16)

            return (0.8 + 0.8 * blk, run)

        return [f(blk, c) for f in (top, power, prob, last) for blk in range(2) for c in range(0, seq, CH)]

    def grads(g):
        b = g % 2
        col, kcol = g * 2 * HD, g * HD

        def dq():
            r.dqf[b, 0:seq, :] = dot(r.ds[b, 0:seq, 0:half], r.rot[g, 2 * seq:2 * seq + half, :])
            r.dqf[b, seq:, :] = dot(r.ds[b, seq:, :], r.rot[g, 2 * seq:, :])

        def dk():
            tb = dot(r.ds[b, seq:, :], r.rot[g, seq:2 * seq, :], TN)
            ta = dot(r.ds[b, 0:seq, 0:half], r.rot[g, 0:seq, :], TN)
            r.dkf[b, :half, :] = tb[:half] + ta
            r.dkf[b, half:, :] = tb[half:]

        def o():
            ta = dot(r.p[b, 0:seq, 0:half], r.v[g, :half, :])
            tb = dot(r.p[b, seq:, :], r.v[g])
            for h in range(2):
                r.o[0:half, col + h * HD:col + (h + 1) * HD] = ta[h * half:(h + 1) * half].astype(BF16)
                r.o[half:seq, col + h * HD:col + (h + 1) * HD] = tb[h * half:(h + 1) * half].astype(BF16)

        def dv():
            tb = dot(r.p[b, seq:, :], r.do[g, seq:, :], TN)
            ta = dot(r.p[b, 0:seq, 0:half], r.do[g, :seq, :], TN)
            r.dv[0:half, kcol:kcol + HD] = (tb[:half] + ta).astype(BF16)
            r.dv[half:seq, kcol:kcol + HD] = tb[half:].astype(BF16)

        return [(1, dq), (1, dk), (1, o), (1, dv)]

    def back(g):
        b = g % 2

        def place(h, c):
            if h == 2:
                return r.dkf, c, r.dk, g * HD, r.kg
            return r.dqf, stacked(h, c), r.dq, (2 * g + h) * HD, r.qg

        def turn(h, c):
            src, o, _, _, g_ref = place(h, c)

            def run():
                d = src[b, o:o + CH, :].astype(BF16).astype(F32)
                that = r.raw[g, h, c:c + CH, :].astype(F32) * r.inv[g, h, c:c + CH, :]
                du = d[:, :HD] * r.tab[2, c:c + CH, :] - d[:, HD:] * r.tab[3, c:c + CH, :]
                src[b, o:o + CH, 0:HD] = du
                pr = du * that
                dg_ref = r.dgk if h == 2 else r.dgq
                dg_ref[...] += jnp.sum(pr.reshape(CH // 8, 8, HD), axis=0)
                r.sb[h, c:c + CH, :] = jnp.broadcast_to(jnp.mean(pr * g_ref[0:1, :], axis=-1, keepdims=True), (CH, HD))

            return (0.6, run)

        def out(h, c):
            src, o, out_ref, col, g_ref = place(h, c)

            def run():
                inv = r.inv[g, h, c:c + CH, :]
                that = r.raw[g, h, c:c + CH, :].astype(F32) * inv
                out_ref[c:c + CH, col:col + HD] = (inv * (src[b, o:o + CH, 0:HD] * g_ref[0:1, :] - that * r.sb[h, c:c + CH, :])).astype(BF16)

            return (0.5, run)

        return [f(h, c) for f in (turn, out) for h in (0, 1, 2) for c in range(0, seq, CH)]

    return SimpleNamespace(norm=norm_rows, proj=proj, rope=rope, scores=scores, soft=soft, grads=grads, back=back)


def attn_tick(st, g, n_grp, more=()):
    gr = st.grads(g)
    for _, f in gr[:2]:
        f()
    weave(st.soft((g - 3) % n_grp), st.rope((g - 1) % n_grp), st.back(g), st.scores((g - 2) % n_grp) + gr[2:] + st.proj(g) + list(more))


def attn_scratch(seq, n_grp):
    return dict(
        qnew=pltpu.VMEM((2, 2, seq, HD), BF16),
        knew=pltpu.VMEM((n_grp, seq, HD), BF16),
        vnew=pltpu.VMEM((n_grp, seq, HD), BF16),
        raw=pltpu.VMEM((n_grp, 3, seq, HD), BF16),
        inv=pltpu.VMEM((n_grp, 3, seq, HD), F32),
        rot=pltpu.VMEM((n_grp, 3 * seq, 2 * HD), BF16),
        do=pltpu.VMEM((n_grp, 2 * seq, HD), BF16),
        v=pltpu.VMEM((n_grp, seq, HD), BF16),
        s=pltpu.VMEM((2, 2 * seq, seq), F32),
        dp=pltpu.VMEM((2, 2 * seq, seq), F32),
        p=pltpu.VMEM((2, 2 * seq, seq), BF16),
        ds=pltpu.VMEM((2, 2 * seq, seq), BF16),
        dkf=pltpu.VMEM((2, seq, 2 * HD), F32),
        dqf=pltpu.VMEM((2, 2 * seq, 2 * HD), F32),
        st=pltpu.VMEM((3, 2 * seq, HD), F32),
        sb=pltpu.VMEM((3, seq, HD), F32),
        tab=pltpu.VMEM((4, seq, HD), F32),
    )


EARLY = 4


def tail_kernel(seq, n_grp, rows, keys, sel_ref, n_in, dy_in, cos_in, sin_in, x_in, dyx_in, gain_ref, qg_ref, kg_ref, dgq_own, dgk_own, *refs):
    own_w, oth_w, own_a = refs[:4], refs[4:8], refs[8:12]
    y_out, dx_out, sums_out = refs[12:15]
    r = SimpleNamespace(n=n_in, dy=dy_in, qg=qg_ref, kg=kg_ref, gain=gain_ref, **dict(zip(keys, refs[15:])))
    step = pl.program_id(0)
    me = sel_ref[0]
    oth = 1 - me
    D = x_in.shape[1]
    r.wq = lambda c: r.wq_all[oth, :, c]
    r.wk = lambda c: r.wk_all[oth, :, c]
    r.wv = lambda c: r.wv_all[oth, :, c]
    r.do_dot = lambda c: dot(dy_in[...], r.wo_all[oth, c, :], NT)
    r.o, r.dq, r.dk, r.dv = r.oc.at[oth], r.dqc.at[oth], r.dkc.at[oth], r.dvc.at[oth]
    st = attn_stages(seq, n_grp, r)

    def fetch(row):
        return [pltpu.make_async_copy(src.at[me, pl.ds(row * seq, seq), :], dst.at[me], r.sem.at[8 + k])
                for k, (src, dst) in enumerate(zip(own_a[1:], (r.dqc, r.dkc, r.dvc)))]

    def fetch_o(row):
        return pltpu.make_async_copy(own_a[0].at[me, pl.ds(row * seq, seq), :], r.o_next, r.sem.at[11])

    weights = (r.wq_all, r.wk_all, r.wv_all, r.wo_all)
    theirs = [pltpu.make_async_copy(oth_w[k], dst.at[oth], r.sem.at[4 + k]) for k, dst in enumerate(weights)]
    mine = [pltpu.make_async_copy(own_w[k], dst.at[me], r.sem.at[k]) for k, dst in enumerate(weights)]

    @pl.when(step == 0)
    def _():
        for c in theirs + mine[3:] + mine[:3]:
            c.start()
        r.dg[...] = jnp.zeros_like(r.dg)
        r.oc[...] = jnp.zeros_like(r.oc)
        for c in theirs + mine[3:]:
            c.wait()

    @pl.when(step > 0)
    def _():
        for c in fetch(step - 1):
            c.start()
        fetch_o(step - 1).wait()
        r.oc[me] = r.o_next[...]

    @pl.when(step < rows)
    def _():
        fetch_o(step).start()

    CR, NC = 32, 256
    nn = D // NC
    lines = range(0, seq, CR)

    def wide(v):
        return jnp.concatenate([v] * (NC // HD), axis=1)

    def stat(c):
        def run():
            xf = x_in[c:c + CR, :].astype(F32)
            r.xs[0, c:c + CR, :] = jnp.broadcast_to(lax.rsqrt(jnp.mean(xf * xf, axis=-1, keepdims=True) + EPS), (CR, HD))
            r.xs[1, c:c + CR, :] = jnp.zeros((CR, HD), F32)

        return (1, run)

    def dn_dot(n):
        def run():
            cols = slice(n * NC, (n + 1) * NC)
            t = None
            for s in range(2):
                for a_ref, w_ref in ((r.dqc, r.wq_all), (r.dkc, r.wk_all), (r.dvc, r.wv_all)):
                    u = dot(a_ref[s], w_ref[s, cols, :], NT)
                    t = u if t is None else t + u
            r.dn[:, cols] = t

        return (2, run)

    def first(n, c):
        def run():
            cols = slice(n * NC, (n + 1) * NC)
            inv = wide(r.xs[0, c:c + CR, :])
            d = r.dn[c:c + CR, cols]
            w = d * (x_in[c:c + CR, cols].astype(F32) * inv)
            r.dg[:, cols] += jnp.sum(w.reshape(CR // 8, 8, NC), axis=0)
            w = w * gain_ref[0:1, cols]
            r.xs[1, c:c + CR, :] += w[:, :HD] + w[:, HD:]
            r.dn[c:c + CR, cols] = dyx_in[c:c + CR, cols].astype(F32) + inv * (d * gain_ref[0:1, cols])

        return (1, run)

    def mean(c):
        def run():
            inv = r.xs[0, c:c + CR, :]
            r.xs[2, c:c + CR, :] = jnp.sum(r.xs[1, c:c + CR, :], axis=-1, keepdims=True) * (1.0 / D) * (inv * inv)

        return (0.2, run)

    def second(n, c):
        def run():
            cols = slice(n * NC, (n + 1) * NC)
            dx_out[c:c + CR, cols] = (r.dn[c:c + CR, cols] - x_in[c:c + CR, cols].astype(F32) * wide(r.xs[2, c:c + CR, :])).astype(BF16)

        return (1, run)

    def y_dot(n):
        def run():
            cols = slice(n * NC, (n + 1) * NC)
            t = dot(r.oc[0], r.wo_all[0, :, cols]) + dot(r.oc[1], r.wo_all[1, :, cols])
            y_out[:, cols] = (x_in[:, cols].astype(F32) + t).astype(BF16)

        return (1, run)

    r.tab[2:4] = r.tab[0:2]
    r.tab[0] = cos_in[...]
    r.tab[1] = sin_in[...]
    yd = [y_dot(n) for n in range(nn)]
    for g in range(n_grp):
        attn_tick(st, g, n_grp, yd[:EARLY] if g == n_grp - 1 else [])
    for acc in (r.dgq, r.dgk):
        acc[...] = jnp.where(step > 0, acc[...], 0.0)

    @pl.when(step == 0)
    def _():
        for c in mine[:3]:
            c.wait()

    @pl.when(step > 0)
    def _():
        for c in fetch(step - 1):
            c.wait()
        dn = [dn_dot(n) for n in range(nn)]
        for _, f in dn[:1]:
            f()
        weave([stat(c) for c in lines], dn[1:2])
        for n in range(2, nn):
            weave([first(n - 2, c) for c in lines], dn[n:n + 1])
        weave([first(nn - 2, c) for c in lines], yd[EARLY:EARLY + 1])
        weave([first(nn - 1, c) for c in lines] + [mean(c) for c in lines], yd[EARLY + 1:EARLY + 2])
        weave([second(n, c) for n in range(nn) for c in lines], yd[EARLY + 2:])

    @pl.when(step == rows)
    def _():
        sums_out[:, 0:D] = r.dg[...]
        sums_out[:, D:D + HD] = r.dgq[...] + dgq_own[...]
        sums_out[:, D + HD:] = r.dgk[...] + dgk_own[...]


def tail_call(sel, n, x, dy, cosd, sind, o, dq, dk, dv, gain, qg, kg, dgq, dgk, own, oth, seq=256):
    T, D = x.shape
    nq, nk = dq.shape[2], dk.shape[2]
    n_grp = nk // HD
    rows = T // seq
    lag = lambda k, c: pl.BlockSpec((seq, c), lambda i, s: (jnp.clip(i - k, 0, rows - 1), 0))
    const = lambda *b: pl.BlockSpec(b, lambda i, s: (0,) * len(b), pipeline_mode=pl.Buffered(1))
    hbm = pl.BlockSpec(memory_space=pl.ANY)
    scratch = attn_scratch(seq, n_grp)
    scratch.update(
        wq_all=pltpu.VMEM((2, D, nq), BF16), wk_all=pltpu.VMEM((2, D, nk), BF16), wv_all=pltpu.VMEM((2, D, nk), BF16), wo_all=pltpu.VMEM((2, nq, D), BF16),
        dn=pltpu.VMEM((seq, D), F32), oc=pltpu.VMEM((2, seq, nq), BF16), dqc=pltpu.VMEM((2, seq, nq), BF16), dkc=pltpu.VMEM((2, seq, nk), BF16), dvc=pltpu.VMEM((2, seq, nk), BF16),
        o_next=pltpu.VMEM((seq, nq), BF16), xs=pltpu.VMEM((3, seq, HD), F32), dg=pltpu.VMEM((8, D), F32), dgq=pltpu.VMEM((8, HD), F32), dgk=pltpu.VMEM((8, HD), F32), sem=pltpu.SemaphoreType.DMA((12,)))
    flops = 2 * T * D * (nq + 2 * nk + nq) * 3 + 12 * T * nq * seq
    return pl.pallas_call(
        functools.partial(tail_kernel, seq, n_grp, rows, tuple(scratch)),
        grid_spec=pltpu.PrefetchScalarGridSpec(
            num_scalar_prefetch=1,
            grid=(rows + 1,),
            in_specs=[lag(0, D), lag(0, D), lag(0, HD), lag(0, HD), lag(1, D), lag(1, D), const(1, D), const(1, HD), const(1, HD), const(8, HD), const(8, HD)] + [hbm] * 12,
            out_specs=[lag(1, D), lag(1, D), pl.BlockSpec((8, D + 2 * HD), lambda i, s: (0, 0))],
            scratch_shapes=list(scratch.values()),
        ),
        out_shape=[jax.ShapeDtypeStruct((T, D), BF16)] * 2 + [jax.ShapeDtypeStruct((8, D + 2 * HD), F32)],
        compiler_params=pltpu.CompilerParams(dimension_semantics=("arbitrary",), vmem_limit_bytes=67043328),
        cost_estimate=pl.CostEstimate(flops=flops, bytes_accessed=T * D * 14, transcendentals=T * nq * 2),
        name="tail",
    )(sel, n, dy, cosd, sind, x, dy, gain, qg, kg, dgq, dgk, *own, *oth, o, dq, dk, dv)


def solution(mesh):
    tok_spec = P("dp", None, None)
    col_spec = P(None, "tp")
    row_spec = P("tp", None)
    n_dp = mesh.shape["dp"]

    def per_device(x_in, dy_in, positions, g_attn, q_gain, k_gain, w_q, w_k, w_v, w_o):
        n_batch, n_seq, D = x_in.shape
        T = n_batch * n_seq
        nk = w_k.shape[1]
        x, dy = x_in.reshape(T, D), dy_in.reshape(T, D)
        me = lax.axis_index("tp").astype(jnp.int32)
        own = me.reshape(1)

        part = lax.axis_index("dp").astype(jnp.int32).reshape(1)
        share, cosd, sind = pre_call(part, w_q, w_k, w_v, w_o, positions, parts=n_dp)
        gathered = lax.all_gather(share, ("tp", "dp"), tiled=True)

        gain = g_attn.astype(F32).reshape(1, D)
        qg, kg = q_gain.astype(F32).reshape(1, HD), k_gain.astype(F32).reshape(1, HD)

        n, o, dq, dk, dv, dgq, dgk = attn_call(True, own, x, dy, cosd, sind, gain, qg, kg, w_q, w_k, w_v, w_o, seq=n_seq)
        dw_q, dw_k, dw_v = dw_call(own, n, [dq, dk, dv], 512)
        dw_o, *theirs = dw_call(own, o, [dy], 1024, gathered=gathered, nk=nk)
        dw_o, dw_q, dw_k, dw_v = lax.psum((dw_o, dw_q, dw_k, dw_v), "dp")

        y, dx, sums = tail_call(own, n, x, dy, cosd, sind, o, dq, dk, dv, gain, qg, kg, dgq, dgk, (w_q, w_k, w_v, w_o), theirs, seq=n_seq)
        g_sum, q_sum, k_sum = (t.reshape(-1) for t in sum_call(sums, (D, HD, HD), n_dp))
        dw_o, dw_q, dw_k, dw_v = copy_call((dw_o, dw_q, dw_k, dw_v))
        return y.reshape(x_in.shape), dx.reshape(x_in.shape), dw_q, dw_k, dw_v, dw_o, q_sum, k_sum, g_sum

    return jax.shard_map(per_device, mesh=mesh, in_specs=(tok_spec, tok_spec, P("dp", None), P(), P(), P(), col_spec, col_spec, col_spec, row_spec), out_specs=(tok_spec, tok_spec, col_spec, col_spec, col_spec, row_spec, P(), P(), P()), check_vma=False)
```

```python
import functools
from types import SimpleNamespace
import jax
import jax.numpy as jnp
from jax import lax
from jax.experimental import pallas as pl
from jax.experimental.pallas import tpu as pltpu
from jax.sharding import PartitionSpec as P


EPS = 1e-6
THETA = 1000000.0
F32 = jnp.float32
BF16 = jnp.bfloat16
HD = 128
NT = (((1,), (1,)), ((), ()))
TN = (((0,), (0,)), ((), ()))
NN = (((1,), (0,)), ((), ()))


def dot(a, b, dims=NN):
    return lax.dot_general(a, b, dims, preferred_element_type=F32)


def weave(*lists):
    order = []
    for n, pieces in enumerate(lists):
        total = sum(c for c, _ in pieces) or 1
        at = 0
        for k, (c, f) in enumerate(pieces):
            order.append(((at + c / 2) / total, n, k, f))
            at += c
    for _, _, _, f in sorted(order, key=lambda e: e[:3]):
        f()


CH = 32


def attn_kernel(own, seq, n_grp, sel_ref, *refs):
    if own:
        (x0_ref, xn_ref, dy_ref, cos_ref, sin_ref, gain_ref, qg_ref, kg_ref, wq_ref, wk_ref, wv_ref, wo_ref,
         n_out, o_out, dq_out, dk_out, dv_out, dgq_out, dgk_out, dwo_out) = refs[:20]
        refs = refs[20:]
    else:
        nin_ref, dy_ref, cos_ref, sin_ref, qg_ref, kg_ref, wq_ref, wk_ref, wv_ref, wo_ref, _, _, _, _, o_out, dq_out, dk_out, dv_out = refs[:18]
        refs = refs[18:]
        n_ref = nin_ref
    (wot_ref, qnew_ref, knew_ref, vnew_ref, raw_ref, inv_ref, rot_ref, do_ref, v_ref, s_ref, dp_ref, p_ref, ds_ref, dkf_ref, dqf_ref, st_ref,
     tab_ref, o_ref, dq_ref, dk_ref, dv_ref) = refs[:21]
    if own:
        n_ref, nn_ref, dgq_ref, dgk_ref, acc_ref, ot_ref, dyp_ref, sem = refs[21:]
    half = seq // 2
    scale = HD ** -0.5
    log2e = 1.4426950408889634
    step = pl.program_id(0)

    def norm_rows(src, dst):
        def piece(c):
            def run():
                xf = src[c:c + 32, :].astype(F32)
                inv = lax.rsqrt(jnp.mean(xf * xf, axis=-1, keepdims=True) + EPS)
                dst[c:c + 32, :] = (xf * inv * gain_ref[0:1, :]).astype(BF16)

            return (1.5, run)

        return [piece(c) for c in range(0, seq, 32)]

    def proj(g):
        def q():
            t = dot(n_ref[...], wq_ref[:, g * 2 * HD:(g + 1) * 2 * HD])
            for h in range(2):
                qnew_ref[g % 2, h] = t[:, h * HD:(h + 1) * HD].astype(BF16)

        def k():
            t = dot(n_ref[...], wk_ref[:, g * HD:(g + 2) * HD])
            for h in range(2):
                knew_ref[g + h] = t[:, h * HD:(h + 1) * HD].astype(BF16)

        def v():
            t = dot(n_ref[...], wv_ref[:, g * HD:(g + 2) * HD])
            for h in range(2):
                vnew_ref[g + h] = t[:, h * HD:(h + 1) * HD].astype(BF16)

        def do():
            t = dot(dy_ref[...], wot_ref[:, g * 2 * HD:(g + 1) * 2 * HD])
            for h in range(2):
                do_ref[g, h * half:(h + 1) * half, :] = t[:half, h * HD:(h + 1) * HD].astype(BF16)
                do_ref[g, seq + h * half:seq + (h + 1) * half, :] = t[half:, h * HD:(h + 1) * HD].astype(BF16)

        return [(1, q)] + ([(1, k), (1, v)] if g % 2 == 0 else []) + [(1, do)]

    def stacked(h, c):
        return (h * half + c) if c < half else (seq + h * half + c - half)

    def rope(g):
        cs, sn = (tab_ref.at[2], tab_ref.at[3]) if g == n_grp - 1 else (tab_ref.at[0], tab_ref.at[1])

        def size(h, c):
            def run():
                raw = knew_ref[g, c:c + CH, :] if h == 2 else qnew_ref[g % 2, h, c:c + CH, :]
                raw_ref[g, h, c:c + CH, :] = raw
                t = raw.astype(F32)
                inv_ref[g, h, c:c + CH, :] = jnp.broadcast_to(lax.rsqrt(jnp.mean(t * t, axis=-1, keepdims=True) + EPS), t.shape)

            return (0.4, run)

        def turn(h, c):
            def run():
                t = raw_ref[g, h, c:c + CH, :].astype(F32)
                w = (t * inv_ref[g, h, c:c + CH, :]) * (kg_ref if h == 2 else qg_ref)[0:1, :]
                o = 2 * seq + c if h == 2 else stacked(h, c)
                x = pltpu.roll(w, HD // 2, 1)
                co, si = cs[c:c + CH, :], sn[c:c + CH, :]
                rot_ref[g, o:o + CH, 0:HD] = (w * co + x * si).astype(BF16)
                rot_ref[g, o:o + CH, HD:] = (x * co - w * si).astype(BF16)
                if h == 2:
                    v_ref[g, c:c + CH, :] = vnew_ref[g, c:c + CH, :]

            return (0.6, run)

        return [f(h, c) for f in (size, turn) for h in (2, 0, 1) for c in range(0, seq, CH)]

    def scores(g):
        b = g % 2

        def s():
            s_ref[b, 0:seq, 0:half] = dot(rot_ref[g, 0:seq, 0:HD], rot_ref[g, 2 * seq:2 * seq + half, 0:HD], NT)
            s_ref[b, seq:, :] = dot(rot_ref[g, seq:2 * seq, 0:HD], rot_ref[g, 2 * seq:, 0:HD], NT)

        def dp():
            dp_ref[b, 0:seq, 0:half] = dot(do_ref[g, :seq, :], v_ref[g, :half, :], NT)
            dp_ref[b, seq:, :] = dot(do_ref[g, seq:, :], v_ref[g], NT)

        return [(1, s), (1, dp)]

    def soft(g):
        b = g % 2
        c2 = scale * log2e

        def part(blk, c):
            return slice(blk * seq + c, blk * seq + c + CH), half if blk == 0 else seq

        def masked(blk, c, s):
            row_id = lax.broadcasted_iota(jnp.int32, (CH, half), 0) + (c % half)
            keep = row_id >= lax.broadcasted_iota(jnp.int32, (CH, half), 1)
            if blk == 0:
                return jnp.where(keep, s, -jnp.inf)
            return jnp.concatenate([s[:, :half], jnp.where(keep, s[:, half:], -jnp.inf)], axis=1)

        def wide(ref, rows, width):
            t = ref[rows, :]
            return t if width == half else jnp.concatenate([t, t], axis=1)

        def top(blk, c):
            rows, width = part(blk, c)

            def run():
                m = jnp.max(masked(blk, c, s_ref[b, rows, 0:width]), axis=-1, keepdims=True)
                st_ref[0, rows, :] = jnp.broadcast_to(m * c2, (CH, HD))

            return (0.4 + 0.4 * blk, run)

        def power(blk, c):
            rows, width = part(blk, c)

            def run():
                e = jnp.exp2(masked(blk, c, s_ref[b, rows, 0:width] * c2) - wide(st_ref.at[0], rows, width))
                s_ref[b, rows, 0:width] = e
                st_ref[1, rows, :] = jnp.broadcast_to(1.0 / jnp.sum(e, axis=-1, keepdims=True), (CH, HD))

            return (0.8 + 0.8 * blk, run)

        def prob(blk, c):
            rows, width = part(blk, c)

            def run():
                pr = s_ref[b, rows, 0:width] * wide(st_ref.at[1], rows, width)
                s_ref[b, rows, 0:width] = pr
                p_ref[b, rows, 0:width] = pr.astype(BF16)
                st_ref[2, rows, :] = jnp.broadcast_to(jnp.sum(pr * dp_ref[b, rows, 0:width], axis=-1, keepdims=True), (CH, HD))

            return (0.8 + 0.8 * blk, run)

        def last(blk, c):
            rows, width = part(blk, c)

            def run():
                d = dp_ref[b, rows, 0:width] - wide(st_ref.at[2], rows, width)
                ds_ref[b, rows, 0:width] = (s_ref[b, rows, 0:width] * d * scale).astype(BF16)

            return (0.8 + 0.8 * blk, run)

        return [f(blk, c) for f in (top, power, prob, last) for blk in range(2) for c in range(0, seq, CH)]

    def grads(g):
        b = g % 2
        col, kcol = g * 2 * HD, g * HD

        def dq():
            dqf_ref[b, 0:seq, :] = dot(ds_ref[b, 0:seq, 0:half], rot_ref[g, 2 * seq:2 * seq + half, :])
            dqf_ref[b, seq:, :] = dot(ds_ref[b, seq:, :], rot_ref[g, 2 * seq:, :])

        def dk():
            tb = dot(ds_ref[b, seq:, :], rot_ref[g, seq:2 * seq, :], TN)
            ta = dot(ds_ref[b, 0:seq, 0:half], rot_ref[g, 0:seq, :], TN)
            dkf_ref[b, :half, :] = tb[:half] + ta
            dkf_ref[b, half:, :] = tb[half:]

        def o():
            ta = dot(p_ref[b, 0:seq, 0:half], v_ref[g, :half, :])
            tb = dot(p_ref[b, seq:, :], v_ref[g])
            for h in range(2):
                o_ref[0:half, col + h * HD:col + (h + 1) * HD] = ta[h * half:(h + 1) * half].astype(BF16)
                o_ref[half:seq, col + h * HD:col + (h + 1) * HD] = tb[h * half:(h + 1) * half].astype(BF16)

        def dv():
            tb = dot(p_ref[b, seq:, :], do_ref[g, seq:, :], TN)
            ta = dot(p_ref[b, 0:seq, 0:half], do_ref[g, :seq, :], TN)
            dv_ref[0:half, kcol:kcol + HD] = (tb[:half] + ta).astype(BF16)
            dv_ref[half:seq, kcol:kcol + HD] = tb[half:].astype(BF16)

        return [(1, dq), (1, dk), (1, o), (1, dv)]

    def back(g):
        b = g % 2

        def place(h, c):
            if h == 2:
                return dkf_ref, c, dk_ref, g * HD, kg_ref
            return dqf_ref, stacked(h, c), dq_ref, (2 * g + h) * HD, qg_ref

        def turn(h, c):
            src, o, _, _, g_ref = place(h, c)

            def run():
                d = src[b, o:o + CH, :].astype(BF16).astype(F32)
                that = raw_ref[g, h, c:c + CH, :].astype(F32) * inv_ref[g, h, c:c + CH, :]
                du = d[:, :HD] * tab_ref[2, c:c + CH, :] - d[:, HD:] * tab_ref[3, c:c + CH, :]
                src[b, o:o + CH, 0:HD] = du
                pr = du * that
                if own:
                    dg_ref = dgk_ref if h == 2 else dgq_ref
                    dg_ref[...] += jnp.sum(pr.reshape(CH // 8, 8, HD), axis=0)
                st_ref[3 + h, c:c + CH, :] = jnp.broadcast_to(jnp.mean(pr * g_ref[0:1, :], axis=-1, keepdims=True), (CH, HD))

            return (0.6, run)

        def out(h, c):
            src, o, out_ref, col, g_ref = place(h, c)

            def run():
                inv = inv_ref[g, h, c:c + CH, :]
                that = raw_ref[g, h, c:c + CH, :].astype(F32) * inv
                out_ref[c:c + CH, col:col + HD] = (inv * (src[b, o:o + CH, 0:HD] * g_ref[0:1, :] - that * st_ref[3 + h, c:c + CH, :])).astype(BF16)

            return (0.5, run)

        return [f(h, c) for f in (turn, out) for h in (0, 1, 2) for c in range(0, seq, CH)]

    def flip(c):
        def run():
            ot_ref[c:c + 256, :] = o_ref[:, c:c + 256].T

        return (0.1, run)

    def dwo(c):
        def run():
            acc_ref[:, c:c + 256] += dot(ot_ref[...], dyp_ref[:, c:c + 256])

        return (0.5, run)

    @pl.when(step == 0)
    def _():
        @pl.loop(0, wo_ref.shape[0] // 256)
        def _(j):
            c = pl.ds(pl.multiple_of(j * 256, 256), 256)
            for d in range(0, wo_ref.shape[1], 256):
                wot_ref[d:d + 256, c] = wo_ref[c, d:d + 256].T

        if own:
            weave(norm_rows(x0_ref, n_ref))

    tab_ref[2:4] = tab_ref[0:2]
    tab_ref[0] = cos_ref[...]
    tab_ref[1] = sin_ref[...]
    if own:
        norms = norm_rows(xn_ref, nn_ref)
    for g in range(n_grp):
        sc = scores((g - 2) % n_grp)
        gr = grads(g)
        nm = norms[g * len(norms) // n_grp:(g + 1) * len(norms) // n_grp] if own else []
        for _, f in gr[:2]:
            f()
        late = []
        if own and g == n_grp - 1:
            late = [flip(c) for c in range(0, ot_ref.shape[0], 256)], [dwo(c) for c in range(0, acc_ref.shape[1], 256)]
        weave(soft((g - 3) % n_grp), rope((g - 1) % n_grp) + nm, back(g), sc + gr[2:] + (late[0] + proj(g) + late[1] if late else proj(g)))

    for dst, src in ((o_out, o_ref), (dq_out, dq_ref), (dk_out, dk_ref), (dv_out, dv_ref)):
        dst[0] = src[...]
    if own:
        n_out[...] = n_ref[...]
        n_ref[...] = nn_ref[...]
        keep = step > 0
        for dst, acc in ((dgq_out, dgq_ref), (dgk_out, dgk_ref)):
            acc[...] = jnp.where(keep, acc[...], 0.0)
            dst[...] = acc[...]
        dyp_ref[...] = dy_ref[...]

        @pl.when(step == 0)
        def _():
            @pl.loop(0, acc_ref.shape[0] // 64)
            def _(j):
                acc_ref[pl.ds(pl.multiple_of(j * 64, 64), 64), :] = jnp.zeros((64, acc_ref.shape[1]), F32)

        @pl.when(step == pl.num_programs(0) - 1)
        def _():
            c = pltpu.make_async_copy(acc_ref, dwo_out, sem)
            c.start()
            c.wait()


def attn_call(own, sel, x, dy, cosd, sind, gain, qg, kg, wq, wk, wv, wo, prev=None, seq=256):
    T, D = x.shape
    nq, nk = wq.shape[1], wk.shape[1]
    n_grp = nk // HD
    rows = T // seq
    const = lambda *b: pl.BlockSpec(b, lambda i, s: (0,) * len(b), pipeline_mode=pl.Buffered(1))
    now = lambda c: pl.BlockSpec((seq, c), lambda i, s: (jnp.minimum(i, rows - 1), 0))
    nxt = lambda c: pl.BlockSpec((seq, c), lambda i, s: (jnp.minimum(i + 1, rows - 1), 0))
    out3 = lambda c: pl.BlockSpec((1, seq, c), lambda i, s: (s[0], jnp.maximum(i - 1, 0), 0))
    mid = [now(D), now(HD), now(HD)]
    tail = [const(1, HD), const(1, HD), const(D, nq), const(D, nk), const(D, nk), const(nq, D)]
    shapes = [jax.ShapeDtypeStruct((2, T, c), BF16) for c in (nq, nq, nk, nk)]
    specs = [out3(nq), out3(nq), out3(nk), out3(nk)]
    aliases = {}
    if own:
        in_specs = [const(seq, D), nxt(D)] + mid + [const(1, D)] + tail
        args = [x, x, dy, cosd, sind, gain, qg, kg, wq, wk, wv, wo]
        shapes = [jax.ShapeDtypeStruct((T, D), BF16)] + shapes + [jax.ShapeDtypeStruct((8, HD), F32)] * 2 + [jax.ShapeDtypeStruct((nq, D), F32)]
        specs = [now(D)] + specs + [pl.BlockSpec((8, HD), lambda i, s: (0, 0))] * 2 + [pl.BlockSpec(memory_space=pl.ANY)]
    else:
        in_specs = [now(D)] + mid + tail + [pl.BlockSpec(memory_space=pl.ANY)] * 4
        args = [x, dy, cosd, sind, qg, kg, wq, wk, wv, wo]
        aliases = {1 + len(args) + i: i for i in range(4)}
        args += list(prev)
    flops = 2 * T * D * (nq + 2 * nk + nq) + 12 * T * nq * seq
    return pl.pallas_call(
        functools.partial(attn_kernel, own, seq, n_grp),
        grid_spec=pltpu.PrefetchScalarGridSpec(
            num_scalar_prefetch=1,
            grid=(rows + 1,),
            in_specs=in_specs,
            out_specs=specs,
            scratch_shapes=[
                pltpu.VMEM((D, nq), BF16),
                pltpu.VMEM((2, 2, seq, HD), BF16),
                pltpu.VMEM((n_grp, seq, HD), BF16),
                pltpu.VMEM((n_grp, seq, HD), BF16),
                pltpu.VMEM((n_grp, 3, seq, HD), BF16),
                pltpu.VMEM((n_grp, 3, seq, HD), F32),
                pltpu.VMEM((n_grp, 3 * seq, 2 * HD), BF16),
                pltpu.VMEM((n_grp, 2 * seq, HD), BF16),
                pltpu.VMEM((n_grp, seq, HD), BF16),
                pltpu.VMEM((2, 2 * seq, seq), F32),
                pltpu.VMEM((2, 2 * seq, seq), F32),
                pltpu.VMEM((2, 2 * seq, seq), BF16),
                pltpu.VMEM((2, 2 * seq, seq), BF16),
                pltpu.VMEM((2, seq, 2 * HD), F32),
                pltpu.VMEM((2, 2 * seq, 2 * HD), F32),
                pltpu.VMEM((6, 2 * seq, HD), F32),
                pltpu.VMEM((4, seq, HD), F32),
            ] + [pltpu.VMEM((seq, c), BF16) for c in (nq, nq, nk, nk)]
            + ([pltpu.VMEM((seq, D), BF16)] * 2 + [pltpu.VMEM((8, HD), F32)] * 2 + [pltpu.VMEM((nq, D), F32), pltpu.VMEM((nq, seq), BF16), pltpu.VMEM((seq, D), BF16), pltpu.SemaphoreType.DMA] if own else []),
        ),
        out_shape=shapes,
        input_output_aliases=aliases,
        compiler_params=pltpu.CompilerParams(dimension_semantics=("arbitrary",), vmem_limit_bytes=62 << 20),
        cost_estimate=pl.CostEstimate(flops=flops, bytes_accessed=T * D * 6 + T * (2 * nq + 2 * nk) * 2, transcendentals=T * nq * 2),
        name="attn_own" if own else "attn_other",
    )(sel, *args)


def pre_kernel(sel_ref, q_ref, k_ref, v_ref, o_ref, pos_ref, freq_ref, out_ref, cos_ref, sin_ref):
    d, nq, nk = q_ref.shape[0], q_ref.shape[1], k_ref.shape[1]
    out_ref[0, 0:d, 0:nq] = q_ref[...].astype(F32)
    out_ref[0, 0:d, nq:nq + nk] = k_ref[...].astype(F32)
    out_ref[0, 0:d, nq + nk:] = v_ref[...].astype(F32)
    out_ref[0, d:, :] = o_ref[...].astype(F32)
    n, seq = pos_ref.shape
    lane = lax.broadcasted_iota(jnp.int32, (HD, HD), 1)
    for r in range(n):
        for h in range(seq // HD):
            p = pos_ref[r:r + 1, h * HD:(h + 1) * HD].astype(F32)
            a = jnp.broadcast_to(p, (HD, HD)).T * freq_ref[0:1, :]
            k = jnp.round(a * 0.6366197723675814)
            x = ((a - k * 1.5703125) - k * 4.837512969970703125e-4) - k * 7.549789948768648e-8
            z = x * x
            s = ((-1.9515295891e-4 * z + 8.3321608736e-3) * z - 1.6666654611e-1) * z * x + x
            c = ((2.443315711809948e-5 * z - 1.388731625493765e-3) * z + 4.166664568298827e-2) * z * z - 0.5 * z + 1.0
            q = k.astype(jnp.int32)
            odd = (q & 1) == 1
            co, si = jnp.where(odd, s, c), jnp.where(odd, c, s)
            rows = slice((r * (seq // HD) + h) * HD, (r * (seq // HD) + h + 1) * HD)
            cos_ref[rows, :] = jnp.where(((q + 1) & 2) == 0, co, -co)
            sin_ref[rows, :] = jnp.where(((q & 2) == 0) == (lane >= HD // 2), si, -si)


def pre_call(part, w_q, w_k, w_v, w_o, positions, parts=2, cuts=4):
    D, nq = w_q.shape
    n, seq = positions.shape
    rows = n // cuts
    freq = THETA ** (-jnp.arange(0, HD, 2, dtype=F32) / HD)
    freq = jnp.concatenate([freq, freq]).reshape(1, HD)
    spec = lambda w: pl.BlockSpec((w.shape[0] // (parts * cuts), w.shape[1]), lambda i, s: (s[0] * cuts + i, 0))
    r = (D + nq) // (parts * cuts)
    table = pl.BlockSpec((rows * seq, HD), lambda i, s: (i, 0))
    return pl.pallas_call(
        pre_kernel,
        grid_spec=pltpu.PrefetchScalarGridSpec(
            num_scalar_prefetch=1,
            grid=(cuts,),
            in_specs=[spec(w) for w in (w_q, w_k, w_v, w_o)] + [pl.BlockSpec((rows, seq), lambda i, s: (i, 0)), pl.BlockSpec((1, HD), lambda i, s: (0, 0))],
            out_specs=[pl.BlockSpec((1, r, D), lambda i, s: (i, 0, 0)), table, table],
        ),
        out_shape=[jax.ShapeDtypeStruct((cuts, r, D), F32)] + [jax.ShapeDtypeStruct((n * seq, HD), F32)] * 2,
        compiler_params=pltpu.CompilerParams(dimension_semantics=("arbitrary",), vmem_limit_bytes=60 << 20),
        cost_estimate=pl.CostEstimate(flops=n * seq * HD * 30, bytes_accessed=cuts * r * D * 6 + n * seq * HD * 8, transcendentals=0),
        name="pre",
    )(part, w_q, w_k, w_v, w_o, positions, freq)


def dw_kernel(n_b, unpack, sel_ref, a_ref, *refs):
    if unpack:
        f_ref, parts = refs[n_b], refs[2 * n_b + 1:2 * n_b + 5]
        refs = refs[:n_b] + refs[n_b + 1:2 * n_b + 1] + refs[2 * n_b + 5:]
        q_ref, k_ref, v_ref, o_ref = parts
        per, nq, nk = f_ref.shape[0], q_ref.shape[1], k_ref.shape[1]
        d, e = q_ref.shape[0] // per, o_ref.shape[0] // per
        for j in range(per):
            q_ref[j * d:(j + 1) * d, :] = f_ref[j, 0:d, 0:nq].astype(BF16)
            k_ref[j * d:(j + 1) * d, :] = f_ref[j, 0:d, nq:nq + nk].astype(BF16)
            v_ref[j * d:(j + 1) * d, :] = f_ref[j, 0:d, nq + nk:].astype(BF16)
            o_ref[j * e:(j + 1) * e, :] = f_ref[j, d:, :].astype(BF16)
    bs, outs, accs, (at_ref, sem) = refs[:n_b], refs[n_b:2 * n_b], refs[2 * n_b:3 * n_b], refs[3 * n_b:]
    flat = lambda ref: ref.at[0] if len(ref.shape) == 3 else ref
    a, bs = flat(a_ref), [flat(b) for b in bs]
    M, tile = at_ref.shape
    step = pl.program_id(0)

    @pl.when(step == 0)
    def _():
        for acc in accs:
            @pl.loop(0, M // 64)
            def _(j):
                acc[pl.ds(pl.multiple_of(j * 64, 64), 64), :] = jnp.zeros((64, acc.shape[1]), F32)

    def part(acc, b, c):
        def run():
            acc[:, c:c + 256] += dot(at_ref[...], b[:, c:c + 256])

        return (1, run)

    for c in range(0, M, 256):
        for k in range(0, tile, 256):
            at_ref[c:c + 256, k:k + 256] = a[k:k + 256, c:c + 256].T
    weave([part(acc, b, c) for acc, b in zip(accs, bs) for c in range(0, b.shape[1], 256)])

    @pl.when(step == pl.num_programs(0) - 1)
    def _():
        copies = [pltpu.make_async_copy(acc, out, sem.at[k]) for k, (acc, out) in enumerate(zip(accs, outs))]
        for c in copies:
            c.start()
        for c in copies:
            c.wait()


def dw_call(sel, a, bs, tile, gathered=None, nk=0):
    def spec(v):
        if v.ndim == 3:
            return pl.BlockSpec((1, tile, v.shape[2]), lambda i, s: (s[0], i, 0))
        return pl.BlockSpec((tile, v.shape[1]), lambda i, s: (i, 0))

    T, M = a.shape[-2:]
    shapes = [(M, b.shape[-1]) for b in bs]
    width = sum(s[1] for s in shapes)
    steps = T // tile
    more_in, more_out, more_shapes, more = [], [], [], []
    if gathered is not None:
        n, r, D = gathered.shape
        per = n // 2 // steps
        more = [gathered]
        more_in = [pl.BlockSpec((per, r, D), lambda i, s: ((1 - s[0]) * steps + i, 0, 0))]
        nq = D - 2 * nk
        more_shapes = [jax.ShapeDtypeStruct(s, BF16) for s in ((D, nq), (D, nk), (D, nk), (nq, D))]
        more_out = [pl.BlockSpec((s.shape[0] // steps, s.shape[1]), lambda i, s: (i, 0)) for s in more_shapes]
    return pl.pallas_call(
        functools.partial(dw_kernel, len(bs), gathered is not None),
        grid_spec=pltpu.PrefetchScalarGridSpec(
            num_scalar_prefetch=1,
            grid=(steps,),
            in_specs=[spec(a)] + [spec(b) for b in bs] + more_in,
            out_specs=[pl.BlockSpec(memory_space=pl.ANY)] * len(bs) + more_out,
            scratch_shapes=[pltpu.VMEM(s, F32) for s in shapes] + [pltpu.VMEM((M, tile), BF16), pltpu.SemaphoreType.DMA((len(bs),))],
        ),
        out_shape=[jax.ShapeDtypeStruct(s, F32) for s in shapes] + more_shapes,
        compiler_params=pltpu.CompilerParams(dimension_semantics=("arbitrary",), vmem_limit_bytes=60 << 20),
        cost_estimate=pl.CostEstimate(flops=2 * T * M * width, bytes_accessed=2 * T * (M + width) + 4 * M * width, transcendentals=0),
    )(sel, a, *bs, *more)


def sum_kernel(n, widths, part_ref, *refs):
    outs, (slots, local_sem, send_sem, recv_sem) = refs[:-4], refs[-4:]
    me = lax.axis_index("dp")
    barrier = pltpu.get_barrier_semaphore()
    for k in range(1, n):
        pl.semaphore_signal(barrier, inc=1, device_id={"dp": lax.rem(me + k, n)}, device_id_type=pl.DeviceIdType.MESH)
    mine = pltpu.make_async_copy(part_ref, slots.at[0], local_sem)
    mine.start()
    pl.semaphore_wait(barrier, n - 1)
    copies = []
    for k in range(1, n):
        copies.append(pltpu.make_async_remote_copy(
            src_ref=part_ref, dst_ref=slots.at[k], send_sem=send_sem.at[k - 1], recv_sem=recv_sem.at[k - 1],
            device_id={"dp": lax.rem(me + k, n)}, device_id_type=pl.DeviceIdType.MESH))
    for c in copies:
        c.start()
    mine.wait()
    for c in copies:
        c.wait()
    total = slots[lax.rem(me + n, n)]
    for a in range(1, n):
        total = total + slots[lax.rem(me + n - a, n)]
    at = 0
    for out, w in zip(outs, widths):
        out[...] = total[:, at:at + w]
        at += w


def sum_call(part, widths, n):
    return pl.pallas_call(
        functools.partial(sum_kernel, n, widths),
        in_specs=[pl.BlockSpec(memory_space=pl.ANY)],
        out_specs=[pl.BlockSpec(memory_space=pltpu.VMEM)] * len(widths),
        out_shape=[jax.ShapeDtypeStruct((1, w), F32) for w in widths],
        scratch_shapes=[pltpu.VMEM((n, *part.shape), F32), pltpu.SemaphoreType.DMA, pltpu.SemaphoreType.DMA((n - 1,)), pltpu.SemaphoreType.DMA((n - 1,))],
        compiler_params=pltpu.CompilerParams(collective_id=0, has_side_effects=True),
        cost_estimate=pl.CostEstimate(flops=n * part.size, bytes_accessed=8 * n * part.size, transcendentals=0),
        name="small_sum",
    )(part)


def copy_kernel(n, cuts, *refs):
    srcs, dsts, bufs, (in_sem, out_sem) = refs[:n], refs[n:2 * n], refs[2 * n:3 * n], refs[3 * n:]
    ins, outs = [], []
    for a, (src, dst, buf) in enumerate(zip(srcs, dsts, bufs)):
        rows = src.shape[0] // cuts
        for j in range(cuts):
            part = pl.ds(j * rows, rows)
            ins.append(pltpu.make_async_copy(src.at[part], buf.at[part], in_sem.at[a, j]))
            outs.append(pltpu.make_async_copy(buf.at[part], dst.at[part], out_sem.at[a, j]))
    for c in ins:
        c.start()
    for c, d in zip(ins, outs):
        c.wait()
        d.start()
    for d in outs:
        d.wait()


def copy_call(arrays, cuts=4):
    n = len(arrays)
    hbm = [pl.BlockSpec(memory_space=pl.ANY)] * n
    return pl.pallas_call(
        functools.partial(copy_kernel, n, cuts),
        in_specs=hbm,
        out_specs=hbm,
        out_shape=[jax.ShapeDtypeStruct(a.shape, a.dtype) for a in arrays],
        scratch_shapes=[pltpu.VMEM(a.shape, a.dtype) for a in arrays] + [pltpu.SemaphoreType.DMA((n, cuts))] * 2,
        compiler_params=pltpu.CompilerParams(vmem_limit_bytes=60 << 20),
        cost_estimate=pl.CostEstimate(flops=0, bytes_accessed=8 * sum(a.size for a in arrays), transcendentals=0),
        name="results",
    )(*arrays)


def attn_stages(seq, n_grp, r):
    half = seq // 2
    scale = HD ** -0.5
    log2e = 1.4426950408889634

    def norm_rows(src, dst):
        def piece(c):
            def run():
                xf = src[c:c + 32, :].astype(F32)
                inv = lax.rsqrt(jnp.mean(xf * xf, axis=-1, keepdims=True) + EPS)
                dst[c:c + 32, :] = (xf * inv * r.gain[0:1, :]).astype(BF16)

            return (1.5, run)

        return [piece(c) for c in range(0, seq, 32)]

    def proj(g):
        def q():
            t = dot(r.n[...], r.wq(slice(g * 2 * HD, (g + 1) * 2 * HD)))
            for h in range(2):
                r.qnew[g % 2, h] = t[:, h * HD:(h + 1) * HD].astype(BF16)

        def k():
            t = dot(r.n[...], r.wk(slice(g * HD, (g + 2) * HD)))
            for h in range(2):
                r.knew[g + h] = t[:, h * HD:(h + 1) * HD].astype(BF16)

        def v():
            t = dot(r.n[...], r.wv(slice(g * HD, (g + 2) * HD)))
            for h in range(2):
                r.vnew[g + h] = t[:, h * HD:(h + 1) * HD].astype(BF16)

        def do():
            t = r.do_dot(slice(g * 2 * HD, (g + 1) * 2 * HD))
            for h in range(2):
                r.do[g, h * half:(h + 1) * half, :] = t[:half, h * HD:(h + 1) * HD].astype(BF16)
                r.do[g, seq + h * half:seq + (h + 1) * half, :] = t[half:, h * HD:(h + 1) * HD].astype(BF16)

        return [(1, q)] + ([(1, k), (1, v)] if g % 2 == 0 else []) + [(1, do)]

    def stacked(h, c):
        return (h * half + c) if c < half else (seq + h * half + c - half)

    def rope(g):
        cs, sn = (r.tab.at[2], r.tab.at[3]) if g == n_grp - 1 else (r.tab.at[0], r.tab.at[1])

        def size(h, c):
            def run():
                raw = r.knew[g, c:c + CH, :] if h == 2 else r.qnew[g % 2, h, c:c + CH, :]
                r.raw[g, h, c:c + CH, :] = raw
                t = raw.astype(F32)
                r.inv[g, h, c:c + CH, :] = jnp.broadcast_to(lax.rsqrt(jnp.mean(t * t, axis=-1, keepdims=True) + EPS), t.shape)

            return (0.4, run)

        def turn(h, c):
            def run():
                t = r.raw[g, h, c:c + CH, :].astype(F32)
                w = (t * r.inv[g, h, c:c + CH, :]) * (r.kg if h == 2 else r.qg)[0:1, :]
                o = 2 * seq + c if h == 2 else stacked(h, c)
                x = pltpu.roll(w, HD // 2, 1)
                co, si = cs[c:c + CH, :], sn[c:c + CH, :]
                r.rot[g, o:o + CH, 0:HD] = (w * co + x * si).astype(BF16)
                r.rot[g, o:o + CH, HD:] = (x * co - w * si).astype(BF16)
                if h == 2:
                    r.v[g, c:c + CH, :] = r.vnew[g, c:c + CH, :]

            return (0.6, run)

        return [f(h, c) for f in (size, turn) for h in (2, 0, 1) for c in range(0, seq, CH)]

    def scores(g):
        b = g % 2

        def s():
            r.s[b, 0:seq, 0:half] = dot(r.rot[g, 0:seq, 0:HD], r.rot[g, 2 * seq:2 * seq + half, 0:HD], NT)
            r.s[b, seq:, :] = dot(r.rot[g, seq:2 * seq, 0:HD], r.rot[g, 2 * seq:, 0:HD], NT)

        def dp():
            r.dp[b, 0:seq, 0:half] = dot(r.do[g, :seq, :], r.v[g, :half, :], NT)
            r.dp[b, seq:, :] = dot(r.do[g, seq:, :], r.v[g], NT)

        return [(1, s), (1, dp)]

    def soft(g):
        b = g % 2
        c2 = scale * log2e

        def part(blk, c):
            return slice(blk * seq + c, blk * seq + c + CH), half if blk == 0 else seq

        def masked(blk, c, s):
            row_id = lax.broadcasted_iota(jnp.int32, (CH, half), 0) + (c % half)
            keep = row_id >= lax.broadcasted_iota(jnp.int32, (CH, half), 1)
            if blk == 0:
                return jnp.where(keep, s, -jnp.inf)
            return jnp.concatenate([s[:, :half], jnp.where(keep, s[:, half:], -jnp.inf)], axis=1)

        def wide(ref, rows, width):
            t = ref[rows, :]
            return t if width == half else jnp.concatenate([t, t], axis=1)

        def top(blk, c):
            rows, width = part(blk, c)

            def run():
                m = jnp.max(masked(blk, c, r.s[b, rows, 0:width]), axis=-1, keepdims=True)
                r.st[0, rows, :] = jnp.broadcast_to(m * c2, (CH, HD))

            return (0.4 + 0.4 * blk, run)

        def power(blk, c):
            rows, width = part(blk, c)

            def run():
                e = jnp.exp2(masked(blk, c, r.s[b, rows, 0:width] * c2) - wide(r.st.at[0], rows, width))
                r.s[b, rows, 0:width] = e
                r.st[1, rows, :] = jnp.broadcast_to(1.0 / jnp.sum(e, axis=-1, keepdims=True), (CH, HD))

            return (0.8 + 0.8 * blk, run)

        def prob(blk, c):
            rows, width = part(blk, c)

            def run():
                pr = r.s[b, rows, 0:width] * wide(r.st.at[1], rows, width)
                r.s[b, rows, 0:width] = pr
                r.p[b, rows, 0:width] = pr.astype(BF16)
                r.st[2, rows, :] = jnp.broadcast_to(jnp.sum(pr * r.dp[b, rows, 0:width], axis=-1, keepdims=True), (CH, HD))

            return (0.8 + 0.8 * blk, run)

        def last(blk, c):
            rows, width = part(blk, c)

            def run():
                d = r.dp[b, rows, 0:width] - wide(r.st.at[2], rows, width)
                r.ds[b, rows, 0:width] = (r.s[b, rows, 0:width] * d * scale).astype(BF16)

            return (0.8 + 0.8 * blk, run)

        return [f(blk, c) for f in (top, power, prob, last) for blk in range(2) for c in range(0, seq, CH)]

    def grads(g):
        b = g % 2
        col, kcol = g * 2 * HD, g * HD

        def dq():
            r.dqf[b, 0:seq, :] = dot(r.ds[b, 0:seq, 0:half], r.rot[g, 2 * seq:2 * seq + half, :])
            r.dqf[b, seq:, :] = dot(r.ds[b, seq:, :], r.rot[g, 2 * seq:, :])

        def dk():
            tb = dot(r.ds[b, seq:, :], r.rot[g, seq:2 * seq, :], TN)
            ta = dot(r.ds[b, 0:seq, 0:half], r.rot[g, 0:seq, :], TN)
            r.dkf[b, :half, :] = tb[:half] + ta
            r.dkf[b, half:, :] = tb[half:]

        def o():
            ta = dot(r.p[b, 0:seq, 0:half], r.v[g, :half, :])
            tb = dot(r.p[b, seq:, :], r.v[g])
            for h in range(2):
                r.o[0:half, col + h * HD:col + (h + 1) * HD] = ta[h * half:(h + 1) * half].astype(BF16)
                r.o[half:seq, col + h * HD:col + (h + 1) * HD] = tb[h * half:(h + 1) * half].astype(BF16)

        def dv():
            tb = dot(r.p[b, seq:, :], r.do[g, seq:, :], TN)
            ta = dot(r.p[b, 0:seq, 0:half], r.do[g, :seq, :], TN)
            r.dv[0:half, kcol:kcol + HD] = (tb[:half] + ta).astype(BF16)
            r.dv[half:seq, kcol:kcol + HD] = tb[half:].astype(BF16)

        return [(1, dq), (1, dk), (1, o), (1, dv)]

    def back(g):
        b = g % 2

        def place(h, c):
            if h == 2:
                return r.dkf, c, r.dk, g * HD, r.kg
            return r.dqf, stacked(h, c), r.dq, (2 * g + h) * HD, r.qg

        def turn(h, c):
            src, o, _, _, g_ref = place(h, c)

            def run():
                d = src[b, o:o + CH, :].astype(BF16).astype(F32)
                that = r.raw[g, h, c:c + CH, :].astype(F32) * r.inv[g, h, c:c + CH, :]
                du = d[:, :HD] * r.tab[2, c:c + CH, :] - d[:, HD:] * r.tab[3, c:c + CH, :]
                src[b, o:o + CH, 0:HD] = du
                pr = du * that
                dg_ref = r.dgk if h == 2 else r.dgq
                dg_ref[...] += jnp.sum(pr.reshape(CH // 8, 8, HD), axis=0)
                r.sb[h, c:c + CH, :] = jnp.broadcast_to(jnp.mean(pr * g_ref[0:1, :], axis=-1, keepdims=True), (CH, HD))

            return (0.6, run)

        def out(h, c):
            src, o, out_ref, col, g_ref = place(h, c)

            def run():
                inv = r.inv[g, h, c:c + CH, :]
                that = r.raw[g, h, c:c + CH, :].astype(F32) * inv
                out_ref[c:c + CH, col:col + HD] = (inv * (src[b, o:o + CH, 0:HD] * g_ref[0:1, :] - that * r.sb[h, c:c + CH, :])).astype(BF16)

            return (0.5, run)

        return [f(h, c) for f in (turn, out) for h in (0, 1, 2) for c in range(0, seq, CH)]

    return SimpleNamespace(norm=norm_rows, proj=proj, rope=rope, scores=scores, soft=soft, grads=grads, back=back)


def attn_tick(st, g, n_grp, more=()):
    gr = st.grads(g)
    for _, f in gr[:2]:
        f()
    weave(st.soft((g - 3) % n_grp), st.rope((g - 1) % n_grp), st.back(g), st.scores((g - 2) % n_grp) + gr[2:] + st.proj(g) + list(more))


def attn_scratch(seq, n_grp):
    return dict(
        qnew=pltpu.VMEM((2, 2, seq, HD), BF16),
        knew=pltpu.VMEM((n_grp, seq, HD), BF16),
        vnew=pltpu.VMEM((n_grp, seq, HD), BF16),
        raw=pltpu.VMEM((n_grp, 3, seq, HD), BF16),
        inv=pltpu.VMEM((n_grp, 3, seq, HD), F32),
        rot=pltpu.VMEM((n_grp, 3 * seq, 2 * HD), BF16),
        do=pltpu.VMEM((n_grp, 2 * seq, HD), BF16),
        v=pltpu.VMEM((n_grp, seq, HD), BF16),
        s=pltpu.VMEM((2, 2 * seq, seq), F32),
        dp=pltpu.VMEM((2, 2 * seq, seq), F32),
        p=pltpu.VMEM((2, 2 * seq, seq), BF16),
        ds=pltpu.VMEM((2, 2 * seq, seq), BF16),
        dkf=pltpu.VMEM((2, seq, 2 * HD), F32),
        dqf=pltpu.VMEM((2, 2 * seq, 2 * HD), F32),
        st=pltpu.VMEM((3, 2 * seq, HD), F32),
        sb=pltpu.VMEM((3, seq, HD), F32),
        tab=pltpu.VMEM((4, seq, HD), F32),
    )


EARLY = 4


def tail_kernel(seq, n_grp, rows, keys, sel_ref, n_in, dy_in, cos_in, sin_in, x_in, dyx_in, gain_ref, qg_ref, kg_ref, dgq_own, dgk_own, *refs):
    own_w, oth_w, own_a = refs[:4], refs[4:8], refs[8:12]
    y_out, dx_out, sums_out = refs[12:15]
    r = SimpleNamespace(n=n_in, dy=dy_in, qg=qg_ref, kg=kg_ref, gain=gain_ref, **dict(zip(keys, refs[15:])))
    step = pl.program_id(0)
    me = sel_ref[0]
    oth = 1 - me
    D = x_in.shape[1]
    r.wq = lambda c: r.wq_all[oth, :, c]
    r.wk = lambda c: r.wk_all[oth, :, c]
    r.wv = lambda c: r.wv_all[oth, :, c]
    r.do_dot = lambda c: dot(dy_in[...], r.wo_all[oth, c, :], NT)
    r.o, r.dq, r.dk, r.dv = r.oc.at[oth], r.dqc.at[oth], r.dkc.at[oth], r.dvc.at[oth]
    st = attn_stages(seq, n_grp, r)

    def fetch(row):
        return [pltpu.make_async_copy(src.at[me, pl.ds(row * seq, seq), :], dst.at[me], r.sem.at[8 + k])
                for k, (src, dst) in enumerate(zip(own_a[1:], (r.dqc, r.dkc, r.dvc)))]

    def fetch_o(row):
        return pltpu.make_async_copy(own_a[0].at[me, pl.ds(row * seq, seq), :], r.o_next, r.sem.at[11])

    weights = (r.wq_all, r.wk_all, r.wv_all, r.wo_all)
    theirs = [pltpu.make_async_copy(oth_w[k], dst.at[oth], r.sem.at[4 + k]) for k, dst in enumerate(weights)]
    mine = [pltpu.make_async_copy(own_w[k], dst.at[me], r.sem.at[k]) for k, dst in enumerate(weights)]

    @pl.when(step == 0)
    def _():
        for c in theirs + mine[3:] + mine[:3]:
            c.start()
        r.dg[...] = jnp.zeros_like(r.dg)
        r.oc[...] = jnp.zeros_like(r.oc)
        for c in theirs + mine[3:]:
            c.wait()

    @pl.when(step > 0)
    def _():
        for c in fetch(step - 1):
            c.start()
        fetch_o(step - 1).wait()
        r.oc[me] = r.o_next[...]

    @pl.when(step < rows)
    def _():
        fetch_o(step).start()

    CR, NC = 32, 256
    nn = D // NC
    lines = range(0, seq, CR)

    def wide(v):
        return jnp.concatenate([v] * (NC // HD), axis=1)

    def stat(c):
        def run():
            xf = x_in[c:c + CR, :].astype(F32)
            r.xs[0, c:c + CR, :] = jnp.broadcast_to(lax.rsqrt(jnp.mean(xf * xf, axis=-1, keepdims=True) + EPS), (CR, HD))
            r.xs[1, c:c + CR, :] = jnp.zeros((CR, HD), F32)

        return (1, run)

    def dn_dot(n):
        def run():
            cols = slice(n * NC, (n + 1) * NC)
            t = None
            for s in range(2):
                for a_ref, w_ref in ((r.dqc, r.wq_all), (r.dkc, r.wk_all), (r.dvc, r.wv_all)):
                    u = dot(a_ref[s], w_ref[s, cols, :], NT)
                    t = u if t is None else t + u
            r.dn[:, cols] = t

        return (2, run)

    def first(n, c):
        def run():
            cols = slice(n * NC, (n + 1) * NC)
            inv = wide(r.xs[0, c:c + CR, :])
            d = r.dn[c:c + CR, cols]
            w = d * (x_in[c:c + CR, cols].astype(F32) * inv)
            r.dg[:, cols] += jnp.sum(w.reshape(CR // 8, 8, NC), axis=0)
            w = w * gain_ref[0:1, cols]
            r.xs[1, c:c + CR, :] += w[:, :HD] + w[:, HD:]
            r.dn[c:c + CR, cols] = dyx_in[c:c + CR, cols].astype(F32) + inv * (d * gain_ref[0:1, cols])

        return (1, run)

    def mean(c):
        def run():
            inv = r.xs[0, c:c + CR, :]
            r.xs[2, c:c + CR, :] = jnp.sum(r.xs[1, c:c + CR, :], axis=-1, keepdims=True) * (1.0 / D) * (inv * inv)

        return (0.2, run)

    def second(n, c):
        def run():
            cols = slice(n * NC, (n + 1) * NC)
            dx_out[c:c + CR, cols] = (r.dn[c:c + CR, cols] - x_in[c:c + CR, cols].astype(F32) * wide(r.xs[2, c:c + CR, :])).astype(BF16)

        return (1, run)

    def y_dot(n):
        def run():
            cols = slice(n * NC, (n + 1) * NC)
            t = dot(r.oc[0], r.wo_all[0, :, cols]) + dot(r.oc[1], r.wo_all[1, :, cols])
            y_out[:, cols] = (x_in[:, cols].astype(F32) + t).astype(BF16)

        return (1, run)

    r.tab[2:4] = r.tab[0:2]
    r.tab[0] = cos_in[...]
    r.tab[1] = sin_in[...]
    yd = [y_dot(n) for n in range(nn)]
    for g in range(n_grp):
        attn_tick(st, g, n_grp, yd[:EARLY] if g == n_grp - 1 else [])
    for acc in (r.dgq, r.dgk):
        acc[...] = jnp.where(step > 0, acc[...], 0.0)

    @pl.when(step == 0)
    def _():
        for c in mine[:3]:
            c.wait()

    @pl.when(step > 0)
    def _():
        for c in fetch(step - 1):
            c.wait()
        dn = [dn_dot(n) for n in range(nn)]
        for _, f in dn[:1]:
            f()
        weave([stat(c) for c in lines], dn[1:2])
        for n in range(2, nn):
            weave([first(n - 2, c) for c in lines], dn[n:n + 1])
        weave([first(nn - 2, c) for c in lines], yd[EARLY:EARLY + 1])
        weave([first(nn - 1, c) for c in lines] + [mean(c) for c in lines], yd[EARLY + 1:EARLY + 2])
        weave([second(n, c) for n in range(nn) for c in lines], yd[EARLY + 2:])

    @pl.when(step == rows)
    def _():
        at = 0
        for part in (r.dg[...], r.dgq[...] + dgq_own[...], r.dgk[...] + dgk_own[...]):
            sums_out[:, at:at + part.shape[1]] = jnp.sum(part, axis=0, keepdims=True)
            at += part.shape[1]


def tail_call(sel, n, x, dy, cosd, sind, o, dq, dk, dv, gain, qg, kg, dgq, dgk, own, oth, seq=256):
    T, D = x.shape
    nq, nk = dq.shape[2], dk.shape[2]
    n_grp = nk // HD
    rows = T // seq
    lag = lambda k, c: pl.BlockSpec((seq, c), lambda i, s: (jnp.clip(i - k, 0, rows - 1), 0))
    const = lambda *b: pl.BlockSpec(b, lambda i, s: (0,) * len(b), pipeline_mode=pl.Buffered(1))
    hbm = pl.BlockSpec(memory_space=pl.ANY)
    scratch = attn_scratch(seq, n_grp)
    scratch.update(
        wq_all=pltpu.VMEM((2, D, nq), BF16), wk_all=pltpu.VMEM((2, D, nk), BF16), wv_all=pltpu.VMEM((2, D, nk), BF16), wo_all=pltpu.VMEM((2, nq, D), BF16),
        dn=pltpu.VMEM((seq, D), F32), oc=pltpu.VMEM((2, seq, nq), BF16), dqc=pltpu.VMEM((2, seq, nq), BF16), dkc=pltpu.VMEM((2, seq, nk), BF16), dvc=pltpu.VMEM((2, seq, nk), BF16),
        o_next=pltpu.VMEM((seq, nq), BF16), xs=pltpu.VMEM((3, seq, HD), F32), dg=pltpu.VMEM((8, D), F32), dgq=pltpu.VMEM((8, HD), F32), dgk=pltpu.VMEM((8, HD), F32), sem=pltpu.SemaphoreType.DMA((12,)))
    flops = 2 * T * D * (nq + 2 * nk + nq) * 3 + 12 * T * nq * seq
    return pl.pallas_call(
        functools.partial(tail_kernel, seq, n_grp, rows, tuple(scratch)),
        grid_spec=pltpu.PrefetchScalarGridSpec(
            num_scalar_prefetch=1,
            grid=(rows + 1,),
            in_specs=[lag(0, D), lag(0, D), lag(0, HD), lag(0, HD), lag(1, D), lag(1, D), const(1, D), const(1, HD), const(1, HD), const(8, HD), const(8, HD)] + [hbm] * 12,
            out_specs=[lag(1, D), lag(1, D), pl.BlockSpec((1, D + 2 * HD), lambda i, s: (0, 0))],
            scratch_shapes=list(scratch.values()),
        ),
        out_shape=[jax.ShapeDtypeStruct((T, D), BF16)] * 2 + [jax.ShapeDtypeStruct((1, D + 2 * HD), F32)],
        compiler_params=pltpu.CompilerParams(dimension_semantics=("arbitrary",), vmem_limit_bytes=67043328),
        cost_estimate=pl.CostEstimate(flops=flops, bytes_accessed=T * D * 14, transcendentals=T * nq * 2),
        name="tail",
    )(sel, n, dy, cosd, sind, x, dy, gain, qg, kg, dgq, dgk, *own, *oth, o, dq, dk, dv)


def solution(mesh):
    tok_spec = P("dp", None, None)
    col_spec = P(None, "tp")
    row_spec = P("tp", None)
    n_dp = mesh.shape["dp"]

    def per_device(x_in, dy_in, positions, g_attn, q_gain, k_gain, w_q, w_k, w_v, w_o):
        n_batch, n_seq, D = x_in.shape
        T = n_batch * n_seq
        nk = w_k.shape[1]
        x, dy = x_in.reshape(T, D), dy_in.reshape(T, D)
        me = lax.axis_index("tp").astype(jnp.int32)
        own = me.reshape(1)

        part = lax.axis_index("dp").astype(jnp.int32).reshape(1)
        share, cosd, sind = pre_call(part, w_q, w_k, w_v, w_o, positions, parts=n_dp)
        gathered = lax.all_gather(share, ("tp", "dp"), tiled=True)

        gain = g_attn.astype(F32).reshape(1, D)
        qg, kg = q_gain.astype(F32).reshape(1, HD), k_gain.astype(F32).reshape(1, HD)

        n, o, dq, dk, dv, dgq, dgk, dw_o = attn_call(True, own, x, dy, cosd, sind, gain, qg, kg, w_q, w_k, w_v, w_o, seq=n_seq)
        dw_q, dw_k, dw_v, *theirs = dw_call(own, n, [dq, dk, dv], 512, gathered=gathered, nk=nk)
        dw_o, dw_q, dw_k, dw_v = lax.psum((dw_o, dw_q, dw_k, dw_v), "dp")

        y, dx, sums = tail_call(own, n, x, dy, cosd, sind, o, dq, dk, dv, gain, qg, kg, dgq, dgk, (w_q, w_k, w_v, w_o), theirs, seq=n_seq)
        g_sum, q_sum, k_sum = (t.reshape(-1) for t in sum_call(sums, (D, HD, HD), n_dp))
        dw_o, dw_q, dw_k, dw_v = copy_call((dw_o, dw_q, dw_k, dw_v))
        return y.reshape(x_in.shape), dx.reshape(x_in.shape), dw_q, dw_k, dw_v, dw_o, q_sum, k_sum, g_sum

    return jax.shard_map(per_device, mesh=mesh, in_specs=(tok_spec, tok_spec, P("dp", None), P(), P(), P(), col_spec, col_spec, col_spec, row_spec), out_specs=(tok_spec, tok_spec, col_spec, col_spec, col_spec, row_spec, P(), P(), P()), check_vma=False)
```

```python
import functools
from types import SimpleNamespace
import jax
import jax.numpy as jnp
from jax import lax
from jax.experimental import pallas as pl
from jax.experimental.pallas import tpu as pltpu
from jax.sharding import PartitionSpec as P


EPS = 1e-6
THETA = 1000000.0
F32 = jnp.float32
BF16 = jnp.bfloat16
HD = 128
NT = (((1,), (1,)), ((), ()))
TN = (((0,), (0,)), ((), ()))
NN = (((1,), (0,)), ((), ()))


def dot(a, b, dims=NN):
    return lax.dot_general(a, b, dims, preferred_element_type=F32)


def weave(*lists):
    order = []
    for n, pieces in enumerate(lists):
        total = sum(c for c, _ in pieces) or 1
        at = 0
        for k, (c, f) in enumerate(pieces):
            order.append(((at + c / 2) / total, n, k, f))
            at += c
    for _, _, _, f in sorted(order, key=lambda e: e[:3]):
        f()


CH = 32


def attn_kernel(own, seq, n_grp, sel_ref, *refs):
    if own:
        (x0_ref, xn_ref, dy_ref, cos_ref, sin_ref, gain_ref, qg_ref, kg_ref, wq_ref, wk_ref, wv_ref, wo_ref,
         n_out, o_out, dq_out, dk_out, dv_out, dgq_out, dgk_out, dwo_out) = refs[:20]
        refs = refs[20:]
    else:
        nin_ref, dy_ref, cos_ref, sin_ref, qg_ref, kg_ref, wq_ref, wk_ref, wv_ref, wo_ref, _, _, _, _, o_out, dq_out, dk_out, dv_out = refs[:18]
        refs = refs[18:]
        n_ref = nin_ref
    (qnew_ref, knew_ref, vnew_ref, raw_ref, inv_ref, rot_ref, do_ref, v_ref, s_ref, dp_ref, p_ref, ds_ref, dkf_ref, dqf_ref, st_ref,
     tab_ref, o_ref, dq_ref, dk_ref, dv_ref) = refs[:20]
    if own:
        n_ref, nn_ref, dgq_ref, dgk_ref, acc_ref, ot_ref, dyp_ref, sem = refs[20:]
    half = seq // 2
    scale = HD ** -0.5
    log2e = 1.4426950408889634
    step = pl.program_id(0)

    def norm_rows(src, dst):
        def piece(c):
            def run():
                xf = src[c:c + 32, :].astype(F32)
                inv = lax.rsqrt(jnp.mean(xf * xf, axis=-1, keepdims=True) + EPS)
                dst[c:c + 32, :] = (xf * inv * gain_ref[0:1, :]).astype(BF16)

            return (1.5, run)

        return [piece(c) for c in range(0, seq, 32)]

    def proj(g):
        def q():
            t = dot(n_ref[...], wq_ref[:, g * 2 * HD:(g + 1) * 2 * HD])
            for h in range(2):
                qnew_ref[g % 2, h] = t[:, h * HD:(h + 1) * HD].astype(BF16)

        def k():
            t = dot(n_ref[...], wk_ref[:, g * HD:(g + 2) * HD])
            for h in range(2):
                knew_ref[g + h] = t[:, h * HD:(h + 1) * HD].astype(BF16)

        def v():
            t = dot(n_ref[...], wv_ref[:, g * HD:(g + 2) * HD])
            for h in range(2):
                vnew_ref[g + h] = t[:, h * HD:(h + 1) * HD].astype(BF16)

        def do():
            t = dot(dy_ref[...], wo_ref[g * 2 * HD:(g + 1) * 2 * HD, :], NT)
            for h in range(2):
                do_ref[g, h * half:(h + 1) * half, :] = t[:half, h * HD:(h + 1) * HD].astype(BF16)
                do_ref[g, seq + h * half:seq + (h + 1) * half, :] = t[half:, h * HD:(h + 1) * HD].astype(BF16)

        return [(1, q)] + ([(1, k), (1, v)] if g % 2 == 0 else []) + [(1, do)]

    def stacked(h, c):
        return (h * half + c) if c < half else (seq + h * half + c - half)

    def rope(g):
        cs, sn = (tab_ref.at[2], tab_ref.at[3]) if g == n_grp - 1 else (tab_ref.at[0], tab_ref.at[1])

        def size(h, c):
            def run():
                raw = knew_ref[g, c:c + CH, :] if h == 2 else qnew_ref[g % 2, h, c:c + CH, :]
                raw_ref[g, h, c:c + CH, :] = raw
                t = raw.astype(F32)
                inv_ref[g, h, c:c + CH, :] = jnp.broadcast_to(lax.rsqrt(jnp.mean(t * t, axis=-1, keepdims=True) + EPS), t.shape)

            return (0.4, run)

        def turn(h, c):
            def run():
                t = raw_ref[g, h, c:c + CH, :].astype(F32)
                w = (t * inv_ref[g, h, c:c + CH, :]) * (kg_ref if h == 2 else qg_ref)[0:1, :]
                o = 2 * seq + c if h == 2 else stacked(h, c)
                x = pltpu.roll(w, HD // 2, 1)
                co, si = cs[c:c + CH, :], sn[c:c + CH, :]
                rot_ref[g, o:o + CH, 0:HD] = (w * co + x * si).astype(BF16)
                rot_ref[g, o:o + CH, HD:] = (x * co - w * si).astype(BF16)
                if h == 2:
                    v_ref[g, c:c + CH, :] = vnew_ref[g, c:c + CH, :]

            return (0.6, run)

        return [f(h, c) for f in (size, turn) for h in (2, 0, 1) for c in range(0, seq, CH)]

    def scores(g):
        b = g % 2

        def s():
            s_ref[b, 0:seq, 0:half] = dot(rot_ref[g, 0:seq, 0:HD], rot_ref[g, 2 * seq:2 * seq + half, 0:HD], NT)
            s_ref[b, seq:, :] = dot(rot_ref[g, seq:2 * seq, 0:HD], rot_ref[g, 2 * seq:, 0:HD], NT)

        def dp():
            dp_ref[b, 0:seq, 0:half] = dot(do_ref[g, :seq, :], v_ref[g, :half, :], NT)
            dp_ref[b, seq:, :] = dot(do_ref[g, seq:, :], v_ref[g], NT)

        return [(1, s), (1, dp)]

    def soft(g):
        b = g % 2
        c2 = scale * log2e

        def part(blk, c):
            return slice(blk * seq + c, blk * seq + c + CH), half if blk == 0 else seq

        def masked(blk, c, s):
            row_id = lax.broadcasted_iota(jnp.int32, (CH, half), 0) + (c % half)
            keep = row_id >= lax.broadcasted_iota(jnp.int32, (CH, half), 1)
            if blk == 0:
                return jnp.where(keep, s, -jnp.inf)
            return jnp.concatenate([s[:, :half], jnp.where(keep, s[:, half:], -jnp.inf)], axis=1)

        def wide(ref, rows, width):
            t = ref[rows, :]
            return t if width == half else jnp.concatenate([t, t], axis=1)

        def top(blk, c):
            rows, width = part(blk, c)

            def run():
                m = jnp.max(masked(blk, c, s_ref[b, rows, 0:width]), axis=-1, keepdims=True)
                st_ref[0, rows, :] = jnp.broadcast_to(m * c2, (CH, HD))

            return (0.4 + 0.4 * blk, run)

        def power(blk, c):
            rows, width = part(blk, c)

            def run():
                e = jnp.exp2(masked(blk, c, s_ref[b, rows, 0:width] * c2) - wide(st_ref.at[0], rows, width))
                s_ref[b, rows, 0:width] = e
                st_ref[1, rows, :] = jnp.broadcast_to(1.0 / jnp.sum(e, axis=-1, keepdims=True), (CH, HD))

            return (0.8 + 0.8 * blk, run)

        def prob(blk, c):
            rows, width = part(blk, c)

            def run():
                pr = s_ref[b, rows, 0:width] * wide(st_ref.at[1], rows, width)
                s_ref[b, rows, 0:width] = pr
                p_ref[b, rows, 0:width] = pr.astype(BF16)
                st_ref[2, rows, :] = jnp.broadcast_to(jnp.sum(pr * dp_ref[b, rows, 0:width], axis=-1, keepdims=True), (CH, HD))

            return (0.8 + 0.8 * blk, run)

        def last(blk, c):
            rows, width = part(blk, c)

            def run():
                d = dp_ref[b, rows, 0:width] - wide(st_ref.at[2], rows, width)
                ds_ref[b, rows, 0:width] = (s_ref[b, rows, 0:width] * d * scale).astype(BF16)

            return (0.8 + 0.8 * blk, run)

        return [f(blk, c) for f in (top, power, prob, last) for blk in range(2) for c in range(0, seq, CH)]

    def grads(g):
        b = g % 2
        col, kcol = g * 2 * HD, g * HD

        def dq():
            dqf_ref[b, 0:seq, :] = dot(ds_ref[b, 0:seq, 0:half], rot_ref[g, 2 * seq:2 * seq + half, :])
            dqf_ref[b, seq:, :] = dot(ds_ref[b, seq:, :], rot_ref[g, 2 * seq:, :])

        def dk():
            tb = dot(ds_ref[b, seq:, :], rot_ref[g, seq:2 * seq, :], TN)
            ta = dot(ds_ref[b, 0:seq, 0:half], rot_ref[g, 0:seq, :], TN)
            dkf_ref[b, :half, :] = tb[:half] + ta
            dkf_ref[b, half:, :] = tb[half:]

        def o():
            ta = dot(p_ref[b, 0:seq, 0:half], v_ref[g, :half, :])
            tb = dot(p_ref[b, seq:, :], v_ref[g])
            for h in range(2):
                o_ref[0:half, col + h * HD:col + (h + 1) * HD] = ta[h * half:(h + 1) * half].astype(BF16)
                o_ref[half:seq, col + h * HD:col + (h + 1) * HD] = tb[h * half:(h + 1) * half].astype(BF16)

        def dv():
            tb = dot(p_ref[b, seq:, :], do_ref[g, seq:, :], TN)
            ta = dot(p_ref[b, 0:seq, 0:half], do_ref[g, :seq, :], TN)
            dv_ref[0:half, kcol:kcol + HD] = (tb[:half] + ta).astype(BF16)
            dv_ref[half:seq, kcol:kcol + HD] = tb[half:].astype(BF16)

        return [(1, dq), (1, dk), (1, o), (1, dv)]

    def back(g):
        b = g % 2

        def place(h, c):
            if h == 2:
                return dkf_ref, c, dk_ref, g * HD, kg_ref
            return dqf_ref, stacked(h, c), dq_ref, (2 * g + h) * HD, qg_ref

        def turn(h, c):
            src, o, _, _, g_ref = place(h, c)

            def run():
                d = src[b, o:o + CH, :].astype(BF16).astype(F32)
                that = raw_ref[g, h, c:c + CH, :].astype(F32) * inv_ref[g, h, c:c + CH, :]
                du = d[:, :HD] * tab_ref[2, c:c + CH, :] - d[:, HD:] * tab_ref[3, c:c + CH, :]
                src[b, o:o + CH, 0:HD] = du
                pr = du * that
                if own:
                    dg_ref = dgk_ref if h == 2 else dgq_ref
                    dg_ref[...] += jnp.sum(pr.reshape(CH // 8, 8, HD), axis=0)
                st_ref[3 + h, c:c + CH, :] = jnp.broadcast_to(jnp.mean(pr * g_ref[0:1, :], axis=-1, keepdims=True), (CH, HD))

            return (0.6, run)

        def out(h, c):
            src, o, out_ref, col, g_ref = place(h, c)

            def run():
                inv = inv_ref[g, h, c:c + CH, :]
                that = raw_ref[g, h, c:c + CH, :].astype(F32) * inv
                out_ref[c:c + CH, col:col + HD] = (inv * (src[b, o:o + CH, 0:HD] * g_ref[0:1, :] - that * st_ref[3 + h, c:c + CH, :])).astype(BF16)

            return (0.5, run)

        return [f(h, c) for f in (turn, out) for h in (0, 1, 2) for c in range(0, seq, CH)]

    def dwo(g):
        rows = slice(g * 2 * HD, (g + 1) * 2 * HD)

        def flip():
            ot_ref[rows, :] = o_ref[:, rows].T

        def part(c):
            def run():
                acc_ref[rows, c:c + 512] += dot(ot_ref[rows, :], dyp_ref[:, c:c + 512])

            return (0.25, run)

        return [(0.1, flip)] + [part(c) for c in range(0, acc_ref.shape[1], 512)]

    @pl.when(step == 0)
    def _():
        if own:
            weave(norm_rows(x0_ref, n_ref))

    tab_ref[2:4] = tab_ref[0:2]
    tab_ref[0] = cos_ref[...]
    tab_ref[1] = sin_ref[...]
    if own:
        norms = norm_rows(xn_ref, nn_ref)
    for g in range(n_grp):
        sc = scores((g - 2) % n_grp)
        gr = grads(g)
        nm = norms[g * len(norms) // n_grp:(g + 1) * len(norms) // n_grp] if own else []
        for _, f in gr[:2]:
            f()
        weave(soft((g - 3) % n_grp), rope((g - 1) % n_grp) + nm, back(g), sc + gr[2:] + (dwo(g - 1) if own and g > 0 else []) + proj(g) + (dwo(g) if own and g == n_grp - 1 else []))

    for dst, src in ((o_out, o_ref), (dq_out, dq_ref), (dk_out, dk_ref), (dv_out, dv_ref)):
        dst[0] = src[...]
    if own:
        n_out[...] = n_ref[...]
        n_ref[...] = nn_ref[...]
        keep = step > 0
        for dst, acc in ((dgq_out, dgq_ref), (dgk_out, dgk_ref)):
            acc[...] = jnp.where(keep, acc[...], 0.0)
            dst[...] = acc[...]
        dyp_ref[...] = dy_ref[...]

        @pl.when(step == 0)
        def _():
            @pl.loop(0, acc_ref.shape[0] // 64)
            def _(j):
                acc_ref[pl.ds(pl.multiple_of(j * 64, 64), 64), :] = jnp.zeros((64, acc_ref.shape[1]), F32)

        @pl.when(step == pl.num_programs(0) - 1)
        def _():
            c = pltpu.make_async_copy(acc_ref, dwo_out, sem)
            c.start()
            c.wait()


def attn_call(own, sel, x, dy, cosd, sind, gain, qg, kg, wq, wk, wv, wo, prev=None, seq=256):
    T, D = x.shape
    nq, nk = wq.shape[1], wk.shape[1]
    n_grp = nk // HD
    rows = T // seq
    const = lambda *b: pl.BlockSpec(b, lambda i, s: (0,) * len(b), pipeline_mode=pl.Buffered(1))
    now = lambda c: pl.BlockSpec((seq, c), lambda i, s: (jnp.minimum(i, rows - 1), 0))
    nxt = lambda c: pl.BlockSpec((seq, c), lambda i, s: (jnp.minimum(i + 1, rows - 1), 0))
    out3 = lambda c: pl.BlockSpec((1, seq, c), lambda i, s: (s[0], jnp.maximum(i - 1, 0), 0))
    mid = [now(D), now(HD), now(HD)]
    tail = [const(1, HD), const(1, HD), const(D, nq), const(D, nk), const(D, nk), const(nq, D)]
    shapes = [jax.ShapeDtypeStruct((2, T, c), BF16) for c in (nq, nq, nk, nk)]
    specs = [out3(nq), out3(nq), out3(nk), out3(nk)]
    aliases = {}
    if own:
        in_specs = [const(seq, D), nxt(D)] + mid + [const(1, D)] + tail
        args = [x, x, dy, cosd, sind, gain, qg, kg, wq, wk, wv, wo]
        shapes = [jax.ShapeDtypeStruct((T, D), BF16)] + shapes + [jax.ShapeDtypeStruct((8, HD), F32)] * 2 + [jax.ShapeDtypeStruct((nq, D), F32)]
        specs = [now(D)] + specs + [pl.BlockSpec((8, HD), lambda i, s: (0, 0))] * 2 + [pl.BlockSpec(memory_space=pl.ANY)]
    else:
        in_specs = [now(D)] + mid + tail + [pl.BlockSpec(memory_space=pl.ANY)] * 4
        args = [x, dy, cosd, sind, qg, kg, wq, wk, wv, wo]
        aliases = {1 + len(args) + i: i for i in range(4)}
        args += list(prev)
    flops = 2 * T * D * (nq + 2 * nk + nq) + 12 * T * nq * seq
    return pl.pallas_call(
        functools.partial(attn_kernel, own, seq, n_grp),
        grid_spec=pltpu.PrefetchScalarGridSpec(
            num_scalar_prefetch=1,
            grid=(rows + 1,),
            in_specs=in_specs,
            out_specs=specs,
            scratch_shapes=[
                pltpu.VMEM((2, 2, seq, HD), BF16),
                pltpu.VMEM((n_grp, seq, HD), BF16),
                pltpu.VMEM((n_grp, seq, HD), BF16),
                pltpu.VMEM((n_grp, 3, seq, HD), BF16),
                pltpu.VMEM((n_grp, 3, seq, HD), F32),
                pltpu.VMEM((n_grp, 3 * seq, 2 * HD), BF16),
                pltpu.VMEM((n_grp, 2 * seq, HD), BF16),
                pltpu.VMEM((n_grp, seq, HD), BF16),
                pltpu.VMEM((2, 2 * seq, seq), F32),
                pltpu.VMEM((2, 2 * seq, seq), F32),
                pltpu.VMEM((2, 2 * seq, seq), BF16),
                pltpu.VMEM((2, 2 * seq, seq), BF16),
                pltpu.VMEM((2, seq, 2 * HD), F32),
                pltpu.VMEM((2, 2 * seq, 2 * HD), F32),
                pltpu.VMEM((6, 2 * seq, HD), F32),
                pltpu.VMEM((4, seq, HD), F32),
            ] + [pltpu.VMEM((seq, c), BF16) for c in (nq, nq, nk, nk)]
            + ([pltpu.VMEM((seq, D), BF16)] * 2 + [pltpu.VMEM((8, HD), F32)] * 2 + [pltpu.VMEM((nq, D), F32), pltpu.VMEM((nq, seq), BF16), pltpu.VMEM((seq, D), BF16), pltpu.SemaphoreType.DMA] if own else []),
        ),
        out_shape=shapes,
        input_output_aliases=aliases,
        compiler_params=pltpu.CompilerParams(dimension_semantics=("arbitrary",), vmem_limit_bytes=62 << 20),
        cost_estimate=pl.CostEstimate(flops=flops, bytes_accessed=T * D * 6 + T * (2 * nq + 2 * nk) * 2, transcendentals=T * nq * 2),
        name="attn_own" if own else "attn_other",
    )(sel, *args)


def pre_kernel(sel_ref, q_ref, k_ref, v_ref, o_ref, pos_ref, freq_ref, out_ref, cos_ref, sin_ref):
    d, nq, nk = q_ref.shape[0], q_ref.shape[1], k_ref.shape[1]
    out_ref[0, 0:d, 0:nq] = q_ref[...].astype(F32)
    out_ref[0, 0:d, nq:nq + nk] = k_ref[...].astype(F32)
    out_ref[0, 0:d, nq + nk:] = v_ref[...].astype(F32)
    out_ref[0, d:, :] = o_ref[...].astype(F32)
    n, seq = pos_ref.shape
    lane = lax.broadcasted_iota(jnp.int32, (HD, HD), 1)
    for r in range(n):
        for h in range(seq // HD):
            p = pos_ref[r:r + 1, h * HD:(h + 1) * HD].astype(F32)
            a = jnp.broadcast_to(p, (HD, HD)).T * freq_ref[0:1, :]
            k = jnp.round(a * 0.6366197723675814)
            x = ((a - k * 1.5703125) - k * 4.837512969970703125e-4) - k * 7.549789948768648e-8
            z = x * x
            s = ((-1.9515295891e-4 * z + 8.3321608736e-3) * z - 1.6666654611e-1) * z * x + x
            c = ((2.443315711809948e-5 * z - 1.388731625493765e-3) * z + 4.166664568298827e-2) * z * z - 0.5 * z + 1.0
            q = k.astype(jnp.int32)
            odd = (q & 1) == 1
            co, si = jnp.where(odd, s, c), jnp.where(odd, c, s)
            rows = slice((r * (seq // HD) + h) * HD, (r * (seq // HD) + h + 1) * HD)
            cos_ref[rows, :] = jnp.where(((q + 1) & 2) == 0, co, -co)
            sin_ref[rows, :] = jnp.where(((q & 2) == 0) == (lane >= HD // 2), si, -si)


def pre_call(part, w_q, w_k, w_v, w_o, positions, parts=2, cuts=4):
    D, nq = w_q.shape
    n, seq = positions.shape
    rows = n // cuts
    freq = THETA ** (-jnp.arange(0, HD, 2, dtype=F32) / HD)
    freq = jnp.concatenate([freq, freq]).reshape(1, HD)
    spec = lambda w: pl.BlockSpec((w.shape[0] // (parts * cuts), w.shape[1]), lambda i, s: (s[0] * cuts + i, 0))
    r = (D + nq) // (parts * cuts)
    table = pl.BlockSpec((rows * seq, HD), lambda i, s: (i, 0))
    return pl.pallas_call(
        pre_kernel,
        grid_spec=pltpu.PrefetchScalarGridSpec(
            num_scalar_prefetch=1,
            grid=(cuts,),
            in_specs=[spec(w) for w in (w_q, w_k, w_v, w_o)] + [pl.BlockSpec((rows, seq), lambda i, s: (i, 0)), pl.BlockSpec((1, HD), lambda i, s: (0, 0))],
            out_specs=[pl.BlockSpec((1, r, D), lambda i, s: (i, 0, 0)), table, table],
        ),
        out_shape=[jax.ShapeDtypeStruct((cuts, r, D), F32)] + [jax.ShapeDtypeStruct((n * seq, HD), F32)] * 2,
        compiler_params=pltpu.CompilerParams(dimension_semantics=("arbitrary",), vmem_limit_bytes=60 << 20),
        cost_estimate=pl.CostEstimate(flops=n * seq * HD * 30, bytes_accessed=cuts * r * D * 6 + n * seq * HD * 8, transcendentals=0),
        name="pre",
    )(part, w_q, w_k, w_v, w_o, positions, freq)


def dw_kernel(n_b, unpack, sel_ref, a_ref, *refs):
    if unpack:
        f_ref, parts = refs[n_b], refs[2 * n_b + 1:2 * n_b + 5]
        refs = refs[:n_b] + refs[n_b + 1:2 * n_b + 1] + refs[2 * n_b + 5:]
        q_ref, k_ref, v_ref, o_ref = parts
        per, nq, nk = f_ref.shape[0], q_ref.shape[1], k_ref.shape[1]
        d, e = q_ref.shape[0] // per, o_ref.shape[0] // per
        for j in range(per):
            q_ref[j * d:(j + 1) * d, :] = f_ref[j, 0:d, 0:nq].astype(BF16)
            k_ref[j * d:(j + 1) * d, :] = f_ref[j, 0:d, nq:nq + nk].astype(BF16)
            v_ref[j * d:(j + 1) * d, :] = f_ref[j, 0:d, nq + nk:].astype(BF16)
            o_ref[j * e:(j + 1) * e, :] = f_ref[j, d:, :].astype(BF16)
    bs, outs, accs, (at_ref, sem) = refs[:n_b], refs[n_b:2 * n_b], refs[2 * n_b:3 * n_b], refs[3 * n_b:]
    flat = lambda ref: ref.at[0] if len(ref.shape) == 3 else ref
    a, bs = flat(a_ref), [flat(b) for b in bs]
    M, tile = at_ref.shape
    step = pl.program_id(0)

    @pl.when(step == 0)
    def _():
        for acc in accs:
            @pl.loop(0, M // 64)
            def _(j):
                acc[pl.ds(pl.multiple_of(j * 64, 64), 64), :] = jnp.zeros((64, acc.shape[1]), F32)

    def part(acc, b, c):
        def run():
            acc[:, c:c + 256] += dot(at_ref[...], b[:, c:c + 256])

        return (1, run)

    for c in range(0, M, 256):
        for k in range(0, tile, 256):
            at_ref[c:c + 256, k:k + 256] = a[k:k + 256, c:c + 256].T
    weave([part(acc, b, c) for acc, b in zip(accs, bs) for c in range(0, b.shape[1], 256)])

    @pl.when(step == pl.num_programs(0) - 1)
    def _():
        copies = [pltpu.make_async_copy(acc, out, sem.at[k]) for k, (acc, out) in enumerate(zip(accs, outs))]
        for c in copies:
            c.start()
        for c in copies:
            c.wait()


def dw_call(sel, a, bs, tile, gathered=None, nk=0):
    def spec(v):
        if v.ndim == 3:
            return pl.BlockSpec((1, tile, v.shape[2]), lambda i, s: (s[0], i, 0))
        return pl.BlockSpec((tile, v.shape[1]), lambda i, s: (i, 0))

    T, M = a.shape[-2:]
    shapes = [(M, b.shape[-1]) for b in bs]
    width = sum(s[1] for s in shapes)
    steps = T // tile
    more_in, more_out, more_shapes, more = [], [], [], []
    if gathered is not None:
        n, r, D = gathered.shape
        per = n // 2 // steps
        more = [gathered]
        more_in = [pl.BlockSpec((per, r, D), lambda i, s: ((1 - s[0]) * steps + i, 0, 0))]
        nq = D - 2 * nk
        more_shapes = [jax.ShapeDtypeStruct(s, BF16) for s in ((D, nq), (D, nk), (D, nk), (nq, D))]
        more_out = [pl.BlockSpec((s.shape[0] // steps, s.shape[1]), lambda i, s: (i, 0)) for s in more_shapes]
    return pl.pallas_call(
        functools.partial(dw_kernel, len(bs), gathered is not None),
        grid_spec=pltpu.PrefetchScalarGridSpec(
            num_scalar_prefetch=1,
            grid=(steps,),
            in_specs=[spec(a)] + [spec(b) for b in bs] + more_in,
            out_specs=[pl.BlockSpec(memory_space=pl.ANY)] * len(bs) + more_out,
            scratch_shapes=[pltpu.VMEM(s, F32) for s in shapes] + [pltpu.VMEM((M, tile), BF16), pltpu.SemaphoreType.DMA((len(bs),))],
        ),
        out_shape=[jax.ShapeDtypeStruct(s, F32) for s in shapes] + more_shapes,
        compiler_params=pltpu.CompilerParams(dimension_semantics=("arbitrary",), vmem_limit_bytes=60 << 20),
        cost_estimate=pl.CostEstimate(flops=2 * T * M * width, bytes_accessed=2 * T * (M + width) + 4 * M * width, transcendentals=0),
    )(sel, a, *bs, *more)


def sum_kernel(n, widths, part_ref, *refs):
    outs, (slots, local_sem, send_sem, recv_sem) = refs[:-4], refs[-4:]
    me = lax.axis_index("dp")
    barrier = pltpu.get_barrier_semaphore()
    for k in range(1, n):
        pl.semaphore_signal(barrier, inc=1, device_id={"dp": lax.rem(me + k, n)}, device_id_type=pl.DeviceIdType.MESH)
    mine = pltpu.make_async_copy(part_ref, slots.at[0], local_sem)
    mine.start()
    pl.semaphore_wait(barrier, n - 1)
    copies = []
    for k in range(1, n):
        copies.append(pltpu.make_async_remote_copy(
            src_ref=part_ref, dst_ref=slots.at[k], send_sem=send_sem.at[k - 1], recv_sem=recv_sem.at[k - 1],
            device_id={"dp": lax.rem(me + k, n)}, device_id_type=pl.DeviceIdType.MESH))
    for c in copies:
        c.start()
    mine.wait()
    for c in copies:
        c.wait()
    total = slots[lax.rem(me + n, n)]
    for a in range(1, n):
        total = total + slots[lax.rem(me + n - a, n)]
    at = 0
    for out, w in zip(outs, widths):
        out[...] = total[:, at:at + w]
        at += w


def sum_call(part, widths, n):
    return pl.pallas_call(
        functools.partial(sum_kernel, n, widths),
        in_specs=[pl.BlockSpec(memory_space=pl.ANY)],
        out_specs=[pl.BlockSpec(memory_space=pltpu.VMEM)] * len(widths),
        out_shape=[jax.ShapeDtypeStruct((1, w), F32) for w in widths],
        scratch_shapes=[pltpu.VMEM((n, *part.shape), F32), pltpu.SemaphoreType.DMA, pltpu.SemaphoreType.DMA((n - 1,)), pltpu.SemaphoreType.DMA((n - 1,))],
        compiler_params=pltpu.CompilerParams(collective_id=0, has_side_effects=True),
        cost_estimate=pl.CostEstimate(flops=n * part.size, bytes_accessed=8 * n * part.size, transcendentals=0),
        name="small_sum",
    )(part)


def copy_kernel(n, cuts, *refs):
    srcs, dsts, bufs, (in_sem, out_sem) = refs[:n], refs[n:2 * n], refs[2 * n:3 * n], refs[3 * n:]
    ins, outs = [], []
    for a, (src, dst, buf) in enumerate(zip(srcs, dsts, bufs)):
        rows = src.shape[0] // cuts
        for j in range(cuts):
            part = pl.ds(j * rows, rows)
            ins.append(pltpu.make_async_copy(src.at[part], buf.at[part], in_sem.at[a, j]))
            outs.append(pltpu.make_async_copy(buf.at[part], dst.at[part], out_sem.at[a, j]))
    for c in ins:
        c.start()
    for c, d in zip(ins, outs):
        c.wait()
        d.start()
    for d in outs:
        d.wait()


def copy_call(arrays, cuts=4):
    n = len(arrays)
    hbm = [pl.BlockSpec(memory_space=pl.ANY)] * n
    return pl.pallas_call(
        functools.partial(copy_kernel, n, cuts),
        in_specs=hbm,
        out_specs=hbm,
        out_shape=[jax.ShapeDtypeStruct(a.shape, a.dtype) for a in arrays],
        scratch_shapes=[pltpu.VMEM(a.shape, a.dtype) for a in arrays] + [pltpu.SemaphoreType.DMA((n, cuts))] * 2,
        compiler_params=pltpu.CompilerParams(vmem_limit_bytes=60 << 20),
        cost_estimate=pl.CostEstimate(flops=0, bytes_accessed=8 * sum(a.size for a in arrays), transcendentals=0),
        name="results",
    )(*arrays)


def attn_stages(seq, n_grp, r):
    half = seq // 2
    scale = HD ** -0.5
    log2e = 1.4426950408889634

    def norm_rows(src, dst):
        def piece(c):
            def run():
                xf = src[c:c + 32, :].astype(F32)
                inv = lax.rsqrt(jnp.mean(xf * xf, axis=-1, keepdims=True) + EPS)
                dst[c:c + 32, :] = (xf * inv * r.gain[0:1, :]).astype(BF16)

            return (1.5, run)

        return [piece(c) for c in range(0, seq, 32)]

    def proj(g):
        def q():
            t = dot(r.n[...], r.wq(slice(g * 2 * HD, (g + 1) * 2 * HD)))
            for h in range(2):
                r.qnew[g % 2, h] = t[:, h * HD:(h + 1) * HD].astype(BF16)

        def k():
            t = dot(r.n[...], r.wk(slice(g * HD, (g + 2) * HD)))
            for h in range(2):
                r.knew[g + h] = t[:, h * HD:(h + 1) * HD].astype(BF16)

        def v():
            t = dot(r.n[...], r.wv(slice(g * HD, (g + 2) * HD)))
            for h in range(2):
                r.vnew[g + h] = t[:, h * HD:(h + 1) * HD].astype(BF16)

        def do():
            t = r.do_dot(slice(g * 2 * HD, (g + 1) * 2 * HD))
            for h in range(2):
                r.do[g, h * half:(h + 1) * half, :] = t[:half, h * HD:(h + 1) * HD].astype(BF16)
                r.do[g, seq + h * half:seq + (h + 1) * half, :] = t[half:, h * HD:(h + 1) * HD].astype(BF16)

        return [(1, q)] + ([(1, k), (1, v)] if g % 2 == 0 else []) + [(1, do)]

    def stacked(h, c):
        return (h * half + c) if c < half else (seq + h * half + c - half)

    def rope(g):
        cs, sn = (r.tab.at[2], r.tab.at[3]) if g == n_grp - 1 else (r.tab.at[0], r.tab.at[1])

        def size(h, c):
            def run():
                raw = r.knew[g, c:c + CH, :] if h == 2 else r.qnew[g % 2, h, c:c + CH, :]
                r.raw[g, h, c:c + CH, :] = raw
                t = raw.astype(F32)
                r.inv[g, h, c:c + CH, :] = jnp.broadcast_to(lax.rsqrt(jnp.mean(t * t, axis=-1, keepdims=True) + EPS), t.shape)

            return (0.4, run)

        def turn(h, c):
            def run():
                t = r.raw[g, h, c:c + CH, :].astype(F32)
                w = (t * r.inv[g, h, c:c + CH, :]) * (r.kg if h == 2 else r.qg)[0:1, :]
                o = 2 * seq + c if h == 2 else stacked(h, c)
                x = pltpu.roll(w, HD // 2, 1)
                co, si = cs[c:c + CH, :], sn[c:c + CH, :]
                r.rot[g, o:o + CH, 0:HD] = (w * co + x * si).astype(BF16)
                r.rot[g, o:o + CH, HD:] = (x * co - w * si).astype(BF16)
                if h == 2:
                    r.v[g, c:c + CH, :] = r.vnew[g, c:c + CH, :]

            return (0.6, run)

        return [f(h, c) for f in (size, turn) for h in (2, 0, 1) for c in range(0, seq, CH)]

    def scores(g):
        b = g % 2

        def s():
            r.s[b, 0:seq, 0:half] = dot(r.rot[g, 0:seq, 0:HD], r.rot[g, 2 * seq:2 * seq + half, 0:HD], NT)
            r.s[b, seq:, :] = dot(r.rot[g, seq:2 * seq, 0:HD], r.rot[g, 2 * seq:, 0:HD], NT)

        def dp():
            r.dp[b, 0:seq, 0:half] = dot(r.do[g, :seq, :], r.v[g, :half, :], NT)
            r.dp[b, seq:, :] = dot(r.do[g, seq:, :], r.v[g], NT)

        return [(1, s), (1, dp)]

    def soft(g):
        b = g % 2
        c2 = scale * log2e

        def part(blk, c):
            return slice(blk * seq + c, blk * seq + c + CH), half if blk == 0 else seq

        def masked(blk, c, s):
            row_id = lax.broadcasted_iota(jnp.int32, (CH, half), 0) + (c % half)
            keep = row_id >= lax.broadcasted_iota(jnp.int32, (CH, half), 1)
            if blk == 0:
                return jnp.where(keep, s, -jnp.inf)
            return jnp.concatenate([s[:, :half], jnp.where(keep, s[:, half:], -jnp.inf)], axis=1)

        def wide(ref, rows, width):
            t = ref[rows, :]
            return t if width == half else jnp.concatenate([t, t], axis=1)

        def top(blk, c):
            rows, width = part(blk, c)

            def run():
                m = jnp.max(masked(blk, c, r.s[b, rows, 0:width]), axis=-1, keepdims=True)
                r.st[0, rows, :] = jnp.broadcast_to(m * c2, (CH, HD))

            return (0.4 + 0.4 * blk, run)

        def power(blk, c):
            rows, width = part(blk, c)

            def run():
                e = jnp.exp2(masked(blk, c, r.s[b, rows, 0:width] * c2) - wide(r.st.at[0], rows, width))
                r.s[b, rows, 0:width] = e
                r.st[1, rows, :] = jnp.broadcast_to(1.0 / jnp.sum(e, axis=-1, keepdims=True), (CH, HD))

            return (0.8 + 0.8 * blk, run)

        def prob(blk, c):
            rows, width = part(blk, c)

            def run():
                pr = r.s[b, rows, 0:width] * wide(r.st.at[1], rows, width)
                r.s[b, rows, 0:width] = pr
                r.p[b, rows, 0:width] = pr.astype(BF16)
                r.st[2, rows, :] = jnp.broadcast_to(jnp.sum(pr * r.dp[b, rows, 0:width], axis=-1, keepdims=True), (CH, HD))

            return (0.8 + 0.8 * blk, run)

        def last(blk, c):
            rows, width = part(blk, c)

            def run():
                d = r.dp[b, rows, 0:width] - wide(r.st.at[2], rows, width)
                r.ds[b, rows, 0:width] = (r.s[b, rows, 0:width] * d * scale).astype(BF16)

            return (0.8 + 0.8 * blk, run)

        return [f(blk, c) for f in (top, power, prob, last) for blk in range(2) for c in range(0, seq, CH)]

    def grads(g):
        b = g % 2
        col, kcol = g * 2 * HD, g * HD

        def dq():
            r.dqf[b, 0:seq, :] = dot(r.ds[b, 0:seq, 0:half], r.rot[g, 2 * seq:2 * seq + half, :])
            r.dqf[b, seq:, :] = dot(r.ds[b, seq:, :], r.rot[g, 2 * seq:, :])

        def dk():
            tb = dot(r.ds[b, seq:, :], r.rot[g, seq:2 * seq, :], TN)
            ta = dot(r.ds[b, 0:seq, 0:half], r.rot[g, 0:seq, :], TN)
            r.dkf[b, :half, :] = tb[:half] + ta
            r.dkf[b, half:, :] = tb[half:]

        def o():
            ta = dot(r.p[b, 0:seq, 0:half], r.v[g, :half, :])
            tb = dot(r.p[b, seq:, :], r.v[g])
            for h in range(2):
                r.o[0:half, col + h * HD:col + (h + 1) * HD] = ta[h * half:(h + 1) * half].astype(BF16)
                r.o[half:seq, col + h * HD:col + (h + 1) * HD] = tb[h * half:(h + 1) * half].astype(BF16)

        def dv():
            tb = dot(r.p[b, seq:, :], r.do[g, seq:, :], TN)
            ta = dot(r.p[b, 0:seq, 0:half], r.do[g, :seq, :], TN)
            r.dv[0:half, kcol:kcol + HD] = (tb[:half] + ta).astype(BF16)
            r.dv[half:seq, kcol:kcol + HD] = tb[half:].astype(BF16)

        return [(1, dq), (1, dk), (1, o), (1, dv)]

    def back(g):
        b = g % 2

        def place(h, c):
            if h == 2:
                return r.dkf, c, r.dk, g * HD, r.kg
            return r.dqf, stacked(h, c), r.dq, (2 * g + h) * HD, r.qg

        def turn(h, c):
            src, o, _, _, g_ref = place(h, c)

            def run():
                d = src[b, o:o + CH, :].astype(BF16).astype(F32)
                that = r.raw[g, h, c:c + CH, :].astype(F32) * r.inv[g, h, c:c + CH, :]
                du = d[:, :HD] * r.tab[2, c:c + CH, :] - d[:, HD:] * r.tab[3, c:c + CH, :]
                src[b, o:o + CH, 0:HD] = du
                pr = du * that
                dg_ref = r.dgk if h == 2 else r.dgq
                dg_ref[...] += jnp.sum(pr.reshape(CH // 8, 8, HD), axis=0)
                r.sb[h, c:c + CH, :] = jnp.broadcast_to(jnp.mean(pr * g_ref[0:1, :], axis=-1, keepdims=True), (CH, HD))

            return (0.6, run)

        def out(h, c):
            src, o, out_ref, col, g_ref = place(h, c)

            def run():
                inv = r.inv[g, h, c:c + CH, :]
                that = r.raw[g, h, c:c + CH, :].astype(F32) * inv
                out_ref[c:c + CH, col:col + HD] = (inv * (src[b, o:o + CH, 0:HD] * g_ref[0:1, :] - that * r.sb[h, c:c + CH, :])).astype(BF16)

            return (0.5, run)

        return [f(h, c) for f in (turn, out) for h in (0, 1, 2) for c in range(0, seq, CH)]

    return SimpleNamespace(norm=norm_rows, proj=proj, rope=rope, scores=scores, soft=soft, grads=grads, back=back)


def attn_tick(st, g, n_grp, more=()):
    gr = st.grads(g)
    for _, f in gr[:2]:
        f()
    weave(st.soft((g - 3) % n_grp), st.rope((g - 1) % n_grp), st.back(g), st.scores((g - 2) % n_grp) + gr[2:] + st.proj(g) + list(more))


def attn_scratch(seq, n_grp):
    return dict(
        qnew=pltpu.VMEM((2, 2, seq, HD), BF16),
        knew=pltpu.VMEM((n_grp, seq, HD), BF16),
        vnew=pltpu.VMEM((n_grp, seq, HD), BF16),
        raw=pltpu.VMEM((n_grp, 3, seq, HD), BF16),
        inv=pltpu.VMEM((n_grp, 3, seq, HD), F32),
        rot=pltpu.VMEM((n_grp, 3 * seq, 2 * HD), BF16),
        do=pltpu.VMEM((n_grp, 2 * seq, HD), BF16),
        v=pltpu.VMEM((n_grp, seq, HD), BF16),
        s=pltpu.VMEM((2, 2 * seq, seq), F32),
        dp=pltpu.VMEM((2, 2 * seq, seq), F32),
        p=pltpu.VMEM((2, 2 * seq, seq), BF16),
        ds=pltpu.VMEM((2, 2 * seq, seq), BF16),
        dkf=pltpu.VMEM((2, seq, 2 * HD), F32),
        dqf=pltpu.VMEM((2, 2 * seq, 2 * HD), F32),
        st=pltpu.VMEM((3, 2 * seq, HD), F32),
        sb=pltpu.VMEM((3, seq, HD), F32),
        tab=pltpu.VMEM((4, seq, HD), F32),
    )


EARLY = 4


def tail_kernel(seq, n_grp, rows, keys, sel_ref, n_in, dy_in, cos_in, sin_in, x_in, dyx_in, gain_ref, qg_ref, kg_ref, dgq_own, dgk_own, *refs):
    own_w, oth_w, own_a = refs[:4], refs[4:8], refs[8:12]
    y_out, dx_out, sums_out = refs[12:15]
    r = SimpleNamespace(n=n_in, dy=dy_in, qg=qg_ref, kg=kg_ref, gain=gain_ref, **dict(zip(keys, refs[15:])))
    step = pl.program_id(0)
    me = sel_ref[0]
    oth = 1 - me
    D = x_in.shape[1]
    r.wq = lambda c: r.wq_all[oth, :, c]
    r.wk = lambda c: r.wk_all[oth, :, c]
    r.wv = lambda c: r.wv_all[oth, :, c]
    r.do_dot = lambda c: dot(dy_in[...], r.wo_all[oth, c, :], NT)
    r.o, r.dq, r.dk, r.dv = r.oc.at[oth], r.dqc.at[oth], r.dkc.at[oth], r.dvc.at[oth]
    st = attn_stages(seq, n_grp, r)

    def fetch(row):
        return [pltpu.make_async_copy(src.at[me, pl.ds(row * seq, seq), :], dst.at[me], r.sem.at[8 + k])
                for k, (src, dst) in enumerate(zip(own_a[1:], (r.dqc, r.dkc, r.dvc)))]

    def fetch_o(row):
        return pltpu.make_async_copy(own_a[0].at[me, pl.ds(row * seq, seq), :], r.o_next, r.sem.at[11])

    weights = (r.wq_all, r.wk_all, r.wv_all, r.wo_all)
    theirs = [pltpu.make_async_copy(oth_w[k], dst.at[oth], r.sem.at[4 + k]) for k, dst in enumerate(weights)]
    mine = [pltpu.make_async_copy(own_w[k], dst.at[me], r.sem.at[k]) for k, dst in enumerate(weights)]

    @pl.when(step == 0)
    def _():
        for c in theirs + mine[3:] + mine[:3]:
            c.start()
        r.dg[...] = jnp.zeros_like(r.dg)
        r.oc[...] = jnp.zeros_like(r.oc)
        for c in theirs + mine[3:]:
            c.wait()

    @pl.when(step > 0)
    def _():
        for c in fetch(step - 1):
            c.start()
        fetch_o(step - 1).wait()
        r.oc[me] = r.o_next[...]

    @pl.when(step < rows)
    def _():
        fetch_o(step).start()

    CR, NC = 32, 256
    nn = D // NC
    lines = range(0, seq, CR)

    def wide(v):
        return jnp.concatenate([v] * (NC // HD), axis=1)

    def stat(c):
        def run():
            xf = x_in[c:c + CR, :].astype(F32)
            r.xs[0, c:c + CR, :] = jnp.broadcast_to(lax.rsqrt(jnp.mean(xf * xf, axis=-1, keepdims=True) + EPS), (CR, HD))
            r.xs[1, c:c + CR, :] = jnp.zeros((CR, HD), F32)

        return (1, run)

    def dn_dot(n):
        def run():
            cols = slice(n * NC, (n + 1) * NC)
            t = None
            for s in range(2):
                for a_ref, w_ref in ((r.dqc, r.wq_all), (r.dkc, r.wk_all), (r.dvc, r.wv_all)):
                    u = dot(a_ref[s], w_ref[s, cols, :], NT)
                    t = u if t is None else t + u
            r.dn[:, cols] = t

        return (2, run)

    def first(n, c):
        def run():
            cols = slice(n * NC, (n + 1) * NC)
            inv = wide(r.xs[0, c:c + CR, :])
            d = r.dn[c:c + CR, cols]
            w = d * (x_in[c:c + CR, cols].astype(F32) * inv)
            r.dg[:, cols] += jnp.sum(w.reshape(CR // 8, 8, NC), axis=0)
            w = w * gain_ref[0:1, cols]
            r.xs[1, c:c + CR, :] += w[:, :HD] + w[:, HD:]
            r.dn[c:c + CR, cols] = dyx_in[c:c + CR, cols].astype(F32) + inv * (d * gain_ref[0:1, cols])

        return (1, run)

    def mean(c):
        def run():
            inv = r.xs[0, c:c + CR, :]
            r.xs[2, c:c + CR, :] = jnp.sum(r.xs[1, c:c + CR, :], axis=-1, keepdims=True) * (1.0 / D) * (inv * inv)

        return (0.2, run)

    def second(n, c):
        def run():
            cols = slice(n * NC, (n + 1) * NC)
            dx_out[c:c + CR, cols] = (r.dn[c:c + CR, cols] - x_in[c:c + CR, cols].astype(F32) * wide(r.xs[2, c:c + CR, :])).astype(BF16)

        return (1, run)

    def y_dot(n):
        def run():
            cols = slice(n * NC, (n + 1) * NC)
            t = dot(r.oc[0], r.wo_all[0, :, cols]) + dot(r.oc[1], r.wo_all[1, :, cols])
            y_out[:, cols] = (x_in[:, cols].astype(F32) + t).astype(BF16)

        return (1, run)

    r.tab[2:4] = r.tab[0:2]
    r.tab[0] = cos_in[...]
    r.tab[1] = sin_in[...]
    yd = [y_dot(n) for n in range(nn)]
    for g in range(n_grp):
        attn_tick(st, g, n_grp, yd[:EARLY] if g == n_grp - 1 else [])
    for acc in (r.dgq, r.dgk):
        acc[...] = jnp.where(step > 0, acc[...], 0.0)

    @pl.when(step == 0)
    def _():
        for c in mine[:3]:
            c.wait()

    @pl.when(step > 0)
    def _():
        for c in fetch(step - 1):
            c.wait()
        dn = [dn_dot(n) for n in range(nn)]
        for _, f in dn[:1]:
            f()
        weave([stat(c) for c in lines], dn[1:2])
        for n in range(2, nn):
            weave([first(n - 2, c) for c in lines], dn[n:n + 1])
        weave([first(nn - 2, c) for c in lines], yd[EARLY:EARLY + 1])
        weave([first(nn - 1, c) for c in lines] + [mean(c) for c in lines], yd[EARLY + 1:EARLY + 2])
        weave([second(n, c) for n in range(nn) for c in lines], yd[EARLY + 2:])

    @pl.when(step == rows)
    def _():
        at = 0
        for part in (r.dg[...], r.dgq[...] + dgq_own[...], r.dgk[...] + dgk_own[...]):
            sums_out[:, at:at + part.shape[1]] = jnp.sum(part, axis=0, keepdims=True)
            at += part.shape[1]


def tail_call(sel, n, x, dy, cosd, sind, o, dq, dk, dv, gain, qg, kg, dgq, dgk, own, oth, seq=256):
    T, D = x.shape
    nq, nk = dq.shape[2], dk.shape[2]
    n_grp = nk // HD
    rows = T // seq
    lag = lambda k, c: pl.BlockSpec((seq, c), lambda i, s: (jnp.clip(i - k, 0, rows - 1), 0))
    const = lambda *b: pl.BlockSpec(b, lambda i, s: (0,) * len(b), pipeline_mode=pl.Buffered(1))
    hbm = pl.BlockSpec(memory_space=pl.ANY)
    scratch = attn_scratch(seq, n_grp)
    scratch.update(
        wq_all=pltpu.VMEM((2, D, nq), BF16), wk_all=pltpu.VMEM((2, D, nk), BF16), wv_all=pltpu.VMEM((2, D, nk), BF16), wo_all=pltpu.VMEM((2, nq, D), BF16),
        dn=pltpu.VMEM((seq, D), F32), oc=pltpu.VMEM((2, seq, nq), BF16), dqc=pltpu.VMEM((2, seq, nq), BF16), dkc=pltpu.VMEM((2, seq, nk), BF16), dvc=pltpu.VMEM((2, seq, nk), BF16),
        o_next=pltpu.VMEM((seq, nq), BF16), xs=pltpu.VMEM((3, seq, HD), F32), dg=pltpu.VMEM((8, D), F32), dgq=pltpu.VMEM((8, HD), F32), dgk=pltpu.VMEM((8, HD), F32), sem=pltpu.SemaphoreType.DMA((12,)))
    flops = 2 * T * D * (nq + 2 * nk + nq) * 3 + 12 * T * nq * seq
    return pl.pallas_call(
        functools.partial(tail_kernel, seq, n_grp, rows, tuple(scratch)),
        grid_spec=pltpu.PrefetchScalarGridSpec(
            num_scalar_prefetch=1,
            grid=(rows + 1,),
            in_specs=[lag(0, D), lag(0, D), lag(0, HD), lag(0, HD), lag(1, D), lag(1, D), const(1, D), const(1, HD), const(1, HD), const(8, HD), const(8, HD)] + [hbm] * 12,
            out_specs=[lag(1, D), lag(1, D), pl.BlockSpec((1, D + 2 * HD), lambda i, s: (0, 0))],
            scratch_shapes=list(scratch.values()),
        ),
        out_shape=[jax.ShapeDtypeStruct((T, D), BF16)] * 2 + [jax.ShapeDtypeStruct((1, D + 2 * HD), F32)],
        compiler_params=pltpu.CompilerParams(dimension_semantics=("arbitrary",), vmem_limit_bytes=67043328),
        cost_estimate=pl.CostEstimate(flops=flops, bytes_accessed=T * D * 14, transcendentals=T * nq * 2),
        name="tail",
    )(sel, n, dy, cosd, sind, x, dy, gain, qg, kg, dgq, dgk, *own, *oth, o, dq, dk, dv)


def solution(mesh):
    tok_spec = P("dp", None, None)
    col_spec = P(None, "tp")
    row_spec = P("tp", None)
    n_dp = mesh.shape["dp"]

    def per_device(x_in, dy_in, positions, g_attn, q_gain, k_gain, w_q, w_k, w_v, w_o):
        n_batch, n_seq, D = x_in.shape
        T = n_batch * n_seq
        nk = w_k.shape[1]
        x, dy = x_in.reshape(T, D), dy_in.reshape(T, D)
        me = lax.axis_index("tp").astype(jnp.int32)
        own = me.reshape(1)

        part = lax.axis_index("dp").astype(jnp.int32).reshape(1)
        share, cosd, sind = pre_call(part, w_q, w_k, w_v, w_o, positions, parts=n_dp)
        gathered = lax.all_gather(share, ("tp", "dp"), tiled=True)

        gain = g_attn.astype(F32).reshape(1, D)
        qg, kg = q_gain.astype(F32).reshape(1, HD), k_gain.astype(F32).reshape(1, HD)

        n, o, dq, dk, dv, dgq, dgk, dw_o = attn_call(True, own, x, dy, cosd, sind, gain, qg, kg, w_q, w_k, w_v, w_o, seq=n_seq)
        dw_q, dw_k, dw_v, *theirs = dw_call(own, n, [dq, dk, dv], 512, gathered=gathered, nk=nk)
        dw_o, dw_q, dw_k, dw_v = lax.psum((dw_o, dw_q, dw_k, dw_v), "dp")

        y, dx, sums = tail_call(own, n, x, dy, cosd, sind, o, dq, dk, dv, gain, qg, kg, dgq, dgk, (w_q, w_k, w_v, w_o), theirs, seq=n_seq)
        g_sum, q_sum, k_sum = (t.reshape(-1) for t in sum_call(sums, (D, HD, HD), n_dp))
        dw_o, dw_q, dw_k, dw_v = copy_call((dw_o, dw_q, dw_k, dw_v))
        return y.reshape(x_in.shape), dx.reshape(x_in.shape), dw_q, dw_k, dw_v, dw_o, q_sum, k_sum, g_sum

    return jax.shard_map(per_device, mesh=mesh, in_specs=(tok_spec, tok_spec, P("dp", None), P(), P(), P(), col_spec, col_spec, col_spec, row_spec), out_specs=(tok_spec, tok_spec, col_spec, col_spec, col_spec, row_spec, P(), P(), P()), check_vma=False)
```

```python
import functools
from types import SimpleNamespace
import jax
import jax.numpy as jnp
from jax import lax
from jax.experimental import pallas as pl
from jax.experimental.pallas import tpu as pltpu
from jax.sharding import PartitionSpec as P


EPS = 1e-6
THETA = 1000000.0
F32 = jnp.float32
BF16 = jnp.bfloat16
HD = 128
NT = (((1,), (1,)), ((), ()))
TN = (((0,), (0,)), ((), ()))
NN = (((1,), (0,)), ((), ()))


def dot(a, b, dims=NN):
    return lax.dot_general(a, b, dims, preferred_element_type=F32)


def weave(*lists):
    order = []
    for n, pieces in enumerate(lists):
        total = sum(c for c, _ in pieces) or 1
        at = 0
        for k, (c, f) in enumerate(pieces):
            order.append(((at + c / 2) / total, n, k, f))
            at += c
    for _, _, _, f in sorted(order, key=lambda e: e[:3]):
        f()


CH = 32


def attn_kernel(own, seq, n_grp, sel_ref, *refs):
    if own:
        (x0_ref, xn_ref, dy_ref, cos_ref, sin_ref, gain_ref, qg_ref, kg_ref, wq_ref, wk_ref, wv_ref, wo_ref,
         n_out, o_out, dq_out, dk_out, dv_out, dgq_out, dgk_out, dwo_out) = refs[:20]
        refs = refs[20:]
    else:
        nin_ref, dy_ref, cos_ref, sin_ref, qg_ref, kg_ref, wq_ref, wk_ref, wv_ref, wo_ref, _, _, _, _, o_out, dq_out, dk_out, dv_out = refs[:18]
        refs = refs[18:]
        n_ref = nin_ref
    (qnew_ref, knew_ref, vnew_ref, raw_ref, inv_ref, rot_ref, do_ref, v_ref, s_ref, dp_ref, p_ref, ds_ref, dkf_ref, dqf_ref, st_ref,
     tab_ref, o_ref, dq_ref, dk_ref, dv_ref) = refs[:20]
    if own:
        n_ref, nn_ref, dgq_ref, dgk_ref, acc_ref, ot_ref, dyp_ref, sem = refs[20:]
    half = seq // 2
    scale = HD ** -0.5
    log2e = 1.4426950408889634
    step = pl.program_id(0)

    def norm_rows(src, dst):
        def piece(c):
            def run():
                xf = src[c:c + 32, :].astype(F32)
                inv = lax.rsqrt(jnp.mean(xf * xf, axis=-1, keepdims=True) + EPS)
                dst[c:c + 32, :] = (xf * inv * gain_ref[0:1, :]).astype(BF16)

            return (1.5, run)

        return [piece(c) for c in range(0, seq, 32)]

    def proj(g):
        def q():
            t = dot(n_ref[...], wq_ref[:, g * 2 * HD:(g + 1) * 2 * HD])
            for h in range(2):
                qnew_ref[g % 2, h] = t[:, h * HD:(h + 1) * HD].astype(BF16)

        def k():
            t = dot(n_ref[...], wk_ref[:, g * HD:(g + 2) * HD])
            for h in range(2):
                knew_ref[g + h] = t[:, h * HD:(h + 1) * HD].astype(BF16)

        def v():
            t = dot(n_ref[...], wv_ref[:, g * HD:(g + 2) * HD])
            for h in range(2):
                vnew_ref[g + h] = t[:, h * HD:(h + 1) * HD].astype(BF16)

        def do():
            t = dot(dy_ref[...], wo_ref[g * 2 * HD:(g + 1) * 2 * HD, :], NT)
            for h in range(2):
                do_ref[g, h * half:(h + 1) * half, :] = t[:half, h * HD:(h + 1) * HD].astype(BF16)
                do_ref[g, seq + h * half:seq + (h + 1) * half, :] = t[half:, h * HD:(h + 1) * HD].astype(BF16)

        return [(1, q)] + ([(1, k), (1, v)] if g % 2 == 0 else []) + [(1, do)]

    def stacked(h, c):
        return (h * half + c) if c < half else (seq + h * half + c - half)

    def rope(g):
        cs, sn = (tab_ref.at[2], tab_ref.at[3]) if g == n_grp - 1 else (tab_ref.at[0], tab_ref.at[1])

        def size(h, c):
            def run():
                raw = knew_ref[g, c:c + CH, :] if h == 2 else qnew_ref[g % 2, h, c:c + CH, :]
                raw_ref[g, h, c:c + CH, :] = raw
                t = raw.astype(F32)
                inv_ref[g, h, c:c + CH, :] = jnp.broadcast_to(lax.rsqrt(jnp.mean(t * t, axis=-1, keepdims=True) + EPS), t.shape)

            return (0.4, run)

        def turn(h, c):
            def run():
                t = raw_ref[g, h, c:c + CH, :].astype(F32)
                w = (t * inv_ref[g, h, c:c + CH, :]) * (kg_ref if h == 2 else qg_ref)[0:1, :]
                o = 2 * seq + c if h == 2 else stacked(h, c)
                x = pltpu.roll(w, HD // 2, 1)
                co, si = cs[c:c + CH, :], sn[c:c + CH, :]
                rot_ref[g, o:o + CH, 0:HD] = (w * co + x * si).astype(BF16)
                rot_ref[g, o:o + CH, HD:] = (x * co - w * si).astype(BF16)
                if h == 2:
                    v_ref[g, c:c + CH, :] = vnew_ref[g, c:c + CH, :]

            return (0.6, run)

        return [f(h, c) for f in (size, turn) for h in (2, 0, 1) for c in range(0, seq, CH)]

    def scores(g):
        b = g % 2

        def s():
            s_ref[b, 0:seq, 0:half] = dot(rot_ref[g, 0:seq, 0:HD], rot_ref[g, 2 * seq:2 * seq + half, 0:HD], NT)
            s_ref[b, seq:, :] = dot(rot_ref[g, seq:2 * seq, 0:HD], rot_ref[g, 2 * seq:, 0:HD], NT)

        def dp():
            dp_ref[b, 0:seq, 0:half] = dot(do_ref[g, :seq, :], v_ref[g, :half, :], NT)
            dp_ref[b, seq:, :] = dot(do_ref[g, seq:, :], v_ref[g], NT)

        return [(1, s), (1, dp)]

    def soft(g):
        b = g % 2
        c2 = scale * log2e

        def part(blk, c):
            return slice(blk * seq + c, blk * seq + c + CH), half if blk == 0 else seq

        def masked(blk, c, s):
            row_id = lax.broadcasted_iota(jnp.int32, (CH, half), 0) + (c % half)
            keep = row_id >= lax.broadcasted_iota(jnp.int32, (CH, half), 1)
            if blk == 0:
                return jnp.where(keep, s, -jnp.inf)
            return jnp.concatenate([s[:, :half], jnp.where(keep, s[:, half:], -jnp.inf)], axis=1)

        def wide(ref, rows, width):
            t = ref[rows, :]
            return t if width == half else jnp.concatenate([t, t], axis=1)

        def top(blk, c):
            rows, width = part(blk, c)

            def run():
                m = jnp.max(masked(blk, c, s_ref[b, rows, 0:width]), axis=-1, keepdims=True)
                st_ref[0, rows, :] = jnp.broadcast_to(m * c2, (CH, HD))

            return (0.4 + 0.4 * blk, run)

        def power(blk, c):
            rows, width = part(blk, c)

            def run():
                e = jnp.exp2(masked(blk, c, s_ref[b, rows, 0:width] * c2) - wide(st_ref.at[0], rows, width))
                s_ref[b, rows, 0:width] = e
                st_ref[1, rows, :] = jnp.broadcast_to(1.0 / jnp.sum(e, axis=-1, keepdims=True), (CH, HD))

            return (0.8 + 0.8 * blk, run)

        def prob(blk, c):
            rows, width = part(blk, c)

            def run():
                pr = s_ref[b, rows, 0:width] * wide(st_ref.at[1], rows, width)
                s_ref[b, rows, 0:width] = pr
                p_ref[b, rows, 0:width] = pr.astype(BF16)
                st_ref[2, rows, :] = jnp.broadcast_to(jnp.sum(pr * dp_ref[b, rows, 0:width], axis=-1, keepdims=True), (CH, HD))

            return (0.8 + 0.8 * blk, run)

        def last(blk, c):
            rows, width = part(blk, c)

            def run():
                d = dp_ref[b, rows, 0:width] - wide(st_ref.at[2], rows, width)
                ds_ref[b, rows, 0:width] = (s_ref[b, rows, 0:width] * d * scale).astype(BF16)

            return (0.8 + 0.8 * blk, run)

        return [f(blk, c) for f in (top, power, prob, last) for blk in range(2) for c in range(0, seq, CH)]

    def grads(g):
        b = g % 2
        col, kcol = g * 2 * HD, g * HD

        def dq():
            dqf_ref[b, 0:seq, :] = dot(ds_ref[b, 0:seq, 0:half], rot_ref[g, 2 * seq:2 * seq + half, :])
            dqf_ref[b, seq:, :] = dot(ds_ref[b, seq:, :], rot_ref[g, 2 * seq:, :])

        def dk():
            tb = dot(ds_ref[b, seq:, :], rot_ref[g, seq:2 * seq, :], TN)
            ta = dot(ds_ref[b, 0:seq, 0:half], rot_ref[g, 0:seq, :], TN)
            dkf_ref[b, :half, :] = tb[:half] + ta
            dkf_ref[b, half:, :] = tb[half:]

        def o():
            ta = dot(p_ref[b, 0:seq, 0:half], v_ref[g, :half, :])
            tb = dot(p_ref[b, seq:, :], v_ref[g])
            for h in range(2):
                o_ref[0:half, col + h * HD:col + (h + 1) * HD] = ta[h * half:(h + 1) * half].astype(BF16)
                o_ref[half:seq, col + h * HD:col + (h + 1) * HD] = tb[h * half:(h + 1) * half].astype(BF16)

        def dv():
            tb = dot(p_ref[b, seq:, :], do_ref[g, seq:, :], TN)
            ta = dot(p_ref[b, 0:seq, 0:half], do_ref[g, :seq, :], TN)
            dv_ref[0:half, kcol:kcol + HD] = (tb[:half] + ta).astype(BF16)
            dv_ref[half:seq, kcol:kcol + HD] = tb[half:].astype(BF16)

        return [(1, dq), (1, dk), (1, o), (1, dv)]

    def back(g):
        b = g % 2

        def place(h, c):
            if h == 2:
                return dkf_ref, c, dk_ref, g * HD, kg_ref
            return dqf_ref, stacked(h, c), dq_ref, (2 * g + h) * HD, qg_ref

        def turn(h, c):
            src, o, _, _, g_ref = place(h, c)

            def run():
                d = src[b, o:o + CH, :].astype(BF16).astype(F32)
                that = raw_ref[g, h, c:c + CH, :].astype(F32) * inv_ref[g, h, c:c + CH, :]
                du = d[:, :HD] * tab_ref[2, c:c + CH, :] - d[:, HD:] * tab_ref[3, c:c + CH, :]
                src[b, o:o + CH, 0:HD] = du
                pr = du * that
                if own:
                    dg_ref = dgk_ref if h == 2 else dgq_ref
                    dg_ref[...] += jnp.sum(pr.reshape(CH // 8, 8, HD), axis=0)
                st_ref[3 + h, c:c + CH, :] = jnp.broadcast_to(jnp.mean(pr * g_ref[0:1, :], axis=-1, keepdims=True), (CH, HD))

            return (0.6, run)

        def out(h, c):
            src, o, out_ref, col, g_ref = place(h, c)

            def run():
                inv = inv_ref[g, h, c:c + CH, :]
                that = raw_ref[g, h, c:c + CH, :].astype(F32) * inv
                out_ref[c:c + CH, col:col + HD] = (inv * (src[b, o:o + CH, 0:HD] * g_ref[0:1, :] - that * st_ref[3 + h, c:c + CH, :])).astype(BF16)

            return (0.5, run)

        return [f(h, c) for f in (turn, out) for h in (0, 1, 2) for c in range(0, seq, CH)]

    def dwo(g):
        rows = slice(g * 2 * HD, (g + 1) * 2 * HD)

        def flip():
            ot_ref[rows, :] = o_ref[:, rows].T

        def part(c):
            def run():
                acc_ref[rows, c:c + 512] += dot(ot_ref[rows, :], dyp_ref[:, c:c + 512])

            return (0.25, run)

        return [(0.1, flip)] + [part(c) for c in range(0, acc_ref.shape[1], 512)]

    @pl.when(step == 0)
    def _():
        if own:
            weave(norm_rows(x0_ref, n_ref))

    tab_ref[2:4] = tab_ref[0:2]
    tab_ref[0] = cos_ref[...]
    tab_ref[1] = sin_ref[...]
    if own:
        norms = norm_rows(xn_ref, nn_ref)
    for g in range(n_grp):
        sc = scores((g - 2) % n_grp)
        gr = grads(g)
        nm = (norms[:4], norms[4:], [], [])[g] if own else []
        for _, f in gr[:2]:
            f()
        weave(soft((g - 3) % n_grp), rope((g - 1) % n_grp) + nm, back(g), sc + gr[2:] + (dwo(g - 1) if own and g > 0 else []) + proj(g) + (dwo(g) if own and g == n_grp - 1 else []))

    for dst, src in ((o_out, o_ref), (dq_out, dq_ref), (dk_out, dk_ref), (dv_out, dv_ref)):
        dst[0] = src[...]
    if own:
        n_out[...] = n_ref[...]
        n_ref[...] = nn_ref[...]
        keep = step > 0
        for dst, acc in ((dgq_out, dgq_ref), (dgk_out, dgk_ref)):
            acc[...] = jnp.where(keep, acc[...], 0.0)
            dst[...] = acc[...]
        dyp_ref[...] = dy_ref[...]

        @pl.when(step == 0)
        def _():
            @pl.loop(0, acc_ref.shape[0] // 64)
            def _(j):
                acc_ref[pl.ds(pl.multiple_of(j * 64, 64), 64), :] = jnp.zeros((64, acc_ref.shape[1]), F32)

        @pl.when(step == pl.num_programs(0) - 1)
        def _():
            c = pltpu.make_async_copy(acc_ref, dwo_out, sem)
            c.start()
            c.wait()


def attn_call(own, sel, x, dy, cosd, sind, gain, qg, kg, wq, wk, wv, wo, prev=None, seq=256):
    T, D = x.shape
    nq, nk = wq.shape[1], wk.shape[1]
    n_grp = nk // HD
    rows = T // seq
    const = lambda *b: pl.BlockSpec(b, lambda i, s: (0,) * len(b), pipeline_mode=pl.Buffered(1))
    now = lambda c: pl.BlockSpec((seq, c), lambda i, s: (jnp.minimum(i, rows - 1), 0))
    nxt = lambda c: pl.BlockSpec((seq, c), lambda i, s: (jnp.minimum(i + 1, rows - 1), 0))
    out3 = lambda c: pl.BlockSpec((1, seq, c), lambda i, s: (s[0], jnp.maximum(i - 1, 0), 0))
    mid = [now(D), now(HD), now(HD)]
    tail = [const(1, HD), const(1, HD), const(D, nq), const(D, nk), const(D, nk), const(nq, D)]
    shapes = [jax.ShapeDtypeStruct((2, T, c), BF16) for c in (nq, nq, nk, nk)]
    specs = [out3(nq), out3(nq), out3(nk), out3(nk)]
    aliases = {}
    if own:
        in_specs = [const(seq, D), nxt(D)] + mid + [const(1, D)] + tail
        args = [x, x, dy, cosd, sind, gain, qg, kg, wq, wk, wv, wo]
        shapes = [jax.ShapeDtypeStruct((T, D), BF16)] + shapes + [jax.ShapeDtypeStruct((8, HD), F32)] * 2 + [jax.ShapeDtypeStruct((nq, D), F32)]
        specs = [now(D)] + specs + [pl.BlockSpec((8, HD), lambda i, s: (0, 0))] * 2 + [pl.BlockSpec(memory_space=pl.ANY)]
    else:
        in_specs = [now(D)] + mid + tail + [pl.BlockSpec(memory_space=pl.ANY)] * 4
        args = [x, dy, cosd, sind, qg, kg, wq, wk, wv, wo]
        aliases = {1 + len(args) + i: i for i in range(4)}
        args += list(prev)
    flops = 2 * T * D * (nq + 2 * nk + nq) + 12 * T * nq * seq
    return pl.pallas_call(
        functools.partial(attn_kernel, own, seq, n_grp),
        grid_spec=pltpu.PrefetchScalarGridSpec(
            num_scalar_prefetch=1,
            grid=(rows + 1,),
            in_specs=in_specs,
            out_specs=specs,
            scratch_shapes=[
                pltpu.VMEM((2, 2, seq, HD), BF16),
                pltpu.VMEM((n_grp, seq, HD), BF16),
                pltpu.VMEM((n_grp, seq, HD), BF16),
                pltpu.VMEM((n_grp, 3, seq, HD), BF16),
                pltpu.VMEM((n_grp, 3, seq, HD), F32),
                pltpu.VMEM((n_grp, 3 * seq, 2 * HD), BF16),
                pltpu.VMEM((n_grp, 2 * seq, HD), BF16),
                pltpu.VMEM((n_grp, seq, HD), BF16),
                pltpu.VMEM((2, 2 * seq, seq), F32),
                pltpu.VMEM((2, 2 * seq, seq), F32),
                pltpu.VMEM((2, 2 * seq, seq), BF16),
                pltpu.VMEM((2, 2 * seq, seq), BF16),
                pltpu.VMEM((2, seq, 2 * HD), F32),
                pltpu.VMEM((2, 2 * seq, 2 * HD), F32),
                pltpu.VMEM((6, 2 * seq, HD), F32),
                pltpu.VMEM((4, seq, HD), F32),
            ] + [pltpu.VMEM((seq, c), BF16) for c in (nq, nq, nk, nk)]
            + ([pltpu.VMEM((seq, D), BF16)] * 2 + [pltpu.VMEM((8, HD), F32)] * 2 + [pltpu.VMEM((nq, D), F32), pltpu.VMEM((nq, seq), BF16), pltpu.VMEM((seq, D), BF16), pltpu.SemaphoreType.DMA] if own else []),
        ),
        out_shape=shapes,
        input_output_aliases=aliases,
        compiler_params=pltpu.CompilerParams(dimension_semantics=("arbitrary",), vmem_limit_bytes=62 << 20),
        cost_estimate=pl.CostEstimate(flops=flops, bytes_accessed=T * D * 6 + T * (2 * nq + 2 * nk) * 2, transcendentals=T * nq * 2),
        name="attn_own" if own else "attn_other",
    )(sel, *args)


def pre_kernel(sel_ref, q_ref, k_ref, v_ref, o_ref, pos_ref, freq_ref, out_ref, cos_ref, sin_ref):
    d, nq, nk = q_ref.shape[0], q_ref.shape[1], k_ref.shape[1]
    out_ref[0, 0:d, 0:nq] = q_ref[...].astype(F32)
    out_ref[0, 0:d, nq:nq + nk] = k_ref[...].astype(F32)
    out_ref[0, 0:d, nq + nk:] = v_ref[...].astype(F32)
    out_ref[0, d:, :] = o_ref[...].astype(F32)
    n, seq = pos_ref.shape[1:]
    low = lax.broadcasted_iota(jnp.int32, (HD, HD), 1) < HD // 2
    for r in range(n):
        for h in range(0, seq // HD, 2):
            p = [jnp.broadcast_to(pos_ref[0, r:r + 1, (h + b) * HD:(h + b + 1) * HD].astype(F32), (HD, HD)).T for b in range(2)]
            a = jnp.where(low, p[0], p[1]) * freq_ref[0:1, :]
            k = jnp.round(a * 0.6366197723675814)
            x = ((a - k * 1.5703125) - k * 4.837512969970703125e-4) - k * 7.549789948768648e-8
            z = x * x
            s = ((-1.9515295891e-4 * z + 8.3321608736e-3) * z - 1.6666654611e-1) * z * x + x
            c = ((2.443315711809948e-5 * z - 1.388731625493765e-3) * z + 4.166664568298827e-2) * z * z - 0.5 * z + 1.0
            q = k.astype(jnp.int32)
            odd = (q & 1) == 1
            co, si = jnp.where(odd, s, c), jnp.where(odd, c, s)
            co = jnp.where(((q + 1) & 2) == 0, co, -co)
            si = jnp.where((q & 2) == 0, si, -si)
            cx, sx = pltpu.roll(co, HD // 2, 1), pltpu.roll(si, HD // 2, 1)
            for b in range(2):
                at = (r * (seq // HD) + h + b) * HD
                cos_ref[at:at + HD, :] = jnp.where(low, co, cx) if b == 0 else jnp.where(low, cx, co)
                sin_ref[at:at + HD, :] = jnp.where(low, -si, sx) if b == 0 else jnp.where(low, -sx, si)


def pre_call(part, w_q, w_k, w_v, w_o, positions, parts=2, cuts=8):
    D, nq = w_q.shape
    n, seq = positions.shape
    rows = n // cuts
    freq = THETA ** (-jnp.arange(0, HD, 2, dtype=F32) / HD)
    freq = jnp.concatenate([freq, freq]).reshape(1, HD)
    spec = lambda w: pl.BlockSpec((w.shape[0] // (parts * cuts), w.shape[1]), lambda i, s: (s[0] * cuts + i, 0))
    r = (D + nq) // (parts * cuts)
    table = pl.BlockSpec((rows * seq, HD), lambda i, s: (i, 0))
    return pl.pallas_call(
        pre_kernel,
        grid_spec=pltpu.PrefetchScalarGridSpec(
            num_scalar_prefetch=1,
            grid=(cuts,),
            in_specs=[spec(w) for w in (w_q, w_k, w_v, w_o)] + [pl.BlockSpec((1, rows, seq), lambda i, s: (i, 0, 0)), pl.BlockSpec((1, HD), lambda i, s: (0, 0))],
            out_specs=[pl.BlockSpec((1, r, D), lambda i, s: (i, 0, 0)), table, table],
        ),
        out_shape=[jax.ShapeDtypeStruct((cuts, r, D), F32)] + [jax.ShapeDtypeStruct((n * seq, HD), F32)] * 2,
        compiler_params=pltpu.CompilerParams(dimension_semantics=("arbitrary",), vmem_limit_bytes=60 << 20),
        cost_estimate=pl.CostEstimate(flops=n * seq * HD * 30, bytes_accessed=cuts * r * D * 6 + n * seq * HD * 8, transcendentals=0),
        name="pre",
    )(part, w_q, w_k, w_v, w_o, positions.reshape(cuts, rows, seq), freq)


def dw_kernel(n_b, unpack, sel_ref, a_ref, *refs):
    if unpack:
        f_ref, parts = refs[n_b], refs[2 * n_b + 1:2 * n_b + 5]
        refs = refs[:n_b] + refs[n_b + 1:2 * n_b + 1] + refs[2 * n_b + 5:]
        q_ref, k_ref, v_ref, o_ref = parts
        per, nq, nk = f_ref.shape[0], q_ref.shape[1], k_ref.shape[1]
        d, e = q_ref.shape[0] // per, o_ref.shape[0] // per
        for j in range(per):
            q_ref[j * d:(j + 1) * d, :] = f_ref[j, 0:d, 0:nq].astype(BF16)
            k_ref[j * d:(j + 1) * d, :] = f_ref[j, 0:d, nq:nq + nk].astype(BF16)
            v_ref[j * d:(j + 1) * d, :] = f_ref[j, 0:d, nq + nk:].astype(BF16)
            o_ref[j * e:(j + 1) * e, :] = f_ref[j, d:, :].astype(BF16)
    bs, outs, accs, (at_ref, sem) = refs[:n_b], refs[n_b:2 * n_b], refs[2 * n_b:3 * n_b], refs[3 * n_b:]
    flat = lambda ref: ref.at[0] if len(ref.shape) == 3 else ref
    a, bs = flat(a_ref), [flat(b) for b in bs]
    M, tile = at_ref.shape
    step = pl.program_id(0)

    @pl.when(step == 0)
    def _():
        for acc in accs:
            @pl.loop(0, M // 64)
            def _(j):
                acc[pl.ds(pl.multiple_of(j * 64, 64), 64), :] = jnp.zeros((64, acc.shape[1]), F32)

    def part(acc, b, c):
        def run():
            acc[:, c:c + 256] += dot(at_ref[...], b[:, c:c + 256])

        return (1, run)

    for c in range(0, M, 256):
        for k in range(0, tile, 256):
            at_ref[c:c + 256, k:k + 256] = a[k:k + 256, c:c + 256].T
    weave([part(acc, b, c) for acc, b in zip(accs, bs) for c in range(0, b.shape[1], 256)])

    @pl.when(step == pl.num_programs(0) - 1)
    def _():
        copies = [pltpu.make_async_copy(acc, out, sem.at[k]) for k, (acc, out) in enumerate(zip(accs, outs))]
        for c in copies:
            c.start()
        for c in copies:
            c.wait()


def dw_call(sel, a, bs, tile, gathered=None, nk=0):
    def spec(v):
        if v.ndim == 3:
            return pl.BlockSpec((1, tile, v.shape[2]), lambda i, s: (s[0], i, 0))
        return pl.BlockSpec((tile, v.shape[1]), lambda i, s: (i, 0))

    T, M = a.shape[-2:]
    shapes = [(M, b.shape[-1]) for b in bs]
    width = sum(s[1] for s in shapes)
    steps = T // tile
    more_in, more_out, more_shapes, more = [], [], [], []
    if gathered is not None:
        n, r, D = gathered.shape
        per = n // 2 // steps
        more = [gathered]
        more_in = [pl.BlockSpec((per, r, D), lambda i, s: ((1 - s[0]) * steps + i, 0, 0))]
        nq = D - 2 * nk
        more_shapes = [jax.ShapeDtypeStruct(s, BF16) for s in ((D, nq), (D, nk), (D, nk), (nq, D))]
        more_out = [pl.BlockSpec((s.shape[0] // steps, s.shape[1]), lambda i, s: (i, 0)) for s in more_shapes]
    return pl.pallas_call(
        functools.partial(dw_kernel, len(bs), gathered is not None),
        grid_spec=pltpu.PrefetchScalarGridSpec(
            num_scalar_prefetch=1,
            grid=(steps,),
            in_specs=[spec(a)] + [spec(b) for b in bs] + more_in,
            out_specs=[pl.BlockSpec(memory_space=pl.ANY)] * len(bs) + more_out,
            scratch_shapes=[pltpu.VMEM(s, F32) for s in shapes] + [pltpu.VMEM((M, tile), BF16), pltpu.SemaphoreType.DMA((len(bs),))],
        ),
        out_shape=[jax.ShapeDtypeStruct(s, F32) for s in shapes] + more_shapes,
        compiler_params=pltpu.CompilerParams(dimension_semantics=("arbitrary",), vmem_limit_bytes=60 << 20),
        cost_estimate=pl.CostEstimate(flops=2 * T * M * width, bytes_accessed=2 * T * (M + width) + 4 * M * width, transcendentals=0),
    )(sel, a, *bs, *more)


def sum_kernel(n, widths, part_ref, *refs):
    outs, (slots, local_sem, send_sem, recv_sem) = refs[:-4], refs[-4:]
    me = lax.axis_index("dp")
    barrier = pltpu.get_barrier_semaphore()
    for k in range(1, n):
        pl.semaphore_signal(barrier, inc=1, device_id={"dp": lax.rem(me + k, n)}, device_id_type=pl.DeviceIdType.MESH)
    mine = pltpu.make_async_copy(part_ref, slots.at[0], local_sem)
    mine.start()
    pl.semaphore_wait(barrier, n - 1)
    copies = []
    for k in range(1, n):
        copies.append(pltpu.make_async_remote_copy(
            src_ref=part_ref, dst_ref=slots.at[k], send_sem=send_sem.at[k - 1], recv_sem=recv_sem.at[k - 1],
            device_id={"dp": lax.rem(me + k, n)}, device_id_type=pl.DeviceIdType.MESH))
    for c in copies:
        c.start()
    mine.wait()
    for c in copies:
        c.wait()
    total = slots[lax.rem(me + n, n)]
    for a in range(1, n):
        total = total + slots[lax.rem(me + n - a, n)]
    at = 0
    for out, w in zip(outs, widths):
        out[...] = total[:, at:at + w]
        at += w


def sum_call(part, widths, n):
    return pl.pallas_call(
        functools.partial(sum_kernel, n, widths),
        in_specs=[pl.BlockSpec(memory_space=pl.ANY)],
        out_specs=[pl.BlockSpec(memory_space=pltpu.VMEM)] * len(widths),
        out_shape=[jax.ShapeDtypeStruct((1, w), F32) for w in widths],
        scratch_shapes=[pltpu.VMEM((n, *part.shape), F32), pltpu.SemaphoreType.DMA, pltpu.SemaphoreType.DMA((n - 1,)), pltpu.SemaphoreType.DMA((n - 1,))],
        compiler_params=pltpu.CompilerParams(collective_id=0, has_side_effects=True),
        cost_estimate=pl.CostEstimate(flops=n * part.size, bytes_accessed=8 * n * part.size, transcendentals=0),
        name="small_sum",
    )(part)


def copy_kernel(n, cuts, *refs):
    srcs, dsts, bufs, (in_sem, out_sem) = refs[:n], refs[n:2 * n], refs[2 * n:3 * n], refs[3 * n:]
    ins, outs = [], []
    for a, (src, dst, buf) in enumerate(zip(srcs, dsts, bufs)):
        rows = src.shape[0] // cuts
        for j in range(cuts):
            part = pl.ds(j * rows, rows)
            ins.append(pltpu.make_async_copy(src.at[part], buf.at[part], in_sem.at[a, j]))
            outs.append(pltpu.make_async_copy(buf.at[part], dst.at[part], out_sem.at[a, j]))
    for c in ins:
        c.start()
    for c, d in zip(ins, outs):
        c.wait()
        d.start()
    for d in outs:
        d.wait()


def copy_call(arrays, cuts=4):
    n = len(arrays)
    hbm = [pl.BlockSpec(memory_space=pl.ANY)] * n
    return pl.pallas_call(
        functools.partial(copy_kernel, n, cuts),
        in_specs=hbm,
        out_specs=hbm,
        out_shape=[jax.ShapeDtypeStruct(a.shape, a.dtype) for a in arrays],
        scratch_shapes=[pltpu.VMEM(a.shape, a.dtype) for a in arrays] + [pltpu.SemaphoreType.DMA((n, cuts))] * 2,
        compiler_params=pltpu.CompilerParams(vmem_limit_bytes=60 << 20),
        cost_estimate=pl.CostEstimate(flops=0, bytes_accessed=8 * sum(a.size for a in arrays), transcendentals=0),
        name="results",
    )(*arrays)


def attn_stages(seq, n_grp, r):
    half = seq // 2
    scale = HD ** -0.5
    log2e = 1.4426950408889634

    def norm_rows(src, dst):
        def piece(c):
            def run():
                xf = src[c:c + 32, :].astype(F32)
                inv = lax.rsqrt(jnp.mean(xf * xf, axis=-1, keepdims=True) + EPS)
                dst[c:c + 32, :] = (xf * inv * r.gain[0:1, :]).astype(BF16)

            return (1.5, run)

        return [piece(c) for c in range(0, seq, 32)]

    def proj(g):
        def q():
            t = dot(r.n[...], r.wq(slice(g * 2 * HD, (g + 1) * 2 * HD)))
            for h in range(2):
                r.qnew[g % 2, h] = t[:, h * HD:(h + 1) * HD].astype(BF16)

        def k():
            t = dot(r.n[...], r.wk(slice(g * HD, (g + 2) * HD)))
            for h in range(2):
                r.knew[g + h] = t[:, h * HD:(h + 1) * HD].astype(BF16)

        def v():
            t = dot(r.n[...], r.wv(slice(g * HD, (g + 2) * HD)))
            for h in range(2):
                r.vnew[g + h] = t[:, h * HD:(h + 1) * HD].astype(BF16)

        def do():
            t = r.do_dot(slice(g * 2 * HD, (g + 1) * 2 * HD))
            for h in range(2):
                r.do[g, h * half:(h + 1) * half, :] = t[:half, h * HD:(h + 1) * HD].astype(BF16)
                r.do[g, seq + h * half:seq + (h + 1) * half, :] = t[half:, h * HD:(h + 1) * HD].astype(BF16)

        return [(1, q)] + ([(1, k), (1, v)] if g % 2 == 0 else []) + [(1, do)]

    def stacked(h, c):
        return (h * half + c) if c < half else (seq + h * half + c - half)

    def rope(g):
        cs, sn = (r.tab.at[2], r.tab.at[3]) if g == n_grp - 1 else (r.tab.at[0], r.tab.at[1])

        def size(h, c):
            def run():
                raw = r.knew[g, c:c + CH, :] if h == 2 else r.qnew[g % 2, h, c:c + CH, :]
                r.raw[g, h, c:c + CH, :] = raw
                t = raw.astype(F32)
                r.inv[g, h, c:c + CH, :] = jnp.broadcast_to(lax.rsqrt(jnp.mean(t * t, axis=-1, keepdims=True) + EPS), t.shape)

            return (0.4, run)

        def turn(h, c):
            def run():
                t = r.raw[g, h, c:c + CH, :].astype(F32)
                w = (t * r.inv[g, h, c:c + CH, :]) * (r.kg if h == 2 else r.qg)[0:1, :]
                o = 2 * seq + c if h == 2 else stacked(h, c)
                x = pltpu.roll(w, HD // 2, 1)
                co, si = cs[c:c + CH, :], sn[c:c + CH, :]
                r.rot[g, o:o + CH, 0:HD] = (w * co + x * si).astype(BF16)
                r.rot[g, o:o + CH, HD:] = (x * co - w * si).astype(BF16)
                if h == 2:
                    r.v[g, c:c + CH, :] = r.vnew[g, c:c + CH, :]

            return (0.6, run)

        return [f(h, c) for f in (size, turn) for h in (2, 0, 1) for c in range(0, seq, CH)]

    def scores(g):
        b = g % 2

        def s():
            r.s[b, 0:seq, 0:half] = dot(r.rot[g, 0:seq, 0:HD], r.rot[g, 2 * seq:2 * seq + half, 0:HD], NT)
            r.s[b, seq:, :] = dot(r.rot[g, seq:2 * seq, 0:HD], r.rot[g, 2 * seq:, 0:HD], NT)

        def dp():
            r.dp[b, 0:seq, 0:half] = dot(r.do[g, :seq, :], r.v[g, :half, :], NT)
            r.dp[b, seq:, :] = dot(r.do[g, seq:, :], r.v[g], NT)

        return [(1, s), (1, dp)]

    def soft(g):
        b = g % 2
        c2 = scale * log2e

        def part(blk, c):
            return slice(blk * seq + c, blk * seq + c + CH), half if blk == 0 else seq

        def masked(blk, c, s):
            row_id = lax.broadcasted_iota(jnp.int32, (CH, half), 0) + (c % half)
            keep = row_id >= lax.broadcasted_iota(jnp.int32, (CH, half), 1)
            if blk == 0:
                return jnp.where(keep, s, -jnp.inf)
            return jnp.concatenate([s[:, :half], jnp.where(keep, s[:, half:], -jnp.inf)], axis=1)

        def wide(ref, rows, width):
            t = ref[rows, :]
            return t if width == half else jnp.concatenate([t, t], axis=1)

        def top(blk, c):
            rows, width = part(blk, c)

            def run():
                m = jnp.max(masked(blk, c, r.s[b, rows, 0:width]), axis=-1, keepdims=True)
                r.st[0, rows, :] = jnp.broadcast_to(m * c2, (CH, HD))

            return (0.4 + 0.4 * blk, run)

        def power(blk, c):
            rows, width = part(blk, c)

            def run():
                e = jnp.exp2(masked(blk, c, r.s[b, rows, 0:width] * c2) - wide(r.st.at[0], rows, width))
                r.s[b, rows, 0:width] = e
                r.st[1, rows, :] = jnp.broadcast_to(1.0 / jnp.sum(e, axis=-1, keepdims=True), (CH, HD))

            return (0.8 + 0.8 * blk, run)

        def prob(blk, c):
            rows, width = part(blk, c)

            def run():
                pr = r.s[b, rows, 0:width] * wide(r.st.at[1], rows, width)
                r.s[b, rows, 0:width] = pr
                r.p[b, rows, 0:width] = pr.astype(BF16)
                r.st[2, rows, :] = jnp.broadcast_to(jnp.sum(pr * r.dp[b, rows, 0:width], axis=-1, keepdims=True), (CH, HD))

            return (0.8 + 0.8 * blk, run)

        def last(blk, c):
            rows, width = part(blk, c)

            def run():
                d = r.dp[b, rows, 0:width] - wide(r.st.at[2], rows, width)
                r.ds[b, rows, 0:width] = (r.s[b, rows, 0:width] * d * scale).astype(BF16)

            return (0.8 + 0.8 * blk, run)

        return [f(blk, c) for f in (top, power, prob, last) for blk in range(2) for c in range(0, seq, CH)]

    def grads(g):
        b = g % 2
        col, kcol = g * 2 * HD, g * HD

        def dq():
            r.dqf[b, 0:seq, :] = dot(r.ds[b, 0:seq, 0:half], r.rot[g, 2 * seq:2 * seq + half, :])
            r.dqf[b, seq:, :] = dot(r.ds[b, seq:, :], r.rot[g, 2 * seq:, :])

        def dk():
            tb = dot(r.ds[b, seq:, :], r.rot[g, seq:2 * seq, :], TN)
            ta = dot(r.ds[b, 0:seq, 0:half], r.rot[g, 0:seq, :], TN)
            r.dkf[b, :half, :] = tb[:half] + ta
            r.dkf[b, half:, :] = tb[half:]

        def o():
            ta = dot(r.p[b, 0:seq, 0:half], r.v[g, :half, :])
            tb = dot(r.p[b, seq:, :], r.v[g])
            for h in range(2):
                r.o[0:half, col + h * HD:col + (h + 1) * HD] = ta[h * half:(h + 1) * half].astype(BF16)
                r.o[half:seq, col + h * HD:col + (h + 1) * HD] = tb[h * half:(h + 1) * half].astype(BF16)

        def dv():
            tb = dot(r.p[b, seq:, :], r.do[g, seq:, :], TN)
            ta = dot(r.p[b, 0:seq, 0:half], r.do[g, :seq, :], TN)
            r.dv[0:half, kcol:kcol + HD] = (tb[:half] + ta).astype(BF16)
            r.dv[half:seq, kcol:kcol + HD] = tb[half:].astype(BF16)

        return [(1, dq), (1, dk), (1, o), (1, dv)]

    def back(g):
        b = g % 2

        def place(h, c):
            if h == 2:
                return r.dkf, c, r.dk, g * HD, r.kg
            return r.dqf, stacked(h, c), r.dq, (2 * g + h) * HD, r.qg

        def turn(h, c):
            src, o, _, _, g_ref = place(h, c)

            def run():
                d = src[b, o:o + CH, :].astype(BF16).astype(F32)
                that = r.raw[g, h, c:c + CH, :].astype(F32) * r.inv[g, h, c:c + CH, :]
                du = d[:, :HD] * r.tab[2, c:c + CH, :] - d[:, HD:] * r.tab[3, c:c + CH, :]
                src[b, o:o + CH, 0:HD] = du
                pr = du * that
                dg_ref = r.dgk if h == 2 else r.dgq
                dg_ref[...] += jnp.sum(pr.reshape(CH // 8, 8, HD), axis=0)
                r.sb[h, c:c + CH, :] = jnp.broadcast_to(jnp.mean(pr * g_ref[0:1, :], axis=-1, keepdims=True), (CH, HD))

            return (0.6, run)

        def out(h, c):
            src, o, out_ref, col, g_ref = place(h, c)

            def run():
                inv = r.inv[g, h, c:c + CH, :]
                that = r.raw[g, h, c:c + CH, :].astype(F32) * inv
                out_ref[c:c + CH, col:col + HD] = (inv * (src[b, o:o + CH, 0:HD] * g_ref[0:1, :] - that * r.sb[h, c:c + CH, :])).astype(BF16)

            return (0.5, run)

        return [f(h, c) for f in (turn, out) for h in (0, 1, 2) for c in range(0, seq, CH)]

    return SimpleNamespace(norm=norm_rows, proj=proj, rope=rope, scores=scores, soft=soft, grads=grads, back=back)


def attn_tick(st, g, n_grp, more=()):
    gr = st.grads(g)
    for _, f in gr[:2]:
        f()
    weave(st.soft((g - 3) % n_grp), st.rope((g - 1) % n_grp), st.back(g), st.scores((g - 2) % n_grp) + gr[2:] + st.proj(g) + list(more))


def attn_scratch(seq, n_grp):
    return dict(
        qnew=pltpu.VMEM((2, 2, seq, HD), BF16),
        knew=pltpu.VMEM((n_grp, seq, HD), BF16),
        vnew=pltpu.VMEM((n_grp, seq, HD), BF16),
        raw=pltpu.VMEM((n_grp, 3, seq, HD), BF16),
        inv=pltpu.VMEM((n_grp, 3, seq, HD), F32),
        rot=pltpu.VMEM((n_grp, 3 * seq, 2 * HD), BF16),
        do=pltpu.VMEM((n_grp, 2 * seq, HD), BF16),
        v=pltpu.VMEM((n_grp, seq, HD), BF16),
        s=pltpu.VMEM((2, 2 * seq, seq), F32),
        dp=pltpu.VMEM((2, 2 * seq, seq), F32),
        p=pltpu.VMEM((2, 2 * seq, seq), BF16),
        ds=pltpu.VMEM((2, 2 * seq, seq), BF16),
        dkf=pltpu.VMEM((2, seq, 2 * HD), F32),
        dqf=pltpu.VMEM((2, 2 * seq, 2 * HD), F32),
        st=pltpu.VMEM((3, 2 * seq, HD), F32),
        sb=pltpu.VMEM((3, seq, HD), F32),
        tab=pltpu.VMEM((4, seq, HD), F32),
    )


EARLY = 4


def tail_kernel(seq, n_grp, rows, keys, sel_ref, n_in, dy_in, cos_in, sin_in, x_in, dyx_in, gain_ref, qg_ref, kg_ref, dgq_own, dgk_own, *refs):
    own_w, oth_w, own_a = refs[:4], refs[4:8], refs[8:12]
    y_out, dx_out, sums_out = refs[12:15]
    r = SimpleNamespace(n=n_in, dy=dy_in, qg=qg_ref, kg=kg_ref, gain=gain_ref, **dict(zip(keys, refs[15:])))
    step = pl.program_id(0)
    me = sel_ref[0]
    oth = 1 - me
    D = x_in.shape[1]
    r.wq = lambda c: r.wq_all[oth, :, c]
    r.wk = lambda c: r.wk_all[oth, :, c]
    r.wv = lambda c: r.wv_all[oth, :, c]
    r.do_dot = lambda c: dot(dy_in[...], r.wo_all[oth, c, :], NT)
    r.o, r.dq, r.dk, r.dv = r.oc.at[oth], r.dqc.at[oth], r.dkc.at[oth], r.dvc.at[oth]
    st = attn_stages(seq, n_grp, r)

    def fetch(row):
        return [pltpu.make_async_copy(src.at[me, pl.ds(row * seq, seq), :], dst.at[me], r.sem.at[8 + k])
                for k, (src, dst) in enumerate(zip(own_a[1:], (r.dqc, r.dkc, r.dvc)))]

    def fetch_o(row):
        return pltpu.make_async_copy(own_a[0].at[me, pl.ds(row * seq, seq), :], r.o_next, r.sem.at[11])

    weights = (r.wq_all, r.wk_all, r.wv_all, r.wo_all)
    theirs = [pltpu.make_async_copy(oth_w[k], dst.at[oth], r.sem.at[4 + k]) for k, dst in enumerate(weights)]
    mine = [pltpu.make_async_copy(own_w[k], dst.at[me], r.sem.at[k]) for k, dst in enumerate(weights)]

    @pl.when(step == 0)
    def _():
        for c in theirs + mine[3:] + mine[:3]:
            c.start()
        r.dg[...] = jnp.zeros_like(r.dg)
        r.oc[...] = jnp.zeros_like(r.oc)
        for c in theirs + mine[3:]:
            c.wait()

    @pl.when(step > 0)
    def _():
        for c in fetch(step - 1):
            c.start()
        fetch_o(step - 1).wait()
        r.oc[me] = r.o_next[...]

    @pl.when(step < rows)
    def _():
        fetch_o(step).start()

    CR, NC = 32, 256
    nn = D // NC
    lines = range(0, seq, CR)

    def wide(v):
        return jnp.concatenate([v] * (NC // HD), axis=1)

    def stat(c):
        def run():
            xf = x_in[c:c + CR, :].astype(F32)
            r.xs[0, c:c + CR, :] = jnp.broadcast_to(lax.rsqrt(jnp.mean(xf * xf, axis=-1, keepdims=True) + EPS), (CR, HD))
            r.xs[1, c:c + CR, :] = jnp.zeros((CR, HD), F32)

        return (1, run)

    def dn_dot(n):
        def run():
            cols = slice(n * NC, (n + 1) * NC)
            t = None
            for s in range(2):
                for a_ref, w_ref in ((r.dqc, r.wq_all), (r.dkc, r.wk_all), (r.dvc, r.wv_all)):
                    u = dot(a_ref[s], w_ref[s, cols, :], NT)
                    t = u if t is None else t + u
            r.dn[:, cols] = t

        return (2, run)

    def first(n, c):
        def run():
            cols = slice(n * NC, (n + 1) * NC)
            inv = wide(r.xs[0, c:c + CR, :])
            d = r.dn[c:c + CR, cols]
            w = d * (x_in[c:c + CR, cols].astype(F32) * inv)
            r.dg[:, cols] += jnp.sum(w.reshape(CR // 8, 8, NC), axis=0)
            w = w * gain_ref[0:1, cols]
            r.xs[1, c:c + CR, :] += w[:, :HD] + w[:, HD:]
            r.dn[c:c + CR, cols] = dyx_in[c:c + CR, cols].astype(F32) + inv * (d * gain_ref[0:1, cols])

        return (1, run)

    def mean(c):
        def run():
            inv = r.xs[0, c:c + CR, :]
            r.xs[2, c:c + CR, :] = jnp.sum(r.xs[1, c:c + CR, :], axis=-1, keepdims=True) * (1.0 / D) * (inv * inv)

        return (0.2, run)

    def second(n, c):
        def run():
            cols = slice(n * NC, (n + 1) * NC)
            dx_out[c:c + CR, cols] = (r.dn[c:c + CR, cols] - x_in[c:c + CR, cols].astype(F32) * wide(r.xs[2, c:c + CR, :])).astype(BF16)

        return (1, run)

    def y_dot(n):
        def run():
            cols = slice(n * NC, (n + 1) * NC)
            t = dot(r.oc[0], r.wo_all[0, :, cols]) + dot(r.oc[1], r.wo_all[1, :, cols])
            y_out[:, cols] = (x_in[:, cols].astype(F32) + t).astype(BF16)

        return (1, run)

    r.tab[2:4] = r.tab[0:2]
    r.tab[0] = cos_in[...]
    r.tab[1] = sin_in[...]
    yd = [y_dot(n) for n in range(nn)]
    for g in range(n_grp):
        attn_tick(st, g, n_grp, yd[:EARLY] if g == n_grp - 1 else [])
    for acc in (r.dgq, r.dgk):
        acc[...] = jnp.where(step > 0, acc[...], 0.0)

    @pl.when(step == 0)
    def _():
        for c in mine[:3]:
            c.wait()

    @pl.when(step > 0)
    def _():
        for c in fetch(step - 1):
            c.wait()
        dn = [dn_dot(n) for n in range(nn)]
        for _, f in dn[:1]:
            f()
        weave([stat(c) for c in lines], dn[1:2])
        for n in range(2, nn):
            weave([first(n - 2, c) for c in lines], dn[n:n + 1])
        weave([first(nn - 2, c) for c in lines], yd[EARLY:EARLY + 1])
        weave([first(nn - 1, c) for c in lines] + [mean(c) for c in lines], yd[EARLY + 1:EARLY + 2])
        weave([second(n, c) for n in range(nn) for c in lines], yd[EARLY + 2:])

    @pl.when(step == rows)
    def _():
        at = 0
        for part in (r.dg[...], r.dgq[...] + dgq_own[...], r.dgk[...] + dgk_own[...]):
            sums_out[:, at:at + part.shape[1]] = jnp.sum(part, axis=0, keepdims=True)
            at += part.shape[1]


def tail_call(sel, n, x, dy, cosd, sind, o, dq, dk, dv, gain, qg, kg, dgq, dgk, own, oth, seq=256):
    T, D = x.shape
    nq, nk = dq.shape[2], dk.shape[2]
    n_grp = nk // HD
    rows = T // seq
    lag = lambda k, c: pl.BlockSpec((seq, c), lambda i, s: (jnp.clip(i - k, 0, rows - 1), 0))
    const = lambda *b: pl.BlockSpec(b, lambda i, s: (0,) * len(b), pipeline_mode=pl.Buffered(1))
    hbm = pl.BlockSpec(memory_space=pl.ANY)
    scratch = attn_scratch(seq, n_grp)
    scratch.update(
        wq_all=pltpu.VMEM((2, D, nq), BF16), wk_all=pltpu.VMEM((2, D, nk), BF16), wv_all=pltpu.VMEM((2, D, nk), BF16), wo_all=pltpu.VMEM((2, nq, D), BF16),
        dn=pltpu.VMEM((seq, D), F32), oc=pltpu.VMEM((2, seq, nq), BF16), dqc=pltpu.VMEM((2, seq, nq), BF16), dkc=pltpu.VMEM((2, seq, nk), BF16), dvc=pltpu.VMEM((2, seq, nk), BF16),
        o_next=pltpu.VMEM((seq, nq), BF16), xs=pltpu.VMEM((3, seq, HD), F32), dg=pltpu.VMEM((8, D), F32), dgq=pltpu.VMEM((8, HD), F32), dgk=pltpu.VMEM((8, HD), F32), sem=pltpu.SemaphoreType.DMA((12,)))
    flops = 2 * T * D * (nq + 2 * nk + nq) * 3 + 12 * T * nq * seq
    return pl.pallas_call(
        functools.partial(tail_kernel, seq, n_grp, rows, tuple(scratch)),
        grid_spec=pltpu.PrefetchScalarGridSpec(
            num_scalar_prefetch=1,
            grid=(rows + 1,),
            in_specs=[lag(0, D), lag(0, D), lag(0, HD), lag(0, HD), lag(1, D), lag(1, D), const(1, D), const(1, HD), const(1, HD), const(8, HD), const(8, HD)] + [hbm] * 12,
            out_specs=[lag(1, D), lag(1, D), pl.BlockSpec((1, D + 2 * HD), lambda i, s: (0, 0))],
            scratch_shapes=list(scratch.values()),
        ),
        out_shape=[jax.ShapeDtypeStruct((T, D), BF16)] * 2 + [jax.ShapeDtypeStruct((1, D + 2 * HD), F32)],
        compiler_params=pltpu.CompilerParams(dimension_semantics=("arbitrary",), vmem_limit_bytes=67043328),
        cost_estimate=pl.CostEstimate(flops=flops, bytes_accessed=T * D * 14, transcendentals=T * nq * 2),
        name="tail",
    )(sel, n, dy, cosd, sind, x, dy, gain, qg, kg, dgq, dgk, *own, *oth, o, dq, dk, dv)


def solution(mesh):
    tok_spec = P("dp", None, None)
    col_spec = P(None, "tp")
    row_spec = P("tp", None)
    n_dp = mesh.shape["dp"]

    def per_device(x_in, dy_in, positions, g_attn, q_gain, k_gain, w_q, w_k, w_v, w_o):
        n_batch, n_seq, D = x_in.shape
        T = n_batch * n_seq
        nk = w_k.shape[1]
        x, dy = x_in.reshape(T, D), dy_in.reshape(T, D)
        me = lax.axis_index("tp").astype(jnp.int32)
        own = me.reshape(1)

        part = lax.axis_index("dp").astype(jnp.int32).reshape(1)
        share, cosd, sind = pre_call(part, w_q, w_k, w_v, w_o, positions, parts=n_dp)
        gathered = lax.all_gather(share, ("tp", "dp"), tiled=True)

        gain = g_attn.astype(F32).reshape(1, D)
        qg, kg = q_gain.astype(F32).reshape(1, HD), k_gain.astype(F32).reshape(1, HD)

        n, o, dq, dk, dv, dgq, dgk, dw_o = attn_call(True, own, x, dy, cosd, sind, gain, qg, kg, w_q, w_k, w_v, w_o, seq=n_seq)
        dw_q, dw_k, dw_v, *theirs = dw_call(own, n, [dq, dk, dv], 512, gathered=gathered, nk=nk)
        dw_o, dw_q, dw_k, dw_v = lax.psum((dw_o, dw_q, dw_k, dw_v), "dp")

        y, dx, sums = tail_call(own, n, x, dy, cosd, sind, o, dq, dk, dv, gain, qg, kg, dgq, dgk, (w_q, w_k, w_v, w_o), theirs, seq=n_seq)
        g_sum, q_sum, k_sum = (t.reshape(-1) for t in sum_call(sums, (D, HD, HD), n_dp))
        dw_o, dw_q, dw_k, dw_v = copy_call((dw_o, dw_q, dw_k, dw_v))
        return y.reshape(x_in.shape), dx.reshape(x_in.shape), dw_q, dw_k, dw_v, dw_o, q_sum, k_sum, g_sum

    return jax.shard_map(per_device, mesh=mesh, in_specs=(tok_spec, tok_spec, P("dp", None), P(), P(), P(), col_spec, col_spec, col_spec, row_spec), out_specs=(tok_spec, tok_spec, col_spec, col_spec, col_spec, row_spec, P(), P(), P()), check_vma=False)
```

```python
import functools
from types import SimpleNamespace
import jax
import jax.numpy as jnp
from jax import lax
from jax.experimental import pallas as pl
from jax.experimental.pallas import tpu as pltpu
from jax.sharding import PartitionSpec as P


EPS = 1e-6
THETA = 1000000.0
F32 = jnp.float32
BF16 = jnp.bfloat16
HD = 128
NT = (((1,), (1,)), ((), ()))
TN = (((0,), (0,)), ((), ()))
NN = (((1,), (0,)), ((), ()))


def dot(a, b, dims=NN):
    return lax.dot_general(a, b, dims, preferred_element_type=F32)


def weave(*lists):
    order = []
    for n, pieces in enumerate(lists):
        total = sum(c for c, _ in pieces) or 1
        at = 0
        for k, (c, f) in enumerate(pieces):
            order.append(((at + c / 2) / total, n, k, f))
            at += c
    for _, _, _, f in sorted(order, key=lambda e: e[:3]):
        f()


CH = 32


def attn_kernel(own, seq, n_grp, sel_ref, *refs):
    if own:
        (x0_ref, xn_ref, dy_ref, cos_ref, sin_ref, gain_ref, qg_ref, kg_ref, wq_ref, wk_ref, wv_ref, wo_ref,
         n_out, o_out, dq_out, dk_out, dv_out, dgq_out, dgk_out, dwo_out) = refs[:20]
        refs = refs[20:]
    else:
        nin_ref, dy_ref, cos_ref, sin_ref, qg_ref, kg_ref, wq_ref, wk_ref, wv_ref, wo_ref, _, _, _, _, o_out, dq_out, dk_out, dv_out = refs[:18]
        refs = refs[18:]
        n_ref = nin_ref
    (qnew_ref, knew_ref, vnew_ref, raw_ref, inv_ref, rot_ref, do_ref, v_ref, s_ref, dp_ref, p_ref, ds_ref, dkf_ref, dqf_ref, st_ref,
     tab_ref, o_ref, dq_ref, dk_ref, dv_ref) = refs[:20]
    if own:
        n_ref, nn_ref, dgq_ref, dgk_ref, acc_ref, ot_ref, dyp_ref, sem = refs[20:]
    half = seq // 2
    scale = HD ** -0.5
    log2e = 1.4426950408889634
    step = pl.program_id(0)

    def norm_rows(src, dst):
        def piece(c):
            def run():
                xf = src[c:c + 32, :].astype(F32)
                inv = lax.rsqrt(jnp.mean(xf * xf, axis=-1, keepdims=True) + EPS)
                dst[c:c + 32, :] = (xf * inv * gain_ref[0:1, :]).astype(BF16)

            return (1.5, run)

        return [piece(c) for c in range(0, seq, 32)]

    def proj(g):
        def q():
            t = dot(n_ref[...], wq_ref[:, g * 2 * HD:(g + 1) * 2 * HD])
            for h in range(2):
                qnew_ref[g % 2, h] = t[:, h * HD:(h + 1) * HD].astype(BF16)

        def k():
            t = dot(n_ref[...], wk_ref[:, g * HD:(g + 2) * HD])
            for h in range(2):
                knew_ref[g + h] = t[:, h * HD:(h + 1) * HD].astype(BF16)

        def v():
            t = dot(n_ref[...], wv_ref[:, g * HD:(g + 2) * HD])
            for h in range(2):
                vnew_ref[g + h] = t[:, h * HD:(h + 1) * HD].astype(BF16)

        def do():
            t = dot(dy_ref[...], wo_ref[g * 2 * HD:(g + 1) * 2 * HD, :], NT)
            for h in range(2):
                do_ref[g, h * half:(h + 1) * half, :] = t[:half, h * HD:(h + 1) * HD].astype(BF16)
                do_ref[g, seq + h * half:seq + (h + 1) * half, :] = t[half:, h * HD:(h + 1) * HD].astype(BF16)

        return [(1, q)] + ([(1, k), (1, v)] if g % 2 == 0 else []) + [(1, do)]

    def stacked(h, c):
        return (h * half + c) if c < half else (seq + h * half + c - half)

    def rope(g):
        cs, sn = (tab_ref.at[2], tab_ref.at[3]) if g == n_grp - 1 else (tab_ref.at[0], tab_ref.at[1])

        def size(h, c):
            def run():
                raw = knew_ref[g, c:c + CH, :] if h == 2 else qnew_ref[g % 2, h, c:c + CH, :]
                raw_ref[g, h, c:c + CH, :] = raw
                t = raw.astype(F32)
                inv_ref[g, h, c:c + CH, :] = jnp.broadcast_to(lax.rsqrt(jnp.mean(t * t, axis=-1, keepdims=True) + EPS), t.shape)

            return (0.4, run)

        def turn(h, c):
            def run():
                t = raw_ref[g, h, c:c + CH, :].astype(F32)
                w = (t * inv_ref[g, h, c:c + CH, :]) * (kg_ref if h == 2 else qg_ref)[0:1, :]
                o = 2 * seq + c if h == 2 else stacked(h, c)
                x = pltpu.roll(w, HD // 2, 1)
                co, si = cs[c:c + CH, :], sn[c:c + CH, :]
                rot_ref[g, o:o + CH, 0:HD] = (w * co + x * si).astype(BF16)
                rot_ref[g, o:o + CH, HD:] = (x * co - w * si).astype(BF16)
                if h == 2:
                    v_ref[g, c:c + CH, :] = vnew_ref[g, c:c + CH, :]

            return (0.6, run)

        return [f(h, c) for f in (size, turn) for h in (2, 0, 1) for c in range(0, seq, CH)]

    def scores(g):
        b = g % 2

        def s():
            s_ref[b, 0:seq, 0:half] = dot(rot_ref[g, 0:seq, 0:HD], rot_ref[g, 2 * seq:2 * seq + half, 0:HD], NT)
            s_ref[b, seq:, :] = dot(rot_ref[g, seq:2 * seq, 0:HD], rot_ref[g, 2 * seq:, 0:HD], NT)

        def dp():
            dp_ref[b, 0:seq, 0:half] = dot(do_ref[g, :seq, :], v_ref[g, :half, :], NT)
            dp_ref[b, seq:, :] = dot(do_ref[g, seq:, :], v_ref[g], NT)

        return [(1, s), (1, dp)]

    def soft(g):
        b = g % 2
        c2 = scale * log2e

        def part(blk, c):
            return slice(blk * seq + c, blk * seq + c + CH), half if blk == 0 else seq

        def masked(blk, c, s):
            row_id = lax.broadcasted_iota(jnp.int32, (CH, half), 0) + (c % half)
            keep = row_id >= lax.broadcasted_iota(jnp.int32, (CH, half), 1)
            if blk == 0:
                return jnp.where(keep, s, -jnp.inf)
            return jnp.concatenate([s[:, :half], jnp.where(keep, s[:, half:], -jnp.inf)], axis=1)

        def wide(ref, rows, width):
            t = ref[rows, :]
            return t if width == half else jnp.concatenate([t, t], axis=1)

        def top(blk, c):
            rows, width = part(blk, c)

            def run():
                m = jnp.max(masked(blk, c, s_ref[b, rows, 0:width]), axis=-1, keepdims=True)
                st_ref[0, rows, :] = jnp.broadcast_to(m * c2, (CH, HD))

            return (0.4 + 0.4 * blk, run)

        def power(blk, c):
            rows, width = part(blk, c)

            def run():
                e = jnp.exp2(masked(blk, c, s_ref[b, rows, 0:width] * c2) - wide(st_ref.at[0], rows, width))
                s_ref[b, rows, 0:width] = e
                st_ref[1, rows, :] = jnp.broadcast_to(1.0 / jnp.sum(e, axis=-1, keepdims=True), (CH, HD))

            return (0.8 + 0.8 * blk, run)

        def prob(blk, c):
            rows, width = part(blk, c)

            def run():
                pr = s_ref[b, rows, 0:width] * wide(st_ref.at[1], rows, width)
                s_ref[b, rows, 0:width] = pr
                p_ref[b, rows, 0:width] = pr.astype(BF16)
                st_ref[2, rows, :] = jnp.broadcast_to(jnp.sum(pr * dp_ref[b, rows, 0:width], axis=-1, keepdims=True), (CH, HD))

            return (0.8 + 0.8 * blk, run)

        def last(blk, c):
            rows, width = part(blk, c)

            def run():
                d = dp_ref[b, rows, 0:width] - wide(st_ref.at[2], rows, width)
                ds_ref[b, rows, 0:width] = (s_ref[b, rows, 0:width] * d * scale).astype(BF16)

            return (0.8 + 0.8 * blk, run)

        return [f(blk, c) for f in (top, power, prob, last) for blk in range(2) for c in range(0, seq, CH)]

    def grads(g):
        b = g % 2
        col, kcol = g * 2 * HD, g * HD

        def dq():
            dqf_ref[b, 0:seq, :] = dot(ds_ref[b, 0:seq, 0:half], rot_ref[g, 2 * seq:2 * seq + half, :])
            dqf_ref[b, seq:, :] = dot(ds_ref[b, seq:, :], rot_ref[g, 2 * seq:, :])

        def dk():
            tb = dot(ds_ref[b, seq:, :], rot_ref[g, seq:2 * seq, :], TN)
            ta = dot(ds_ref[b, 0:seq, 0:half], rot_ref[g, 0:seq, :], TN)
            dkf_ref[b, :half, :] = tb[:half] + ta
            dkf_ref[b, half:, :] = tb[half:]

        def o():
            ta = dot(p_ref[b, 0:seq, 0:half], v_ref[g, :half, :])
            tb = dot(p_ref[b, seq:, :], v_ref[g])
            for h in range(2):
                o_ref[0:half, col + h * HD:col + (h + 1) * HD] = ta[h * half:(h + 1) * half].astype(BF16)
                o_ref[half:seq, col + h * HD:col + (h + 1) * HD] = tb[h * half:(h + 1) * half].astype(BF16)

        def dv():
            tb = dot(p_ref[b, seq:, :], do_ref[g, seq:, :], TN)
            ta = dot(p_ref[b, 0:seq, 0:half], do_ref[g, :seq, :], TN)
            dv_ref[0:half, kcol:kcol + HD] = (tb[:half] + ta).astype(BF16)
            dv_ref[half:seq, kcol:kcol + HD] = tb[half:].astype(BF16)

        return [(1, dq), (1, dk), (1, o), (1, dv)]

    def back(g):
        b = g % 2

        def place(h, c):
            if h == 2:
                return dkf_ref, c, dk_ref, g * HD, kg_ref
            return dqf_ref, stacked(h, c), dq_ref, (2 * g + h) * HD, qg_ref

        def turn(h, c):
            src, o, _, _, g_ref = place(h, c)

            def run():
                d = src[b, o:o + CH, :].astype(BF16).astype(F32)
                that = raw_ref[g, h, c:c + CH, :].astype(F32) * inv_ref[g, h, c:c + CH, :]
                du = d[:, :HD] * tab_ref[2, c:c + CH, :] - d[:, HD:] * tab_ref[3, c:c + CH, :]
                src[b, o:o + CH, 0:HD] = du
                pr = du * that
                if own:
                    dg_ref = dgk_ref if h == 2 else dgq_ref
                    dg_ref[...] += jnp.sum(pr.reshape(CH // 8, 8, HD), axis=0)
                st_ref[3 + h, c:c + CH, :] = jnp.broadcast_to(jnp.mean(pr * g_ref[0:1, :], axis=-1, keepdims=True), (CH, HD))

            return (0.6, run)

        def out(h, c):
            src, o, out_ref, col, g_ref = place(h, c)

            def run():
                inv = inv_ref[g, h, c:c + CH, :]
                that = raw_ref[g, h, c:c + CH, :].astype(F32) * inv
                out_ref[c:c + CH, col:col + HD] = (inv * (src[b, o:o + CH, 0:HD] * g_ref[0:1, :] - that * st_ref[3 + h, c:c + CH, :])).astype(BF16)

            return (0.5, run)

        return [f(h, c) for f in (turn, out) for h in (0, 1, 2) for c in range(0, seq, CH)]

    def dwo(g):
        rows = slice(g * 2 * HD, (g + 1) * 2 * HD)

        def flip():
            ot_ref[rows, :] = o_ref[:, rows].T

        def part(c):
            def run():
                acc_ref[rows, c:c + 512] += dot(ot_ref[rows, :], dyp_ref[:, c:c + 512])

            return (0.25, run)

        return [(0.1, flip)] + [part(c) for c in range(0, acc_ref.shape[1], 512)]

    @pl.when(step == 0)
    def _():
        if own:
            weave(norm_rows(x0_ref, n_ref))

    tab_ref[2:4] = tab_ref[0:2]
    tab_ref[0] = cos_ref[...]
    tab_ref[1] = sin_ref[...]
    if own:
        norms = norm_rows(xn_ref, nn_ref)
    for g in range(n_grp):
        sc = scores((g - 2) % n_grp)
        gr = grads(g)
        nm = (norms[:4], norms[4:], [], [])[g] if own else []
        for _, f in gr[:2]:
            f()
        weave(soft((g - 3) % n_grp), rope((g - 1) % n_grp) + nm, back(g), sc + gr[2:] + (dwo(g - 1) if own and g > 0 else []) + proj(g) + (dwo(g) if own and g == n_grp - 1 else []))

    for dst, src in ((o_out, o_ref), (dq_out, dq_ref), (dk_out, dk_ref), (dv_out, dv_ref)):
        dst[0] = src[...]
    if own:
        n_out[...] = n_ref[...]
        n_ref[...] = nn_ref[...]
        keep = step > 0
        for dst, acc in ((dgq_out, dgq_ref), (dgk_out, dgk_ref)):
            acc[...] = jnp.where(keep, acc[...], 0.0)
            dst[...] = acc[...]
        dyp_ref[...] = dy_ref[...]

        @pl.when(step == 0)
        def _():
            @pl.loop(0, acc_ref.shape[0] // 64)
            def _(j):
                acc_ref[pl.ds(pl.multiple_of(j * 64, 64), 64), :] = jnp.zeros((64, acc_ref.shape[1]), F32)

        @pl.when(step == pl.num_programs(0) - 1)
        def _():
            c = pltpu.make_async_copy(acc_ref, dwo_out, sem)
            c.start()
            c.wait()


def attn_call(own, sel, x, dy, cosd, sind, gain, qg, kg, wq, wk, wv, wo, prev=None, seq=256):
    T, D = x.shape
    nq, nk = wq.shape[1], wk.shape[1]
    n_grp = nk // HD
    rows = T // seq
    const = lambda *b: pl.BlockSpec(b, lambda i, s: (0,) * len(b), pipeline_mode=pl.Buffered(1))
    now = lambda c: pl.BlockSpec((seq, c), lambda i, s: (jnp.minimum(i, rows - 1), 0))
    nxt = lambda c: pl.BlockSpec((seq, c), lambda i, s: (jnp.minimum(i + 1, rows - 1), 0))
    out3 = lambda c: pl.BlockSpec((1, seq, c), lambda i, s: (s[0], jnp.maximum(i - 1, 0), 0))
    mid = [now(D), now(HD), now(HD)]
    tail = [const(1, HD), const(1, HD), const(D, nq), const(D, nk), const(D, nk), const(nq, D)]
    shapes = [jax.ShapeDtypeStruct((2, T, c), BF16) for c in (nq, nq, nk, nk)]
    specs = [out3(nq), out3(nq), out3(nk), out3(nk)]
    aliases = {}
    if own:
        in_specs = [const(seq, D), nxt(D)] + mid + [const(1, D)] + tail
        args = [x, x, dy, cosd, sind, gain, qg, kg, wq, wk, wv, wo]
        shapes = [jax.ShapeDtypeStruct((T, D), BF16)] + shapes + [jax.ShapeDtypeStruct((8, HD), F32)] * 2 + [jax.ShapeDtypeStruct((nq, D), F32)]
        specs = [now(D)] + specs + [pl.BlockSpec((8, HD), lambda i, s: (0, 0))] * 2 + [pl.BlockSpec(memory_space=pl.ANY)]
    else:
        in_specs = [now(D)] + mid + tail + [pl.BlockSpec(memory_space=pl.ANY)] * 4
        args = [x, dy, cosd, sind, qg, kg, wq, wk, wv, wo]
        aliases = {1 + len(args) + i: i for i in range(4)}
        args += list(prev)
    flops = 2 * T * D * (nq + 2 * nk + nq) + 12 * T * nq * seq
    return pl.pallas_call(
        functools.partial(attn_kernel, own, seq, n_grp),
        grid_spec=pltpu.PrefetchScalarGridSpec(
            num_scalar_prefetch=1,
            grid=(rows + 1,),
            in_specs=in_specs,
            out_specs=specs,
            scratch_shapes=[
                pltpu.VMEM((2, 2, seq, HD), BF16),
                pltpu.VMEM((n_grp, seq, HD), BF16),
                pltpu.VMEM((n_grp, seq, HD), BF16),
                pltpu.VMEM((n_grp, 3, seq, HD), BF16),
                pltpu.VMEM((n_grp, 3, seq, HD), F32),
                pltpu.VMEM((n_grp, 3 * seq, 2 * HD), BF16),
                pltpu.VMEM((n_grp, 2 * seq, HD), BF16),
                pltpu.VMEM((n_grp, seq, HD), BF16),
                pltpu.VMEM((2, 2 * seq, seq), F32),
                pltpu.VMEM((2, 2 * seq, seq), F32),
                pltpu.VMEM((2, 2 * seq, seq), BF16),
                pltpu.VMEM((2, 2 * seq, seq), BF16),
                pltpu.VMEM((2, seq, 2 * HD), F32),
                pltpu.VMEM((2, 2 * seq, 2 * HD), F32),
                pltpu.VMEM((6, 2 * seq, HD), F32),
                pltpu.VMEM((4, seq, HD), F32),
            ] + [pltpu.VMEM((seq, c), BF16) for c in (nq, nq, nk, nk)]
            + ([pltpu.VMEM((seq, D), BF16)] * 2 + [pltpu.VMEM((8, HD), F32)] * 2 + [pltpu.VMEM((nq, D), F32), pltpu.VMEM((nq, seq), BF16), pltpu.VMEM((seq, D), BF16), pltpu.SemaphoreType.DMA] if own else []),
        ),
        out_shape=shapes,
        input_output_aliases=aliases,
        compiler_params=pltpu.CompilerParams(dimension_semantics=("arbitrary",), vmem_limit_bytes=62 << 20),
        cost_estimate=pl.CostEstimate(flops=flops, bytes_accessed=T * D * 6 + T * (2 * nq + 2 * nk) * 2, transcendentals=T * nq * 2),
        name="attn_own" if own else "attn_other",
    )(sel, *args)


def pre_kernel(sel_ref, q_ref, k_ref, v_ref, o_ref, pos_ref, freq_ref, out_ref, cos_ref, sin_ref):
    d, nq, nk = q_ref.shape[0], q_ref.shape[1], k_ref.shape[1]
    out_ref[0, 0:d, 0:nq] = q_ref[...].astype(F32)
    out_ref[0, 0:d, nq:nq + nk] = k_ref[...].astype(F32)
    out_ref[0, 0:d, nq + nk:] = v_ref[...].astype(F32)
    out_ref[0, d:, :] = o_ref[...].astype(F32)
    n, seq = pos_ref.shape
    low = lax.broadcasted_iota(jnp.int32, (HD, HD), 1) < HD // 2
    for r in range(n):
        for h in range(0, seq // HD, 2):
            p = [jnp.broadcast_to(pos_ref[r:r + 1, (h + b) * HD:(h + b + 1) * HD].astype(F32), (HD, HD)).T for b in range(2)]
            a = jnp.where(low, p[0], p[1]) * freq_ref[0:1, :]
            k = jnp.round(a * 0.6366197723675814)
            x = ((a - k * 1.5703125) - k * 4.837512969970703125e-4) - k * 7.549789948768648e-8
            z = x * x
            s = ((-1.9515295891e-4 * z + 8.3321608736e-3) * z - 1.6666654611e-1) * z * x + x
            c = ((2.443315711809948e-5 * z - 1.388731625493765e-3) * z + 4.166664568298827e-2) * z * z - 0.5 * z + 1.0
            q = k.astype(jnp.int32)
            odd = (q & 1) == 1
            co, si = jnp.where(odd, s, c), jnp.where(odd, c, s)
            co = jnp.where(((q + 1) & 2) == 0, co, -co)
            si = jnp.where((q & 2) == 0, si, -si)
            cx, sx = pltpu.roll(co, HD // 2, 1), pltpu.roll(si, HD // 2, 1)
            for b in range(2):
                at = (r * (seq // HD) + h + b) * HD
                cos_ref[at:at + HD, :] = jnp.where(low, co, cx) if b == 0 else jnp.where(low, cx, co)
                sin_ref[at:at + HD, :] = jnp.where(low, -si, sx) if b == 0 else jnp.where(low, -sx, si)


def pre_call(part, w_q, w_k, w_v, w_o, positions, parts=2, cuts=4):
    D, nq = w_q.shape
    n, seq = positions.shape
    rows = n // cuts
    freq = THETA ** (-jnp.arange(0, HD, 2, dtype=F32) / HD)
    freq = jnp.concatenate([freq, freq]).reshape(1, HD)
    spec = lambda w: pl.BlockSpec((w.shape[0] // (parts * cuts), w.shape[1]), lambda i, s: (s[0] * cuts + i, 0))
    r = (D + nq) // (parts * cuts)
    table = pl.BlockSpec((rows * seq, HD), lambda i, s: (i, 0))
    return pl.pallas_call(
        pre_kernel,
        grid_spec=pltpu.PrefetchScalarGridSpec(
            num_scalar_prefetch=1,
            grid=(cuts,),
            in_specs=[spec(w) for w in (w_q, w_k, w_v, w_o)] + [pl.BlockSpec((rows, seq), lambda i, s: (i, 0)), pl.BlockSpec((1, HD), lambda i, s: (0, 0))],
            out_specs=[pl.BlockSpec((1, r, D), lambda i, s: (i, 0, 0)), table, table],
        ),
        out_shape=[jax.ShapeDtypeStruct((cuts, r, D), F32)] + [jax.ShapeDtypeStruct((n * seq, HD), F32)] * 2,
        compiler_params=pltpu.CompilerParams(dimension_semantics=("arbitrary",), vmem_limit_bytes=60 << 20),
        cost_estimate=pl.CostEstimate(flops=n * seq * HD * 30, bytes_accessed=cuts * r * D * 6 + n * seq * HD * 8, transcendentals=0),
        name="pre",
    )(part, w_q, w_k, w_v, w_o, positions, freq)


def dw_kernel(n_b, unpack, sel_ref, a_ref, *refs):
    if unpack:
        f_ref, parts = refs[n_b], refs[2 * n_b + 1:2 * n_b + 5]
        refs = refs[:n_b] + refs[n_b + 1:2 * n_b + 1] + refs[2 * n_b + 5:]
        q_ref, k_ref, v_ref, o_ref = parts
        per, nq, nk = f_ref.shape[0], q_ref.shape[1], k_ref.shape[1]
        d, e = q_ref.shape[0] // per, o_ref.shape[0] // per
        for j in range(per):
            q_ref[j * d:(j + 1) * d, :] = f_ref[j, 0:d, 0:nq].astype(BF16)
            k_ref[j * d:(j + 1) * d, :] = f_ref[j, 0:d, nq:nq + nk].astype(BF16)
            v_ref[j * d:(j + 1) * d, :] = f_ref[j, 0:d, nq + nk:].astype(BF16)
            o_ref[j * e:(j + 1) * e, :] = f_ref[j, d:, :].astype(BF16)
    bs, outs, accs, (at_ref, sem) = refs[:n_b], refs[n_b:2 * n_b], refs[2 * n_b:3 * n_b], refs[3 * n_b:]
    flat = lambda ref: ref.at[0] if len(ref.shape) == 3 else ref
    a, bs = flat(a_ref), [flat(b) for b in bs]
    M, tile = at_ref.shape
    step = pl.program_id(0)

    @pl.when(step == 0)
    def _():
        for acc in accs:
            @pl.loop(0, M // 64)
            def _(j):
                acc[pl.ds(pl.multiple_of(j * 64, 64), 64), :] = jnp.zeros((64, acc.shape[1]), F32)

    def part(acc, b, c):
        def run():
            acc[:, c:c + 256] += dot(at_ref[...], b[:, c:c + 256])

        return (1, run)

    for c in range(0, M, 256):
        for k in range(0, tile, 256):
            at_ref[c:c + 256, k:k + 256] = a[k:k + 256, c:c + 256].T
    weave([part(acc, b, c) for acc, b in zip(accs, bs) for c in range(0, b.shape[1], 256)])

    @pl.when(step == pl.num_programs(0) - 1)
    def _():
        copies = [pltpu.make_async_copy(acc, out, sem.at[k]) for k, (acc, out) in enumerate(zip(accs, outs))]
        for c in copies:
            c.start()
        for c in copies:
            c.wait()


def dw_call(sel, a, bs, tile, gathered=None, nk=0):
    def spec(v):
        if v.ndim == 3:
            return pl.BlockSpec((1, tile, v.shape[2]), lambda i, s: (s[0], i, 0))
        return pl.BlockSpec((tile, v.shape[1]), lambda i, s: (i, 0))

    T, M = a.shape[-2:]
    shapes = [(M, b.shape[-1]) for b in bs]
    width = sum(s[1] for s in shapes)
    steps = T // tile
    more_in, more_out, more_shapes, more = [], [], [], []
    if gathered is not None:
        n, r, D = gathered.shape
        per = n // 2 // steps
        more = [gathered]
        more_in = [pl.BlockSpec((per, r, D), lambda i, s: ((1 - s[0]) * steps + i, 0, 0))]
        nq = D - 2 * nk
        more_shapes = [jax.ShapeDtypeStruct(s, BF16) for s in ((D, nq), (D, nk), (D, nk), (nq, D))]
        more_out = [pl.BlockSpec((s.shape[0] // steps, s.shape[1]), lambda i, s: (i, 0)) for s in more_shapes]
    return pl.pallas_call(
        functools.partial(dw_kernel, len(bs), gathered is not None),
        grid_spec=pltpu.PrefetchScalarGridSpec(
            num_scalar_prefetch=1,
            grid=(steps,),
            in_specs=[spec(a)] + [spec(b) for b in bs] + more_in,
            out_specs=[pl.BlockSpec(memory_space=pl.ANY)] * len(bs) + more_out,
            scratch_shapes=[pltpu.VMEM(s, F32) for s in shapes] + [pltpu.VMEM((M, tile), BF16), pltpu.SemaphoreType.DMA((len(bs),))],
        ),
        out_shape=[jax.ShapeDtypeStruct(s, F32) for s in shapes] + more_shapes,
        compiler_params=pltpu.CompilerParams(dimension_semantics=("arbitrary",), vmem_limit_bytes=60 << 20),
        cost_estimate=pl.CostEstimate(flops=2 * T * M * width, bytes_accessed=2 * T * (M + width) + 4 * M * width, transcendentals=0),
    )(sel, a, *bs, *more)


def sum_kernel(n, widths, part_ref, *refs):
    outs, (slots, local_sem, send_sem, recv_sem) = refs[:-4], refs[-4:]
    me = lax.axis_index("dp")
    barrier = pltpu.get_barrier_semaphore()
    for k in range(1, n):
        pl.semaphore_signal(barrier, inc=1, device_id={"dp": lax.rem(me + k, n)}, device_id_type=pl.DeviceIdType.MESH)
    mine = pltpu.make_async_copy(part_ref, slots.at[0], local_sem)
    mine.start()
    pl.semaphore_wait(barrier, n - 1)
    copies = []
    for k in range(1, n):
        copies.append(pltpu.make_async_remote_copy(
            src_ref=part_ref, dst_ref=slots.at[k], send_sem=send_sem.at[k - 1], recv_sem=recv_sem.at[k - 1],
            device_id={"dp": lax.rem(me + k, n)}, device_id_type=pl.DeviceIdType.MESH))
    for c in copies:
        c.start()
    mine.wait()
    for c in copies:
        c.wait()
    total = slots[lax.rem(me + n, n)]
    for a in range(1, n):
        total = total + slots[lax.rem(me + n - a, n)]
    at = 0
    for out, w in zip(outs, widths):
        out[...] = total[:, at:at + w]
        at += w


def sum_call(part, widths, n):
    return pl.pallas_call(
        functools.partial(sum_kernel, n, widths),
        in_specs=[pl.BlockSpec(memory_space=pl.ANY)],
        out_specs=[pl.BlockSpec(memory_space=pltpu.VMEM)] * len(widths),
        out_shape=[jax.ShapeDtypeStruct((1, w), F32) for w in widths],
        scratch_shapes=[pltpu.VMEM((n, *part.shape), F32), pltpu.SemaphoreType.DMA, pltpu.SemaphoreType.DMA((n - 1,)), pltpu.SemaphoreType.DMA((n - 1,))],
        compiler_params=pltpu.CompilerParams(collective_id=0, has_side_effects=True),
        cost_estimate=pl.CostEstimate(flops=n * part.size, bytes_accessed=8 * n * part.size, transcendentals=0),
        name="small_sum",
    )(part)


def copy_kernel(n, cuts, *refs):
    srcs, dsts, bufs, (in_sem, out_sem) = refs[:n], refs[n:2 * n], refs[2 * n:3 * n], refs[3 * n:]
    ins, outs = [], []
    for a, (src, dst, buf) in enumerate(zip(srcs, dsts, bufs)):
        rows = src.shape[0] // cuts
        for j in range(cuts):
            part = pl.ds(j * rows, rows)
            ins.append(pltpu.make_async_copy(src.at[part], buf.at[part], in_sem.at[a, j]))
            outs.append(pltpu.make_async_copy(buf.at[part], dst.at[part], out_sem.at[a, j]))
    for c in ins:
        c.start()
    for c, d in zip(ins, outs):
        c.wait()
        d.start()
    for d in outs:
        d.wait()


def copy_call(arrays, cuts=4):
    n = len(arrays)
    hbm = [pl.BlockSpec(memory_space=pl.ANY)] * n
    return pl.pallas_call(
        functools.partial(copy_kernel, n, cuts),
        in_specs=hbm,
        out_specs=hbm,
        out_shape=[jax.ShapeDtypeStruct(a.shape, a.dtype) for a in arrays],
        scratch_shapes=[pltpu.VMEM(a.shape, a.dtype) for a in arrays] + [pltpu.SemaphoreType.DMA((n, cuts))] * 2,
        compiler_params=pltpu.CompilerParams(vmem_limit_bytes=60 << 20),
        cost_estimate=pl.CostEstimate(flops=0, bytes_accessed=8 * sum(a.size for a in arrays), transcendentals=0),
        name="results",
    )(*arrays)


def attn_stages(seq, n_grp, r):
    half = seq // 2
    scale = HD ** -0.5
    log2e = 1.4426950408889634

    def norm_rows(src, dst):
        def piece(c):
            def run():
                xf = src[c:c + 32, :].astype(F32)
                inv = lax.rsqrt(jnp.mean(xf * xf, axis=-1, keepdims=True) + EPS)
                dst[c:c + 32, :] = (xf * inv * r.gain[0:1, :]).astype(BF16)

            return (1.5, run)

        return [piece(c) for c in range(0, seq, 32)]

    def proj(g):
        def q():
            t = dot(r.n[...], r.wq(slice(g * 2 * HD, (g + 1) * 2 * HD)))
            for h in range(2):
                r.qnew[g % 2, h] = t[:, h * HD:(h + 1) * HD].astype(BF16)

        def k():
            t = dot(r.n[...], r.wk(slice(g * HD, (g + 2) * HD)))
            for h in range(2):
                r.knew[g + h] = t[:, h * HD:(h + 1) * HD].astype(BF16)

        def v():
            t = dot(r.n[...], r.wv(slice(g * HD, (g + 2) * HD)))
            for h in range(2):
                r.vnew[g + h] = t[:, h * HD:(h + 1) * HD].astype(BF16)

        def do():
            t = r.do_dot(slice(g * 2 * HD, (g + 1) * 2 * HD))
            for h in range(2):
                r.do[g, h * half:(h + 1) * half, :] = t[:half, h * HD:(h + 1) * HD].astype(BF16)
                r.do[g, seq + h * half:seq + (h + 1) * half, :] = t[half:, h * HD:(h + 1) * HD].astype(BF16)

        return [(1, q)] + ([(1, k), (1, v)] if g % 2 == 0 else []) + [(1, do)]

    def stacked(h, c):
        return (h * half + c) if c < half else (seq + h * half + c - half)

    def rope(g):
        cs, sn = (r.tab.at[2], r.tab.at[3]) if g == n_grp - 1 else (r.tab.at[0], r.tab.at[1])

        def size(h, c):
            def run():
                raw = r.knew[g, c:c + CH, :] if h == 2 else r.qnew[g % 2, h, c:c + CH, :]
                r.raw[g, h, c:c + CH, :] = raw
                t = raw.astype(F32)
                r.inv[g, h, c:c + CH, :] = jnp.broadcast_to(lax.rsqrt(jnp.mean(t * t, axis=-1, keepdims=True) + EPS), t.shape)

            return (0.4, run)

        def turn(h, c):
            def run():
                t = r.raw[g, h, c:c + CH, :].astype(F32)
                w = (t * r.inv[g, h, c:c + CH, :]) * (r.kg if h == 2 else r.qg)[0:1, :]
                o = 2 * seq + c if h == 2 else stacked(h, c)
                x = pltpu.roll(w, HD // 2, 1)
                co, si = cs[c:c + CH, :], sn[c:c + CH, :]
                r.rot[g, o:o + CH, 0:HD] = (w * co + x * si).astype(BF16)
                r.rot[g, o:o + CH, HD:] = (x * co - w * si).astype(BF16)
                if h == 2:
                    r.v[g, c:c + CH, :] = r.vnew[g, c:c + CH, :]

            return (0.6, run)

        return [f(h, c) for f in (size, turn) for h in (2, 0, 1) for c in range(0, seq, CH)]

    def scores(g):
        b = g % 2

        def s():
            r.s[b, 0:seq, 0:half] = dot(r.rot[g, 0:seq, 0:HD], r.rot[g, 2 * seq:2 * seq + half, 0:HD], NT)
            r.s[b, seq:, :] = dot(r.rot[g, seq:2 * seq, 0:HD], r.rot[g, 2 * seq:, 0:HD], NT)

        def dp():
            r.dp[b, 0:seq, 0:half] = dot(r.do[g, :seq, :], r.v[g, :half, :], NT)
            r.dp[b, seq:, :] = dot(r.do[g, seq:, :], r.v[g], NT)

        return [(1, s), (1, dp)]

    def soft(g):
        b = g % 2
        c2 = scale * log2e

        def part(blk, c):
            return slice(blk * seq + c, blk * seq + c + CH), half if blk == 0 else seq

        def masked(blk, c, s):
            row_id = lax.broadcasted_iota(jnp.int32, (CH, half), 0) + (c % half)
            keep = row_id >= lax.broadcasted_iota(jnp.int32, (CH, half), 1)
            if blk == 0:
                return jnp.where(keep, s, -jnp.inf)
            return jnp.concatenate([s[:, :half], jnp.where(keep, s[:, half:], -jnp.inf)], axis=1)

        def wide(ref, rows, width):
            t = ref[rows, :]
            return t if width == half else jnp.concatenate([t, t], axis=1)

        def top(blk, c):
            rows, width = part(blk, c)

            def run():
                m = jnp.max(masked(blk, c, r.s[b, rows, 0:width]), axis=-1, keepdims=True)
                r.st[0, rows, :] = jnp.broadcast_to(m * c2, (CH, HD))

            return (0.4 + 0.4 * blk, run)

        def power(blk, c):
            rows, width = part(blk, c)

            def run():
                e = jnp.exp2(masked(blk, c, r.s[b, rows, 0:width] * c2) - wide(r.st.at[0], rows, width))
                r.s[b, rows, 0:width] = e
                r.st[1, rows, :] = jnp.broadcast_to(1.0 / jnp.sum(e, axis=-1, keepdims=True), (CH, HD))

            return (0.8 + 0.8 * blk, run)

        def prob(blk, c):
            rows, width = part(blk, c)

            def run():
                pr = r.s[b, rows, 0:width] * wide(r.st.at[1], rows, width)
                r.s[b, rows, 0:width] = pr
                r.p[b, rows, 0:width] = pr.astype(BF16)
                r.st[2, rows, :] = jnp.broadcast_to(jnp.sum(pr * r.dp[b, rows, 0:width], axis=-1, keepdims=True), (CH, HD))

            return (0.8 + 0.8 * blk, run)

        def last(blk, c):
            rows, width = part(blk, c)

            def run():
                d = r.dp[b, rows, 0:width] - wide(r.st.at[2], rows, width)
                r.ds[b, rows, 0:width] = (r.s[b, rows, 0:width] * d * scale).astype(BF16)

            return (0.8 + 0.8 * blk, run)

        return [f(blk, c) for f in (top, power, prob, last) for blk in range(2) for c in range(0, seq, CH)]

    def grads(g):
        b = g % 2
        col, kcol = g * 2 * HD, g * HD

        def dq():
            r.dqf[b, 0:seq, :] = dot(r.ds[b, 0:seq, 0:half], r.rot[g, 2 * seq:2 * seq + half, :])
            r.dqf[b, seq:, :] = dot(r.ds[b, seq:, :], r.rot[g, 2 * seq:, :])

        def dk():
            tb = dot(r.ds[b, seq:, :], r.rot[g, seq:2 * seq, :], TN)
            ta = dot(r.ds[b, 0:seq, 0:half], r.rot[g, 0:seq, :], TN)
            r.dkf[b, :half, :] = tb[:half] + ta
            r.dkf[b, half:, :] = tb[half:]

        def o():
            ta = dot(r.p[b, 0:seq, 0:half], r.v[g, :half, :])
            tb = dot(r.p[b, seq:, :], r.v[g])
            for h in range(2):
                r.o[0:half, col + h * HD:col + (h + 1) * HD] = ta[h * half:(h + 1) * half].astype(BF16)
                r.o[half:seq, col + h * HD:col + (h + 1) * HD] = tb[h * half:(h + 1) * half].astype(BF16)

        def dv():
            tb = dot(r.p[b, seq:, :], r.do[g, seq:, :], TN)
            ta = dot(r.p[b, 0:seq, 0:half], r.do[g, :seq, :], TN)
            r.dv[0:half, kcol:kcol + HD] = (tb[:half] + ta).astype(BF16)
            r.dv[half:seq, kcol:kcol + HD] = tb[half:].astype(BF16)

        return [(1, dq), (1, dk), (1, o), (1, dv)]

    def back(g):
        b = g % 2

        def place(h, c):
            if h == 2:
                return r.dkf, c, r.dk, g * HD, r.kg
            return r.dqf, stacked(h, c), r.dq, (2 * g + h) * HD, r.qg

        def turn(h, c):
            src, o, _, _, g_ref = place(h, c)

            def run():
                d = src[b, o:o + CH, :].astype(BF16).astype(F32)
                that = r.raw[g, h, c:c + CH, :].astype(F32) * r.inv[g, h, c:c + CH, :]
                du = d[:, :HD] * r.tab[2, c:c + CH, :] - d[:, HD:] * r.tab[3, c:c + CH, :]
                src[b, o:o + CH, 0:HD] = du
                pr = du * that
                dg_ref = r.dgk if h == 2 else r.dgq
                dg_ref[...] += jnp.sum(pr.reshape(CH // 8, 8, HD), axis=0)
                r.sb[h, c:c + CH, :] = jnp.broadcast_to(jnp.mean(pr * g_ref[0:1, :], axis=-1, keepdims=True), (CH, HD))

            return (0.6, run)

        def out(h, c):
            src, o, out_ref, col, g_ref = place(h, c)

            def run():
                inv = r.inv[g, h, c:c + CH, :]
                that = r.raw[g, h, c:c + CH, :].astype(F32) * inv
                out_ref[c:c + CH, col:col + HD] = (inv * (src[b, o:o + CH, 0:HD] * g_ref[0:1, :] - that * r.sb[h, c:c + CH, :])).astype(BF16)

            return (0.5, run)

        return [f(h, c) for f in (turn, out) for h in (0, 1, 2) for c in range(0, seq, CH)]

    return SimpleNamespace(norm=norm_rows, proj=proj, rope=rope, scores=scores, soft=soft, grads=grads, back=back)


def attn_tick(st, g, n_grp, more=()):
    gr = st.grads(g)
    for _, f in gr[:2]:
        f()
    weave(st.soft((g - 3) % n_grp), st.rope((g - 1) % n_grp), st.back(g), st.scores((g - 2) % n_grp) + gr[2:] + st.proj(g) + list(more))


def attn_scratch(seq, n_grp):
    return dict(
        qnew=pltpu.VMEM((2, 2, seq, HD), BF16),
        knew=pltpu.VMEM((n_grp, seq, HD), BF16),
        vnew=pltpu.VMEM((n_grp, seq, HD), BF16),
        raw=pltpu.VMEM((n_grp, 3, seq, HD), BF16),
        inv=pltpu.VMEM((n_grp, 3, seq, HD), F32),
        rot=pltpu.VMEM((n_grp, 3 * seq, 2 * HD), BF16),
        do=pltpu.VMEM((n_grp, 2 * seq, HD), BF16),
        v=pltpu.VMEM((n_grp, seq, HD), BF16),
        s=pltpu.VMEM((2, 2 * seq, seq), F32),
        dp=pltpu.VMEM((2, 2 * seq, seq), F32),
        p=pltpu.VMEM((2, 2 * seq, seq), BF16),
        ds=pltpu.VMEM((2, 2 * seq, seq), BF16),
        dkf=pltpu.VMEM((2, seq, 2 * HD), F32),
        dqf=pltpu.VMEM((2, 2 * seq, 2 * HD), F32),
        st=pltpu.VMEM((3, 2 * seq, HD), F32),
        sb=pltpu.VMEM((3, seq, HD), F32),
        tab=pltpu.VMEM((4, seq, HD), F32),
    )


EARLY = 4


def tail_kernel(seq, n_grp, rows, keys, sel_ref, n_in, dy_in, cos_in, sin_in, x_in, dyx_in, gain_ref, qg_ref, kg_ref, dgq_own, dgk_own, *refs):
    own_w, oth_w, own_a = refs[:4], refs[4:8], refs[8:12]
    y_out, dx_out, sums_out = refs[12:15]
    r = SimpleNamespace(n=n_in, dy=dy_in, qg=qg_ref, kg=kg_ref, gain=gain_ref, **dict(zip(keys, refs[15:])))
    step = pl.program_id(0)
    me = sel_ref[0]
    oth = 1 - me
    D = x_in.shape[1]
    r.wq = lambda c: r.wq_all[oth, :, c]
    r.wk = lambda c: r.wk_all[oth, :, c]
    r.wv = lambda c: r.wv_all[oth, :, c]
    r.do_dot = lambda c: dot(dy_in[...], r.wo_all[oth, c, :], NT)
    r.o, r.dq, r.dk, r.dv = r.oc.at[oth], r.dqc.at[oth], r.dkc.at[oth], r.dvc.at[oth]
    st = attn_stages(seq, n_grp, r)

    def fetch(row):
        return [pltpu.make_async_copy(src.at[me, pl.ds(row * seq, seq), :], dst.at[me], r.sem.at[8 + k])
                for k, (src, dst) in enumerate(zip(own_a[1:], (r.dqc, r.dkc, r.dvc)))]

    def fetch_o(row):
        return pltpu.make_async_copy(own_a[0].at[me, pl.ds(row * seq, seq), :], r.o_next, r.sem.at[11])

    weights = (r.wq_all, r.wk_all, r.wv_all, r.wo_all)
    theirs = [pltpu.make_async_copy(oth_w[k], dst.at[oth], r.sem.at[4 + k]) for k, dst in enumerate(weights)]
    mine = [pltpu.make_async_copy(own_w[k], dst.at[me], r.sem.at[k]) for k, dst in enumerate(weights)]

    @pl.when(step == 0)
    def _():
        for c in theirs + mine[3:] + mine[:3]:
            c.start()
        r.dg[...] = jnp.zeros_like(r.dg)
        r.oc[...] = jnp.zeros_like(r.oc)
        for c in theirs + mine[3:]:
            c.wait()

    @pl.when(step > 0)
    def _():
        for c in fetch(step - 1):
            c.start()
        fetch_o(step - 1).wait()
        r.oc[me] = r.o_next[...]

    @pl.when(step < rows)
    def _():
        fetch_o(step).start()

    CR, NC = 32, 256
    nn = D // NC
    lines = range(0, seq, CR)

    def wide(v):
        return jnp.concatenate([v] * (NC // HD), axis=1)

    def stat(c):
        def run():
            xf = x_in[c:c + CR, :].astype(F32)
            r.xs[0, c:c + CR, :] = jnp.broadcast_to(lax.rsqrt(jnp.mean(xf * xf, axis=-1, keepdims=True) + EPS), (CR, HD))
            r.xs[1, c:c + CR, :] = jnp.zeros((CR, HD), F32)

        return (1, run)

    def dn_dot(n):
        def run():
            cols = slice(n * NC, (n + 1) * NC)
            t = None
            for s in range(2):
                for a_ref, w_ref in ((r.dqc, r.wq_all), (r.dkc, r.wk_all), (r.dvc, r.wv_all)):
                    u = dot(a_ref[s], w_ref[s, cols, :], NT)
                    t = u if t is None else t + u
            r.dn[:, cols] = t

        return (2, run)

    def first(n, c):
        def run():
            cols = slice(n * NC, (n + 1) * NC)
            inv = wide(r.xs[0, c:c + CR, :])
            d = r.dn[c:c + CR, cols]
            w = d * (x_in[c:c + CR, cols].astype(F32) * inv)
            r.dg[:, cols] += jnp.sum(w.reshape(CR // 8, 8, NC), axis=0)
            w = w * gain_ref[0:1, cols]
            r.xs[1, c:c + CR, :] += w[:, :HD] + w[:, HD:]
            r.dn[c:c + CR, cols] = dyx_in[c:c + CR, cols].astype(F32) + inv * (d * gain_ref[0:1, cols])

        return (1, run)

    def mean(c):
        def run():
            inv = r.xs[0, c:c + CR, :]
            r.xs[2, c:c + CR, :] = jnp.sum(r.xs[1, c:c + CR, :], axis=-1, keepdims=True) * (1.0 / D) * (inv * inv)

        return (0.2, run)

    def second(n, c):
        def run():
            cols = slice(n * NC, (n + 1) * NC)
            dx_out[c:c + CR, cols] = (r.dn[c:c + CR, cols] - x_in[c:c + CR, cols].astype(F32) * wide(r.xs[2, c:c + CR, :])).astype(BF16)

        return (1, run)

    def y_dot(n):
        def run():
            cols = slice(n * NC, (n + 1) * NC)
            t = dot(r.oc[0], r.wo_all[0, :, cols]) + dot(r.oc[1], r.wo_all[1, :, cols])
            y_out[:, cols] = (x_in[:, cols].astype(F32) + t).astype(BF16)

        return (1, run)

    r.tab[2:4] = r.tab[0:2]
    r.tab[0] = cos_in[...]
    r.tab[1] = sin_in[...]
    yd = [y_dot(n) for n in range(nn)]
    for g in range(n_grp):
        attn_tick(st, g, n_grp, yd[:EARLY] if g == n_grp - 1 else [])
    for acc in (r.dgq, r.dgk):
        acc[...] = jnp.where(step > 0, acc[...], 0.0)

    @pl.when(step == 0)
    def _():
        for c in mine[:3]:
            c.wait()

    @pl.when(step > 0)
    def _():
        for c in fetch(step - 1):
            c.wait()
        dn = [dn_dot(n) for n in range(nn)]
        for _, f in dn[:1]:
            f()
        weave([stat(c) for c in lines], dn[1:2])
        for n in range(2, nn):
            weave([first(n - 2, c) for c in lines], dn[n:n + 1])
        weave([first(nn - 2, c) for c in lines], yd[EARLY:EARLY + 1])
        weave([first(nn - 1, c) for c in lines] + [mean(c) for c in lines], yd[EARLY + 1:EARLY + 2])
        weave([second(n, c) for n in range(nn) for c in lines], yd[EARLY + 2:])

    @pl.when(step == rows)
    def _():
        at = 0
        for part in (r.dg[...], r.dgq[...] + dgq_own[...], r.dgk[...] + dgk_own[...]):
            sums_out[:, at:at + part.shape[1]] = jnp.sum(part, axis=0, keepdims=True)
            at += part.shape[1]


def tail_call(sel, n, x, dy, cosd, sind, o, dq, dk, dv, gain, qg, kg, dgq, dgk, own, oth, seq=256):
    T, D = x.shape
    nq, nk = dq.shape[2], dk.shape[2]
    n_grp = nk // HD
    rows = T // seq
    lag = lambda k, c: pl.BlockSpec((seq, c), lambda i, s: (jnp.clip(i - k, 0, rows - 1), 0))
    const = lambda *b: pl.BlockSpec(b, lambda i, s: (0,) * len(b), pipeline_mode=pl.Buffered(1))
    hbm = pl.BlockSpec(memory_space=pl.ANY)
    scratch = attn_scratch(seq, n_grp)
    scratch.update(
        wq_all=pltpu.VMEM((2, D, nq), BF16), wk_all=pltpu.VMEM((2, D, nk), BF16), wv_all=pltpu.VMEM((2, D, nk), BF16), wo_all=pltpu.VMEM((2, nq, D), BF16),
        dn=pltpu.VMEM((seq, D), F32), oc=pltpu.VMEM((2, seq, nq), BF16), dqc=pltpu.VMEM((2, seq, nq), BF16), dkc=pltpu.VMEM((2, seq, nk), BF16), dvc=pltpu.VMEM((2, seq, nk), BF16),
        o_next=pltpu.VMEM((seq, nq), BF16), xs=pltpu.VMEM((3, seq, HD), F32), dg=pltpu.VMEM((8, D), F32), dgq=pltpu.VMEM((8, HD), F32), dgk=pltpu.VMEM((8, HD), F32), sem=pltpu.SemaphoreType.DMA((12,)))
    flops = 2 * T * D * (nq + 2 * nk + nq) * 3 + 12 * T * nq * seq
    return pl.pallas_call(
        functools.partial(tail_kernel, seq, n_grp, rows, tuple(scratch)),
        grid_spec=pltpu.PrefetchScalarGridSpec(
            num_scalar_prefetch=1,
            grid=(rows + 1,),
            in_specs=[lag(0, D), lag(0, D), lag(0, HD), lag(0, HD), lag(1, D), lag(1, D), const(1, D), const(1, HD), const(1, HD), const(8, HD), const(8, HD)] + [hbm] * 12,
            out_specs=[lag(1, D), lag(1, D), pl.BlockSpec((1, D + 2 * HD), lambda i, s: (0, 0))],
            scratch_shapes=list(scratch.values()),
        ),
        out_shape=[jax.ShapeDtypeStruct((T, D), BF16)] * 2 + [jax.ShapeDtypeStruct((1, D + 2 * HD), F32)],
        compiler_params=pltpu.CompilerParams(dimension_semantics=("arbitrary",), vmem_limit_bytes=67043328),
        cost_estimate=pl.CostEstimate(flops=flops, bytes_accessed=T * D * 14, transcendentals=T * nq * 2),
        name="tail",
    )(sel, n, dy, cosd, sind, x, dy, gain, qg, kg, dgq, dgk, *own, *oth, o, dq, dk, dv)


def solution(mesh):
    tok_spec = P("dp", None, None)
    col_spec = P(None, "tp")
    row_spec = P("tp", None)
    n_dp = mesh.shape["dp"]

    def per_device(x_in, dy_in, positions, g_attn, q_gain, k_gain, w_q, w_k, w_v, w_o):
        n_batch, n_seq, D = x_in.shape
        T = n_batch * n_seq
        nk = w_k.shape[1]
        x, dy = x_in.reshape(T, D), dy_in.reshape(T, D)
        me = lax.axis_index("tp").astype(jnp.int32)
        own = me.reshape(1)

        part = lax.axis_index("dp").astype(jnp.int32).reshape(1)
        share, cosd, sind = pre_call(part, w_q, w_k, w_v, w_o, positions, parts=n_dp)
        gathered = lax.all_gather(share, ("tp", "dp"), tiled=True)

        gain = g_attn.astype(F32).reshape(1, D)
        qg, kg = q_gain.astype(F32).reshape(1, HD), k_gain.astype(F32).reshape(1, HD)

        n, o, dq, dk, dv, dgq, dgk, dw_o = attn_call(True, own, x, dy, cosd, sind, gain, qg, kg, w_q, w_k, w_v, w_o, seq=n_seq)
        dw_q, dw_k, dw_v, *theirs = dw_call(own, n, [dq, dk, dv], 512, gathered=gathered, nk=nk)
        dw_o, dw_q, dw_k, dw_v = lax.psum((dw_o, dw_q, dw_k, dw_v), "dp")

        y, dx, sums = tail_call(own, n, x, dy, cosd, sind, o, dq, dk, dv, gain, qg, kg, dgq, dgk, (w_q, w_k, w_v, w_o), theirs, seq=n_seq)
        g_sum, q_sum, k_sum = (t.reshape(-1) for t in sum_call(sums, (D, HD, HD), n_dp))
        dw_o, dw_q, dw_k, dw_v = copy_call((dw_o, dw_q, dw_k, dw_v))
        return y.reshape(x_in.shape), dx.reshape(x_in.shape), dw_q, dw_k, dw_v, dw_o, q_sum, k_sum, g_sum

    return jax.shard_map(per_device, mesh=mesh, in_specs=(tok_spec, tok_spec, P("dp", None), P(), P(), P(), col_spec, col_spec, col_spec, row_spec), out_specs=(tok_spec, tok_spec, col_spec, col_spec, col_spec, row_spec, P(), P(), P()), check_vma=False)
```
